16 devices in a mesh: dp: 2 (over z), sp: 8 (over y, x, core).
Axes of the slice: x: 2, y: 2, z: 2, core: 2. Of those that a mesh axis runs over, the one named last changes fastest.
Arguments:
- x: bfloat16 [8192, 3072], P(('dp', 'sp')), parts along dimension 0
- grad_out: bfloat16 [8192, 3072], P(('dp', 'sp')), parts along dimension 0
- positions: int32 [8192], P(('dp', 'sp')), parts along dimension 0
- gain: bfloat16 [3072], replicated
- w_q: bfloat16 [3072, 3072], replicated
- w_k: bfloat16 [3072, 1024], replicated
- w_v: bfloat16 [3072, 1024], replicated
- w_o: bfloat16 [3072, 3072], replicated
Outputs:
- output 1: bfloat16 [8192, 3072], P(('dp', 'sp')), parts along dimension 0
- output 2: bfloat16 [8192, 3072], P(('dp', 'sp')), parts along dimension 0
- output 3: float32 [6144, 3072], P('dp'), parts along dimension 0
- output 4: float32 [6144, 1024], P('dp'), parts along dimension 0
- output 5: float32 [6144, 1024], P('dp'), parts along dimension 0
- output 6: float32 [6144, 3072], P('dp'), parts along dimension 0
- output 7: float32 [6144], P('dp'), parts along dimension 0
There are 2 independent parts. The reference program is written for one: setup_inputs(seed, part) draws one part's arguments, and reference() takes and returns one part's arrays. A program takes and returns all parts, laid end to end along the dimension named above; an argument that names none is the same for every part.
All inputs are finite; a program needn't handle non-finite values.
Results may differ from the reference program's by a relative error of at most 0.0182909.
Values are sent between devices in bfloat16 or wider.
A program may use at most 1 GiB of HBM per device.

```python
import jax
import jax.numpy as jnp
from jax import lax

D = 3072
HEADS = 24
KV_HEADS = 8
HEAD = 128
SEQ = 4096
GROUP = HEADS // KV_HEADS
ROPE_THETA = 1000000.0
NORM_EPS = 1e-05
NEG_LARGE = -1e30


def block_rows(seq_len, row_cost):
    row_count = seq_len
    while row_count > 8 and row_count * row_cost > 2 ** 24:
        row_count = row_count // 2
    return row_count


def setup_inputs(seed: int = 0, part: int = 0) -> dict:
    base_key = jax.random.key(seed)
    part_key = jax.random.fold_in(base_key, part)
    key_x, key_dy, key_start, key_step = jax.random.split(part_key, 4)
    shared = jax.random.split(jax.random.key(seed + 1), 5)
    x = jax.random.normal(key_x, (SEQ, D), jnp.float32).astype(jnp.bfloat16)
    grad_out = jax.random.normal(key_dy, (SEQ, D), jnp.float32).astype(jnp.bfloat16)
    pos_start = jax.random.randint(key_start, (), 0, SEQ)
    pos_steps = jax.random.randint(key_step, (SEQ,), 1, 4)
    positions = (pos_start + jnp.cumsum(pos_steps) - pos_steps[0]).astype(jnp.int32)
    gain = (1.0 + 0.3 * jax.random.normal(shared[0], (D,), jnp.float32)).astype(jnp.bfloat16)
    w_q = (jax.random.normal(shared[1], (D, HEADS * HEAD), jnp.float32) * D ** -0.5).astype(jnp.bfloat16)
    w_k = (jax.random.normal(shared[2], (D, KV_HEADS * HEAD), jnp.float32) * D ** -0.5).astype(jnp.bfloat16)
    w_v = (jax.random.normal(shared[3], (D, KV_HEADS * HEAD), jnp.float32) * D ** -0.5).astype(jnp.bfloat16)
    w_o = (jax.random.normal(shared[4], (HEADS * HEAD, D), jnp.float32) * (HEADS * HEAD) ** -0.5).astype(jnp.bfloat16)
    return {'x': x, 'grad_out': grad_out, 'positions': positions, 'gain': gain, 'w_q': w_q, 'w_k': w_k, 'w_v': w_v, 'w_o': w_o}


def rope(values, cos_t, sin_t):
    half_dim = HEAD // 2
    lower_half = values[..., :half_dim]
    upper_half = values[..., half_dim:]
    return jnp.concatenate([lower_half * cos_t - upper_half * sin_t, upper_half * cos_t + lower_half * sin_t], axis=-1)


def attend(q_all, k_all, v_all):
    row_count = block_rows(SEQ, HEADS * SEQ)
    n_blocks = SEQ // row_count
    key_f = k_all.astype(jnp.float32)
    val_f = v_all.astype(jnp.float32)
    key_index = jnp.arange(SEQ)
    q_blocks = q_all.reshape(n_blocks, row_count, KV_HEADS, GROUP, HEAD)
    blk_starts = jnp.arange(n_blocks) * row_count

    def one_block(block_args):
        q_blk, blk_start = block_args
        scores = jnp.einsum('qhgd,khd->hgqk', q_blk.astype(jnp.float32), key_f) * HEAD ** -0.5
        causal = (blk_start + jnp.arange(row_count))[:, None] >= key_index[None, :]
        attn_prob = jax.nn.softmax(jnp.where(causal, scores, NEG_LARGE), axis=-1)
        blk_out = jnp.einsum('hgqk,khd->qhgd', attn_prob.astype(jnp.bfloat16).astype(jnp.float32), val_f)
        return blk_out.astype(jnp.bfloat16)

    outputs = lax.map(jax.checkpoint(one_block), (q_blocks, blk_starts))
    return outputs.reshape(SEQ, KV_HEADS, GROUP, HEAD)


def reference(x, grad_out, positions, gain, w_q, w_k, w_v, w_o):
    inv_freq = ROPE_THETA ** (-jnp.arange(0, HEAD, 2).astype(jnp.float32) / HEAD)
    angles = positions.astype(jnp.float32)[:, None] * inv_freq[None, :]
    cos_t = jnp.cos(angles)[:, None, :]
    sin_t = jnp.sin(angles)[:, None, :]

    def forward(x_f, gain_f, wq_f, wk_f, wv_f, wo_f):
        normed = x_f * lax.rsqrt(jnp.mean(x_f * x_f, axis=-1, keepdims=True) + NORM_EPS)
        hidden = (normed * gain_f).astype(jnp.bfloat16).astype(jnp.float32)
        q_proj = jnp.dot(hidden, wq_f, preferred_element_type=jnp.float32).reshape(SEQ, HEADS, HEAD)
        k_proj = jnp.dot(hidden, wk_f, preferred_element_type=jnp.float32).reshape(SEQ, KV_HEADS, HEAD)
        v_all = jnp.dot(hidden, wv_f, preferred_element_type=jnp.float32).astype(jnp.bfloat16).reshape(SEQ, KV_HEADS, HEAD)
        q_all = rope(q_proj, cos_t, sin_t).astype(jnp.bfloat16).reshape(SEQ, KV_HEADS, GROUP, HEAD)
        k_all = rope(k_proj, cos_t, sin_t).astype(jnp.bfloat16)
        attn = attend(q_all, k_all, v_all).reshape(SEQ, HEADS * HEAD)
        mixed = jnp.dot(attn.astype(jnp.float32), wo_f, preferred_element_type=jnp.float32)
        return (x_f + mixed).astype(jnp.bfloat16)

    result, pullback = jax.vjp(forward, x.astype(jnp.float32), gain.astype(jnp.float32), w_q.astype(jnp.float32), w_k.astype(jnp.float32), w_v.astype(jnp.float32), w_o.astype(jnp.float32))
    grad_xf, grad_gain, grad_wq, grad_wk, grad_wv, grad_wo = pullback(grad_out)
    return result, grad_xf.astype(jnp.bfloat16), grad_wq, grad_wk, grad_wv, grad_wo, grad_gain
```

```python
import functools

import jax
import jax.numpy as jnp
from jax import lax
from jax.experimental import pallas as pl
from jax.experimental.pallas import tpu as pltpu
from jax.sharding import PartitionSpec as P


HEAD_DIM = 128
HALF = HEAD_DIM // 2
ROPE_THETA = 1000000.0
NORM_EPS = 1e-05
NEG_LARGE = -1e30
LOG2E = 1.4426950408889634
BLK = 512
F32 = jnp.float32
BF16 = jnp.bfloat16
ROWS_ROWS = (((0,), (0,)), ((), ()))
COLS_COLS = (((1,), (1,)), ((), ()))
ROWS_COLS = (((0,), (1,)), ((), ()))
VMEM_LIMIT = 60 * 1024 * 1024


def dot(a, b, dims=(((1,), (0,)), ((), ()))):
    return lax.dot_general(a, b, dims, preferred_element_type=F32)


def params():
    return pltpu.CompilerParams(dimension_semantics=("arbitrary",), vmem_limit_bytes=VMEM_LIMIT)


def rope_tables(positions):
    inv_freq = ROPE_THETA ** (-jnp.arange(0, HEAD_DIM, 2).astype(F32) / HEAD_DIM)
    angles = positions.astype(F32)[:, None] * inv_freq[None, :]
    return jnp.cos(angles), jnp.sin(angles)


def project_kernel(heads, h_ref, w_ref, cos_ref, sin_ref, q_ref, k_ref, v_ref):
    prod = dot(h_ref[...], w_ref[...])
    cos_t, sin_t = cos_ref[...], sin_ref[...]
    for i in range(heads + 1):
        val = prod[:, i * HEAD_DIM:(i + 1) * HEAD_DIM]
        rot = (val * cos_t + pltpu.roll(val, HALF, 1) * sin_t).astype(BF16)
        if i < heads:
            q_ref[:, i * HEAD_DIM:(i + 1) * HEAD_DIM] = rot
        else:
            k_ref[...] = rot
    v_ref[...] = prod[:, (heads + 1) * HEAD_DIM:].astype(BF16)


def project(hidden, w_all, cos_t, sin_t, heads):
    seq_len, width = hidden.shape
    rows = lambda i: (i, 0)
    q_cols = heads * HEAD_DIM
    return pl.pallas_call(
        functools.partial(project_kernel, heads),
        grid=(seq_len // BLK,),
        in_specs=[pl.BlockSpec((BLK, width), rows), pl.BlockSpec(w_all.shape, lambda i: (0, 0)),
                  pl.BlockSpec((BLK, HEAD_DIM), rows), pl.BlockSpec((BLK, HEAD_DIM), rows)],
        out_specs=[pl.BlockSpec((BLK, q_cols), rows), pl.BlockSpec((BLK, HEAD_DIM), rows), pl.BlockSpec((BLK, HEAD_DIM), rows)],
        out_shape=[jax.ShapeDtypeStruct((seq_len, q_cols), BF16), jax.ShapeDtypeStruct((seq_len, HEAD_DIM), BF16),
                   jax.ShapeDtypeStruct((seq_len, HEAD_DIM), BF16)],
        compiler_params=params(),
        cost_estimate=pl.CostEstimate(flops=2 * seq_len * width * w_all.shape[1], bytes_accessed=2 * seq_len * width, transcendentals=0),
        name="project",
    )(hidden, w_all, cos_t, sin_t)


def masked(scores):
    key = lax.broadcasted_iota(jnp.int32, scores.shape, 0)
    query = lax.broadcasted_iota(jnp.int32, scores.shape, 1)
    return jnp.where(key <= query, scores, NEG_LARGE)


def attn_fwd_kernel(heads, q_ref, k_ref, v_ref, o_ref, lse_ref, vt, acc):
    i = pl.program_id(0)
    n_blocks = k_ref.shape[0] // BLK
    to_log2 = HEAD_DIM ** -0.5 * LOG2E

    @pl.when(i == 0)
    def _():
        @pl.loop(0, n_blocks)
        def _(c):
            vt[c] = v_ref[pl.ds(c * BLK, BLK), :].T

    acc[...] = jnp.zeros_like(acc)

    def chunk(c, carry, diagonal):
        k_c = k_ref[pl.ds(pl.multiple_of(c * BLK, BLK), BLK), :]
        vt_c = vt[c]
        scores = [dot(k_c, q_ref[:, a * HEAD_DIM:(a + 1) * HEAD_DIM], COLS_COLS) * to_log2 for a in range(heads)]
        out = []
        for a in range(heads):
            s = masked(scores[a]) if diagonal else scores[a]
            m_old, l_old = carry[a]
            m_new = jnp.maximum(m_old, jnp.max(s, axis=0, keepdims=True))
            alpha = jnp.exp2(m_old - m_new)
            p = jnp.exp2(s - m_new)
            l_new = l_old * alpha + jnp.sum(p, axis=0, keepdims=True)
            acc[a] = acc[a] * alpha + dot(vt_c, p.astype(BF16))
            out.append((m_new, l_new))
        return tuple(out)

    start = tuple((jnp.full((1, BLK), NEG_LARGE, F32), jnp.zeros((1, BLK), F32)) for _ in range(heads))
    carry = lax.fori_loop(0, i, lambda c, carry: chunk(c, carry, False), start)
    carry = chunk(i, carry, True)
    for a in range(heads):
        m_a, l_a = carry[a]
        o_ref[a * HEAD_DIM:(a + 1) * HEAD_DIM, :] = (acc[a] / l_a).astype(BF16)
        lse_ref[a:a + 1, :] = m_a + jnp.log2(l_a)


def attn_forward(q, k, v, heads):
    seq_len = k.shape[0]
    n_blocks = seq_len // BLK
    whole = lambda i: (0, 0)
    pairs = heads * seq_len * (seq_len + BLK) // 2
    return pl.pallas_call(
        functools.partial(attn_fwd_kernel, heads),
        grid=(n_blocks,),
        in_specs=[pl.BlockSpec((BLK, heads * HEAD_DIM), lambda i: (i, 0)), pl.BlockSpec(k.shape, whole), pl.BlockSpec(v.shape, whole)],
        out_specs=[pl.BlockSpec((heads * HEAD_DIM, BLK), lambda i: (0, i)), pl.BlockSpec((8, BLK), lambda i: (0, i))],
        out_shape=[jax.ShapeDtypeStruct((heads * HEAD_DIM, seq_len), BF16), jax.ShapeDtypeStruct((8, seq_len), F32)],
        scratch_shapes=[pltpu.VMEM((n_blocks, HEAD_DIM, BLK), BF16), pltpu.VMEM((heads, HEAD_DIM, BLK), F32)],
        compiler_params=params(),
        cost_estimate=pl.CostEstimate(flops=8 * pairs * HEAD_DIM, bytes_accessed=4 * seq_len * heads * HEAD_DIM, transcendentals=pairs),
        name="attn_fwd",
    )(q, k, v)


def unrotate_t(val, cos_t, sin_t):
    lower, upper = val[:HALF], val[HALF:]
    return jnp.concatenate([lower * cos_t + upper * sin_t, upper * cos_t - lower * sin_t], axis=0)


def attn_bwd_kernel(heads, q_ref, k_ref, v_ref, do_ref, ot_ref, lse_ref, cos_ref, sin_ref, dq_ref, dk_ref, dv_ref, kt, dk_acc, dv_acc, dqt):
    i = pl.program_id(0)
    n_blocks = k_ref.shape[0] // BLK
    qk_scale = HEAD_DIM ** -0.5
    to_log2 = qk_scale * LOG2E

    @pl.when(i == 0)
    def _():
        @pl.loop(0, n_blocks)
        def _(c):
            kt[c] = k_ref[pl.ds(c * BLK, BLK), :].T

    dqt[...] = jnp.zeros_like(dqt)
    cols = [slice(a * HEAD_DIM, (a + 1) * HEAD_DIM) for a in range(heads)]
    delta = [jnp.sum(ot_ref[cols[a], :].astype(F32) * do_ref[:, cols[a]].T.astype(F32), axis=0, keepdims=True) for a in range(heads)]

    def chunk(c, diagonal):
        rows = pl.ds(pl.multiple_of(c * BLK, BLK), BLK)
        k_c, v_c, kt_c = k_ref[rows, :], v_ref[rows, :], kt[c]
        dk_c = dv_c = None
        for a in range(heads):
            q_a, do_a = q_ref[:, cols[a]], do_ref[:, cols[a]]
            s = dot(k_c, q_a, COLS_COLS) * to_log2
            if diagonal:
                s = masked(s)
            p = jnp.exp2(s - lse_ref[a:a + 1, :])
            d_p = dot(v_c, do_a, COLS_COLS)
            d_s = (p * (d_p - delta[a])).astype(BF16)
            dv_a = dot(p.astype(BF16), do_a)
            dk_a = dot(d_s, q_a)
            dv_c = dv_a if dv_c is None else dv_c + dv_a
            dk_c = dk_a if dk_c is None else dk_c + dk_a
            dqt[a] += dot(kt_c, d_s)
        if diagonal:
            dk_acc[c] = dk_c
            dv_acc[c] = dv_c
        else:
            dk_acc[c] += dk_c
            dv_acc[c] += dv_c

    @pl.loop(0, i)
    def _(c):
        chunk(c, False)

    chunk(i, True)
    for a in range(heads):
        dq_ref[cols[a], :] = unrotate_t(dqt[a] * qk_scale, cos_ref[i], sin_ref[i]).astype(BF16)

    @pl.when(i == n_blocks - 1)
    def _():
        for c in range(n_blocks):
            dk_ref[:, c * BLK:(c + 1) * BLK] = unrotate_t(dk_acc[c].T * qk_scale, cos_ref[c], sin_ref[c]).astype(BF16)
            dv_ref[:, c * BLK:(c + 1) * BLK] = dv_acc[c].astype(BF16).T


def attn_backward(q, k, v, d_o, ot, lse, cos_t, sin_t, heads):
    seq_len = k.shape[0]
    n_blocks = seq_len // BLK
    whole = lambda i: (0, 0)
    blocks = lambda t: t.T.reshape(HALF, n_blocks, BLK).transpose(1, 0, 2)
    pairs = heads * seq_len * (seq_len + BLK) // 2
    q_cols = heads * HEAD_DIM
    row_spec = pl.BlockSpec((BLK, q_cols), lambda i: (i, 0))
    col_spec = pl.BlockSpec((q_cols, BLK), lambda i: (0, i))
    table_spec = pl.BlockSpec((n_blocks, HALF, BLK), lambda i: (0, 0, 0))
    kv_spec = pl.BlockSpec(k.shape, whole)
    kvt_spec = pl.BlockSpec((HEAD_DIM, seq_len), whole)
    return pl.pallas_call(
        functools.partial(attn_bwd_kernel, heads),
        grid=(n_blocks,),
        in_specs=[row_spec, kv_spec, kv_spec, row_spec, col_spec, pl.BlockSpec((8, BLK), lambda i: (0, i)), table_spec, table_spec],
        out_specs=[col_spec, kvt_spec, kvt_spec],
        out_shape=[jax.ShapeDtypeStruct((q_cols, seq_len), BF16), jax.ShapeDtypeStruct((HEAD_DIM, seq_len), BF16),
                   jax.ShapeDtypeStruct((HEAD_DIM, seq_len), BF16)],
        scratch_shapes=[pltpu.VMEM((n_blocks, HEAD_DIM, BLK), BF16), pltpu.VMEM((n_blocks, BLK, HEAD_DIM), F32),
                        pltpu.VMEM((n_blocks, BLK, HEAD_DIM), F32), pltpu.VMEM((heads, HEAD_DIM, BLK), F32)],
        compiler_params=params(),
        cost_estimate=pl.CostEstimate(flops=20 * pairs * HEAD_DIM, bytes_accessed=8 * seq_len * q_cols, transcendentals=pairs),
        name="attn_bwd",
    )(q, k, v, d_o, ot, lse, blocks(cos_t), blocks(sin_t))


def solution(mesh):
    sp_size = mesh.shape['sp']
    seq_spec = P(('dp', 'sp'), None)
    pos_spec = P(('dp', 'sp'))
    replicated = P(None, None)
    part_rows = P('dp', None)

    def gather(val):
        return lax.all_gather(val, 'sp', axis=0, tiled=True)

    def local_step(x, grad_out, positions, gain, w_q, w_k, w_v, w_o):
        tok_count = x.shape[0]
        n_heads = w_q.shape[1] // HEAD_DIM
        heads = n_heads // sp_size
        me = lax.axis_index('sp')
        q_cols = heads * HEAD_DIM
        x_f = x.astype(F32)
        inv_rms = lax.rsqrt(jnp.mean(x_f * x_f, axis=-1, keepdims=True) + NORM_EPS)
        normed = x_f * inv_rms
        gain_f = gain.astype(F32)
        hidden = gather((normed * gain_f).astype(BF16))
        d_out = gather(grad_out)
        cos_h, sin_h = rope_tables(gather(positions))
        cos_t = jnp.concatenate([cos_h, cos_h], axis=1)
        sin_t = jnp.concatenate([-sin_h, sin_h], axis=1)
        take_cols = lambda w, n: lax.dynamic_slice_in_dim(w, me * n, n, axis=1)
        w_all = jnp.concatenate([take_cols(w_q, q_cols), take_cols(w_k, HEAD_DIM), take_cols(w_v, HEAD_DIM)], axis=1)
        w_o_loc = lax.dynamic_slice_in_dim(w_o, me * q_cols, q_cols, axis=0)

        q, k, v = project(hidden, w_all, cos_t, sin_t, heads)
        ot, lse = attn_forward(q, k, v, heads)
        ot_all = gather(ot)
        d_o = dot(d_out, w_o_loc, COLS_COLS).astype(BF16)
        dqt, dkt, dvt = attn_backward(q, k, v, d_o, ot, lse, cos_h, sin_h, heads)
        dqt_all, dkt_all, dvt_all = gather(dqt), gather(dkt), gather(dvt)

        own = lambda t: lax.dynamic_slice_in_dim(t, me * tok_count, tok_count, axis=1)
        result = (x_f + dot(own(ot_all), w_o, ROWS_ROWS)).astype(BF16)
        grad_wo = dot(ot_all, d_out)
        grad_wq = dot(hidden, dqt_all, ROWS_COLS)
        grad_wk = dot(hidden, dkt_all, ROWS_COLS)
        grad_wv = dot(hidden, dvt_all, ROWS_COLS)
        d_hidden = (dot(own(dqt_all), w_q, ROWS_COLS) + dot(own(dkt_all), w_k, ROWS_COLS) + dot(own(dvt_all), w_v, ROWS_COLS))
        grad_gain = lax.psum(jnp.sum(d_hidden * normed, axis=0), 'sp')
        d_normed = d_hidden * gain_f
        d_xnorm = inv_rms * (d_normed - normed * jnp.mean(d_normed * normed, axis=-1, keepdims=True))
        grad_x = (grad_out.astype(F32) + d_xnorm).astype(BF16)
        return result, grad_x, grad_wq, grad_wk, grad_wv, grad_wo, grad_gain

    return jax.shard_map(local_step, mesh=mesh,
                         in_specs=(seq_spec, seq_spec, pos_spec, P(None), replicated, replicated, replicated, replicated),
                         out_specs=(seq_spec, seq_spec, part_rows, part_rows, part_rows, part_rows, P('dp')),
                         check_vma=False)
```

```python
import functools

import jax
import jax.numpy as jnp
from jax import lax
from jax.experimental import pallas as pl
from jax.experimental.pallas import tpu as pltpu
from jax.sharding import PartitionSpec as P

HEAD_DIM = 128
HALF = HEAD_DIM // 2
ROPE_THETA = 1000000.0
NORM_EPS = 1e-05
NEG_LARGE = -1e30
LOG2E = 1.4426950408889634
BLK = 512
CHUNKS = 4
FWD_MIDDLE, BWD_MIDDLE, BWD_LATE = 5, 4, 5
MROWS = 1024
RING = 3
ROWS = 64
F32 = jnp.float32
BF16 = jnp.bfloat16
ROWS_ROWS = (((0,), (0,)), ((), ()))
COLS_COLS = (((1,), (1,)), ((), ()))
ROWS_COLS = (((0,), (1,)), ((), ()))
VMEM_LIMIT = 60 * 1024 * 1024


def dot(a, b, dims=(((1,), (0,)), ((), ()))):
    return lax.dot_general(a, b, dims, preferred_element_type=F32)


def params(axes=1):
    return pltpu.CompilerParams(dimension_semantics=("arbitrary",) * axes, vmem_limit_bytes=VMEM_LIMIT)


class Neighbours:
    def __init__(self):
        self.me = lax.axis_index('sp')
        core, col, row = lax.rem(self.me, 2), lax.rem(self.me // 2, 2), self.me // 4
        self.sib = self.me + 1 - 2 * core
        self.xn = self.me + 2 - 4 * col
        self.yn = self.me + 4 - 8 * row
        self.diag = self.xn + self.yn - self.me

    def meet(self, peers):
        barrier = pltpu.get_barrier_semaphore()
        for peer in peers:
            pl.semaphore_signal(barrier, inc=1, device_id={'sp': peer}, device_id_type=pl.DeviceIdType.MESH)
        pl.semaphore_wait(barrier, len(peers))

    def others(self):
        flip = lambda dev: dev + 1 - 2 * lax.rem(dev, 2)
        return [self.sib, self.xn, flip(self.xn), self.yn, flip(self.yn), self.diag, flip(self.diag)]


def send(src, dst, sems, index, peer):
    return pltpu.make_async_remote_copy(src_ref=src, dst_ref=dst, send_sem=sems.at[0, index], recv_sem=sems.at[1, index],
                                        device_id={'sp': peer}, device_id_type=pl.DeviceIdType.MESH)


class Gather:
    COPIES = 22

    def __init__(self, near, own, dst, rows, sems):
        self.near, self.own, self.dst, self.rows, self.sems = near, own, dst, rows, sems

    def block(self, dev, chunk, count=1):
        size = self.rows // CHUNKS
        return self.dst.at[pl.ds(pl.multiple_of(dev * self.rows + chunk * size, size), count * size), :]

    def first(self, chunk, kind):
        peer = (self.near.xn, self.near.yn, self.near.sib)[kind]
        return send(self.own(chunk), self.block(self.near.me, chunk), self.sems, kind * CHUNKS + chunk, peer)

    def onward(self, chunk):
        over_y = chunk < CHUNKS // 2
        rows = self.block(self.near.xn if over_y else self.near.yn, chunk)
        return send(rows, rows, self.sems, 12 + chunk, self.near.yn if over_y else self.near.xn)

    def share(self, kind):
        rows = self.block((self.near.xn, self.near.yn)[kind], 0, CHUNKS)
        return send(rows, rows, self.sems, 16 + kind, self.near.sib)

    def share_diag(self, chunk):
        rows = self.block(self.near.diag, chunk)
        return send(rows, rows, self.sems, 18 + chunk, self.near.sib)

    def begin(self):
        self.near.meet([self.near.sib, self.near.xn, self.near.yn])
        for chunk in range(CHUNKS):
            self.start(chunk)

    def start(self, chunk):
        for kind in range(3):
            self.first(chunk, kind).start()

    def middle(self):
        for chunk in (0, 1):
            self.first(chunk, 0).wait_recv()
            self.onward(chunk).start()
        self.first(2, 1).wait_recv()
        self.onward(2).start()

    def late(self):
        self.first(3, 1).wait_recv()
        self.onward(3).start()
        for chunk in (2, 3):
            self.first(chunk, 0).wait_recv()
        self.share(0).start()
        for chunk in (0, 1):
            self.first(chunk, 1).wait_recv()
        self.share(1).start()

    def end(self):
        for chunk in (0, 2, 1, 3):
            self.onward(chunk).wait_recv()
            self.share_diag(chunk).start()
        sent = [self.first(chunk, kind) for chunk in range(CHUNKS) for kind in range(3)]
        for copy in sent:
            copy.wait_send()
        for chunk in range(CHUNKS):
            self.first(chunk, 2).wait_recv()
            self.onward(chunk).wait_send()
        for copy in [self.share(0), self.share(1)] + [self.share_diag(chunk) for chunk in range(CHUNKS)]:
            copy.wait()


SEMS = pltpu.SemaphoreType.DMA((2, Gather.COPIES))


def comm_params(collective_id):
    return pltpu.CompilerParams(dimension_semantics=("arbitrary",), vmem_limit_bytes=VMEM_LIMIT, collective_id=collective_id,
                                has_side_effects=True)


def gather_h_kernel(x_ref, gain_ref, pos_ref, freq_ref, h_all, cos_ref, sin_ref, x_v, h_v, pos_all, in_sems, out_sem, pos_sems, sems):
    near = Neighbours()
    rows = x_ref.shape[0]
    size = rows // CHUNKS
    part = lambda ref, chunk: ref.at[pl.ds(chunk * size, size), :]
    gather = Gather(near, lambda chunk: part(h_v, chunk), h_all, rows, sems)
    loads = [pltpu.make_async_copy(part(x_ref, chunk), part(x_v, chunk), in_sems.at[chunk]) for chunk in range(CHUNKS)]
    for load in loads:
        load.start()
    others = near.others()
    near.meet(others)
    pos_all[near.me] = pos_ref[...]
    positions = [send(pos_ref, pos_all.at[near.me], pos_sems, r, peer) for r, peer in enumerate(others)]
    for copy in positions:
        copy.start()
    for chunk in range(CHUNKS):
        loads[chunk].wait()

        @pl.loop(0, size // 32)
        def _(r):
            at = pl.ds(pl.multiple_of(chunk * size + r * 32, 32), 32)
            x_f = x_v[at, :].astype(F32)
            normed = x_f * lax.rsqrt(jnp.mean(x_f * x_f, axis=-1, keepdims=True) + NORM_EPS)
            h_v[at, :] = (normed * gain_ref[...]).astype(BF16)

        gather.start(chunk)
    own = pltpu.make_async_copy(h_v, gather.block(near.me, 0, CHUNKS), out_sem)
    own.start()
    for copy in positions:
        copy.wait()
    sign = jnp.where(lax.broadcasted_iota(jnp.int32, (1, HEAD_DIM), 1) < HALF, -1.0, 1.0)

    @pl.loop(0, pos_all.shape[0])
    def _(b):
        at = pl.ds(pl.multiple_of(b * rows, rows), rows)
        pos = jnp.broadcast_to(pos_all[b, 0:1, :].astype(F32), (HEAD_DIM, rows)).T
        angles = pos * freq_ref[...]
        cos_ref[at, :] = jnp.cos(angles)
        sin_ref[at, :] = jnp.sin(angles) * sign

    gather.middle()
    gather.late()
    own.wait()
    gather.end()


def gather_h(x, gain_f, positions, sp_size):
    rows, width = x.shape
    any_spec = pl.BlockSpec(memory_space=pl.ANY)
    vmem = pl.BlockSpec(memory_space=pltpu.VMEM)
    inv_freq = ROPE_THETA ** (-jnp.arange(0, HEAD_DIM, 2).astype(F32) / HEAD_DIM)
    freq = jnp.concatenate([inv_freq, inv_freq])[None, :]
    table = jax.ShapeDtypeStruct((rows * sp_size, HEAD_DIM), F32)
    return pl.pallas_call(
        gather_h_kernel,
        in_specs=[any_spec, vmem, vmem, vmem],
        out_specs=[any_spec, vmem, vmem],
        out_shape=[jax.ShapeDtypeStruct((rows * sp_size, width), BF16), table, table],
        scratch_shapes=[pltpu.VMEM((rows, width), BF16), pltpu.VMEM((rows, width), BF16), pltpu.VMEM((sp_size, 8, rows), jnp.int32),
                        pltpu.SemaphoreType.DMA((CHUNKS,)), pltpu.SemaphoreType.DMA, pltpu.SemaphoreType.DMA((2, 7)), SEMS],
        compiler_params=pltpu.CompilerParams(vmem_limit_bytes=VMEM_LIMIT, collective_id=0, has_side_effects=True),
        name="gather_h",
    )(x, gain_f, jnp.broadcast_to(positions[None, :], (8, rows)), freq)


def masked(scores):
    key = lax.broadcasted_iota(jnp.int32, scores.shape, 0)
    query = lax.broadcasted_iota(jnp.int32, scores.shape, 1)
    return jnp.where(key <= query, scores, NEG_LARGE)


def forward_kernel(heads, h_ref, wq_ref, wk_ref, wv_ref, cos_ref, sin_ref, dy_ref, q_ref, k_ref, v_ref, ht_ref, o_ref, lse_ref, dy_all,
                   w_v, w_sems, k_s, vt, acc, stage, stage_sems, sems):
    i = pl.program_id(0)
    near = Neighbours()
    rows = dy_ref.shape[0]
    size = rows // CHUNKS
    gather = Gather(near, lambda chunk: dy_ref.at[pl.ds(chunk * size, size), :], dy_all, rows, sems)
    stage_in = pltpu.make_async_copy(dy_ref, stage, stage_sems.at[0])
    stage_out = pltpu.make_async_copy(stage, gather.block(near.me, 0, CHUNKS), stage_sems.at[1])
    to_log2 = HEAD_DIM ** -0.5 * LOG2E
    q_cols = heads * HEAD_DIM

    @pl.when(i == 0)
    def _():
        loads, col = [], 0
        for n, (ref, count) in enumerate(((wq_ref, q_cols), (wk_ref, HEAD_DIM), (wv_ref, HEAD_DIM))):
            at = pl.ds(pl.multiple_of(near.me * count, HEAD_DIM), count)
            loads.append(pltpu.make_async_copy(ref.at[:, at], w_v.at[:, pl.ds(col, count)], w_sems.at[n]))
            col += count
        for load in loads:
            load.start()
        gather.begin()
        stage_in.start()
        for load in loads:
            load.wait()

    ht_ref[...] = h_ref[...].T
    prod = dot(h_ref[...], w_v[...])
    cos_t, sin_t = cos_ref[...], sin_ref[...]
    for a in range(heads + 1):
        val = prod[:, a * HEAD_DIM:(a + 1) * HEAD_DIM]
        rot = (val * cos_t + pltpu.roll(val, HALF, 1) * sin_t).astype(BF16)
        if a < heads:
            q_ref[:, a * HEAD_DIM:(a + 1) * HEAD_DIM] = rot
        else:
            k_ref[...] = rot
            k_s[i] = rot
    v_i = prod[:, q_cols + HEAD_DIM:].astype(BF16)
    v_ref[...] = v_i
    vt[i] = v_i.T
    acc[...] = jnp.zeros_like(acc)

    def chunk(c, carry, diagonal):
        k_c, vt_c = k_s[c], vt[c]
        scores = [dot(k_c, q_ref[:, a * HEAD_DIM:(a + 1) * HEAD_DIM], COLS_COLS) * to_log2 for a in range(heads)]
        out = []
        for a in range(heads):
            s = masked(scores[a]) if diagonal else scores[a]
            m_old, l_old = carry[a]
            m_new = jnp.maximum(m_old, jnp.max(s, axis=0, keepdims=True))
            alpha = jnp.exp2(m_old - m_new)
            p = jnp.exp2(s - m_new)
            l_new = l_old * alpha + jnp.sum(p, axis=0, keepdims=True)
            acc[a] = acc[a] * alpha + dot(vt_c, p.astype(BF16))
            out.append((m_new, l_new))
        return tuple(out)

    start = tuple((jnp.full((1, BLK), NEG_LARGE, F32), jnp.zeros((1, BLK), F32)) for _ in range(heads))
    carry = lax.fori_loop(0, i, lambda c, carry: chunk(c, carry, False), start)
    carry = chunk(i, carry, True)
    for a in range(heads):
        m_a, l_a = carry[a]
        o_ref[a * HEAD_DIM:(a + 1) * HEAD_DIM, :] = (acc[a] / l_a).astype(BF16)
        lse_ref[a:a + 1, :] = m_a + jnp.log2(l_a)

    @pl.when(i == FWD_MIDDLE)
    def _():
        gather.middle()
        stage_in.wait()
        stage_out.start()

    @pl.when(i == pl.num_programs(0) - 1)
    def _():
        gather.late()
        stage_out.wait()
        gather.end()


def forward(hidden, w_q, w_k, w_v, cos_t, sin_t, grad_out, heads):
    seq_len, width = hidden.shape
    n_blocks = seq_len // BLK
    q_cols = heads * HEAD_DIM
    pairs = heads * seq_len * (seq_len + BLK) // 2
    any_spec = pl.BlockSpec(memory_space=pl.ANY)
    rows = lambda cols: pl.BlockSpec((BLK, cols), lambda i: (i, 0))
    cols = lambda rows: pl.BlockSpec((rows, BLK), lambda i: (0, i))
    out = lambda *shape, dtype=BF16: jax.ShapeDtypeStruct(shape, dtype)
    return pl.pallas_call(
        functools.partial(forward_kernel, heads),
        grid=(n_blocks,),
        in_specs=[rows(width), any_spec, any_spec, any_spec, rows(HEAD_DIM), rows(HEAD_DIM), any_spec],
        out_specs=[rows(q_cols), rows(HEAD_DIM), rows(HEAD_DIM), cols(width), cols(q_cols), cols(8), any_spec],
        out_shape=[out(seq_len, q_cols), out(seq_len, HEAD_DIM), out(seq_len, HEAD_DIM), out(width, seq_len), out(q_cols, seq_len),
                   out(8, seq_len, dtype=F32), out(seq_len, width)],
        scratch_shapes=[pltpu.VMEM((width, q_cols + 2 * HEAD_DIM), BF16), pltpu.SemaphoreType.DMA((3,)), pltpu.VMEM((n_blocks, BLK, HEAD_DIM), BF16),
                        pltpu.VMEM((n_blocks, HEAD_DIM, BLK), BF16), pltpu.VMEM((heads, HEAD_DIM, BLK), F32), pltpu.VMEM(grad_out.shape, BF16),
                        pltpu.SemaphoreType.DMA((2,)), SEMS],
        compiler_params=comm_params(1),
        cost_estimate=pl.CostEstimate(flops=8 * pairs * HEAD_DIM + 4 * seq_len * width * q_cols, bytes_accessed=8 * seq_len * width, transcendentals=pairs),
        name="forward",
    )(hidden, w_q, w_k, w_v, cos_t, sin_t, grad_out)


def unrotate(val, cos_t, sin_t):
    return (val * cos_t - pltpu.roll(val, HALF, 1) * sin_t).astype(BF16)


def backward_kernel(heads, q_ref, k_ref, v_ref, dy_ref, wo_ref, ot_ref, lse_ref, cos_ref, sin_ref, o_ref, dkv_ref, dq_a_ref, dq_b_ref, o_all,
                    wo_v, w_sem, do_s, kt, dk_acc, dv_acc, dqt, stage, stage_sems, sems):
    i = pl.program_id(0)
    n_blocks = k_ref.shape[0] // BLK
    qk_scale = HEAD_DIM ** -0.5
    to_log2 = qk_scale * LOG2E
    near = Neighbours()
    own_rows = o_ref.shape[0]
    size = own_rows // CHUNKS
    gather = Gather(near, lambda chunk: o_ref.at[pl.ds(chunk * size, size), :], o_all, own_rows, sems)
    stage_in = pltpu.make_async_copy(o_ref, stage, stage_sems.at[0])
    stage_out = pltpu.make_async_copy(stage, gather.block(near.me, 0, CHUNKS), stage_sems.at[1])

    @pl.when(i == 0)
    def _():
        q_cols = heads * HEAD_DIM
        load = pltpu.make_async_copy(wo_ref.at[pl.ds(pl.multiple_of(near.me * q_cols, q_cols), q_cols), :], wo_v, w_sem)
        load.start()
        gather.begin()
        stage_in.start()

        @pl.loop(0, n_blocks)
        def _(c):
            kt[c] = k_ref[pl.ds(pl.multiple_of(c * BLK, BLK), BLK), :].T

        load.wait()

    cols = [slice(a * HEAD_DIM, (a + 1) * HEAD_DIM) for a in range(heads)]
    d_o = dot(dy_ref[...], wo_v[...], COLS_COLS).astype(BF16)
    do_s[...] = d_o
    dqt[...] = jnp.zeros_like(dqt)
    delta = [jnp.sum(ot_ref[cols[a], :].astype(F32) * d_o[:, cols[a]].T.astype(F32), axis=0, keepdims=True) for a in range(heads)]

    def chunk(c, diagonal):
        rows = pl.ds(pl.multiple_of(c * BLK, BLK), BLK)
        k_c, v_c, kt_c = k_ref[rows, :], v_ref[rows, :], kt[c]
        dk_c = dv_c = None
        for a in range(heads):
            q_a, do_a = q_ref[:, cols[a]], do_s[:, cols[a]]
            s = dot(k_c, q_a, COLS_COLS) * to_log2
            if diagonal:
                s = masked(s)
            p = jnp.exp2(s - lse_ref[a:a + 1, :])
            d_p = dot(v_c, do_a, COLS_COLS)
            d_s = (p * (d_p - delta[a])).astype(BF16)
            dv_a = dot(p.astype(BF16), do_a)
            dk_a = dot(d_s, q_a)
            dv_c = dv_a if dv_c is None else dv_c + dv_a
            dk_c = dk_a if dk_c is None else dk_c + dk_a
            dqt[a] += dot(kt_c, d_s)
        if diagonal:
            dk_acc[c] = dk_c
            dv_acc[c] = dv_c
        else:
            dk_acc[c] += dk_c
            dv_acc[c] += dv_c

    @pl.loop(0, i)
    def _(c):
        chunk(c, False)

    chunk(i, True)
    rows = pl.ds(pl.multiple_of(i * BLK, BLK), BLK)
    for a in range(heads):
        d_q = unrotate(dqt[a].T * qk_scale, cos_ref[rows, :], sin_ref[rows, :])
        if a < heads - 1:
            dq_a_ref[:, cols[a]] = d_q
        else:
            dq_b_ref[...] = d_q

    @pl.when(i == BWD_MIDDLE)
    def _():
        gather.middle()
        stage_in.wait()
        stage_out.start()

    @pl.when(i == BWD_LATE)
    def _():
        gather.late()

    @pl.when(i == n_blocks - 1)
    def _():
        @pl.loop(0, n_blocks)
        def _(c):
            rows_c = pl.ds(pl.multiple_of(c * BLK, BLK), BLK)
            dkv_ref[rows_c, :HEAD_DIM] = unrotate(dk_acc[c] * qk_scale, cos_ref[rows_c, :], sin_ref[rows_c, :])
            dkv_ref[rows_c, HEAD_DIM:] = dv_acc[c].astype(BF16)

        stage_out.wait()
        gather.end()


def backward(q, k, v, d_out, w_o, ot, lse, cos_t, sin_t, heads, sp_size):
    seq_len, width = d_out.shape
    n_blocks = seq_len // BLK
    whole = lambda i: (0, 0)
    pairs = heads * seq_len * (seq_len + BLK) // 2
    q_cols = heads * HEAD_DIM
    any_spec = pl.BlockSpec(memory_space=pl.ANY)
    rows = lambda cols: pl.BlockSpec((BLK, cols), lambda i: (i, 0))
    cols = lambda rows: pl.BlockSpec((rows, BLK), lambda i: (0, i))
    kv_spec = pl.BlockSpec(k.shape, whole)
    last = (heads - 1) * HEAD_DIM
    out = lambda *shape: jax.ShapeDtypeStruct(shape, BF16)
    return pl.pallas_call(
        functools.partial(backward_kernel, heads),
        grid=(n_blocks,),
        in_specs=[rows(q_cols), kv_spec, kv_spec, rows(width), any_spec, cols(q_cols), cols(8), kv_spec, kv_spec, any_spec],
        out_specs=[pl.BlockSpec((seq_len, 2 * HEAD_DIM), whole), rows(last), rows(HEAD_DIM), any_spec],
        out_shape=[out(seq_len, 2 * HEAD_DIM), out(seq_len, last), out(seq_len, HEAD_DIM), out(q_cols * sp_size, seq_len)],
        scratch_shapes=[pltpu.VMEM((q_cols, width), BF16), pltpu.SemaphoreType.DMA, pltpu.VMEM((BLK, q_cols), BF16),
                        pltpu.VMEM((n_blocks, HEAD_DIM, BLK), BF16), pltpu.VMEM((n_blocks, BLK, HEAD_DIM), F32),
                        pltpu.VMEM((n_blocks, BLK, HEAD_DIM), F32), pltpu.VMEM((heads, HEAD_DIM, BLK), F32), pltpu.VMEM(ot.shape, BF16),
                        pltpu.SemaphoreType.DMA((2,)), SEMS],
        compiler_params=comm_params(2),
        cost_estimate=pl.CostEstimate(flops=20 * pairs * HEAD_DIM + 2 * seq_len * width * q_cols, bytes_accessed=8 * seq_len * q_cols, transcendentals=pairs),
        name="backward",
    )(q, k, v, d_out, w_o, ot, lse, cos_t, sin_t, ot)


def lanes(*parts):
    return jnp.concatenate(parts, axis=1)


def products_kernel(ot_ref, ht_ref, dy_ref, d_kv_ref, d_qa_ref, d_qb_ref, tiles, kv_all, qa_all, qb_all,
                    a_buf, b_buf, tile, a_sems, b_sems, t_sems, x_sems, kv_s, qa_s, qb_s, stage_sems, kv_sems, qa_sems, qb_sems):
    near = Neighbours()
    core = lax.rem(near.me, 2)
    half = a_buf.shape[1]
    seq_len = d_kv_ref.shape[0]
    chunk = seq_len // CHUNKS
    n_cols = d_kv_ref.shape[1]
    n_o, n_all = dy_ref.shape[1] // (2 * n_cols), tiles.shape[1]
    n_kv = (n_all - n_o) // 2

    def gather_of(src, dst, sems):
        return Gather(near, lambda c: src.at[pl.ds(c * chunk, chunk), :], dst, seq_len, sems)

    gathers = [gather_of(d_kv_ref, kv_all, kv_sems), gather_of(d_qa_ref, qa_all, qa_sems), gather_of(d_qb_ref, qb_all, qb_sems)]
    stage_in = [pltpu.make_async_copy(src, dst, stage_sems.at[0, n]) for n, (src, dst) in enumerate(((d_kv_ref, kv_s), (d_qa_ref, qa_s), (d_qb_ref, qb_s)))]
    stage_out = [pltpu.make_async_copy(src, gather.block(near.me, 0, CHUNKS), stage_sems.at[1, n])
                 for n, (src, gather) in enumerate(zip((kv_s, qa_s, qb_s), gathers))]
    own_rows = pl.ds(pl.multiple_of(core * half, half), half)
    a_loads = [pltpu.make_async_copy(ref.at[own_rows, :], a_buf.at[n], a_sems.at[n]) for n, ref in enumerate((ot_ref, ht_ref))]

    def b_load(source, p, slot, g):
        if source is dy_ref:
            src = dy_ref.at[:, pl.ds(pl.multiple_of((2 * p + g) * n_cols, n_cols), n_cols)]
        else:
            src = source.at[pl.ds(pl.multiple_of((2 * p + g) * seq_len, seq_len), seq_len), :]
        return pltpu.make_async_copy(src, b_buf.at[slot, :, pl.ds(g * n_cols, n_cols)], b_sems.at[slot, g])

    def start_b(step):
        slot = lax.rem(step, 2)
        for source, low, high in ((dy_ref, 0, n_o), (kv_all, n_o, n_o + n_kv), (qa_all, n_o + n_kv, n_all)):
            @pl.when(jnp.logical_and(step >= low, step < high))
            def _():
                for g in range(2):
                    b_load(source, step - low, slot, g).start()

    def keep(step):
        return pltpu.make_async_copy(tile.at[lax.rem(step, 2)], tiles.at[core, step], t_sems.at[lax.rem(step, 2)])

    def give(step):
        return send(tile.at[lax.rem(step, 2)], tiles.at[core, step], x_sems, step, near.sib)

    near.meet([near.sib, near.xn, near.yn])
    for c in range(CHUNKS):
        gathers[0].start(c)
    a_loads[0].start()
    start_b(jnp.int32(0))
    for load in stage_in:
        load.start()
    a_loads[1].start()
    a_loads[0].wait()

    @pl.loop(0, n_all)
    def _(step):
        slot = lax.rem(step, 2)
        for g in range(2):
            b_load(dy_ref, 0, slot, g).wait()

        @pl.when(jnp.logical_and(step != n_o - 1, step != n_o + n_kv - 1))
        def _():
            start_b(step + 1)

        @pl.when(step >= 2)
        def _():
            keep(step - 2).wait()
            give(step - 2).wait_send()

        @pl.when(step == n_o)
        def _():
            a_loads[1].wait()

        tile[slot] = dot(a_buf[jnp.where(step < n_o, 0, 1)], b_buf[slot])
        keep(step).start()
        give(step).start()

        @pl.when(step == n_o - 2)
        def _():
            for load, store in zip(stage_in, stage_out):
                load.wait()
                store.start()
            gathers[0].middle()

        @pl.when(step == n_o - 1)
        def _():
            gathers[0].late()
            for c in range(CHUNKS):
                gathers[1].start(c)
            stage_out[0].wait()
            gathers[0].end()
            start_b(step + 1)

        @pl.when(step == n_o + n_kv - 1)
        def _():
            gathers[1].middle()
            gathers[1].late()
            for c in range(CHUNKS):
                gathers[2].start(c)
            stage_out[1].wait()
            gathers[1].end()
            start_b(step + 1)

        @pl.when(step == n_all - 3)
        def _():
            gathers[2].middle()

        @pl.when(step == n_all - 2)
        def _():
            gathers[2].late()

    stage_out[2].wait()
    gathers[2].end()
    for step in (n_all - 2, n_all - 1):
        keep(step).wait()
        give(step).wait_send()

    @pl.loop(0, n_all)
    def _(step):
        give(step).wait_recv()


def products(ot_all, ht, d_out, d_kv, d_qa, d_qb, sp_size):
    width, seq_len = ht.shape
    half = width // 2
    cols = 2 * d_kv.shape[1]
    n_all = d_out.shape[1] // cols + 2 * sp_size * d_kv.shape[1] // cols
    any_spec = pl.BlockSpec(memory_space=pl.ANY)
    gathered = [jax.ShapeDtypeStruct((sp_size * seq_len, d.shape[1]), BF16) for d in (d_kv, d_qa, d_qb)]
    return pl.pallas_call(
        products_kernel,
        in_specs=[any_spec] * 6,
        out_specs=[any_spec] * 4,
        out_shape=[jax.ShapeDtypeStruct((2, n_all, half, cols), F32)] + gathered,
        scratch_shapes=[pltpu.VMEM((2, half, seq_len), BF16), pltpu.VMEM((2, seq_len, cols), BF16), pltpu.VMEM((2, half, cols), F32),
                        pltpu.SemaphoreType.DMA((2,)), pltpu.SemaphoreType.DMA((2, 2)), pltpu.SemaphoreType.DMA((2,)),
                        pltpu.SemaphoreType.DMA((2, n_all)), pltpu.VMEM(d_kv.shape, BF16), pltpu.VMEM(d_qa.shape, BF16), pltpu.VMEM(d_qb.shape, BF16),
                        pltpu.SemaphoreType.DMA((2, 3)), SEMS, SEMS, SEMS],
        compiler_params=pltpu.CompilerParams(vmem_limit_bytes=VMEM_LIMIT, collective_id=3, has_side_effects=True),
        cost_estimate=pl.CostEstimate(flops=2 * half * cols * seq_len * n_all, bytes_accessed=8 * half * cols * n_all, transcendentals=0),
        name="products",
    )(ot_all, ht, d_out, d_kv, d_qa, d_qb)


def finish_kernel(heads, n_o, n_kv, ht_ref, d_ref, tiles, wq_ref, wk_ref, wv_ref, wo_ref, tile, sems, ring, ring_sems):
    n_cols = d_ref.shape[2]
    n_j = pl.num_programs(1)
    step = pl.program_id(0) * n_j + pl.program_id(1)
    slot = lax.rem(step, 2)
    half = ring.shape[2]
    every = [(c, t) for t in range(tiles.shape[1]) for c in range(2)]
    groups = [every[g:g + RING] for g in range(0, len(every), RING)]

    def pieces(c, t):
        rows = pl.ds(c * half, half)
        cols = ring.shape[3]
        if t < n_o:
            return [(0, cols, wo_ref.at[rows, pl.ds(t * cols, cols)])]
        if t < n_o + n_kv:
            return [(n * HEAD_DIM, HEAD_DIM, (wk_ref, wv_ref)[n % 2].at[rows, pl.ds(((t - n_o) * 2 + n // 2) * HEAD_DIM, HEAD_DIM)]) for n in range(4)]
        wide = (heads - 1) * HEAD_DIM
        return [(n * wide, wide, wq_ref.at[rows, pl.ds(((t - n_o - n_kv) * 2 + n) * heads * HEAD_DIM, wide)]) for n in range(2)]

    def ins(g):
        return [pltpu.make_async_copy(tiles.at[c, t], ring.at[g % 2, n], ring_sems.at[0, g % 2, n, 0]) for n, (c, t) in enumerate(groups[g])]

    def outs(g):
        return [pltpu.make_async_copy(ring.at[g % 2, n, :, pl.ds(col, count)], dst, ring_sems.at[1, g % 2, n, m])
                for n, (c, t) in enumerate(groups[g]) for m, (col, count, dst) in enumerate(pieces(c, t))]

    for g in range(len(groups) + 2):
        @pl.when(step == g)
        def _():
            if 0 <= g - 1 < len(groups):
                for copy in ins(g - 1):
                    copy.wait()
                for copy in outs(g - 1):
                    copy.start()
            if 0 <= g - 2 < len(groups):
                for copy in outs(g - 2):
                    copy.wait()
            if g < len(groups):
                for copy in ins(g):
                    copy.start()

    def copies(step, slot):
        rows = pl.ds(pl.multiple_of((step // n_j) * MROWS, MROWS), MROWS)
        out = []
        for g in range(2):
            col = ((lax.rem(step, n_j) * 2 + g + 1) * heads - 1) * HEAD_DIM
            out.append(pltpu.make_async_copy(tile.at[slot, :, pl.ds(g * n_cols, n_cols)],
                                             wq_ref.at[rows, pl.ds(pl.multiple_of(col, HEAD_DIM), n_cols)], sems.at[slot, g]))
        return out

    @pl.when(step >= 2)
    def _():
        for copy in copies(step - 2, slot):
            copy.wait()

    tile[slot] = dot(ht_ref[...], lanes(d_ref[0], d_ref[1]))
    for copy in copies(step, slot):
        copy.start()

    @pl.when(step == pl.num_programs(0) * n_j - 1)
    def _():
        for copy in copies(step - 1, 1 - slot) + copies(step, slot):
            copy.wait()


def finish(ht, d_q, tiles, heads, n_o, n_kv):
    width, seq_len = ht.shape
    groups, _, n_cols = d_q.shape
    steps = (width // MROWS) * (groups // 2)
    assert -(-2 * tiles.shape[1] // RING) + 2 <= steps
    any_spec = pl.BlockSpec(memory_space=pl.ANY)
    out = lambda cols: jax.ShapeDtypeStruct((width, cols), F32)
    return pl.pallas_call(
        functools.partial(finish_kernel, heads, n_o, n_kv),
        grid=(width // MROWS, groups // 2),
        in_specs=[pl.BlockSpec((MROWS, seq_len), lambda m, j: (m, 0)), pl.BlockSpec((2, seq_len, n_cols), lambda m, j: (j, 0, 0)), any_spec],
        out_specs=[any_spec] * 4,
        out_shape=[out(groups * heads * HEAD_DIM), out(groups * HEAD_DIM), out(groups * HEAD_DIM),
                   jax.ShapeDtypeStruct((groups * heads * HEAD_DIM, width), F32)],
        scratch_shapes=[pltpu.VMEM((2, MROWS, 2 * n_cols), F32), pltpu.SemaphoreType.DMA((2, 2)), pltpu.VMEM((2, RING) + tiles.shape[2:], F32),
                        pltpu.SemaphoreType.DMA((2, 2, RING, 4))],
        compiler_params=params(2),
        cost_estimate=pl.CostEstimate(flops=2 * width * seq_len * groups * n_cols, bytes_accessed=2 * width * seq_len, transcendentals=0),
        name="finish",
    )(ht, d_q, tiles)


def d_hidden_kernel(me_ref, dkv_ref, dq_ref, wk_ref, wv_ref, wq0_ref, wq1_ref, acc_ref):
    prod = dot(lanes(dkv_ref[0], dq_ref[0]), lanes(wk_ref[...], wv_ref[...], wq0_ref[...], wq1_ref[...]), COLS_COLS)

    @pl.when(pl.program_id(0) == 0)
    def _():
        acc_ref[...] = prod

    @pl.when(pl.program_id(0) > 0)
    def _():
        acc_ref[...] += prod


def d_hidden(me, d_kv, d_q, w_k, w_v, w_q, tok_count, heads):
    width = w_q.shape[0]
    groups = d_kv.shape[0]
    own_spec = pl.BlockSpec((1, tok_count, 2 * HEAD_DIM), lambda j, me_ref: (j, me_ref[0], 0))
    w_spec = lambda scale, off: pl.BlockSpec((width, HEAD_DIM), lambda j, me_ref: (0, j * scale + off))
    return pl.pallas_call(
        d_hidden_kernel,
        grid_spec=pltpu.PrefetchScalarGridSpec(
            num_scalar_prefetch=1, grid=(groups,),
            in_specs=[own_spec, own_spec, w_spec(1, 0), w_spec(1, 0), w_spec(heads, 0), w_spec(heads, 1)],
            out_specs=pl.BlockSpec((tok_count, width), lambda j, me_ref: (0, 0))),
        out_shape=jax.ShapeDtypeStruct((tok_count, width), F32),
        compiler_params=params(),
        cost_estimate=pl.CostEstimate(flops=8 * tok_count * width * groups * HEAD_DIM, bytes_accessed=8 * width * groups * HEAD_DIM, transcendentals=0),
        name="d_hidden",
    )(me, d_kv, d_q, w_k, w_v, w_q, w_q)


def grad_x_kernel(me_ref, dq_ref, wq0_ref, wq1_ref, part_ref, x_ref, dy_ref, gain_ref, gx_ref, gg_ref, acc):
    j = pl.program_id(0)
    prod = dot(lanes(dq_ref[0], dq_ref[1]), lanes(wq0_ref[...], wq1_ref[...]), COLS_COLS)

    @pl.when(j == 0)
    def _():
        acc[...] = part_ref[...] + prod

    @pl.when(j > 0)
    def _():
        acc[...] += prod

    @pl.when(j == pl.num_programs(0) - 1)
    def _():
        gain = gain_ref[...]
        gg_ref[...] = jnp.zeros_like(gg_ref)

        @pl.loop(0, x_ref.shape[0] // ROWS)
        def _(r):
            rows = pl.ds(pl.multiple_of(r * ROWS, ROWS), ROWS)
            x_f = x_ref[rows, :].astype(F32)
            inv_rms = lax.rsqrt(jnp.mean(x_f * x_f, axis=-1, keepdims=True) + NORM_EPS)
            normed = x_f * inv_rms
            d_hid = acc[rows, :]
            both = d_hid * normed
            gg_ref[...] += jnp.sum(both.reshape(ROWS // 8, 8, both.shape[1]), axis=0)
            mean = jnp.mean(both * gain, axis=-1, keepdims=True)
            d_x = inv_rms * (d_hid * gain - normed * mean)
            gx_ref[rows, :] = (dy_ref[rows, :].astype(F32) + d_x).astype(BF16)


def grad_x_final(me, d_q, w_q, part, x, grad_out, gain_f, heads):
    tok_count, width = x.shape
    groups = d_q.shape[0]
    whole = lambda j, me_ref: (0, 0)
    w_spec = lambda g: pl.BlockSpec((width, HEAD_DIM), lambda j, me_ref: (0, (2 * j + g + 1) * heads - 1))
    full = pl.BlockSpec((tok_count, width), whole)
    return pl.pallas_call(
        grad_x_kernel,
        grid_spec=pltpu.PrefetchScalarGridSpec(
            num_scalar_prefetch=1, grid=(groups // 2,),
            in_specs=[pl.BlockSpec((2, tok_count, HEAD_DIM), lambda j, me_ref: (j, me_ref[0], 0)), w_spec(0), w_spec(1), full, full, full,
                      pl.BlockSpec((1, width), whole)],
            out_specs=[full, pl.BlockSpec((8, width), whole)],
            scratch_shapes=[pltpu.VMEM((tok_count, width), F32)]),
        out_shape=[jax.ShapeDtypeStruct((tok_count, width), BF16), jax.ShapeDtypeStruct((8, width), F32)],
        compiler_params=params(),
        cost_estimate=pl.CostEstimate(flops=2 * tok_count * width * groups * HEAD_DIM, bytes_accessed=8 * width * tok_count, transcendentals=0),
        name="grad_x",
    )(me, d_q, w_q, w_q, part, x, grad_out, gain_f)


def solution(mesh):
    sp_size = mesh.shape['sp']
    seq_spec = P(('dp', 'sp'), None)
    pos_spec = P(('dp', 'sp'))
    replicated = P(None, None)
    part_rows = P('dp', None)

    def local_step(x, grad_out, positions, gain, w_q, w_k, w_v, w_o):
        tok_count = x.shape[0]
        n_heads = w_q.shape[1] // HEAD_DIM
        heads = n_heads // sp_size
        me = lax.axis_index('sp')
        gain_f = gain.astype(F32).reshape(1, -1)
        hidden, cos_t, sin_t = gather_h(x, gain_f, positions, sp_size)
        q, k, v, ht, ot, lse, d_out = forward(hidden, w_q, w_k, w_v, cos_t, sin_t, grad_out, heads)
        *grads, ot_all = backward(q, k, v, d_out, w_o, ot, lse, cos_t, sin_t, heads, sp_size)
        tiles, *gathered = products(ot_all, ht, d_out, *grads, sp_size)
        dkv_all, dqa_all, dqb_all = [val.reshape(sp_size, -1, val.shape[1]) for val in gathered]
        n_kv = sp_size // 2
        grad_wq, grad_wk, grad_wv, grad_wo = finish(ht, dqb_all, tiles, heads, tiles.shape[1] - 2 * n_kv, n_kv)
        o_own = lax.dynamic_slice_in_dim(ot_all, me * tok_count, tok_count, axis=1)
        result = (x.astype(F32) + dot(o_own, w_o, ROWS_ROWS)).astype(BF16)
        me_arr = me.reshape(1).astype(jnp.int32)
        part = d_hidden(me_arr, dkv_all, dqa_all, w_k, w_v, w_q, tok_count, heads)
        grad_x, gg = grad_x_final(me_arr, dqb_all, w_q, part, x, grad_out, gain_f, heads)
        grad_gain = jnp.sum(lax.all_gather(gg, 'sp', axis=0, tiled=True), axis=0)
        return result, grad_x, grad_wq, grad_wk, grad_wv, grad_wo, grad_gain

    return jax.shard_map(local_step, mesh=mesh,
                         in_specs=(seq_spec, seq_spec, pos_spec, P(None), replicated, replicated, replicated, replicated),
                         out_specs=(seq_spec, seq_spec, part_rows, part_rows, part_rows, part_rows, P('dp')),
                         check_vma=False)
```

```python
import functools

import jax
import jax.numpy as jnp
from jax import lax
from jax.experimental import pallas as pl
from jax.experimental.pallas import tpu as pltpu
from jax.sharding import PartitionSpec as P

HEAD_DIM = 128
HALF = HEAD_DIM // 2
ROPE_THETA = 1000000.0
NORM_EPS = 1e-05
NEG_LARGE = -1e30
LOG2E = 1.4426950408889634
BLK = 512
CHUNKS = 4
FWD_MIDDLE, BWD_MIDDLE, BWD_LATE = 5, 4, 5
MROWS = 1024
RING = 3
ROW_STEPS = 8
F32 = jnp.float32
BF16 = jnp.bfloat16
ROWS_ROWS = (((0,), (0,)), ((), ()))
COLS_COLS = (((1,), (1,)), ((), ()))
ROWS_COLS = (((0,), (1,)), ((), ()))
VMEM_LIMIT = 63 * 1024 * 1024


def dot(a, b, dims=(((1,), (0,)), ((), ()))):
    return lax.dot_general(a, b, dims, preferred_element_type=F32)


def params(axes=1):
    return pltpu.CompilerParams(dimension_semantics=("arbitrary",) * axes, vmem_limit_bytes=VMEM_LIMIT)


class Neighbours:
    def __init__(self):
        self.me = lax.axis_index('sp')
        core, col, row = lax.rem(self.me, 2), lax.rem(self.me // 2, 2), self.me // 4
        self.sib = self.me + 1 - 2 * core
        self.xn = self.me + 2 - 4 * col
        self.yn = self.me + 4 - 8 * row
        self.diag = self.xn + self.yn - self.me

    def meet(self, peers):
        barrier = pltpu.get_barrier_semaphore()
        for peer in peers:
            pl.semaphore_signal(barrier, inc=1, device_id={'sp': peer}, device_id_type=pl.DeviceIdType.MESH)
        pl.semaphore_wait(barrier, len(peers))

    def others(self):
        flip = lambda dev: dev + 1 - 2 * lax.rem(dev, 2)
        return [self.sib, self.xn, flip(self.xn), self.yn, flip(self.yn), self.diag, flip(self.diag)]


def send(src, dst, sems, index, peer):
    return pltpu.make_async_remote_copy(src_ref=src, dst_ref=dst, send_sem=sems.at[0, index], recv_sem=sems.at[1, index],
                                        device_id={'sp': peer}, device_id_type=pl.DeviceIdType.MESH)


class Gather:
    COPIES = 22

    def __init__(self, near, own, dst, rows, sems):
        self.near, self.own, self.dst, self.rows, self.sems = near, own, dst, rows, sems

    def block(self, dev, chunk, count=1):
        size = self.rows // CHUNKS
        return self.dst.at[pl.ds(pl.multiple_of(dev * self.rows + chunk * size, size), count * size), :]

    def first(self, chunk, kind):
        peer = (self.near.xn, self.near.yn, self.near.sib)[kind]
        return send(self.own(chunk), self.block(self.near.me, chunk), self.sems, kind * CHUNKS + chunk, peer)

    def onward(self, chunk):
        over_y = chunk < CHUNKS // 2
        rows = self.block(self.near.xn if over_y else self.near.yn, chunk)
        return send(rows, rows, self.sems, 12 + chunk, self.near.yn if over_y else self.near.xn)

    def share(self, kind):
        rows = self.block((self.near.xn, self.near.yn)[kind], 0, CHUNKS)
        return send(rows, rows, self.sems, 16 + kind, self.near.sib)

    def share_diag(self, chunk):
        rows = self.block(self.near.diag, chunk)
        return send(rows, rows, self.sems, 18 + chunk, self.near.sib)

    def begin(self):
        self.near.meet([self.near.sib, self.near.xn, self.near.yn])
        for chunk in range(CHUNKS):
            self.start(chunk)

    def start(self, chunk):
        for kind in range(3):
            self.first(chunk, kind).start()

    def middle(self):
        for chunk in (0, 1):
            self.first(chunk, 0).wait_recv()
            self.onward(chunk).start()
        self.first(2, 1).wait_recv()
        self.onward(2).start()

    def late(self):
        self.first(3, 1).wait_recv()
        self.onward(3).start()
        for chunk in (2, 3):
            self.first(chunk, 0).wait_recv()
        self.share(0).start()
        for chunk in (0, 1):
            self.first(chunk, 1).wait_recv()
        self.share(1).start()

    def end(self):
        for chunk in (0, 2, 1, 3):
            self.onward(chunk).wait_recv()
            self.share_diag(chunk).start()
        sent = [self.first(chunk, kind) for chunk in range(CHUNKS) for kind in range(3)]
        for copy in sent:
            copy.wait_send()
        for chunk in range(CHUNKS):
            self.first(chunk, 2).wait_recv()
            self.onward(chunk).wait_send()
        for copy in [self.share(0), self.share(1)] + [self.share_diag(chunk) for chunk in range(CHUNKS)]:
            copy.wait()


SEMS = pltpu.SemaphoreType.DMA((2, Gather.COPIES))


def comm_params(collective_id):
    return pltpu.CompilerParams(dimension_semantics=("arbitrary",), vmem_limit_bytes=VMEM_LIMIT, collective_id=collective_id,
                                has_side_effects=True)


def gather_h_kernel(x_ref, gain_ref, pos_ref, freq_ref, h_all, cos_ref, sin_ref, x_v, h_v, pos_all, in_sems, out_sem, pos_sems, sems):
    near = Neighbours()
    rows = x_ref.shape[0]
    size = rows // CHUNKS
    part = lambda ref, chunk: ref.at[pl.ds(chunk * size, size), :]
    gather = Gather(near, lambda chunk: part(h_v, chunk), h_all, rows, sems)
    loads = [pltpu.make_async_copy(part(x_ref, chunk), part(x_v, chunk), in_sems.at[chunk]) for chunk in range(CHUNKS)]
    for load in loads:
        load.start()
    others = near.others()
    near.meet(others)
    pos_all[near.me] = pos_ref[...]
    positions = [send(pos_ref, pos_all.at[near.me], pos_sems, r, peer) for r, peer in enumerate(others)]
    for copy in positions:
        copy.start()
    for chunk in range(CHUNKS):
        loads[chunk].wait()

        @pl.loop(0, size // 32)
        def _(r):
            at = pl.ds(pl.multiple_of(chunk * size + r * 32, 32), 32)
            x_f = x_v[at, :].astype(F32)
            normed = x_f * lax.rsqrt(jnp.mean(x_f * x_f, axis=-1, keepdims=True) + NORM_EPS)
            h_v[at, :] = (normed * gain_ref[...]).astype(BF16)

        gather.start(chunk)
    own = pltpu.make_async_copy(h_v, gather.block(near.me, 0, CHUNKS), out_sem)
    own.start()
    for copy in positions:
        copy.wait()
    sign = jnp.where(lax.broadcasted_iota(jnp.int32, (1, HEAD_DIM), 1) < HALF, -1.0, 1.0)

    @pl.loop(0, pos_all.shape[0])
    def _(b):
        at = pl.ds(pl.multiple_of(b * rows, rows), rows)
        pos = jnp.broadcast_to(pos_all[b, 0:1, :].astype(F32), (HEAD_DIM, rows)).T
        angles = pos * freq_ref[...]
        cos_ref[at, :] = jnp.cos(angles)
        sin_ref[at, :] = jnp.sin(angles) * sign

    gather.middle()
    gather.late()
    own.wait()
    gather.end()


def gather_h(x, gain_f, positions, sp_size):
    rows, width = x.shape
    any_spec = pl.BlockSpec(memory_space=pl.ANY)
    vmem = pl.BlockSpec(memory_space=pltpu.VMEM)
    inv_freq = ROPE_THETA ** (-jnp.arange(0, HEAD_DIM, 2).astype(F32) / HEAD_DIM)
    freq = jnp.concatenate([inv_freq, inv_freq])[None, :]
    table = jax.ShapeDtypeStruct((rows * sp_size, HEAD_DIM), F32)
    return pl.pallas_call(
        gather_h_kernel,
        in_specs=[any_spec, vmem, vmem, vmem],
        out_specs=[any_spec, vmem, vmem],
        out_shape=[jax.ShapeDtypeStruct((rows * sp_size, width), BF16), table, table],
        scratch_shapes=[pltpu.VMEM((rows, width), BF16), pltpu.VMEM((rows, width), BF16), pltpu.VMEM((sp_size, 8, rows), jnp.int32),
                        pltpu.SemaphoreType.DMA((CHUNKS,)), pltpu.SemaphoreType.DMA, pltpu.SemaphoreType.DMA((2, 7)), SEMS],
        compiler_params=pltpu.CompilerParams(vmem_limit_bytes=VMEM_LIMIT, collective_id=0, has_side_effects=True),
        name="gather_h",
    )(x, gain_f, jnp.broadcast_to(positions[None, :], (8, rows)), freq)


def masked(scores):
    key = lax.broadcasted_iota(jnp.int32, scores.shape, 0)
    query = lax.broadcasted_iota(jnp.int32, scores.shape, 1)
    return jnp.where(key <= query, scores, NEG_LARGE)


def forward_kernel(heads, h_ref, wq_ref, wk_ref, wv_ref, cos_ref, sin_ref, dy_ref, q_ref, k_ref, v_ref, ht_ref, o_ref, lse_ref, dy_all,
                   w_v, w_sems, k_s, vt, acc, stage, stage_sems, sems):
    i = pl.program_id(0)
    near = Neighbours()
    rows = dy_ref.shape[0]
    size = rows // CHUNKS
    gather = Gather(near, lambda chunk: dy_ref.at[pl.ds(chunk * size, size), :], dy_all, rows, sems)
    stage_in = pltpu.make_async_copy(dy_ref, stage, stage_sems.at[0])
    stage_out = pltpu.make_async_copy(stage, gather.block(near.me, 0, CHUNKS), stage_sems.at[1])
    to_log2 = HEAD_DIM ** -0.5 * LOG2E
    q_cols = heads * HEAD_DIM

    @pl.when(i == 0)
    def _():
        loads, col = [], 0
        for n, (ref, count) in enumerate(((wq_ref, q_cols), (wk_ref, HEAD_DIM), (wv_ref, HEAD_DIM))):
            at = pl.ds(pl.multiple_of(near.me * count, HEAD_DIM), count)
            loads.append(pltpu.make_async_copy(ref.at[:, at], w_v.at[:, pl.ds(col, count)], w_sems.at[n]))
            col += count
        for load in loads:
            load.start()
        gather.begin()
        stage_in.start()
        for load in loads:
            load.wait()

    ht_ref[...] = h_ref[...].T
    prod = dot(h_ref[...], w_v[...])
    cos_t, sin_t = cos_ref[...], sin_ref[...]
    for a in range(heads + 1):
        val = prod[:, a * HEAD_DIM:(a + 1) * HEAD_DIM]
        rot = (val * cos_t + pltpu.roll(val, HALF, 1) * sin_t).astype(BF16)
        if a < heads:
            q_ref[:, a * HEAD_DIM:(a + 1) * HEAD_DIM] = rot
        else:
            k_ref[...] = rot
            k_s[i] = rot
    v_i = prod[:, q_cols + HEAD_DIM:].astype(BF16)
    v_ref[...] = v_i
    vt[i] = v_i.T
    acc[...] = jnp.zeros_like(acc)

    def chunk(c, carry, diagonal):
        k_c, vt_c = k_s[c], vt[c]
        scores = [dot(k_c, q_ref[:, a * HEAD_DIM:(a + 1) * HEAD_DIM], COLS_COLS) * to_log2 for a in range(heads)]
        out = []
        for a in range(heads):
            s = masked(scores[a]) if diagonal else scores[a]
            m_old, l_old = carry[a]
            m_new = jnp.maximum(m_old, jnp.max(s, axis=0, keepdims=True))
            alpha = jnp.exp2(m_old - m_new)
            p = jnp.exp2(s - m_new)
            l_new = l_old * alpha + jnp.sum(p, axis=0, keepdims=True)
            acc[a] = acc[a] * alpha + dot(vt_c, p.astype(BF16))
            out.append((m_new, l_new))
        return tuple(out)

    start = tuple((jnp.full((1, BLK), NEG_LARGE, F32), jnp.zeros((1, BLK), F32)) for _ in range(heads))
    carry = lax.fori_loop(0, i, lambda c, carry: chunk(c, carry, False), start)
    carry = chunk(i, carry, True)
    for a in range(heads):
        m_a, l_a = carry[a]
        o_ref[a * HEAD_DIM:(a + 1) * HEAD_DIM, :] = (acc[a] / l_a).astype(BF16)
        lse_ref[a:a + 1, :] = m_a + jnp.log2(l_a)

    @pl.when(i == FWD_MIDDLE)
    def _():
        gather.middle()
        stage_in.wait()
        stage_out.start()

    @pl.when(i == pl.num_programs(0) - 1)
    def _():
        gather.late()
        stage_out.wait()
        gather.end()


def forward(hidden, w_q, w_k, w_v, cos_t, sin_t, grad_out, heads):
    seq_len, width = hidden.shape
    n_blocks = seq_len // BLK
    q_cols = heads * HEAD_DIM
    pairs = heads * seq_len * (seq_len + BLK) // 2
    any_spec = pl.BlockSpec(memory_space=pl.ANY)
    rows = lambda cols: pl.BlockSpec((BLK, cols), lambda i: (i, 0))
    cols = lambda rows: pl.BlockSpec((rows, BLK), lambda i: (0, i))
    out = lambda *shape, dtype=BF16: jax.ShapeDtypeStruct(shape, dtype)
    return pl.pallas_call(
        functools.partial(forward_kernel, heads),
        grid=(n_blocks,),
        in_specs=[rows(width), any_spec, any_spec, any_spec, rows(HEAD_DIM), rows(HEAD_DIM), any_spec],
        out_specs=[rows(q_cols), rows(HEAD_DIM), rows(HEAD_DIM), cols(width), cols(q_cols), cols(8), any_spec],
        out_shape=[out(seq_len, q_cols), out(seq_len, HEAD_DIM), out(seq_len, HEAD_DIM), out(width, seq_len), out(q_cols, seq_len),
                   out(8, seq_len, dtype=F32), out(seq_len, width)],
        scratch_shapes=[pltpu.VMEM((width, q_cols + 2 * HEAD_DIM), BF16), pltpu.SemaphoreType.DMA((3,)), pltpu.VMEM((n_blocks, BLK, HEAD_DIM), BF16),
                        pltpu.VMEM((n_blocks, HEAD_DIM, BLK), BF16), pltpu.VMEM((heads, HEAD_DIM, BLK), F32), pltpu.VMEM(grad_out.shape, BF16),
                        pltpu.SemaphoreType.DMA((2,)), SEMS],
        compiler_params=comm_params(1),
        cost_estimate=pl.CostEstimate(flops=8 * pairs * HEAD_DIM + 4 * seq_len * width * q_cols, bytes_accessed=8 * seq_len * width, transcendentals=pairs),
        name="forward",
    )(hidden, w_q, w_k, w_v, cos_t, sin_t, grad_out)


def unrotate(val, cos_t, sin_t):
    return (val * cos_t - pltpu.roll(val, HALF, 1) * sin_t).astype(BF16)


def backward_kernel(heads, q_ref, k_ref, v_ref, dy_ref, wo_ref, ot_ref, lse_ref, cos_ref, sin_ref, o_ref, dkv_ref, dq_a_ref, dq_b_ref, o_all,
                    wo_v, w_sem, do_s, kt, dk_acc, dv_acc, dqt, stage, stage_sems, sems):
    i = pl.program_id(0)
    n_blocks = k_ref.shape[0] // BLK
    qk_scale = HEAD_DIM ** -0.5
    to_log2 = qk_scale * LOG2E
    near = Neighbours()
    own_rows = o_ref.shape[0]
    size = own_rows // CHUNKS
    gather = Gather(near, lambda chunk: o_ref.at[pl.ds(chunk * size, size), :], o_all, own_rows, sems)
    stage_in = pltpu.make_async_copy(o_ref, stage, stage_sems.at[0])
    stage_out = pltpu.make_async_copy(stage, gather.block(near.me, 0, CHUNKS), stage_sems.at[1])

    @pl.when(i == 0)
    def _():
        q_cols = heads * HEAD_DIM
        load = pltpu.make_async_copy(wo_ref.at[pl.ds(pl.multiple_of(near.me * q_cols, q_cols), q_cols), :], wo_v, w_sem)
        load.start()
        gather.begin()
        stage_in.start()

        @pl.loop(0, n_blocks)
        def _(c):
            kt[c] = k_ref[pl.ds(pl.multiple_of(c * BLK, BLK), BLK), :].T

        load.wait()

    cols = [slice(a * HEAD_DIM, (a + 1) * HEAD_DIM) for a in range(heads)]
    d_o = dot(dy_ref[...], wo_v[...], COLS_COLS).astype(BF16)
    do_s[...] = d_o
    dqt[...] = jnp.zeros_like(dqt)
    delta = [jnp.sum(ot_ref[cols[a], :].astype(F32) * d_o[:, cols[a]].T.astype(F32), axis=0, keepdims=True) for a in range(heads)]

    def chunk(c, diagonal):
        rows = pl.ds(pl.multiple_of(c * BLK, BLK), BLK)
        k_c, v_c, kt_c = k_ref[rows, :], v_ref[rows, :], kt[c]
        dk_c = dv_c = None
        for a in range(heads):
            q_a, do_a = q_ref[:, cols[a]], do_s[:, cols[a]]
            s = dot(k_c, q_a, COLS_COLS) * to_log2
            if diagonal:
                s = masked(s)
            p = jnp.exp2(s - lse_ref[a:a + 1, :])
            d_p = dot(v_c, do_a, COLS_COLS)
            d_s = (p * (d_p - delta[a])).astype(BF16)
            dv_a = dot(p.astype(BF16), do_a)
            dk_a = dot(d_s, q_a)
            dv_c = dv_a if dv_c is None else dv_c + dv_a
            dk_c = dk_a if dk_c is None else dk_c + dk_a
            dqt[a] += dot(kt_c, d_s)
        if diagonal:
            dk_acc[c] = dk_c
            dv_acc[c] = dv_c
        else:
            dk_acc[c] += dk_c
            dv_acc[c] += dv_c

    @pl.loop(0, i)
    def _(c):
        chunk(c, False)

    chunk(i, True)
    rows = pl.ds(pl.multiple_of(i * BLK, BLK), BLK)
    for a in range(heads):
        d_q = unrotate(dqt[a].T * qk_scale, cos_ref[rows, :], sin_ref[rows, :])
        if a < heads - 1:
            dq_a_ref[:, cols[a]] = d_q
        else:
            dq_b_ref[...] = d_q

    @pl.when(i == BWD_MIDDLE)
    def _():
        gather.middle()
        stage_in.wait()
        stage_out.start()

    @pl.when(i == BWD_LATE)
    def _():
        gather.late()

    @pl.when(i == n_blocks - 1)
    def _():
        @pl.loop(0, n_blocks)
        def _(c):
            rows_c = pl.ds(pl.multiple_of(c * BLK, BLK), BLK)
            dkv_ref[rows_c, :HEAD_DIM] = unrotate(dk_acc[c] * qk_scale, cos_ref[rows_c, :], sin_ref[rows_c, :])
            dkv_ref[rows_c, HEAD_DIM:] = dv_acc[c].astype(BF16)

        stage_out.wait()
        gather.end()


def backward(q, k, v, d_out, w_o, ot, lse, cos_t, sin_t, heads, sp_size):
    seq_len, width = d_out.shape
    n_blocks = seq_len // BLK
    whole = lambda i: (0, 0)
    pairs = heads * seq_len * (seq_len + BLK) // 2
    q_cols = heads * HEAD_DIM
    any_spec = pl.BlockSpec(memory_space=pl.ANY)
    rows = lambda cols: pl.BlockSpec((BLK, cols), lambda i: (i, 0))
    cols = lambda rows: pl.BlockSpec((rows, BLK), lambda i: (0, i))
    kv_spec = pl.BlockSpec(k.shape, whole)
    last = (heads - 1) * HEAD_DIM
    out = lambda *shape: jax.ShapeDtypeStruct(shape, BF16)
    return pl.pallas_call(
        functools.partial(backward_kernel, heads),
        grid=(n_blocks,),
        in_specs=[rows(q_cols), kv_spec, kv_spec, rows(width), any_spec, cols(q_cols), cols(8), kv_spec, kv_spec, any_spec],
        out_specs=[pl.BlockSpec((seq_len, 2 * HEAD_DIM), whole), rows(last), rows(HEAD_DIM), any_spec],
        out_shape=[out(seq_len, 2 * HEAD_DIM), out(seq_len, last), out(seq_len, HEAD_DIM), out(q_cols * sp_size, seq_len)],
        scratch_shapes=[pltpu.VMEM((q_cols, width), BF16), pltpu.SemaphoreType.DMA, pltpu.VMEM((BLK, q_cols), BF16),
                        pltpu.VMEM((n_blocks, HEAD_DIM, BLK), BF16), pltpu.VMEM((n_blocks, BLK, HEAD_DIM), F32),
                        pltpu.VMEM((n_blocks, BLK, HEAD_DIM), F32), pltpu.VMEM((heads, HEAD_DIM, BLK), F32), pltpu.VMEM(ot.shape, BF16),
                        pltpu.SemaphoreType.DMA((2,)), SEMS],
        compiler_params=comm_params(2),
        cost_estimate=pl.CostEstimate(flops=20 * pairs * HEAD_DIM + 2 * seq_len * width * q_cols, bytes_accessed=8 * seq_len * q_cols, transcendentals=pairs),
        name="backward",
    )(q, k, v, d_out, w_o, ot, lse, cos_t, sin_t, ot)


def lanes(*parts):
    return jnp.concatenate(parts, axis=1)


def products_kernel(heads, ot_ref, ht_ref, dy_ref, d_kv_ref, d_qa_ref, d_qb_ref, x_ref, wo_ref, wk_ref, wv_ref, wq_ref,
                    tiles, kv_all, qa_all, qb_all, res_ref, hid_ref,
                    a_buf, b_buf, tile, a_sem, b_sems, t_sems, x_sems, stage, stage_sems, ot_v, o_v, x_v, io_sems, own, own_sems, w_v, w_sems, acc,
                    kv_sems, qa_sems, qb_sems):
    near = Neighbours()
    core = lax.rem(near.me, 2)
    half = a_buf.shape[0]
    seq_len = d_kv_ref.shape[0]
    rows, width = x_ref.shape
    chunk = seq_len // CHUNKS
    n_cols = d_kv_ref.shape[1]
    n_o, n_all = width // (2 * n_cols), tiles.shape[1]
    n_kv = (n_all - n_o) // 2

    def gather_of(src, dst, sems):
        return Gather(near, lambda c: src.at[pl.ds(c * chunk, chunk), :], dst, seq_len, sems)

    local = (d_kv_ref, d_qa_ref, d_qb_ref)
    gathers = [gather_of(d_kv_ref, kv_all, kv_sems), gather_of(d_qa_ref, qa_all, qa_sems), gather_of(d_qb_ref, qb_all, qb_sems)]

    def stage_in(n):
        return pltpu.make_async_copy(local[n], stage.at[:, pl.ds(0, local[n].shape[1])], stage_sems.at[0])

    def stage_out(n):
        return pltpu.make_async_copy(stage.at[:, pl.ds(0, local[n].shape[1])], gathers[n].block(near.me, 0, CHUNKS), stage_sems.at[1])

    def copy_own(n):
        stage_in(n).wait()
        stage_out(n).start()

    own_rows = pl.ds(pl.multiple_of(core * half, half), half)
    tokens = pl.ds(pl.multiple_of(near.me * rows, rows), rows)
    ot_load = pltpu.make_async_copy(ot_ref.at[:, tokens], ot_v, io_sems.at[0])
    x_load = pltpu.make_async_copy(x_ref, x_v, io_sems.at[1])
    res_store = pltpu.make_async_copy(x_v, res_ref, io_sems.at[2])
    hid_store = pltpu.make_async_copy(acc, hid_ref, io_sems.at[3])

    def a_load(ref):
        return pltpu.make_async_copy(ref.at[own_rows, :], a_buf, a_sem)

    def b_load(source, p, slot, g):
        if source is dy_ref:
            src = dy_ref.at[:, pl.ds(pl.multiple_of((2 * p + g) * n_cols, n_cols), n_cols)]
        else:
            src = source.at[pl.ds(pl.multiple_of((2 * p + g) * seq_len, seq_len), seq_len), :]
        return pltpu.make_async_copy(src, b_buf.at[slot, :, pl.ds(g * n_cols, n_cols)], b_sems.at[slot, g])

    def start_b(step):
        slot = lax.rem(step, 2)
        for source, low, high in ((dy_ref, 0, n_o), (kv_all, n_o, n_o + n_kv), (qa_all, n_o + n_kv, n_all)):
            @pl.when(jnp.logical_and(step >= low, step < high))
            def _():
                for g in range(2):
                    b_load(source, step - low, slot, g).start()

    def keep(step):
        return pltpu.make_async_copy(tile.at[lax.rem(step, 2)], tiles.at[core, step], t_sems.at[lax.rem(step, 2)])

    def give(step):
        return send(tile.at[lax.rem(step, 2)], tiles.at[core, step], x_sems, step, near.sib)

    def result_part():
        cols = b_buf.shape[2]

        def w_load(n):
            slot = lax.rem(n, 2)
            return pltpu.make_async_copy(wo_ref.at[:, pl.ds(pl.multiple_of(n * cols, cols), cols)], b_buf.at[slot, pl.ds(0, wo_ref.shape[0]), :],
                                         b_sems.at[slot, 0])

        w_load(jnp.int32(0)).start()
        ot_load.wait()

        @pl.loop(0, ot_v.shape[0] // BLK)
        def _(r):
            at = pl.ds(pl.multiple_of(r * BLK, BLK), BLK)
            o_v[:, at] = ot_v[at, :].T

        x_load.wait()

        @pl.loop(0, n_o)
        def _(n):
            w_load(n).wait()

            @pl.when(n + 1 < n_o)
            def _():
                w_load(n + 1).start()

            at = pl.ds(pl.multiple_of(n * cols, cols), cols)
            x_v[:, at] = (x_v[:, at].astype(F32) + dot(o_v[...], b_buf[lax.rem(n, 2), :wo_ref.shape[0], :])).astype(BF16)

        res_store.start()

    def hidden_parts(kind):
        per = 2 if kind == 2 else 1
        count = own.shape[0] // per

        def own_load(j, g):
            source = (kv_all, qa_all, qb_all)[kind]
            device, col = (2 * j + g, 0) if kind == 2 else (j, g * HEAD_DIM)
            at = pl.ds(pl.multiple_of(device * seq_len + near.me * rows, rows), rows)
            return pltpu.make_async_copy(source.at[at, pl.ds(col, HEAD_DIM)], own.at[j, :, pl.ds(g * HEAD_DIM, HEAD_DIM)], own_sems.at[j, g])

        def w_load(j, g):
            source = (wk_ref, wv_ref)[g] if kind == 0 else wq_ref
            col = j if kind == 0 else heads * j + g if kind == 1 else heads * (2 * j + g + 1) - 1
            slot = lax.rem(j, 2)
            return pltpu.make_async_copy(source.at[:, pl.ds(pl.multiple_of(col * HEAD_DIM, HEAD_DIM), HEAD_DIM)],
                                         w_v.at[slot, :, pl.ds(g * HEAD_DIM, HEAD_DIM)], w_sems.at[slot, g])

        return count, own_load, w_load

    def hidden_start(kind):
        count, own_load, w_load = hidden_parts(kind)
        for g in range(2):
            w_load(jnp.int32(0), g).start()

            @pl.loop(0, count)
            def _(j):
                own_load(j, g).start()

    def hidden_add(kind):
        count, own_load, w_load = hidden_parts(kind)

        @pl.loop(0, count)
        def _(j):
            for g in range(2):
                w_load(j, g).wait()
                own_load(j, g).wait()

            @pl.when(j + 1 < count)
            def _():
                for g in range(2):
                    w_load(j + 1, g).start()

            prod = dot(own[j], w_v[lax.rem(j, 2)], COLS_COLS)
            if kind == 0:
                @pl.when(j == 0)
                def _():
                    acc[...] = prod

                @pl.when(j > 0)
                def _():
                    acc[...] += prod
            else:
                acc[...] += prod

    near.meet([near.sib, near.xn, near.yn])
    for c in range(CHUNKS):
        gathers[0].start(c)
    a_load(ot_ref).start()
    start_b(jnp.int32(0))
    stage_in(0).start()
    ot_load.start()
    x_load.start()
    a_load(ot_ref).wait()

    @pl.loop(0, n_all)
    def _(step):
        slot = lax.rem(step, 2)
        for g in range(2):
            b_load(dy_ref, 0, slot, g).wait()

        @pl.when(jnp.logical_and(step != n_o - 1, step != n_o + n_kv - 1))
        def _():
            start_b(step + 1)

        @pl.when(step >= 2)
        def _():
            keep(step - 2).wait()
            give(step - 2).wait_send()

        @pl.when(step == n_o)
        def _():
            a_load(ht_ref).wait()

        tile[slot] = dot(a_buf[...], b_buf[slot])
        keep(step).start()
        give(step).start()

        @pl.when(step == n_o - 2)
        def _():
            copy_own(0)
            gathers[0].middle()

        @pl.when(step == n_o - 1)
        def _():
            a_load(ht_ref).start()
            gathers[0].late()
            for c in range(CHUNKS):
                gathers[1].start(c)
            stage_out(0).wait()
            stage_in(1).start()
            result_part()
            gathers[0].end()
            start_b(step + 1)
            hidden_start(0)

        @pl.when(step == n_o + n_kv - 1)
        def _():
            gathers[1].middle()
            copy_own(1)
            hidden_add(0)
            gathers[1].late()
            for c in range(CHUNKS):
                gathers[2].start(c)
            stage_out(1).wait()
            stage_in(2).start()
            gathers[1].end()
            start_b(step + 1)
            hidden_start(1)

        @pl.when(step == n_all - 3)
        def _():
            copy_own(2)
            gathers[2].middle()

        @pl.when(step == n_all - 2)
        def _():
            gathers[2].late()

    hidden_add(1)
    stage_out(2).wait()
    gathers[2].end()
    hidden_start(2)
    for step in (n_all - 2, n_all - 1):
        keep(step).wait()
        give(step).wait_send()
    hidden_add(2)
    hid_store.start()

    @pl.loop(0, n_all)
    def _(step):
        give(step).wait_recv()

    res_store.wait()
    hid_store.wait()


def products(ot_all, ht, d_out, d_kv, d_qa, d_qb, x, w_o, w_k, w_v, w_q, sp_size, heads):
    width, seq_len = ht.shape
    half = width // 2
    cols = 2 * d_kv.shape[1]
    n_all = width // cols + 2 * sp_size * d_kv.shape[1] // cols
    any_spec = pl.BlockSpec(memory_space=pl.ANY)
    dma = pltpu.SemaphoreType.DMA
    gathered = [jax.ShapeDtypeStruct((sp_size * seq_len, d.shape[1]), BF16) for d in (d_kv, d_qa, d_qb)]
    return pl.pallas_call(
        functools.partial(products_kernel, heads),
        in_specs=[any_spec] * 11,
        out_specs=[any_spec] * 6,
        out_shape=[jax.ShapeDtypeStruct((2, n_all, half, cols), F32)] + gathered
        + [jax.ShapeDtypeStruct(x.shape, BF16), jax.ShapeDtypeStruct(x.shape, F32)],
        scratch_shapes=[pltpu.VMEM((half, seq_len), BF16), pltpu.VMEM((2, seq_len, cols), BF16), pltpu.VMEM((2, half, cols), F32),
                        dma, dma((2, 2)), dma((2,)), dma((2, n_all)), pltpu.VMEM(d_kv.shape, BF16), dma((2,)),
                        pltpu.VMEM((ot_all.shape[0], x.shape[0]), BF16), pltpu.VMEM((x.shape[0], ot_all.shape[0]), BF16), pltpu.VMEM(x.shape, BF16),
                        dma((4,)), pltpu.VMEM((sp_size, x.shape[0], 2 * HEAD_DIM), BF16), dma((sp_size, 2)),
                        pltpu.VMEM((2, width, 2 * HEAD_DIM), BF16), dma((2, 2)), pltpu.VMEM(x.shape, F32), SEMS, SEMS, SEMS],
        compiler_params=pltpu.CompilerParams(vmem_limit_bytes=VMEM_LIMIT, collective_id=3, has_side_effects=True),
        cost_estimate=pl.CostEstimate(flops=2 * half * cols * seq_len * n_all, bytes_accessed=8 * half * cols * n_all, transcendentals=0),
        name="products",
    )(ot_all, ht, d_out, d_kv, d_qa, d_qb, x, w_o, w_k, w_v, w_q)


def finish_kernel(heads, n_o, n_kv, ht_ref, d_ref, hid_ref, x_ref, dy_ref, gain_ref, part_ref, tiles,
                  wq_ref, wk_ref, wv_ref, wo_ref, gx_ref, gg_ref, res_ref, tile, sems, ring, ring_sems):
    n_cols = d_ref.shape[2]
    n_j = pl.num_programs(1)
    step = pl.program_id(0) * n_j + pl.program_id(1)
    slot = lax.rem(step, 2)
    half = ring.shape[2]
    every = [(c, t) for t in range(tiles.shape[1]) for c in range(2)]
    groups = [every[g:g + RING] for g in range(0, len(every), RING)]

    def pieces(c, t):
        rows = pl.ds(c * half, half)
        cols = ring.shape[3]
        if t < n_o:
            return [(0, cols, wo_ref.at[rows, pl.ds(t * cols, cols)])]
        if t < n_o + n_kv:
            return [(n * HEAD_DIM, HEAD_DIM, (wk_ref, wv_ref)[n % 2].at[rows, pl.ds(((t - n_o) * 2 + n // 2) * HEAD_DIM, HEAD_DIM)]) for n in range(4)]
        wide = (heads - 1) * HEAD_DIM
        return [(n * wide, wide, wq_ref.at[rows, pl.ds(((t - n_o - n_kv) * 2 + n) * heads * HEAD_DIM, wide)]) for n in range(2)]

    def ins(g):
        return [pltpu.make_async_copy(tiles.at[c, t], ring.at[g % 2, n], ring_sems.at[0, g % 2, n, 0]) for n, (c, t) in enumerate(groups[g])]

    def outs(g):
        return [pltpu.make_async_copy(ring.at[g % 2, n, :, pl.ds(col, count)], dst, ring_sems.at[1, g % 2, n, m])
                for n, (c, t) in enumerate(groups[g]) for m, (col, count, dst) in enumerate(pieces(c, t))]

    for g in range(len(groups) + 2):
        @pl.when(step == g)
        def _():
            if 0 <= g - 1 < len(groups):
                for copy in ins(g - 1):
                    copy.wait()
                for copy in outs(g - 1):
                    copy.start()
            if 0 <= g - 2 < len(groups):
                for copy in outs(g - 2):
                    copy.wait()
            if g < len(groups):
                for copy in ins(g):
                    copy.start()

    def copies(step, slot):
        rows = pl.ds(pl.multiple_of((step // n_j) * MROWS, MROWS), MROWS)
        out = []
        for g in range(2):
            col = ((lax.rem(step, n_j) * 2 + g + 1) * heads - 1) * HEAD_DIM
            out.append(pltpu.make_async_copy(tile.at[slot, :, pl.ds(g * n_cols, n_cols)],
                                             wq_ref.at[rows, pl.ds(pl.multiple_of(col, HEAD_DIM), n_cols)], sems.at[slot, g]))
        return out

    @pl.when(step >= 2)
    def _():
        for copy in copies(step - 2, slot):
            copy.wait()

    pair = 2 * pl.program_id(1)
    tile[slot] = dot(ht_ref[...], lanes(d_ref[pair], d_ref[pair + 1]))
    for copy in copies(step, slot):
        copy.start()

    @pl.when(step == 0)
    def _():
        gg_ref[...] = jnp.zeros_like(gg_ref)

    @pl.when(step < ROW_STEPS)
    def _():
        x_f = x_ref[...].astype(F32)
        inv_rms = lax.rsqrt(jnp.mean(x_f * x_f, axis=-1, keepdims=True) + NORM_EPS)
        normed = x_f * inv_rms
        d_hid = hid_ref[...]
        both = d_hid * normed
        gain = gain_ref[...]
        gg_ref[...] += jnp.sum(both.reshape(both.shape[0] // 8, 8, both.shape[1]), axis=0)
        mean = jnp.mean(both * gain, axis=-1, keepdims=True)
        d_x = inv_rms * (d_hid * gain - normed * mean)
        gx_ref[...] = (dy_ref[...].astype(F32) + d_x).astype(BF16)
        res_ref[...] = part_ref[...]

    @pl.when(step == pl.num_programs(0) * n_j - 1)
    def _():
        for copy in copies(step - 1, 1 - slot) + copies(step, slot):
            copy.wait()


def finish(ht, d_q, tiles, d_hid, x, grad_out, gain_f, result, heads, n_o, n_kv):
    width, seq_len = ht.shape
    groups, _, n_cols = d_q.shape
    n_j = groups // 2
    steps = (width // MROWS) * n_j
    assert -(-2 * tiles.shape[1] // RING) + 2 <= steps
    any_spec = pl.BlockSpec(memory_space=pl.ANY)
    rows = pl.BlockSpec((x.shape[0] // ROW_STEPS, width), lambda m, j: (jnp.minimum(m * n_j + j, ROW_STEPS - 1), 0))
    whole = lambda *shape: pl.BlockSpec(shape, lambda m, j: (0,) * len(shape))
    out = lambda cols: jax.ShapeDtypeStruct((width, cols), F32)
    return pl.pallas_call(
        functools.partial(finish_kernel, heads, n_o, n_kv),
        grid=(width // MROWS, n_j),
        in_specs=[pl.BlockSpec((MROWS, seq_len), lambda m, j: (m, 0)),
                  pl.BlockSpec(d_q.shape, lambda m, j: (0, 0, 0), pipeline_mode=pl.Buffered(1)),
                  rows, rows, rows, whole(1, width), rows, any_spec],
        out_specs=[any_spec] * 4 + [rows, whole(8, width), rows],
        out_shape=[out(groups * heads * HEAD_DIM), out(groups * HEAD_DIM), out(groups * HEAD_DIM),
                   jax.ShapeDtypeStruct((groups * heads * HEAD_DIM, width), F32), jax.ShapeDtypeStruct(x.shape, BF16),
                   jax.ShapeDtypeStruct((8, width), F32), jax.ShapeDtypeStruct(x.shape, BF16)],
        scratch_shapes=[pltpu.VMEM((2, MROWS, 2 * n_cols), F32), pltpu.SemaphoreType.DMA((2, 2)), pltpu.VMEM((2, RING) + tiles.shape[2:], F32),
                        pltpu.SemaphoreType.DMA((2, 2, RING, 4))],
        compiler_params=params(2),
        cost_estimate=pl.CostEstimate(flops=2 * width * seq_len * groups * n_cols, bytes_accessed=2 * width * seq_len, transcendentals=0),
        name="finish",
    )(ht, d_q, d_hid, x, grad_out, gain_f, result, tiles)


def solution(mesh):
    sp_size = mesh.shape['sp']
    seq_spec = P(('dp', 'sp'), None)
    pos_spec = P(('dp', 'sp'))
    replicated = P(None, None)
    part_rows = P('dp', None)

    def local_step(x, grad_out, positions, gain, w_q, w_k, w_v, w_o):
        n_heads = w_q.shape[1] // HEAD_DIM
        heads = n_heads // sp_size
        gain_f = gain.astype(F32).reshape(1, -1)
        hidden, cos_t, sin_t = gather_h(x, gain_f, positions, sp_size)
        q, k, v, ht, ot, lse, d_out = forward(hidden, w_q, w_k, w_v, cos_t, sin_t, grad_out, heads)
        *grads, ot_all = backward(q, k, v, d_out, w_o, ot, lse, cos_t, sin_t, heads, sp_size)
        tiles, _, _, dqb_all, part, d_hid = products(ot_all, ht, d_out, *grads, x, w_o, w_k, w_v, w_q, sp_size, heads)
        n_kv = sp_size // 2
        grad_wq, grad_wk, grad_wv, grad_wo, grad_x, gg, result = finish(
            ht, dqb_all.reshape(sp_size, -1, HEAD_DIM), tiles, d_hid, x, grad_out, gain_f, part, heads, tiles.shape[1] - 2 * n_kv, n_kv)
        grad_gain = jnp.sum(lax.all_gather(gg, 'sp', axis=0, tiled=True), axis=0)
        return result, grad_x, grad_wq, grad_wk, grad_wv, grad_wo, grad_gain

    return jax.shard_map(local_step, mesh=mesh,
                         in_specs=(seq_spec, seq_spec, pos_spec, P(None), replicated, replicated, replicated, replicated),
                         out_specs=(seq_spec, seq_spec, part_rows, part_rows, part_rows, part_rows, P('dp')),
                         check_vma=False)
```

```python
import functools

import jax
import jax.numpy as jnp
from jax import lax
from jax.experimental import pallas as pl
from jax.experimental.pallas import tpu as pltpu
from jax.sharding import PartitionSpec as P

HEAD_DIM = 128
HALF = HEAD_DIM // 2
ROPE_THETA = 1000000.0
NORM_EPS = 1e-05
NEG_LARGE = -1e30
LOG2E = 1.4426950408889634
BLK = 512
CHUNKS = 4
FWD_MIDDLE, BWD_MIDDLE, BWD_LATE = 5, 4, 5
MROWS = 768
RING = 2
ROW_STEPS = 8
F32 = jnp.float32
BF16 = jnp.bfloat16
ROWS_ROWS = (((0,), (0,)), ((), ()))
COLS_COLS = (((1,), (1,)), ((), ()))
ROWS_COLS = (((0,), (1,)), ((), ()))
VMEM_LIMIT = 63 * 1024 * 1024


def dot(a, b, dims=(((1,), (0,)), ((), ()))):
    return lax.dot_general(a, b, dims, preferred_element_type=F32)


def params(axes=1):
    return pltpu.CompilerParams(dimension_semantics=("arbitrary",) * axes, vmem_limit_bytes=VMEM_LIMIT)


class Neighbours:
    def __init__(self):
        self.me = lax.axis_index('sp')
        core, col, row = lax.rem(self.me, 2), lax.rem(self.me // 2, 2), self.me // 4
        self.sib = self.me + 1 - 2 * core
        self.xn = self.me + 2 - 4 * col
        self.yn = self.me + 4 - 8 * row
        self.diag = self.xn + self.yn - self.me

    def meet(self, peers):
        barrier = pltpu.get_barrier_semaphore()
        for peer in peers:
            pl.semaphore_signal(barrier, inc=1, device_id={'sp': peer}, device_id_type=pl.DeviceIdType.MESH)
        pl.semaphore_wait(barrier, len(peers))

    def across(self, r):
        core, col, row = lax.rem(self.me, 2), lax.rem(self.me // 2, 2), self.me // 4
        return (self.me + lax.rem(r, 2) * (1 - 2 * core) + lax.rem(r // 2, 2) * (2 - 4 * col) + (r // 4) * (4 - 8 * row))

    def others(self):
        flip = lambda dev: dev + 1 - 2 * lax.rem(dev, 2)
        return [self.sib, self.xn, flip(self.xn), self.yn, flip(self.yn), self.diag, flip(self.diag)]


def send(src, dst, sems, index, peer):
    return pltpu.make_async_remote_copy(src_ref=src, dst_ref=dst, send_sem=sems.at[0, index], recv_sem=sems.at[1, index],
                                        device_id={'sp': peer}, device_id_type=pl.DeviceIdType.MESH)


class Gather:
    COPIES = 22

    def __init__(self, near, own, dst, rows, sems):
        self.near, self.own, self.dst, self.rows, self.sems = near, own, dst, rows, sems

    def block(self, dev, chunk, count=1):
        size = self.rows // CHUNKS
        return self.dst.at[pl.ds(pl.multiple_of(dev * self.rows + chunk * size, size), count * size), :]

    def first(self, chunk, kind):
        peer = (self.near.xn, self.near.yn, self.near.sib)[kind]
        return send(self.own(chunk), self.block(self.near.me, chunk), self.sems, kind * CHUNKS + chunk, peer)

    def onward(self, chunk):
        over_y = chunk < CHUNKS // 2
        rows = self.block(self.near.xn if over_y else self.near.yn, chunk)
        return send(rows, rows, self.sems, 12 + chunk, self.near.yn if over_y else self.near.xn)

    def share(self, kind):
        rows = self.block((self.near.xn, self.near.yn)[kind], 0, CHUNKS)
        return send(rows, rows, self.sems, 16 + kind, self.near.sib)

    def share_diag(self, chunk):
        rows = self.block(self.near.diag, chunk)
        return send(rows, rows, self.sems, 18 + chunk, self.near.sib)

    def begin(self):
        self.near.meet([self.near.sib, self.near.xn, self.near.yn])
        for chunk in range(CHUNKS):
            self.start(chunk)

    def start(self, chunk):
        for kind in range(3):
            self.first(chunk, kind).start()

    def middle(self):
        for chunk in (0, 1):
            self.first(chunk, 0).wait_recv()
            self.onward(chunk).start()
        self.first(2, 1).wait_recv()
        self.onward(2).start()

    def late(self):
        self.first(3, 1).wait_recv()
        self.onward(3).start()
        for chunk in (2, 3):
            self.first(chunk, 0).wait_recv()
        self.share(0).start()
        for chunk in (0, 1):
            self.first(chunk, 1).wait_recv()
        self.share(1).start()

    def end_near(self):
        for chunk in range(CHUNKS):
            self.first(chunk, 2).wait_recv()
        for kind in range(2):
            self.share(kind).wait_recv()

    def end_far(self):
        for chunk in (0, 2, 1, 3):
            self.onward(chunk).wait_recv()
            self.share_diag(chunk).start()
        for chunk in range(CHUNKS):
            for kind in range(3):
                self.first(chunk, kind).wait_send()
            self.onward(chunk).wait_send()
        for kind in range(2):
            self.share(kind).wait_send()
        for chunk in range(CHUNKS):
            self.share_diag(chunk).wait()

    def end(self):
        self.end_near()
        self.end_far()


SEMS = pltpu.SemaphoreType.DMA((2, Gather.COPIES))


def comm_params(collective_id):
    return pltpu.CompilerParams(dimension_semantics=("arbitrary",), vmem_limit_bytes=VMEM_LIMIT, collective_id=collective_id,
                                has_side_effects=True)


def gather_h_kernel(x_ref, gain_ref, pos_ref, freq_ref, h_all, cos_ref, sin_ref, x_v, h_v, pos_all, in_sems, out_sem, pos_sems, sems):
    near = Neighbours()
    rows = x_ref.shape[0]
    size = rows // CHUNKS
    part = lambda ref, chunk: ref.at[pl.ds(chunk * size, size), :]
    gather = Gather(near, lambda chunk: part(h_v, chunk), h_all, rows, sems)
    loads = [pltpu.make_async_copy(part(x_ref, chunk), part(x_v, chunk), in_sems.at[chunk]) for chunk in range(CHUNKS)]
    for load in loads:
        load.start()
    others = near.others()
    near.meet(others)
    pos_all[near.me] = pos_ref[...]
    positions = [send(pos_ref, pos_all.at[near.me], pos_sems, r, peer) for r, peer in enumerate(others)]
    for copy in positions:
        copy.start()
    for chunk in range(CHUNKS):
        loads[chunk].wait()

        @pl.loop(0, size // 32)
        def _(r):
            at = pl.ds(pl.multiple_of(chunk * size + r * 32, 32), 32)
            x_f = x_v[at, :].astype(F32)
            normed = x_f * lax.rsqrt(jnp.mean(x_f * x_f, axis=-1, keepdims=True) + NORM_EPS)
            h_v[at, :] = (normed * gain_ref[...]).astype(BF16)

        gather.start(chunk)
    own = pltpu.make_async_copy(h_v, gather.block(near.me, 0, CHUNKS), out_sem)
    own.start()
    for copy in positions:
        copy.wait()
    sign = jnp.where(lax.broadcasted_iota(jnp.int32, (1, HEAD_DIM), 1) < HALF, -1.0, 1.0)

    @pl.loop(0, pos_all.shape[0])
    def _(b):
        at = pl.ds(pl.multiple_of(b * rows, rows), rows)
        pos = jnp.broadcast_to(pos_all[b, 0:1, :].astype(F32), (HEAD_DIM, rows)).T
        angles = pos * freq_ref[...]
        cos_ref[at, :] = jnp.cos(angles)
        sin_ref[at, :] = jnp.sin(angles) * sign

    gather.middle()
    gather.late()
    own.wait()
    gather.end()


def gather_h(x, gain_f, positions, sp_size):
    rows, width = x.shape
    any_spec = pl.BlockSpec(memory_space=pl.ANY)
    vmem = pl.BlockSpec(memory_space=pltpu.VMEM)
    inv_freq = ROPE_THETA ** (-jnp.arange(0, HEAD_DIM, 2).astype(F32) / HEAD_DIM)
    freq = jnp.concatenate([inv_freq, inv_freq])[None, :]
    table = jax.ShapeDtypeStruct((rows * sp_size, HEAD_DIM), F32)
    return pl.pallas_call(
        gather_h_kernel,
        in_specs=[any_spec, vmem, vmem, vmem],
        out_specs=[any_spec, vmem, vmem],
        out_shape=[jax.ShapeDtypeStruct((rows * sp_size, width), BF16), table, table],
        scratch_shapes=[pltpu.VMEM((rows, width), BF16), pltpu.VMEM((rows, width), BF16), pltpu.VMEM((sp_size, 8, rows), jnp.int32),
                        pltpu.SemaphoreType.DMA((CHUNKS,)), pltpu.SemaphoreType.DMA, pltpu.SemaphoreType.DMA((2, 7)), SEMS],
        compiler_params=pltpu.CompilerParams(vmem_limit_bytes=VMEM_LIMIT, collective_id=0, has_side_effects=True),
        name="gather_h",
    )(x, gain_f, jnp.broadcast_to(positions[None, :], (8, rows)), freq)


def masked(scores):
    key = lax.broadcasted_iota(jnp.int32, scores.shape, 0)
    query = lax.broadcasted_iota(jnp.int32, scores.shape, 1)
    return jnp.where(key <= query, scores, NEG_LARGE)


def forward_kernel(heads, h_ref, wq_ref, wk_ref, wv_ref, cos_ref, sin_ref, dy_ref, q_ref, k_ref, v_ref, ht_ref, o_ref, lse_ref, dy_all,
                   w_v, w_sems, k_s, vt, acc, stage, stage_sems, sems):
    i = pl.program_id(0)
    near = Neighbours()
    rows = dy_ref.shape[0]
    size = rows // CHUNKS
    gather = Gather(near, lambda chunk: dy_ref.at[pl.ds(chunk * size, size), :], dy_all, rows, sems)
    stage_in = pltpu.make_async_copy(dy_ref, stage, stage_sems.at[0])
    stage_out = pltpu.make_async_copy(stage, gather.block(near.me, 0, CHUNKS), stage_sems.at[1])
    to_log2 = HEAD_DIM ** -0.5 * LOG2E
    q_cols = heads * HEAD_DIM

    @pl.when(i == 0)
    def _():
        loads, col = [], 0
        for n, (ref, count) in enumerate(((wq_ref, q_cols), (wk_ref, HEAD_DIM), (wv_ref, HEAD_DIM))):
            at = pl.ds(pl.multiple_of(near.me * count, HEAD_DIM), count)
            loads.append(pltpu.make_async_copy(ref.at[:, at], w_v.at[:, pl.ds(col, count)], w_sems.at[n]))
            col += count
        for load in loads:
            load.start()
        gather.begin()
        stage_in.start()
        for load in loads:
            load.wait()

    ht_ref[...] = h_ref[...].T
    prod = dot(h_ref[...], w_v[...])
    cos_t, sin_t = cos_ref[...], sin_ref[...]
    for a in range(heads + 1):
        val = prod[:, a * HEAD_DIM:(a + 1) * HEAD_DIM]
        rot = (val * cos_t + pltpu.roll(val, HALF, 1) * sin_t).astype(BF16)
        if a < heads:
            q_ref[:, a * HEAD_DIM:(a + 1) * HEAD_DIM] = rot
        else:
            k_ref[...] = rot
            k_s[i] = rot
    v_i = prod[:, q_cols + HEAD_DIM:].astype(BF16)
    v_ref[...] = v_i
    vt[i] = v_i.T
    acc[...] = jnp.zeros_like(acc)

    def chunk(c, carry, diagonal):
        k_c, vt_c = k_s[c], vt[c]
        scores = [dot(k_c, q_ref[:, a * HEAD_DIM:(a + 1) * HEAD_DIM], COLS_COLS) * to_log2 for a in range(heads)]
        out = []
        for a in range(heads):
            s = masked(scores[a]) if diagonal else scores[a]
            m_old, l_old = carry[a]
            m_new = jnp.maximum(m_old, jnp.max(s, axis=0, keepdims=True))
            alpha = jnp.exp2(m_old - m_new)
            p = jnp.exp2(s - m_new)
            l_new = l_old * alpha + jnp.sum(p, axis=0, keepdims=True)
            acc[a] = acc[a] * alpha + dot(vt_c, p.astype(BF16))
            out.append((m_new, l_new))
        return tuple(out)

    start = tuple((jnp.full((1, BLK), NEG_LARGE, F32), jnp.zeros((1, BLK), F32)) for _ in range(heads))
    carry = lax.fori_loop(0, i, lambda c, carry: chunk(c, carry, False), start)
    carry = chunk(i, carry, True)
    for a in range(heads):
        m_a, l_a = carry[a]
        o_ref[a * HEAD_DIM:(a + 1) * HEAD_DIM, :] = (acc[a] / l_a).astype(BF16)
        lse_ref[a:a + 1, :] = m_a + jnp.log2(l_a)

    @pl.when(i == FWD_MIDDLE)
    def _():
        gather.middle()
        stage_in.wait()
        stage_out.start()

    @pl.when(i == pl.num_programs(0) - 1)
    def _():
        gather.late()
        stage_out.wait()
        gather.end()


def forward(hidden, w_q, w_k, w_v, cos_t, sin_t, grad_out, heads):
    seq_len, width = hidden.shape
    n_blocks = seq_len // BLK
    q_cols = heads * HEAD_DIM
    pairs = heads * seq_len * (seq_len + BLK) // 2
    any_spec = pl.BlockSpec(memory_space=pl.ANY)
    rows = lambda cols: pl.BlockSpec((BLK, cols), lambda i: (i, 0))
    cols = lambda rows: pl.BlockSpec((rows, BLK), lambda i: (0, i))
    out = lambda *shape, dtype=BF16: jax.ShapeDtypeStruct(shape, dtype)
    return pl.pallas_call(
        functools.partial(forward_kernel, heads),
        grid=(n_blocks,),
        in_specs=[rows(width), any_spec, any_spec, any_spec, rows(HEAD_DIM), rows(HEAD_DIM), any_spec],
        out_specs=[rows(q_cols), rows(HEAD_DIM), rows(HEAD_DIM), cols(width), cols(q_cols), cols(8), any_spec],
        out_shape=[out(seq_len, q_cols), out(seq_len, HEAD_DIM), out(seq_len, HEAD_DIM), out(width, seq_len), out(q_cols, seq_len),
                   out(8, seq_len, dtype=F32), out(seq_len, width)],
        scratch_shapes=[pltpu.VMEM((width, q_cols + 2 * HEAD_DIM), BF16), pltpu.SemaphoreType.DMA((3,)), pltpu.VMEM((n_blocks, BLK, HEAD_DIM), BF16),
                        pltpu.VMEM((n_blocks, HEAD_DIM, BLK), BF16), pltpu.VMEM((heads, HEAD_DIM, BLK), F32), pltpu.VMEM(grad_out.shape, BF16),
                        pltpu.SemaphoreType.DMA((2,)), SEMS],
        compiler_params=comm_params(1),
        cost_estimate=pl.CostEstimate(flops=8 * pairs * HEAD_DIM + 4 * seq_len * width * q_cols, bytes_accessed=8 * seq_len * width, transcendentals=pairs),
        name="forward",
    )(hidden, w_q, w_k, w_v, cos_t, sin_t, grad_out)


def unrotate(val, cos_t, sin_t):
    return (val * cos_t - pltpu.roll(val, HALF, 1) * sin_t).astype(BF16)


def backward_kernel(heads, q_ref, k_ref, v_ref, dy_ref, wo_ref, ot_ref, lse_ref, cos_ref, sin_ref, o_ref, dkv_ref, dq_a_ref, dq_b_ref, o_all,
                    wo_v, w_sem, do_s, kt, dk_acc, dv_acc, dqt, stage, stage_sems, sems):
    i = pl.program_id(0)
    n_blocks = k_ref.shape[0] // BLK
    qk_scale = HEAD_DIM ** -0.5
    to_log2 = qk_scale * LOG2E
    near = Neighbours()
    own_rows = o_ref.shape[0]
    size = own_rows // CHUNKS
    gather = Gather(near, lambda chunk: o_ref.at[pl.ds(chunk * size, size), :], o_all, own_rows, sems)
    stage_in = pltpu.make_async_copy(o_ref, stage, stage_sems.at[0])
    stage_out = pltpu.make_async_copy(stage, gather.block(near.me, 0, CHUNKS), stage_sems.at[1])

    @pl.when(i == 0)
    def _():
        q_cols = heads * HEAD_DIM
        load = pltpu.make_async_copy(wo_ref.at[pl.ds(pl.multiple_of(near.me * q_cols, q_cols), q_cols), :], wo_v, w_sem)
        load.start()
        gather.begin()
        stage_in.start()

        @pl.loop(0, n_blocks)
        def _(c):
            kt[c] = k_ref[pl.ds(pl.multiple_of(c * BLK, BLK), BLK), :].T

        load.wait()

    cols = [slice(a * HEAD_DIM, (a + 1) * HEAD_DIM) for a in range(heads)]
    d_o = dot(dy_ref[...], wo_v[...], COLS_COLS).astype(BF16)
    do_s[...] = d_o
    dqt[...] = jnp.zeros_like(dqt)
    delta = [jnp.sum(ot_ref[cols[a], :].astype(F32) * d_o[:, cols[a]].T.astype(F32), axis=0, keepdims=True) for a in range(heads)]

    def chunk(c, diagonal):
        rows = pl.ds(pl.multiple_of(c * BLK, BLK), BLK)
        k_c, v_c, kt_c = k_ref[rows, :], v_ref[rows, :], kt[c]
        dk_c = dv_c = None
        for a in range(heads):
            q_a, do_a = q_ref[:, cols[a]], do_s[:, cols[a]]
            s = dot(k_c, q_a, COLS_COLS) * to_log2
            if diagonal:
                s = masked(s)
            p = jnp.exp2(s - lse_ref[a:a + 1, :])
            d_p = dot(v_c, do_a, COLS_COLS)
            d_s = (p * (d_p - delta[a])).astype(BF16)
            dv_a = dot(p.astype(BF16), do_a)
            dk_a = dot(d_s, q_a)
            dv_c = dv_a if dv_c is None else dv_c + dv_a
            dk_c = dk_a if dk_c is None else dk_c + dk_a
            dqt[a] += dot(kt_c, d_s)
        if diagonal:
            dk_acc[c] = dk_c
            dv_acc[c] = dv_c
        else:
            dk_acc[c] += dk_c
            dv_acc[c] += dv_c

    @pl.loop(0, i)
    def _(c):
        chunk(c, False)

    chunk(i, True)
    rows = pl.ds(pl.multiple_of(i * BLK, BLK), BLK)
    for a in range(heads):
        d_q = unrotate(dqt[a].T * qk_scale, cos_ref[rows, :], sin_ref[rows, :])
        if a < heads - 1:
            dq_a_ref[:, cols[a]] = d_q
        else:
            dq_b_ref[...] = d_q

    @pl.when(i == BWD_MIDDLE)
    def _():
        gather.middle()
        stage_in.wait()
        stage_out.start()

    @pl.when(i == BWD_LATE)
    def _():
        gather.late()

    @pl.when(i == n_blocks - 1)
    def _():
        @pl.loop(0, n_blocks)
        def _(c):
            rows_c = pl.ds(pl.multiple_of(c * BLK, BLK), BLK)
            dkv_ref[rows_c, :HEAD_DIM] = unrotate(dk_acc[c] * qk_scale, cos_ref[rows_c, :], sin_ref[rows_c, :])
            dkv_ref[rows_c, HEAD_DIM:] = dv_acc[c].astype(BF16)

        stage_out.wait()
        gather.end()


def backward(q, k, v, d_out, w_o, ot, lse, cos_t, sin_t, heads, sp_size):
    seq_len, width = d_out.shape
    n_blocks = seq_len // BLK
    whole = lambda i: (0, 0)
    pairs = heads * seq_len * (seq_len + BLK) // 2
    q_cols = heads * HEAD_DIM
    any_spec = pl.BlockSpec(memory_space=pl.ANY)
    rows = lambda cols: pl.BlockSpec((BLK, cols), lambda i: (i, 0))
    cols = lambda rows: pl.BlockSpec((rows, BLK), lambda i: (0, i))
    kv_spec = pl.BlockSpec(k.shape, whole)
    last = (heads - 1) * HEAD_DIM
    out = lambda *shape: jax.ShapeDtypeStruct(shape, BF16)
    return pl.pallas_call(
        functools.partial(backward_kernel, heads),
        grid=(n_blocks,),
        in_specs=[rows(q_cols), kv_spec, kv_spec, rows(width), any_spec, cols(q_cols), cols(8), kv_spec, kv_spec, any_spec],
        out_specs=[pl.BlockSpec((seq_len, 2 * HEAD_DIM), whole), rows(last), rows(HEAD_DIM), any_spec],
        out_shape=[out(seq_len, 2 * HEAD_DIM), out(seq_len, last), out(seq_len, HEAD_DIM), out(q_cols * sp_size, seq_len)],
        scratch_shapes=[pltpu.VMEM((q_cols, width), BF16), pltpu.SemaphoreType.DMA, pltpu.VMEM((BLK, q_cols), BF16),
                        pltpu.VMEM((n_blocks, HEAD_DIM, BLK), BF16), pltpu.VMEM((n_blocks, BLK, HEAD_DIM), F32),
                        pltpu.VMEM((n_blocks, BLK, HEAD_DIM), F32), pltpu.VMEM((heads, HEAD_DIM, BLK), F32), pltpu.VMEM(ot.shape, BF16),
                        pltpu.SemaphoreType.DMA((2,)), SEMS],
        compiler_params=comm_params(2),
        cost_estimate=pl.CostEstimate(flops=20 * pairs * HEAD_DIM + 2 * seq_len * width * q_cols, bytes_accessed=8 * seq_len * q_cols, transcendentals=pairs),
        name="backward",
    )(q, k, v, d_out, w_o, ot, lse, cos_t, sin_t, ot)


def lanes(*parts):
    return jnp.concatenate(parts, axis=1)


def products_kernel(heads, ot_ref, ht_ref, dy_ref, d_kv_ref, d_qa_ref, d_qb_ref, x_ref, wo_ref, wk_ref, wv_ref, wq_ref,
                    tiles, kv_all, qa_all, qb_all, res_ref, hid_ref,
                    a_buf, b_buf, tile, a_sem, b_sems, t_sems, x_sems, stage, stage_sems, ot_v, o_v, x_v, io_sems, own, own_sems, w_v, w_sems, acc,
                    kv_sems, qa_sems, qb_sems):
    near = Neighbours()
    core = lax.rem(near.me, 2)
    half = a_buf.shape[0]
    seq_len = d_kv_ref.shape[0]
    rows, width = x_ref.shape
    chunk = seq_len // CHUNKS
    n_cols = d_kv_ref.shape[1]
    n_o, n_all = width // (2 * n_cols), tiles.shape[1]
    n_qa = (n_all - n_o) * 2 // 3
    n_oa = n_o + n_qa

    def gather_of(src, dst, sems):
        return Gather(near, lambda c: src.at[pl.ds(c * chunk, chunk), :], dst, seq_len, sems)

    local = (d_qa_ref, d_qb_ref, d_kv_ref)
    gathers = [gather_of(d_qa_ref, qa_all, qa_sems), gather_of(d_qb_ref, qb_all, qb_sems), gather_of(d_kv_ref, kv_all, kv_sems)]

    def stage_in(n):
        return pltpu.make_async_copy(local[n], stage.at[:, pl.ds(0, local[n].shape[1])], stage_sems.at[0])

    def stage_out(n):
        return pltpu.make_async_copy(stage.at[:, pl.ds(0, local[n].shape[1])], gathers[n].block(near.me, 0, CHUNKS), stage_sems.at[1])

    def copy_own(n):
        stage_in(n).wait()
        stage_out(n).start()

    own_rows = pl.ds(pl.multiple_of(core * half, half), half)
    tokens = pl.ds(pl.multiple_of(near.me * rows, rows), rows)
    ot_load = pltpu.make_async_copy(ot_ref.at[:, tokens], ot_v, io_sems.at[0])
    x_load = pltpu.make_async_copy(x_ref, x_v, io_sems.at[1])
    res_store = pltpu.make_async_copy(x_v, res_ref, io_sems.at[2])
    hid_store = pltpu.make_async_copy(acc, hid_ref, io_sems.at[3])

    def a_load(ref):
        return pltpu.make_async_copy(ref.at[own_rows, :], a_buf, a_sem)

    def b_loads(source, p, slot, g):
        if source is dy_ref:
            srcs = [dy_ref.at[:, pl.ds(pl.multiple_of((2 * p + g) * n_cols, n_cols), n_cols)]]
        else:
            per = n_cols // source.shape[1]
            srcs = [source.at[pl.ds(pl.multiple_of(((2 * p + g) * per + n) * seq_len, seq_len), seq_len), :] for n in range(per)]
        return [pltpu.make_async_copy(src, b_buf.at[slot, :, pl.ds(g * n_cols + n * src.shape[1], src.shape[1])], b_sems.at[slot, g])
                for n, src in enumerate(srcs)]

    def start_b(step):
        slot = lax.rem(step, 2)
        for source, low, high in ((dy_ref, 0, n_o), (qa_all, n_o, n_oa), (qb_all, n_oa, n_all)):
            @pl.when(jnp.logical_and(step >= low, step < high))
            def _():
                for g in range(2):
                    for load in b_loads(source, step - low, slot, g):
                        load.start()

    def keep(step):
        return pltpu.make_async_copy(tile.at[lax.rem(step, 2)], tiles.at[core, step], t_sems.at[lax.rem(step, 2)])

    def give(step):
        return send(tile.at[lax.rem(step, 2)], tiles.at[core, step], x_sems, step, near.sib)

    def result_part():
        cols = b_buf.shape[2]

        def w_load(n):
            slot = lax.rem(n, 2)
            return pltpu.make_async_copy(wo_ref.at[:, pl.ds(pl.multiple_of(n * cols, cols), cols)], b_buf.at[slot, pl.ds(0, wo_ref.shape[0]), :],
                                         b_sems.at[slot, 0])

        w_load(jnp.int32(0)).start()
        ot_load.wait()

        @pl.loop(0, ot_v.shape[0] // BLK)
        def _(r):
            at = pl.ds(pl.multiple_of(r * BLK, BLK), BLK)
            o_v[:, at] = ot_v[at, :].T

        x_load.wait()

        @pl.loop(0, n_o)
        def _(n):
            w_load(n).wait()

            @pl.when(n + 1 < n_o)
            def _():
                w_load(n + 1).start()

            at = pl.ds(pl.multiple_of(n * cols, cols), cols)
            x_v[:, at] = (x_v[:, at].astype(F32) + dot(o_v[...], b_buf[lax.rem(n, 2), :wo_ref.shape[0], :])).astype(BF16)

        res_store.start()

    def hidden_parts(kind):
        count = own.shape[0] // (2 if kind == 1 else 1)

        def own_load(r, g):
            source = (qa_all, qb_all, kv_all)[kind]
            device, col = (2 * r + g, 0) if kind == 1 else (near.across(r), g * HEAD_DIM)
            at = pl.ds(pl.multiple_of(device * seq_len + near.me * rows, rows), rows)
            return pltpu.make_async_copy(source.at[at, pl.ds(col, HEAD_DIM)], own.at[r, :, pl.ds(g * HEAD_DIM, HEAD_DIM)], own_sems.at[r, g])

        def w_load(r, g):
            source = (wk_ref, wv_ref)[g] if kind == 2 else wq_ref
            col = near.across(r) if kind == 2 else heads * near.across(r) + g if kind == 0 else heads * (2 * r + g + 1) - 1
            slot = lax.rem(r, 2)
            return pltpu.make_async_copy(source.at[:, pl.ds(pl.multiple_of(col * HEAD_DIM, HEAD_DIM), HEAD_DIM)],
                                         w_v.at[slot, :, pl.ds(g * HEAD_DIM, HEAD_DIM)], w_sems.at[slot, g])

        return count, own_load, w_load

    def hidden_start(kind, low=0, high=None):
        count, own_load, w_load = hidden_parts(kind)
        for g in range(2):
            if low == 0:
                w_load(jnp.int32(0), g).start()

            @pl.loop(low, high or count)
            def _(r):
                own_load(r, g).start()

    def hidden_add(kind, low=0, high=None):
        count, own_load, w_load = hidden_parts(kind)

        @pl.loop(low, high or count)
        def _(r):
            for g in range(2):
                w_load(r, g).wait()
                own_load(r, g).wait()

            @pl.when(r + 1 < count)
            def _():
                for g in range(2):
                    w_load(r + 1, g).start()

            prod = dot(own[r], w_v[lax.rem(r, 2)], COLS_COLS)
            if kind == 0:
                @pl.when(r == 0)
                def _():
                    acc[...] = prod

                @pl.when(r > 0)
                def _():
                    acc[...] += prod
            else:
                acc[...] += prod

    near.meet([near.sib, near.xn, near.yn])
    for c in range(CHUNKS):
        gathers[0].start(c)
    a_load(ot_ref).start()
    start_b(jnp.int32(0))
    stage_in(0).start()
    ot_load.start()
    x_load.start()
    a_load(ot_ref).wait()

    @pl.loop(0, n_all)
    def _(step):
        slot = lax.rem(step, 2)
        for g in range(2):
            b_loads(dy_ref, 0, slot, g)[0].wait()

        @pl.when(jnp.logical_and(step != n_o - 1, step != n_oa - 1))
        def _():
            start_b(step + 1)

        @pl.when(step >= 2)
        def _():
            keep(step - 2).wait()
            give(step - 2).wait_send()

        @pl.when(step == n_o)
        def _():
            a_load(ht_ref).wait()

        tile[slot] = dot(a_buf[...], b_buf[slot])
        keep(step).start()
        give(step).start()

        @pl.when(step == n_o - 2)
        def _():
            copy_own(0)
            gathers[0].middle()

        @pl.when(step == n_o - 1)
        def _():
            a_load(ht_ref).start()
            gathers[0].late()
            for c in range(CHUNKS):
                gathers[1].start(c)
            stage_out(0).wait()
            stage_in(1).start()
            result_part()
            gathers[0].end()
            start_b(step + 1)
            hidden_start(0)

        @pl.when(step == n_oa - 3)
        def _():
            copy_own(1)
            gathers[1].middle()

        @pl.when(step == n_oa - 2)
        def _():
            gathers[1].late()
            for c in range(CHUNKS):
                gathers[2].start(c)
            stage_out(1).wait()
            stage_in(2).start()

        @pl.when(step == n_oa - 1)
        def _():
            gathers[1].end()
            start_b(step + 1)
            hidden_add(0)
            hidden_start(1)

    hidden_add(1)
    copy_own(2)
    gathers[2].middle()
    gathers[2].late()
    stage_out(2).wait()
    gathers[2].end_near()
    near_count = own.shape[0] * 3 // 4
    hidden_start(2, 0, near_count)
    for step in (n_all - 2, n_all - 1):
        keep(step).wait()
        give(step).wait_send()
    hidden_add(2, 0, near_count)
    gathers[2].end_far()
    hidden_start(2, near_count)
    hidden_add(2, near_count)
    hid_store.start()

    @pl.loop(0, n_all)
    def _(step):
        give(step).wait_recv()

    res_store.wait()
    hid_store.wait()


def products(ot_all, ht, d_out, d_kv, d_qa, d_qb, x, w_o, w_k, w_v, w_q, sp_size, heads):
    width, seq_len = ht.shape
    half = width // 2
    cols = 2 * d_kv.shape[1]
    n_all = width // cols + sp_size * (d_qa.shape[1] + d_qb.shape[1]) // cols
    any_spec = pl.BlockSpec(memory_space=pl.ANY)
    dma = pltpu.SemaphoreType.DMA
    gathered = [jax.ShapeDtypeStruct((sp_size * seq_len, d.shape[1]), BF16) for d in (d_kv, d_qa, d_qb)]
    return pl.pallas_call(
        functools.partial(products_kernel, heads),
        in_specs=[any_spec] * 11,
        out_specs=[any_spec] * 6,
        out_shape=[jax.ShapeDtypeStruct((2, n_all, half, cols), F32)] + gathered
        + [jax.ShapeDtypeStruct(x.shape, BF16), jax.ShapeDtypeStruct(x.shape, F32)],
        scratch_shapes=[pltpu.VMEM((half, seq_len), BF16), pltpu.VMEM((2, seq_len, cols), BF16), pltpu.VMEM((2, half, cols), F32),
                        dma, dma((2, 2)), dma((2,)), dma((2, n_all)), pltpu.VMEM(d_kv.shape, BF16), dma((2,)),
                        pltpu.VMEM((ot_all.shape[0], x.shape[0]), BF16), pltpu.VMEM((x.shape[0], ot_all.shape[0]), BF16), pltpu.VMEM(x.shape, BF16),
                        dma((4,)), pltpu.VMEM((sp_size, x.shape[0], 2 * HEAD_DIM), BF16), dma((sp_size, 2)),
                        pltpu.VMEM((2, width, 2 * HEAD_DIM), BF16), dma((2, 2)), pltpu.VMEM(x.shape, F32), SEMS, SEMS, SEMS],
        compiler_params=pltpu.CompilerParams(vmem_limit_bytes=VMEM_LIMIT, collective_id=3, has_side_effects=True),
        cost_estimate=pl.CostEstimate(flops=2 * half * cols * seq_len * n_all, bytes_accessed=8 * half * cols * n_all, transcendentals=0),
        name="products",
    )(ot_all, ht, d_out, d_kv, d_qa, d_qb, x, w_o, w_k, w_v, w_q)


def finish_kernel(heads, n_o, n_qa, ht_ref, d_ref, hid_ref, x_ref, dy_ref, gain_ref, part_ref, tiles,
                  wk_ref, wv_ref, wq_ref, wo_ref, gx_ref, gg_ref, res_ref, ring, ring_sems):
    step = pl.program_id(0) * pl.num_programs(1) + pl.program_id(1)
    half = ring.shape[2]
    every = [(c, t) for t in range(tiles.shape[1]) for c in range(2)]
    groups = [every[g:g + RING] for g in range(0, len(every), RING)]

    def pieces(c, t):
        rows = pl.ds(c * half, half)
        cols = ring.shape[3]
        if t < n_o:
            return [(0, cols, wo_ref.at[rows, pl.ds(t * cols, cols)])]
        wide, first, t = ((heads - 1) * HEAD_DIM, 0, t - n_o) if t < n_o + n_qa else (HEAD_DIM, heads - 1, t - n_o - n_qa)
        per = cols // wide
        return [(n * wide, wide, wq_ref.at[rows, pl.ds(((t * per + n) * heads + first) * HEAD_DIM, wide)]) for n in range(per)]

    def ins(g):
        return [pltpu.make_async_copy(tiles.at[c, t], ring.at[g % 2, n], ring_sems.at[0, g % 2, n, 0]) for n, (c, t) in enumerate(groups[g])]

    def outs(g):
        return [pltpu.make_async_copy(ring.at[g % 2, n, :, pl.ds(col, count)], dst, ring_sems.at[1, g % 2, n, m])
                for n, (c, t) in enumerate(groups[g]) for m, (col, count, dst) in enumerate(pieces(c, t))]

    for g in range(len(groups) + 2):
        @pl.when(step == g)
        def _():
            if 0 <= g - 1 < len(groups):
                for copy in ins(g - 1):
                    copy.wait()
                for copy in outs(g - 1):
                    copy.start()
            if 0 <= g - 2 < len(groups):
                for copy in outs(g - 2):
                    copy.wait()
            if g < len(groups):
                for copy in ins(g):
                    copy.start()

    ht = ht_ref[...]
    pair = 2 * pl.program_id(1)
    wk_ref[...] = dot(ht, lanes(d_ref[pair, :, :HEAD_DIM], d_ref[pair + 1, :, :HEAD_DIM]))
    wv_ref[...] = dot(ht, lanes(d_ref[pair, :, HEAD_DIM:], d_ref[pair + 1, :, HEAD_DIM:]))

    @pl.when(step == 0)
    def _():
        gg_ref[...] = jnp.zeros_like(gg_ref)

    @pl.when(step < ROW_STEPS)
    def _():
        x_f = x_ref[...].astype(F32)
        inv_rms = lax.rsqrt(jnp.mean(x_f * x_f, axis=-1, keepdims=True) + NORM_EPS)
        normed = x_f * inv_rms
        d_hid = hid_ref[...]
        both = d_hid * normed
        gain = gain_ref[...]
        gg_ref[...] += jnp.sum(both.reshape(both.shape[0] // 8, 8, both.shape[1]), axis=0)
        mean = jnp.mean(both * gain, axis=-1, keepdims=True)
        d_x = inv_rms * (d_hid * gain - normed * mean)
        gx_ref[...] = (dy_ref[...].astype(F32) + d_x).astype(BF16)
        res_ref[...] = part_ref[...]


def finish(ht, d_kv, tiles, d_hid, x, grad_out, gain_f, result, heads, n_o, n_qa):
    width, seq_len = ht.shape
    groups = d_kv.shape[0]
    n_j = groups // 2
    steps = (width // MROWS) * n_j
    assert -(-2 * tiles.shape[1] // RING) + 2 <= steps
    any_spec = pl.BlockSpec(memory_space=pl.ANY)
    rows = pl.BlockSpec((x.shape[0] // ROW_STEPS, width), lambda m, j: (jnp.minimum(m * n_j + j, ROW_STEPS - 1), 0))
    whole = lambda *shape: pl.BlockSpec(shape, lambda m, j: (0,) * len(shape))
    kv_out = pl.BlockSpec((MROWS, 2 * HEAD_DIM), lambda m, j: (m, j))
    out = lambda cols: jax.ShapeDtypeStruct((width, cols), F32)
    return pl.pallas_call(
        functools.partial(finish_kernel, heads, n_o, n_qa),
        grid=(width // MROWS, n_j),
        in_specs=[pl.BlockSpec((MROWS, seq_len), lambda m, j: (m, 0)),
                  pl.BlockSpec(d_kv.shape, lambda m, j: (0, 0, 0), pipeline_mode=pl.Buffered(1)),
                  rows, rows, rows, whole(1, width), rows, any_spec],
        out_specs=[kv_out, kv_out, any_spec, any_spec, rows, whole(8, width), rows],
        out_shape=[out(groups * HEAD_DIM), out(groups * HEAD_DIM), out(groups * heads * HEAD_DIM),
                   jax.ShapeDtypeStruct((groups * heads * HEAD_DIM, width), F32), jax.ShapeDtypeStruct(x.shape, BF16),
                   jax.ShapeDtypeStruct((8, width), F32), jax.ShapeDtypeStruct(x.shape, BF16)],
        scratch_shapes=[pltpu.VMEM((2, RING) + tiles.shape[2:], F32), pltpu.SemaphoreType.DMA((2, 2, RING, 4))],
        compiler_params=params(2),
        cost_estimate=pl.CostEstimate(flops=4 * width * seq_len * groups * HEAD_DIM, bytes_accessed=2 * width * seq_len, transcendentals=0),
        name="finish",
    )(ht, d_kv, d_hid, x, grad_out, gain_f, result, tiles)


def solution(mesh):
    sp_size = mesh.shape['sp']
    seq_spec = P(('dp', 'sp'), None)
    pos_spec = P(('dp', 'sp'))
    replicated = P(None, None)
    part_rows = P('dp', None)

    def local_step(x, grad_out, positions, gain, w_q, w_k, w_v, w_o):
        n_heads = w_q.shape[1] // HEAD_DIM
        heads = n_heads // sp_size
        gain_f = gain.astype(F32).reshape(1, -1)
        hidden, cos_t, sin_t = gather_h(x, gain_f, positions, sp_size)
        q, k, v, ht, ot, lse, d_out = forward(hidden, w_q, w_k, w_v, cos_t, sin_t, grad_out, heads)
        *grads, ot_all = backward(q, k, v, d_out, w_o, ot, lse, cos_t, sin_t, heads, sp_size)
        tiles, kv_all, _, _, part, d_hid = products(ot_all, ht, d_out, *grads, x, w_o, w_k, w_v, w_q, sp_size, heads)
        n_o = x.shape[1] // tiles.shape[3]
        grad_wk, grad_wv, grad_wq, grad_wo, grad_x, gg, result = finish(
            ht, kv_all.reshape(sp_size, -1, 2 * HEAD_DIM), tiles, d_hid, x, grad_out, gain_f, part, heads, n_o, (tiles.shape[1] - n_o) * 2 // 3)
        grad_gain = jnp.sum(lax.all_gather(gg, 'sp', axis=0, tiled=True), axis=0)
        return result, grad_x, grad_wq, grad_wk, grad_wv, grad_wo, grad_gain

    return jax.shard_map(local_step, mesh=mesh,
                         in_specs=(seq_spec, seq_spec, pos_spec, P(None), replicated, replicated, replicated, replicated),
                         out_specs=(seq_spec, seq_spec, part_rows, part_rows, part_rows, part_rows, P('dp')),
                         check_vma=False)
```

```python
import functools

import jax
import jax.numpy as jnp
import numpy as np
from jax import lax
from jax.experimental import pallas as pl
from jax.experimental.pallas import tpu as pltpu
from jax.sharding import PartitionSpec as P

HEAD_DIM = 128
HALF = HEAD_DIM // 2
ROPE_THETA = 1000000.0
NORM_EPS = 1e-05
NEG_LARGE = -1e30
LOG2E = 1.4426950408889634
BLK = 512
CHUNKS = 4
FWD_MIDDLE, FWD_LATE, BWD_MIDDLE, BWD_LATE = 5, 6, 5, 6
MROWS = 384
RING = 2
DEPTH = 5
ROW_STEPS = 8
F32 = jnp.float32
BF16 = jnp.bfloat16
ROWS_ROWS = (((0,), (0,)), ((), ()))
COLS_COLS = (((1,), (1,)), ((), ()))
ROWS_COLS = (((0,), (1,)), ((), ()))
VMEM_LIMIT = 63 * 1024 * 1024


def dot(a, b, dims=(((1,), (0,)), ((), ()))):
    return lax.dot_general(a, b, dims, preferred_element_type=F32)


def params(axes=1):
    return pltpu.CompilerParams(dimension_semantics=("arbitrary",) * axes, vmem_limit_bytes=VMEM_LIMIT)


class Neighbours:
    def __init__(self):
        self.me = lax.axis_index('sp')
        core, col, row = lax.rem(self.me, 2), lax.rem(self.me // 2, 2), self.me // 4
        self.sib = self.me + 1 - 2 * core
        self.xn = self.me + 2 - 4 * col
        self.yn = self.me + 4 - 8 * row
        self.diag = self.xn + self.yn - self.me

    def meet(self, peers):
        barrier = pltpu.get_barrier_semaphore()
        for peer in peers:
            pl.semaphore_signal(barrier, inc=1, device_id={'sp': peer}, device_id_type=pl.DeviceIdType.MESH)
        pl.semaphore_wait(barrier, len(peers))

    def across(self, r):
        core, col, row = lax.rem(self.me, 2), lax.rem(self.me // 2, 2), self.me // 4
        return (self.me + lax.rem(r, 2) * (1 - 2 * core) + lax.rem(r // 2, 2) * (2 - 4 * col) + (r // 4) * (4 - 8 * row))

    def others(self):
        flip = lambda dev: dev + 1 - 2 * lax.rem(dev, 2)
        return [self.sib, self.xn, flip(self.xn), self.yn, flip(self.yn), self.diag, flip(self.diag)]


def send(src, dst, sems, index, peer):
    return pltpu.make_async_remote_copy(src_ref=src, dst_ref=dst, send_sem=sems.at[0, index], recv_sem=sems.at[1, index],
                                        device_id={'sp': peer}, device_id_type=pl.DeviceIdType.MESH)


class Gather:
    COPIES = 22

    def __init__(self, near, own, dst, rows, sems):
        self.near, self.own, self.dst, self.rows, self.sems = near, own, dst, rows, sems

    def block(self, dev, chunk, count=1):
        size = self.rows // CHUNKS
        return self.dst.at[pl.ds(pl.multiple_of(dev * self.rows + chunk * size, size), count * size), :]

    def first(self, chunk, kind):
        peer = (self.near.xn, self.near.yn, self.near.sib)[kind]
        return send(self.own(chunk), self.block(self.near.me, chunk), self.sems, kind * CHUNKS + chunk, peer)

    def onward(self, chunk):
        over_y = chunk < CHUNKS // 2
        rows = self.block(self.near.xn if over_y else self.near.yn, chunk)
        return send(rows, rows, self.sems, 12 + chunk, self.near.yn if over_y else self.near.xn)

    def share(self, kind):
        rows = self.block((self.near.xn, self.near.yn)[kind], 0, CHUNKS)
        return send(rows, rows, self.sems, 16 + kind, self.near.sib)

    def share_diag(self, chunk):
        rows = self.block(self.near.diag, chunk)
        return send(rows, rows, self.sems, 18 + chunk, self.near.sib)

    def begin(self):
        self.near.meet([self.near.sib, self.near.xn, self.near.yn])
        for chunk in range(CHUNKS):
            self.start(chunk)

    def start(self, chunk):
        for kind in range(3):
            self.first(chunk, kind).start()

    def middle(self):
        for chunk in (0, 1):
            self.first(chunk, 0).wait_recv()
            self.onward(chunk).start()
        self.first(2, 1).wait_recv()
        self.onward(2).start()

    def late(self):
        self.first(3, 1).wait_recv()
        self.onward(3).start()
        for chunk in (2, 3):
            self.first(chunk, 0).wait_recv()
        self.share(0).start()
        for chunk in (0, 1):
            self.first(chunk, 1).wait_recv()
        self.share(1).start()

    def end_near(self):
        for chunk in range(CHUNKS):
            self.first(chunk, 2).wait_recv()
        for kind in range(2):
            self.share(kind).wait_recv()

    def end_far(self):
        for chunk in (0, 2, 1, 3):
            self.onward(chunk).wait_recv()
            self.share_diag(chunk).start()
        for chunk in range(CHUNKS):
            for kind in range(3):
                self.first(chunk, kind).wait_send()
            self.onward(chunk).wait_send()
        for kind in range(2):
            self.share(kind).wait_send()
        for chunk in range(CHUNKS):
            self.share_diag(chunk).wait()

    def end(self):
        self.end_near()
        self.end_far()


SEMS = pltpu.SemaphoreType.DMA((2, Gather.COPIES))


def masked(scores):
    key = lax.broadcasted_iota(jnp.int32, scores.shape, 0)
    query = lax.broadcasted_iota(jnp.int32, scores.shape, 1)
    return jnp.where(key <= query, scores, NEG_LARGE)


def unrotate(val, cos_t, sin_t):
    return (val * cos_t - pltpu.roll(val, HALF, 1) * sin_t).astype(BF16)


def attention_kernel(heads, x_ref, gain_ref, pos_ref, freq_ref, dy_ref, wq_ref, wk_ref, wv_ref, wo_ref,
                     h_all, dy_all, o_all, ht_ref, dkv_ref, dq_a_ref, dq_b_ref,
                     x_v, h_v, x_sems, own_sems, pos_all, pos_sems, cos_s, sin_s, w_v, wo_v, w_sems, blk, blk_sems, ht_v, ht_sems,
                     q_s, k_s, v_s, vt, kt, ot_s, lse_s, acc, do_s, dk_acc, dv_acc, dq_v, dq_sems, dkv_v, h_sems, dy_sems, o_sems):
    near = Neighbours()
    rows, width = x_ref.shape
    n_blocks = k_s.shape[0]
    q_cols = heads * HEAD_DIM
    size = rows // CHUNKS
    qk_scale = HEAD_DIM ** -0.5
    to_log2 = qk_scale * LOG2E
    cols = [slice(a * HEAD_DIM, (a + 1) * HEAD_DIM) for a in range(heads)]
    part = lambda ref, chunk, count=size: ref.at[pl.ds(chunk * count, count), :]
    gather_h = Gather(near, lambda chunk: part(h_v, chunk), h_all, rows, h_sems)
    gather_dy = Gather(near, lambda chunk: part(dy_ref, chunk), dy_all, rows, dy_sems)
    gather_o = Gather(near, lambda chunk: part(ot_s, chunk, q_cols // CHUNKS), o_all, q_cols, o_sems)

    loads = [pltpu.make_async_copy(part(x_ref, chunk), part(x_v, chunk), x_sems.at[chunk]) for chunk in range(CHUNKS)]
    for load in loads:
        load.start()
    others = near.others()
    near.meet(others)
    pos_all[near.me] = jnp.broadcast_to(pos_ref[...], pos_all.shape[1:])
    positions = [send(pos_ref, pos_all.at[near.me, pl.ds(0, 1), :], pos_sems, r, peer) for r, peer in enumerate(others)]
    gain = gain_ref[...].astype(F32)
    for chunk in range(CHUNKS):
        loads[chunk].wait()

        @pl.loop(0, size // 32)
        def _(r):
            at = pl.ds(pl.multiple_of(chunk * size + r * 32, 32), 32)
            x_f = x_v[at, :].astype(F32)
            normed = x_f * lax.rsqrt(jnp.mean(x_f * x_f, axis=-1, keepdims=True) + NORM_EPS)
            h_v[at, :] = (normed * gain).astype(BF16)

        gather_h.start(chunk)
    for copy in positions:
        copy.start()
    own_h = pltpu.make_async_copy(h_v, gather_h.block(near.me, 0, CHUNKS), own_sems.at[0])
    own_h.start()
    w_loads, col = [], 0
    for n, (ref, count) in enumerate(((wq_ref, q_cols), (wk_ref, HEAD_DIM), (wv_ref, HEAD_DIM))):
        at = pl.ds(pl.multiple_of(near.me * count, HEAD_DIM), count)
        w_loads.append(pltpu.make_async_copy(ref.at[:, at], w_v.at[:, pl.ds(col, count)], w_sems.at[n]))
        col += count
    w_loads.append(pltpu.make_async_copy(wo_ref.at[pl.ds(pl.multiple_of(near.me * q_cols, q_cols), q_cols), :], wo_v, w_sems.at[3]))
    stage_in = pltpu.make_async_copy(dy_ref, x_v, own_sems.at[1])
    stage_out = pltpu.make_async_copy(x_v, gather_dy.block(near.me, 0, CHUNKS), own_sems.at[2])
    for load in w_loads + [stage_in]:
        load.start()
    for copy in positions:
        copy.wait()
    sign = jnp.where(lax.broadcasted_iota(jnp.int32, (1, HEAD_DIM), 1) < HALF, -1.0, 1.0)

    @pl.loop(0, n_blocks)
    def _(b):
        pos = jnp.broadcast_to(pos_all[b, 0:1, :].astype(F32), (HEAD_DIM, rows)).T
        angles = pos * freq_ref[...]
        cos_s[b] = jnp.cos(angles)
        sin_s[b] = jnp.sin(angles) * sign

    gather_h.middle()
    gather_h.late()
    for chunk in range(CHUNKS):
        gather_dy.start(chunk)
    for load in w_loads + [stage_in]:
        load.wait()
    stage_out.start()
    own_h.wait()
    gather_h.end()

    def block_load(ref, block, slot):
        return pltpu.make_async_copy(ref.at[pl.ds(pl.multiple_of(block * rows, rows), rows), :], blk.at[slot], blk_sems.at[slot])

    def fwd_chunk(i, c, carry, diagonal):
        k_c, vt_c = k_s[c], vt[c]
        scores = [dot(k_c, q_s[i, :, cols[a]], COLS_COLS) * to_log2 for a in range(heads)]
        out = []
        for a in range(heads):
            s = masked(scores[a]) if diagonal else scores[a]
            m_old, l_old = carry[a]
            m_new = jnp.maximum(m_old, jnp.max(s, axis=0, keepdims=True))
            alpha = jnp.exp2(m_old - m_new)
            p = jnp.exp2(s - m_new)
            l_new = l_old * alpha + jnp.sum(p, axis=0, keepdims=True)
            acc[a] = acc[a] * alpha + dot(vt_c, p.astype(BF16))
            out.append((m_new, l_new))
        return tuple(out)

    def ht_store(i):
        at = pl.ds(pl.multiple_of(i * rows, rows), rows)
        return pltpu.make_async_copy(ht_v.at[lax.rem(i, 2)], ht_ref.at[:, at], ht_sems.at[lax.rem(i, 2)])

    block_load(h_all, 0, 0).start()

    @pl.loop(0, n_blocks)
    def _(i):
        slot = lax.rem(i, 2)
        block_load(h_all, i, slot).wait()

        @pl.when(i + 1 < n_blocks)
        def _():
            block_load(h_all, i + 1, 1 - slot).start()

        @pl.when(i >= 2)
        def _():
            ht_store(i - 2).wait()

        ht_v[slot] = blk[slot].T
        ht_store(i).start()
        prod = dot(blk[slot], w_v[...])
        cos_t, sin_t = cos_s[i], sin_s[i]
        for a in range(heads + 1):
            val = prod[:, a * HEAD_DIM:(a + 1) * HEAD_DIM]
            rot = (val * cos_t + pltpu.roll(val, HALF, 1) * sin_t).astype(BF16)
            if a < heads:
                q_s[i, :, cols[a]] = rot
            else:
                k_s[i] = rot
                kt[i] = rot.T
        v_i = prod[:, q_cols + HEAD_DIM:].astype(BF16)
        v_s[i] = v_i
        vt[i] = v_i.T
        acc[...] = jnp.zeros_like(acc)
        start = tuple((jnp.full((1, rows), NEG_LARGE, F32), jnp.zeros((1, rows), F32)) for _ in range(heads))
        carry = lax.fori_loop(0, i, lambda c, carry: fwd_chunk(i, c, carry, False), start)
        carry = fwd_chunk(i, i, carry, True)
        at = pl.ds(pl.multiple_of(i * rows, rows), rows)
        for a in range(heads):
            m_a, l_a = carry[a]
            ot_s[cols[a], at] = (acc[a] / l_a).astype(BF16)
            lse_s[i, a:a + 1, :] = m_a + jnp.log2(l_a)

        @pl.when(i == FWD_MIDDLE)
        def _():
            gather_dy.middle()

        @pl.when(i == FWD_LATE)
        def _():
            gather_dy.late()

    for chunk in range(CHUNKS):
        gather_o.start(chunk)
    own_o = pltpu.make_async_copy(ot_s, gather_o.block(near.me, 0, CHUNKS), own_sems.at[0])
    own_o.start()

    def d_o_blocks(low, high):
        block_load(dy_all, near.across(low), 0).start()

        @pl.loop(low, high)
        def _(r):
            slot = lax.rem(r - low, 2)
            block_load(dy_all, 0, slot).wait()

            @pl.when(r + 1 < high)
            def _():
                block_load(dy_all, near.across(r + 1), 1 - slot).start()

            do_s[near.across(r)] = dot(blk[slot], wo_v[...], COLS_COLS).astype(BF16)

    stage_out.wait()
    gather_dy.end_near()
    d_o_blocks(0, n_blocks * 3 // 4)
    gather_dy.end_far()
    d_o_blocks(n_blocks * 3 // 4, n_blocks)

    def bwd_chunk(i, c, delta, diagonal):
        k_c, v_c, kt_c = k_s[c], v_s[c], kt[c]
        dk_c = dv_c = None
        for a in range(heads):
            q_a, do_a = q_s[i, :, cols[a]], do_s[i, :, cols[a]]
            s = dot(k_c, q_a, COLS_COLS) * to_log2
            if diagonal:
                s = masked(s)
            p = jnp.exp2(s - lse_s[i, a:a + 1, :])
            d_p = dot(v_c, do_a, COLS_COLS)
            d_s = (p * (d_p - delta[a])).astype(BF16)
            dv_a = dot(p.astype(BF16), do_a)
            dk_a = dot(d_s, q_a)
            dv_c = dv_a if dv_c is None else dv_c + dv_a
            dk_c = dk_a if dk_c is None else dk_c + dk_a
            acc[a] += dot(kt_c, d_s)
        if diagonal:
            dk_acc[c] = dk_c
            dv_acc[c] = dv_c
        else:
            dk_acc[c] += dk_c
            dv_acc[c] += dv_c

    def dq_stores(i):
        slot = lax.rem(i, 2)
        at = pl.ds(pl.multiple_of(i * rows, rows), rows)
        last = q_cols - HEAD_DIM
        return [pltpu.make_async_copy(dq_v.at[slot, :, pl.ds(0, last)], dq_a_ref.at[at, :], dq_sems.at[slot, 0]),
                pltpu.make_async_copy(dq_v.at[slot, :, pl.ds(last, HEAD_DIM)], dq_b_ref.at[at, :], dq_sems.at[slot, 1])]

    for i in (n_blocks - 2, n_blocks - 1):
        ht_store(i).wait()

    @pl.loop(0, n_blocks)
    def _(i):
        at = pl.ds(pl.multiple_of(i * rows, rows), rows)
        acc[...] = jnp.zeros_like(acc)
        delta = [jnp.sum(ot_s[cols[a], at].astype(F32) * do_s[i, :, cols[a]].T.astype(F32), axis=0, keepdims=True) for a in range(heads)]

        @pl.loop(0, i)
        def _(c):
            bwd_chunk(i, c, delta, False)

        bwd_chunk(i, i, delta, True)

        @pl.when(i >= 2)
        def _():
            for store in dq_stores(i - 2):
                store.wait()

        for a in range(heads):
            dq_v[lax.rem(i, 2), :, cols[a]] = unrotate(acc[a].T * qk_scale, cos_s[i], sin_s[i])
        for store in dq_stores(i):
            store.start()

        @pl.when(i == BWD_MIDDLE)
        def _():
            gather_o.middle()

        @pl.when(i == BWD_LATE)
        def _():
            gather_o.late()

    @pl.loop(0, n_blocks)
    def _(c):
        at = pl.ds(pl.multiple_of(c * rows, rows), rows)
        dkv_v[at, :HEAD_DIM] = unrotate(dk_acc[c] * qk_scale, cos_s[c], sin_s[c])
        dkv_v[at, HEAD_DIM:] = dv_acc[c].astype(BF16)

    dkv_store = pltpu.make_async_copy(dkv_v, dkv_ref, own_sems.at[1])
    dkv_store.start()
    own_o.wait()
    gather_o.end()
    for i in (n_blocks - 2, n_blocks - 1):
        for store in dq_stores(i):
            store.wait()
    dkv_store.wait()


def attention(x, gain, positions, grad_out, w_q, w_k, w_v, w_o, sp_size, heads):
    rows, width = x.shape
    seq_len = rows * sp_size
    q_cols = heads * HEAD_DIM
    any_spec = pl.BlockSpec(memory_space=pl.ANY)
    vmem = pl.BlockSpec(memory_space=pltpu.VMEM)
    dma = pltpu.SemaphoreType.DMA
    inv_freq = ROPE_THETA ** (-np.arange(0, HEAD_DIM, 2) / HEAD_DIM)
    freq = jnp.asarray(np.concatenate([inv_freq, inv_freq])[None, :], F32)
    pairs = heads * seq_len * (seq_len + rows) // 2
    out = lambda *shape: jax.ShapeDtypeStruct(shape, BF16)
    blocks = lambda *shape, dtype=BF16: pltpu.VMEM((sp_size,) + shape, dtype)
    return pl.pallas_call(
        functools.partial(attention_kernel, heads),
        in_specs=[any_spec, vmem, vmem, vmem] + [any_spec] * 5,
        out_specs=[any_spec] * 7,
        out_shape=[out(seq_len, width), out(seq_len, width), out(q_cols * sp_size, seq_len), out(width, seq_len), out(seq_len, 2 * HEAD_DIM),
                   out(seq_len, q_cols - HEAD_DIM), out(seq_len, HEAD_DIM)],
        scratch_shapes=[pltpu.VMEM((rows, width), BF16), pltpu.VMEM((rows, width), BF16), dma((CHUNKS,)), dma((3,)),
                        blocks(8, rows, dtype=jnp.int32), dma((2, 7)), blocks(rows, HEAD_DIM, dtype=F32), blocks(rows, HEAD_DIM, dtype=F32),
                        pltpu.VMEM((width, q_cols + 2 * HEAD_DIM), BF16), pltpu.VMEM((q_cols, width), BF16), dma((4,)),
                        pltpu.VMEM((2, rows, width), BF16), dma((2,)), pltpu.VMEM((2, width, rows), BF16), dma((2,)),
                        blocks(rows, q_cols), blocks(rows, HEAD_DIM), blocks(rows, HEAD_DIM), blocks(HEAD_DIM, rows), blocks(HEAD_DIM, rows),
                        pltpu.VMEM((q_cols, seq_len), BF16), blocks(8, rows, dtype=F32), pltpu.VMEM((heads, HEAD_DIM, rows), F32),
                        blocks(rows, q_cols), blocks(rows, HEAD_DIM, dtype=F32), blocks(rows, HEAD_DIM, dtype=F32),
                        pltpu.VMEM((2, rows, q_cols), BF16), dma((2, 2)), pltpu.VMEM((seq_len, 2 * HEAD_DIM), BF16), SEMS, SEMS, SEMS],
        compiler_params=pltpu.CompilerParams(vmem_limit_bytes=VMEM_LIMIT, collective_id=0, has_side_effects=True),
        cost_estimate=pl.CostEstimate(flops=28 * pairs * HEAD_DIM, bytes_accessed=20 * seq_len * width, transcendentals=2 * pairs),
        name="attention",
    )(x, gain.reshape(1, -1), positions.reshape(1, -1), freq, grad_out, w_q, w_k, w_v, w_o)


def lanes(*parts):
    return jnp.concatenate(parts, axis=1)


def products_kernel(heads, ot_ref, ht_ref, dy_ref, d_kv_ref, d_qa_ref, d_qb_ref, x_ref, wo_ref, wk_ref, wv_ref, wq_ref,
                    tiles, kv_all, qa_all, qb_all, res_ref, hid_ref,
                    a_buf, b_buf, tile, a_sem, b_sems, t_sems, x_sems, stage, stage_sems, ot_v, o_v, x_v, io_sems, own, own_sems, w_v, w_sems, acc,
                    kv_sems, qa_sems, qb_sems):
    near = Neighbours()
    core = lax.rem(near.me, 2)
    half = a_buf.shape[0]
    seq_len = d_kv_ref.shape[0]
    rows, width = x_ref.shape
    chunk = seq_len // CHUNKS
    n_cols = d_kv_ref.shape[1]
    n_o, n_all = width // (2 * n_cols), tiles.shape[1]
    n_qa = (n_all - n_o) * 2 // 3
    n_oa = n_o + n_qa

    def gather_of(src, dst, sems):
        return Gather(near, lambda c: src.at[pl.ds(c * chunk, chunk), :], dst, seq_len, sems)

    local = (d_qa_ref, d_qb_ref, d_kv_ref)
    gathers = [gather_of(d_qa_ref, qa_all, qa_sems), gather_of(d_qb_ref, qb_all, qb_sems), gather_of(d_kv_ref, kv_all, kv_sems)]

    def stage_in(n):
        return pltpu.make_async_copy(local[n], stage.at[:, pl.ds(0, local[n].shape[1])], stage_sems.at[0])

    def stage_out(n):
        return pltpu.make_async_copy(stage.at[:, pl.ds(0, local[n].shape[1])], gathers[n].block(near.me, 0, CHUNKS), stage_sems.at[1])

    def copy_own(n):
        stage_in(n).wait()
        stage_out(n).start()

    own_rows = pl.ds(pl.multiple_of(core * half, half), half)
    tokens = pl.ds(pl.multiple_of(near.me * rows, rows), rows)
    ot_load = pltpu.make_async_copy(ot_ref.at[:, tokens], ot_v, io_sems.at[0])
    x_load = pltpu.make_async_copy(x_ref, x_v, io_sems.at[1])
    res_store = pltpu.make_async_copy(x_v, res_ref, io_sems.at[2])
    hid_store = pltpu.make_async_copy(acc, hid_ref, io_sems.at[3])

    def a_load(ref):
        return pltpu.make_async_copy(ref.at[own_rows, :], a_buf, a_sem)

    def b_loads(source, p, slot, g):
        if source is dy_ref:
            srcs = [dy_ref.at[:, pl.ds(pl.multiple_of((2 * p + g) * n_cols, n_cols), n_cols)]]
        else:
            per = n_cols // source.shape[1]
            srcs = [source.at[pl.ds(pl.multiple_of(((2 * p + g) * per + n) * seq_len, seq_len), seq_len), :] for n in range(per)]
        return [pltpu.make_async_copy(src, b_buf.at[slot, :, pl.ds(g * n_cols + n * src.shape[1], src.shape[1])], b_sems.at[slot, g])
                for n, src in enumerate(srcs)]

    def start_b(step):
        slot = lax.rem(step, 2)
        for source, low, high in ((dy_ref, 0, n_o), (qa_all, n_o, n_oa), (qb_all, n_oa, n_all)):
            @pl.when(jnp.logical_and(step >= low, step < high))
            def _():
                for g in range(2):
                    for load in b_loads(source, step - low, slot, g):
                        load.start()

    def keep(step):
        return pltpu.make_async_copy(tile.at[lax.rem(step, 2)], tiles.at[core, step], t_sems.at[lax.rem(step, 2)])

    def give(step):
        return send(tile.at[lax.rem(step, 2)], tiles.at[core, step], x_sems, step, near.sib)

    def result_part():
        cols = b_buf.shape[2]

        def w_load(n):
            slot = lax.rem(n, 2)
            return pltpu.make_async_copy(wo_ref.at[:, pl.ds(pl.multiple_of(n * cols, cols), cols)], b_buf.at[slot, pl.ds(0, wo_ref.shape[0]), :],
                                         b_sems.at[slot, 0])

        w_load(jnp.int32(0)).start()
        ot_load.wait()

        @pl.loop(0, ot_v.shape[0] // BLK)
        def _(r):
            at = pl.ds(pl.multiple_of(r * BLK, BLK), BLK)
            o_v[:, at] = ot_v[at, :].T

        x_load.wait()

        @pl.loop(0, n_o)
        def _(n):
            w_load(n).wait()

            @pl.when(n + 1 < n_o)
            def _():
                w_load(n + 1).start()

            at = pl.ds(pl.multiple_of(n * cols, cols), cols)
            x_v[:, at] = (x_v[:, at].astype(F32) + dot(o_v[...], b_buf[lax.rem(n, 2), :wo_ref.shape[0], :])).astype(BF16)

        res_store.start()

    def hidden_parts(kind):
        count = own.shape[0] // (2 if kind == 1 else 1)

        def own_load(r, g):
            source = (qa_all, qb_all, kv_all)[kind]
            device, col = (2 * r + g, 0) if kind == 1 else (near.across(r), g * HEAD_DIM)
            at = pl.ds(pl.multiple_of(device * seq_len + near.me * rows, rows), rows)
            return pltpu.make_async_copy(source.at[at, pl.ds(col, HEAD_DIM)], own.at[r, :, pl.ds(g * HEAD_DIM, HEAD_DIM)], own_sems.at[r, g])

        def w_load(r, g):
            source = (wk_ref, wv_ref)[g] if kind == 2 else wq_ref
            col = near.across(r) if kind == 2 else heads * near.across(r) + g if kind == 0 else heads * (2 * r + g + 1) - 1
            slot = lax.rem(r, 2)
            return pltpu.make_async_copy(source.at[:, pl.ds(pl.multiple_of(col * HEAD_DIM, HEAD_DIM), HEAD_DIM)],
                                         w_v.at[slot, :, pl.ds(g * HEAD_DIM, HEAD_DIM)], w_sems.at[slot, g])

        return count, own_load, w_load

    def hidden_start(kind, low=0, high=None):
        count, own_load, w_load = hidden_parts(kind)
        for g in range(2):
            if low == 0:
                w_load(jnp.int32(0), g).start()

            @pl.loop(low, high or count)
            def _(r):
                own_load(r, g).start()

    def hidden_add(kind, low=0, high=None):
        count, own_load, w_load = hidden_parts(kind)

        @pl.loop(low, high or count)
        def _(r):
            for g in range(2):
                w_load(r, g).wait()
                own_load(r, g).wait()

            @pl.when(r + 1 < count)
            def _():
                for g in range(2):
                    w_load(r + 1, g).start()

            prod = dot(own[r], w_v[lax.rem(r, 2)], COLS_COLS)
            if kind == 0:
                @pl.when(r == 0)
                def _():
                    acc[...] = prod

                @pl.when(r > 0)
                def _():
                    acc[...] += prod
            else:
                acc[...] += prod

    near.meet([near.sib, near.xn, near.yn])
    for c in range(CHUNKS):
        gathers[0].start(c)
    a_load(ot_ref).start()
    start_b(jnp.int32(0))
    stage_in(0).start()
    ot_load.start()
    x_load.start()
    a_load(ot_ref).wait()

    @pl.loop(0, n_all)
    def _(step):
        slot = lax.rem(step, 2)
        for g in range(2):
            b_loads(dy_ref, 0, slot, g)[0].wait()

        @pl.when(jnp.logical_and(step != n_o - 1, step != n_oa - 1))
        def _():
            start_b(step + 1)

        @pl.when(step >= 2)
        def _():
            keep(step - 2).wait()
            give(step - 2).wait_send()

        @pl.when(step == n_o)
        def _():
            a_load(ht_ref).wait()

        tile[slot] = dot(a_buf[...], b_buf[slot])
        keep(step).start()
        give(step).start()

        @pl.when(step == n_o - 2)
        def _():
            copy_own(0)
            gathers[0].middle()

        @pl.when(step == n_o - 1)
        def _():
            a_load(ht_ref).start()
            gathers[0].late()
            for c in range(CHUNKS):
                gathers[1].start(c)
            stage_out(0).wait()
            stage_in(1).start()
            result_part()
            gathers[0].end()
            start_b(step + 1)
            hidden_start(0)

        @pl.when(step == n_oa - 3)
        def _():
            copy_own(1)
            gathers[1].middle()

        @pl.when(step == n_oa - 2)
        def _():
            gathers[1].late()
            for c in range(CHUNKS):
                gathers[2].start(c)
            stage_out(1).wait()
            stage_in(2).start()

        @pl.when(step == n_oa - 1)
        def _():
            gathers[1].end()
            start_b(step + 1)
            hidden_add(0)
            hidden_start(1)

    hidden_add(1)
    copy_own(2)
    gathers[2].middle()
    gathers[2].late()
    stage_out(2).wait()
    gathers[2].end_near()
    near_count = own.shape[0] * 3 // 4
    hidden_start(2, 0, near_count)
    for step in (n_all - 2, n_all - 1):
        keep(step).wait()
        give(step).wait_send()
    hidden_add(2, 0, near_count)
    gathers[2].end_far()
    hidden_start(2, near_count)
    hidden_add(2, near_count)
    hid_store.start()

    @pl.loop(0, n_all)
    def _(step):
        give(step).wait_recv()

    res_store.wait()
    hid_store.wait()


def products(ot_all, ht, d_out, d_kv, d_qa, d_qb, x, w_o, w_k, w_v, w_q, sp_size, heads):
    width, seq_len = ht.shape
    half = width // 2
    cols = 2 * d_kv.shape[1]
    n_all = width // cols + sp_size * (d_qa.shape[1] + d_qb.shape[1]) // cols
    any_spec = pl.BlockSpec(memory_space=pl.ANY)
    dma = pltpu.SemaphoreType.DMA
    gathered = [jax.ShapeDtypeStruct((sp_size * seq_len, d.shape[1]), BF16) for d in (d_kv, d_qa, d_qb)]
    return pl.pallas_call(
        functools.partial(products_kernel, heads),
        in_specs=[any_spec] * 11,
        out_specs=[any_spec] * 6,
        out_shape=[jax.ShapeDtypeStruct((2, n_all, half, cols), F32)] + gathered
        + [jax.ShapeDtypeStruct(x.shape, BF16), jax.ShapeDtypeStruct(x.shape, F32)],
        scratch_shapes=[pltpu.VMEM((half, seq_len), BF16), pltpu.VMEM((2, seq_len, cols), BF16), pltpu.VMEM((2, half, cols), F32),
                        dma, dma((2, 2)), dma((2,)), dma((2, n_all)), pltpu.VMEM(d_kv.shape, BF16), dma((2,)),
                        pltpu.VMEM((ot_all.shape[0], x.shape[0]), BF16), pltpu.VMEM((x.shape[0], ot_all.shape[0]), BF16), pltpu.VMEM(x.shape, BF16),
                        dma((4,)), pltpu.VMEM((sp_size, x.shape[0], 2 * HEAD_DIM), BF16), dma((sp_size, 2)),
                        pltpu.VMEM((2, width, 2 * HEAD_DIM), BF16), dma((2, 2)), pltpu.VMEM(x.shape, F32), SEMS, SEMS, SEMS],
        compiler_params=pltpu.CompilerParams(vmem_limit_bytes=VMEM_LIMIT, collective_id=1, has_side_effects=True),
        cost_estimate=pl.CostEstimate(flops=2 * half * cols * seq_len * n_all, bytes_accessed=8 * half * cols * n_all, transcendentals=0),
        name="products",
    )(ot_all, ht, d_out, d_kv, d_qa, d_qb, x, w_o, w_k, w_v, w_q)


def finish_kernel(heads, n_o, n_qa, ht_ref, d_ref, hid_ref, x_ref, dy_ref, gain_ref, part_ref, tiles,
                  wk_ref, wv_ref, wq_ref, wo_ref, gx_ref, gg_ref, res_ref, d_v, d_sems, ring, ring_sems):
    step = pl.program_id(0) * pl.num_programs(1) + pl.program_id(1)
    half, high = tiles.shape[2], ring.shape[2]
    every = [(c, t, n) for t in range(tiles.shape[1]) for c in range(2) for n in range(half // high)]
    groups = [every[g:g + RING] for g in range(0, len(every), RING)]

    def pieces(c, t, part):
        rows = pl.ds(c * half + part * high, high)
        cols = ring.shape[3]
        if t < n_o:
            return [(0, cols, wo_ref.at[rows, pl.ds(t * cols, cols)])]
        wide, first, t = ((heads - 1) * HEAD_DIM, 0, t - n_o) if t < n_o + n_qa else (HEAD_DIM, heads - 1, t - n_o - n_qa)
        per = cols // wide
        return [(n * wide, wide, wq_ref.at[rows, pl.ds(((t * per + n) * heads + first) * HEAD_DIM, wide)]) for n in range(per)]

    def ins(g):
        return [pltpu.make_async_copy(tiles.at[c, t, pl.ds(part * high, high), :], ring.at[g % DEPTH, n], ring_sems.at[0, g % DEPTH, n, 0])
                for n, (c, t, part) in enumerate(groups[g])]

    def outs(g):
        return [pltpu.make_async_copy(ring.at[g % DEPTH, n, :, pl.ds(col, count)], dst, ring_sems.at[1, g % DEPTH, n, m])
                for n, item in enumerate(groups[g]) for m, (col, count, dst) in enumerate(pieces(*item))]

    def pair_load(p):
        at = pl.ds(2 * p, 2)
        return pltpu.make_async_copy(d_ref.at[at], d_v.at[at], d_sems.at[p])

    @pl.when(step == 0)
    def _():
        for p in range(d_v.shape[0] // 2):
            pair_load(p).start()

    for g in range(len(groups) + DEPTH):
        @pl.when(step == g)
        def _():
            if g >= DEPTH:
                for copy in outs(g - DEPTH):
                    copy.wait()
            if g < len(groups):
                for copy in ins(g):
                    copy.start()
            if 2 <= g < len(groups) + 2:
                for copy in ins(g - 2):
                    copy.wait()
                for copy in outs(g - 2):
                    copy.start()

    for p in range(d_v.shape[0] // 2):
        @pl.when(step == p)
        def _():
            pair_load(p).wait()

    ht = ht_ref[...]
    pair = 2 * pl.program_id(1)
    wk_ref[...] = dot(ht, lanes(d_v[pair, :, :HEAD_DIM], d_v[pair + 1, :, :HEAD_DIM]))
    wv_ref[...] = dot(ht, lanes(d_v[pair, :, HEAD_DIM:], d_v[pair + 1, :, HEAD_DIM:]))

    @pl.when(step == 0)
    def _():
        gg_ref[...] = jnp.zeros_like(gg_ref)

    @pl.when(step < ROW_STEPS)
    def _():
        x_f = x_ref[...].astype(F32)
        inv_rms = lax.rsqrt(jnp.mean(x_f * x_f, axis=-1, keepdims=True) + NORM_EPS)
        normed = x_f * inv_rms
        d_hid = hid_ref[...]
        both = d_hid * normed
        gain = gain_ref[...].astype(F32)
        gg_ref[...] += jnp.sum(both.reshape(both.shape[0] // 8, 8, both.shape[1]), axis=0)
        mean = jnp.mean(both * gain, axis=-1, keepdims=True)
        d_x = inv_rms * (d_hid * gain - normed * mean)
        gx_ref[...] = (dy_ref[...].astype(F32) + d_x).astype(BF16)
        res_ref[...] = part_ref[...]


def finish(ht, d_kv, tiles, d_hid, x, grad_out, gain_f, result, heads, n_o, n_qa):
    width, seq_len = ht.shape
    groups = d_kv.shape[0]
    n_j = groups // 2
    steps = (width // MROWS) * n_j
    assert -(-4 * tiles.shape[1] // RING) + DEPTH <= steps
    any_spec = pl.BlockSpec(memory_space=pl.ANY)
    rows = pl.BlockSpec((x.shape[0] // ROW_STEPS, width), lambda m, j: (jnp.minimum(m * n_j + j, ROW_STEPS - 1), 0))
    whole = lambda *shape: pl.BlockSpec(shape, lambda m, j: (0,) * len(shape))
    kv_out = pl.BlockSpec((MROWS, 2 * HEAD_DIM), lambda m, j: (m, j))
    out = lambda cols: jax.ShapeDtypeStruct((width, cols), F32)
    return pl.pallas_call(
        functools.partial(finish_kernel, heads, n_o, n_qa),
        grid=(width // MROWS, n_j),
        in_specs=[pl.BlockSpec((MROWS, seq_len), lambda m, j: (m, 0)),
                  any_spec, rows, rows, rows, whole(1, width), rows, any_spec],
        out_specs=[kv_out, kv_out, any_spec, any_spec, rows, whole(8, width), rows],
        out_shape=[out(groups * HEAD_DIM), out(groups * HEAD_DIM), out(groups * heads * HEAD_DIM),
                   jax.ShapeDtypeStruct((groups * heads * HEAD_DIM, width), F32), jax.ShapeDtypeStruct(x.shape, BF16),
                   jax.ShapeDtypeStruct((8, width), F32), jax.ShapeDtypeStruct(x.shape, BF16)],
        scratch_shapes=[pltpu.VMEM(d_kv.shape, BF16), pltpu.SemaphoreType.DMA((groups // 2,)),
                        pltpu.VMEM((DEPTH, RING, tiles.shape[2] // 2, tiles.shape[3]), F32), pltpu.SemaphoreType.DMA((2, DEPTH, RING, 4))],
        compiler_params=params(2),
        cost_estimate=pl.CostEstimate(flops=4 * width * seq_len * groups * HEAD_DIM, bytes_accessed=2 * width * seq_len, transcendentals=0),
        name="finish",
    )(ht, d_kv, d_hid, x, grad_out, gain_f, result, tiles)


def solution(mesh):
    sp_size = mesh.shape['sp']
    seq_spec = P(('dp', 'sp'), None)
    pos_spec = P(('dp', 'sp'))
    replicated = P(None, None)
    part_rows = P('dp', None)

    def local_step(x, grad_out, positions, gain, w_q, w_k, w_v, w_o):
        n_heads = w_q.shape[1] // HEAD_DIM
        heads = n_heads // sp_size
        _, d_out, ot_all, ht, *grads = attention(x, gain, positions, grad_out, w_q, w_k, w_v, w_o, sp_size, heads)
        tiles, kv_all, _, _, part, d_hid = products(ot_all, ht, d_out, *grads, x, w_o, w_k, w_v, w_q, sp_size, heads)
        n_o = x.shape[1] // tiles.shape[3]
        grad_wk, grad_wv, grad_wq, grad_wo, grad_x, gg, result = finish(
            ht, kv_all.reshape(sp_size, -1, 2 * HEAD_DIM), tiles, d_hid, x, grad_out, gain.reshape(1, -1), part, heads, n_o, (tiles.shape[1] - n_o) * 2 // 3)
        grad_gain = jnp.sum(lax.all_gather(gg, 'sp', axis=0, tiled=True), axis=0)
        return result, grad_x, grad_wq, grad_wk, grad_wv, grad_wo, grad_gain

    return jax.shard_map(local_step, mesh=mesh,
                         in_specs=(seq_spec, seq_spec, pos_spec, P(None), replicated, replicated, replicated, replicated),
                         out_specs=(seq_spec, seq_spec, part_rows, part_rows, part_rows, part_rows, P('dp')),
                         check_vma=False)
```

```python
import functools

import jax
import jax.numpy as jnp
import numpy as np
from jax import lax
from jax.experimental import pallas as pl
from jax.experimental.pallas import tpu as pltpu
from jax.sharding import PartitionSpec as P

HEAD_DIM = 128
HALF = HEAD_DIM // 2
ROPE_THETA = 1000000.0
NORM_EPS = 1e-05
NEG_LARGE = -1e30
LOG2E = 1.4426950408889634
BLK = 512
CHUNKS = 4
FWD_MIDDLE, FWD_LATE, BWD_MIDDLE, BWD_LATE = 5, 6, 5, 6
MROWS = 384
RING = 2
DEPTH = 5
COPY_ROWS = 24
ROW_STEPS = 8
F32 = jnp.float32
BF16 = jnp.bfloat16
ROWS_ROWS = (((0,), (0,)), ((), ()))
COLS_COLS = (((1,), (1,)), ((), ()))
ROWS_COLS = (((0,), (1,)), ((), ()))
VMEM_LIMIT = 63 * 1024 * 1024


def dot(a, b, dims=(((1,), (0,)), ((), ()))):
    return lax.dot_general(a, b, dims, preferred_element_type=F32)


def params(axes=1):
    return pltpu.CompilerParams(dimension_semantics=("arbitrary",) * axes, vmem_limit_bytes=VMEM_LIMIT)


class Neighbours:
    def __init__(self):
        self.me = lax.axis_index('sp')
        core, col, row = lax.rem(self.me, 2), lax.rem(self.me // 2, 2), self.me // 4
        self.sib = self.me + 1 - 2 * core
        self.xn = self.me + 2 - 4 * col
        self.yn = self.me + 4 - 8 * row
        self.diag = self.xn + self.yn - self.me

    def meet(self, peers):
        barrier = pltpu.get_barrier_semaphore()
        for peer in peers:
            pl.semaphore_signal(barrier, inc=1, device_id={'sp': peer}, device_id_type=pl.DeviceIdType.MESH)
        pl.semaphore_wait(barrier, len(peers))

    def across(self, r):
        core, col, row = lax.rem(self.me, 2), lax.rem(self.me // 2, 2), self.me // 4
        return (self.me + lax.rem(r, 2) * (1 - 2 * core) + lax.rem(r // 2, 2) * (2 - 4 * col) + (r // 4) * (4 - 8 * row))

    def others(self):
        flip = lambda dev: dev + 1 - 2 * lax.rem(dev, 2)
        return [self.sib, self.xn, flip(self.xn), self.yn, flip(self.yn), self.diag, flip(self.diag)]


def send(src, dst, sems, index, peer):
    return pltpu.make_async_remote_copy(src_ref=src, dst_ref=dst, send_sem=sems.at[0, index], recv_sem=sems.at[1, index],
                                        device_id={'sp': peer}, device_id_type=pl.DeviceIdType.MESH)


class Gather:
    COPIES = 22

    def __init__(self, near, own, dst, rows, sems):
        self.near, self.own, self.dst, self.rows, self.sems = near, own, dst, rows, sems

    def block(self, dev, chunk, count=1):
        size = self.rows // CHUNKS
        return self.dst.at[pl.ds(pl.multiple_of(dev * self.rows + chunk * size, size), count * size), :]

    def first(self, chunk, kind):
        peer = (self.near.xn, self.near.yn, self.near.sib)[kind]
        return send(self.own(chunk), self.block(self.near.me, chunk), self.sems, kind * CHUNKS + chunk, peer)

    def onward(self, chunk):
        over_y = chunk < CHUNKS // 2
        rows = self.block(self.near.xn if over_y else self.near.yn, chunk)
        return send(rows, rows, self.sems, 12 + chunk, self.near.yn if over_y else self.near.xn)

    def share(self, kind):
        rows = self.block((self.near.xn, self.near.yn)[kind], 0, CHUNKS)
        return send(rows, rows, self.sems, 16 + kind, self.near.sib)

    def share_diag(self, chunk):
        rows = self.block(self.near.diag, chunk)
        return send(rows, rows, self.sems, 18 + chunk, self.near.sib)

    def begin(self):
        self.near.meet([self.near.sib, self.near.xn, self.near.yn])
        for chunk in range(CHUNKS):
            self.start(chunk)

    def start(self, chunk):
        for kind in range(3):
            self.first(chunk, kind).start()

    def middle(self):
        for chunk in (0, 1):
            self.first(chunk, 0).wait_recv()
            self.onward(chunk).start()
        self.first(2, 1).wait_recv()
        self.onward(2).start()

    def late(self):
        self.first(3, 1).wait_recv()
        self.onward(3).start()
        for chunk in (2, 3):
            self.first(chunk, 0).wait_recv()
        self.share(0).start()
        for chunk in (0, 1):
            self.first(chunk, 1).wait_recv()
        self.share(1).start()

    def end_near(self):
        for chunk in range(CHUNKS):
            self.first(chunk, 2).wait_recv()
        for kind in range(2):
            self.share(kind).wait_recv()

    def end_far(self):
        for chunk in (0, 2, 1, 3):
            self.onward(chunk).wait_recv()
            self.share_diag(chunk).start()
        for chunk in range(CHUNKS):
            for kind in range(3):
                self.first(chunk, kind).wait_send()
            self.onward(chunk).wait_send()
        for kind in range(2):
            self.share(kind).wait_send()
        for chunk in range(CHUNKS):
            self.share_diag(chunk).wait()

    def end(self):
        self.end_near()
        self.end_far()


SEMS = pltpu.SemaphoreType.DMA((2, Gather.COPIES))


def masked(scores):
    key = lax.broadcasted_iota(jnp.int32, scores.shape, 0)
    query = lax.broadcasted_iota(jnp.int32, scores.shape, 1)
    return jnp.where(key <= query, scores, NEG_LARGE)


def unrotate(val, cos_t, sin_t):
    return (val * cos_t - pltpu.roll(val, HALF, 1) * sin_t).astype(BF16)


def attention_kernel(heads, x_ref, gain_ref, pos_ref, freq_ref, dy_ref, wq_ref, wk_ref, wv_ref, wo_ref,
                     h_all, dy_all, o_all, ht_ref, dkv_ref, dq_a_ref, dq_b_ref,
                     x_v, h_v, x_sems, own_sems, pos_all, pos_sems, cos_s, sin_s, w_v, wo_v, w_sems, blk, blk_sems, ht_v, ht_sems,
                     q_s, k_s, v_s, vt, kt, ot_s, lse_s, acc, do_s, dk_acc, dv_acc, dq_v, dq_sems, dkv_v, h_sems, dy_sems, o_sems):
    near = Neighbours()
    rows, width = x_ref.shape
    n_blocks = k_s.shape[0]
    q_cols = heads * HEAD_DIM
    size = rows // CHUNKS
    qk_scale = HEAD_DIM ** -0.5
    to_log2 = qk_scale * LOG2E
    cols = [slice(a * HEAD_DIM, (a + 1) * HEAD_DIM) for a in range(heads)]
    part = lambda ref, chunk, count=size: ref.at[pl.ds(chunk * count, count), :]
    gather_h = Gather(near, lambda chunk: part(h_v, chunk), h_all, rows, h_sems)
    gather_dy = Gather(near, lambda chunk: part(dy_ref, chunk), dy_all, rows, dy_sems)
    gather_o = Gather(near, lambda chunk: part(ot_s, chunk, q_cols // CHUNKS), o_all, q_cols, o_sems)

    loads = [pltpu.make_async_copy(part(x_ref, chunk), part(x_v, chunk), x_sems.at[chunk]) for chunk in range(CHUNKS)]
    for load in loads:
        load.start()
    others = near.others()
    near.meet(others)
    pos_all[near.me] = jnp.broadcast_to(pos_ref[...], pos_all.shape[1:])
    positions = [send(pos_ref, pos_all.at[near.me, pl.ds(0, 1), :], pos_sems, r, peer) for r, peer in enumerate(others)]
    gain = gain_ref[...].astype(F32)
    for chunk in range(CHUNKS):
        loads[chunk].wait()

        @pl.loop(0, size // 32)
        def _(r):
            at = pl.ds(pl.multiple_of(chunk * size + r * 32, 32), 32)
            x_f = x_v[at, :].astype(F32)
            normed = x_f * lax.rsqrt(jnp.mean(x_f * x_f, axis=-1, keepdims=True) + NORM_EPS)
            h_v[at, :] = (normed * gain).astype(BF16)

        gather_h.start(chunk)
    for copy in positions:
        copy.start()
    own_h = pltpu.make_async_copy(h_v, gather_h.block(near.me, 0, CHUNKS), own_sems.at[0])
    own_h.start()
    w_loads, col = [], 0
    for n, (ref, count) in enumerate(((wq_ref, q_cols), (wk_ref, HEAD_DIM), (wv_ref, HEAD_DIM))):
        at = pl.ds(pl.multiple_of(near.me * count, HEAD_DIM), count)
        w_loads.append(pltpu.make_async_copy(ref.at[:, at], w_v.at[:, pl.ds(col, count)], w_sems.at[n]))
        col += count
    w_loads.append(pltpu.make_async_copy(wo_ref.at[pl.ds(pl.multiple_of(near.me * q_cols, q_cols), q_cols), :], wo_v, w_sems.at[3]))
    stage_in = pltpu.make_async_copy(dy_ref, x_v, own_sems.at[1])
    stage_out = pltpu.make_async_copy(x_v, gather_dy.block(near.me, 0, CHUNKS), own_sems.at[2])
    for load in w_loads + [stage_in]:
        load.start()
    for copy in positions:
        copy.wait()
    sign = jnp.where(lax.broadcasted_iota(jnp.int32, (1, HEAD_DIM), 1) < HALF, -1.0, 1.0)

    @pl.loop(0, n_blocks)
    def _(b):
        pos = jnp.broadcast_to(pos_all[b, 0:1, :].astype(F32), (HEAD_DIM, rows)).T
        angles = pos * freq_ref[...]
        cos_s[b] = jnp.cos(angles)
        sin_s[b] = jnp.sin(angles) * sign

    gather_h.middle()
    gather_h.late()
    for chunk in range(CHUNKS):
        gather_dy.start(chunk)
    for load in w_loads + [stage_in]:
        load.wait()
    stage_out.start()
    own_h.wait()
    gather_h.end()

    def block_load(ref, block, slot):
        return pltpu.make_async_copy(ref.at[pl.ds(pl.multiple_of(block * rows, rows), rows), :], blk.at[slot], blk_sems.at[slot])

    def fwd_chunk(i, c, carry, diagonal):
        k_c, vt_c = k_s[c], vt[c]
        scores = [dot(k_c, q_s[i, :, cols[a]], COLS_COLS) * to_log2 for a in range(heads)]
        out = []
        for a in range(heads):
            s = masked(scores[a]) if diagonal else scores[a]
            m_old, l_old = carry[a]
            m_new = jnp.maximum(m_old, jnp.max(s, axis=0, keepdims=True))
            alpha = jnp.exp2(m_old - m_new)
            p = jnp.exp2(s - m_new)
            l_new = l_old * alpha + jnp.sum(p, axis=0, keepdims=True)
            acc[a] = acc[a] * alpha + dot(vt_c, p.astype(BF16))
            out.append((m_new, l_new))
        return tuple(out)

    def ht_store(i):
        at = pl.ds(pl.multiple_of(i * rows, rows), rows)
        return pltpu.make_async_copy(ht_v.at[lax.rem(i, 2)], ht_ref.at[:, at], ht_sems.at[lax.rem(i, 2)])

    block_load(h_all, 0, 0).start()

    @pl.loop(0, n_blocks)
    def _(i):
        slot = lax.rem(i, 2)
        block_load(h_all, i, slot).wait()

        @pl.when(i + 1 < n_blocks)
        def _():
            block_load(h_all, i + 1, 1 - slot).start()

        @pl.when(i >= 2)
        def _():
            ht_store(i - 2).wait()

        ht_v[slot] = blk[slot].T
        ht_store(i).start()
        prod = dot(blk[slot], w_v[...])
        cos_t, sin_t = cos_s[i], sin_s[i]
        for a in range(heads + 1):
            val = prod[:, a * HEAD_DIM:(a + 1) * HEAD_DIM]
            rot = (val * cos_t + pltpu.roll(val, HALF, 1) * sin_t).astype(BF16)
            if a < heads:
                q_s[i, :, cols[a]] = rot
            else:
                k_s[i] = rot
                kt[i] = rot.T
        v_i = prod[:, q_cols + HEAD_DIM:].astype(BF16)
        v_s[i] = v_i
        vt[i] = v_i.T
        acc[...] = jnp.zeros_like(acc)
        start = tuple((jnp.full((1, rows), NEG_LARGE, F32), jnp.zeros((1, rows), F32)) for _ in range(heads))
        carry = lax.fori_loop(0, i, lambda c, carry: fwd_chunk(i, c, carry, False), start)
        carry = fwd_chunk(i, i, carry, True)
        at = pl.ds(pl.multiple_of(i * rows, rows), rows)
        for a in range(heads):
            m_a, l_a = carry[a]
            ot_s[cols[a], at] = (acc[a] / l_a).astype(BF16)
            lse_s[i, a:a + 1, :] = m_a + jnp.log2(l_a)

        @pl.when(i == FWD_MIDDLE)
        def _():
            gather_dy.middle()

        @pl.when(i == FWD_LATE)
        def _():
            gather_dy.late()

    for chunk in range(CHUNKS):
        gather_o.start(chunk)
    own_o = pltpu.make_async_copy(ot_s, gather_o.block(near.me, 0, CHUNKS), own_sems.at[0])
    own_o.start()

    def d_o_blocks(low, high):
        block_load(dy_all, near.across(low), 0).start()

        @pl.loop(low, high)
        def _(r):
            slot = lax.rem(r - low, 2)
            block_load(dy_all, 0, slot).wait()

            @pl.when(r + 1 < high)
            def _():
                block_load(dy_all, near.across(r + 1), 1 - slot).start()

            do_s[near.across(r)] = dot(blk[slot], wo_v[...], COLS_COLS).astype(BF16)

    stage_out.wait()
    gather_dy.end_near()
    d_o_blocks(0, n_blocks * 3 // 4)
    gather_dy.end_far()
    d_o_blocks(n_blocks * 3 // 4, n_blocks)

    def bwd_chunk(i, c, delta, diagonal):
        k_c, v_c, kt_c = k_s[c], v_s[c], kt[c]
        dk_c = dv_c = None
        for a in range(heads):
            q_a, do_a = q_s[i, :, cols[a]], do_s[i, :, cols[a]]
            s = dot(k_c, q_a, COLS_COLS) * to_log2
            if diagonal:
                s = masked(s)
            p = jnp.exp2(s - lse_s[i, a:a + 1, :])
            d_p = dot(v_c, do_a, COLS_COLS)
            d_s = (p * (d_p - delta[a])).astype(BF16)
            dv_a = dot(p.astype(BF16), do_a)
            dk_a = dot(d_s, q_a)
            dv_c = dv_a if dv_c is None else dv_c + dv_a
            dk_c = dk_a if dk_c is None else dk_c + dk_a
            acc[a] += dot(kt_c, d_s)
        if diagonal:
            dk_acc[c] = dk_c
            dv_acc[c] = dv_c
        else:
            dk_acc[c] += dk_c
            dv_acc[c] += dv_c

    def dq_stores(i):
        slot = lax.rem(i, 2)
        at = pl.ds(pl.multiple_of(i * rows, rows), rows)
        last = q_cols - HEAD_DIM
        return [pltpu.make_async_copy(dq_v.at[slot, :, pl.ds(0, last)], dq_a_ref.at[at, :], dq_sems.at[slot, 0]),
                pltpu.make_async_copy(dq_v.at[slot, :, pl.ds(last, HEAD_DIM)], dq_b_ref.at[at, :], dq_sems.at[slot, 1])]

    for i in (n_blocks - 2, n_blocks - 1):
        ht_store(i).wait()

    @pl.loop(0, n_blocks)
    def _(i):
        at = pl.ds(pl.multiple_of(i * rows, rows), rows)
        acc[...] = jnp.zeros_like(acc)
        delta = [jnp.sum(ot_s[cols[a], at].astype(F32) * do_s[i, :, cols[a]].T.astype(F32), axis=0, keepdims=True) for a in range(heads)]

        @pl.loop(0, i)
        def _(c):
            bwd_chunk(i, c, delta, False)

        bwd_chunk(i, i, delta, True)

        @pl.when(i >= 2)
        def _():
            for store in dq_stores(i - 2):
                store.wait()

        for a in range(heads):
            dq_v[lax.rem(i, 2), :, cols[a]] = unrotate(acc[a].T * qk_scale, cos_s[i], sin_s[i])
        for store in dq_stores(i):
            store.start()

        @pl.when(i == BWD_MIDDLE)
        def _():
            gather_o.middle()

        @pl.when(i == BWD_LATE)
        def _():
            gather_o.late()

    @pl.loop(0, n_blocks)
    def _(c):
        at = pl.ds(pl.multiple_of(c * rows, rows), rows)
        dkv_v[at, :HEAD_DIM] = unrotate(dk_acc[c] * qk_scale, cos_s[c], sin_s[c])
        dkv_v[at, HEAD_DIM:] = dv_acc[c].astype(BF16)

    dkv_store = pltpu.make_async_copy(dkv_v, dkv_ref, own_sems.at[1])
    dkv_store.start()
    own_o.wait()
    gather_o.end()
    for i in (n_blocks - 2, n_blocks - 1):
        for store in dq_stores(i):
            store.wait()
    dkv_store.wait()


def attention(x, gain, positions, grad_out, w_q, w_k, w_v, w_o, sp_size, heads):
    rows, width = x.shape
    seq_len = rows * sp_size
    q_cols = heads * HEAD_DIM
    any_spec = pl.BlockSpec(memory_space=pl.ANY)
    vmem = pl.BlockSpec(memory_space=pltpu.VMEM)
    dma = pltpu.SemaphoreType.DMA
    inv_freq = ROPE_THETA ** (-np.arange(0, HEAD_DIM, 2) / HEAD_DIM)
    freq = jnp.asarray(np.concatenate([inv_freq, inv_freq])[None, :], F32)
    pairs = heads * seq_len * (seq_len + rows) // 2
    out = lambda *shape: jax.ShapeDtypeStruct(shape, BF16)
    blocks = lambda *shape, dtype=BF16: pltpu.VMEM((sp_size,) + shape, dtype)
    return pl.pallas_call(
        functools.partial(attention_kernel, heads),
        in_specs=[any_spec, vmem, vmem, vmem] + [any_spec] * 5,
        out_specs=[any_spec] * 7,
        out_shape=[out(seq_len, width), out(seq_len, width), out(q_cols * sp_size, seq_len), out(width, seq_len), out(seq_len, 2 * HEAD_DIM),
                   out(seq_len, q_cols - HEAD_DIM), out(seq_len, HEAD_DIM)],
        scratch_shapes=[pltpu.VMEM((rows, width), BF16), pltpu.VMEM((rows, width), BF16), dma((CHUNKS,)), dma((3,)),
                        blocks(8, rows, dtype=jnp.int32), dma((2, 7)), blocks(rows, HEAD_DIM, dtype=F32), blocks(rows, HEAD_DIM, dtype=F32),
                        pltpu.VMEM((width, q_cols + 2 * HEAD_DIM), BF16), pltpu.VMEM((q_cols, width), BF16), dma((4,)),
                        pltpu.VMEM((2, rows, width), BF16), dma((2,)), pltpu.VMEM((2, width, rows), BF16), dma((2,)),
                        blocks(rows, q_cols), blocks(rows, HEAD_DIM), blocks(rows, HEAD_DIM), blocks(HEAD_DIM, rows), blocks(HEAD_DIM, rows),
                        pltpu.VMEM((q_cols, seq_len), BF16), blocks(8, rows, dtype=F32), pltpu.VMEM((heads, HEAD_DIM, rows), F32),
                        blocks(rows, q_cols), blocks(rows, HEAD_DIM, dtype=F32), blocks(rows, HEAD_DIM, dtype=F32),
                        pltpu.VMEM((2, rows, q_cols), BF16), dma((2, 2)), pltpu.VMEM((seq_len, 2 * HEAD_DIM), BF16), SEMS, SEMS, SEMS],
        compiler_params=pltpu.CompilerParams(vmem_limit_bytes=VMEM_LIMIT, collective_id=0, has_side_effects=True),
        cost_estimate=pl.CostEstimate(flops=28 * pairs * HEAD_DIM, bytes_accessed=20 * seq_len * width, transcendentals=2 * pairs),
        name="attention",
    )(x, gain.reshape(1, -1), positions.reshape(1, -1), freq, grad_out, w_q, w_k, w_v, w_o)


def lanes(*parts):
    return jnp.concatenate(parts, axis=1)


def products_kernel(heads, ot_ref, ht_ref, dy_ref, d_kv_ref, d_qa_ref, d_qb_ref, x_ref, own_dy_ref, gain_ref, wo_ref, wk_ref, wv_ref, wq_ref,
                    wo_out, wq_out, kv_all, qa_all, qb_all, res_ref, gx_ref, gg_ref,
                    a_buf, b_buf, tile, a_sem, b_sems, t_sems, x_sems, stage, stage_sems, ot_v, o_v, x_v, io_sems, own, own_sems, w_v, w_sems, acc,
                    gg_v, gg_all, gg_sems, kv_sems, qa_sems, qb_sems):
    near = Neighbours()
    core = lax.rem(near.me, 2)
    half = a_buf.shape[0]
    seq_len = d_kv_ref.shape[0]
    rows, width = x_ref.shape
    chunk = seq_len // CHUNKS
    n_cols = d_kv_ref.shape[1]
    n_o, n_all = width // (2 * n_cols), x_sems.shape[1]
    n_oa = n_o + (n_all - n_o) * 2 // 3

    def gather_of(src, dst, sems):
        return Gather(near, lambda c: src.at[pl.ds(c * chunk, chunk), :], dst, seq_len, sems)

    local = (d_qa_ref, d_qb_ref, d_kv_ref)
    gathers = [gather_of(d_qa_ref, qa_all, qa_sems), gather_of(d_qb_ref, qb_all, qb_sems), gather_of(d_kv_ref, kv_all, kv_sems)]

    def stage_in(n):
        return pltpu.make_async_copy(local[n], stage.at[:, pl.ds(0, local[n].shape[1])], stage_sems.at[0])

    def stage_out(n):
        return pltpu.make_async_copy(stage.at[:, pl.ds(0, local[n].shape[1])], gathers[n].block(near.me, 0, CHUNKS), stage_sems.at[1])

    def copy_own(n):
        stage_in(n).wait()
        stage_out(n).start()

    own_rows = pl.ds(pl.multiple_of(core * half, half), half)
    tokens = pl.ds(pl.multiple_of(near.me * rows, rows), rows)
    ot_load = pltpu.make_async_copy(ot_ref.at[:, tokens], ot_v, io_sems.at[0])
    x_load = pltpu.make_async_copy(x_ref, x_v, io_sems.at[1])
    res_store = pltpu.make_async_copy(x_v, res_ref, io_sems.at[2])
    dy_load = pltpu.make_async_copy(own_dy_ref, o_v, io_sems.at[3])
    gx_store = pltpu.make_async_copy(o_v, gx_ref, io_sems.at[0])

    def a_load(ref):
        return pltpu.make_async_copy(ref.at[own_rows, :], a_buf, a_sem)

    def b_loads(source, p, slot, g):
        if source is dy_ref:
            srcs = [dy_ref.at[:, pl.ds(pl.multiple_of((2 * p + g) * n_cols, n_cols), n_cols)]]
        else:
            per = n_cols // source.shape[1]
            srcs = [source.at[pl.ds(pl.multiple_of(((2 * p + g) * per + n) * seq_len, seq_len), seq_len), :] for n in range(per)]
        return [pltpu.make_async_copy(src, b_buf.at[slot, :, pl.ds(g * n_cols + n * src.shape[1], src.shape[1])], b_sems.at[slot, g])
                for n, src in enumerate(srcs)]

    def start_b(step):
        slot = lax.rem(step, 2)
        for source, low, high in ((dy_ref, 0, n_o), (qa_all, n_o, n_oa), (qb_all, n_oa, n_all)):
            @pl.when(jnp.logical_and(step >= low, step < high))
            def _():
                for g in range(2):
                    for load in b_loads(source, step - low, slot, g):
                        load.start()

    def pieces(kind, step):
        wide = (2 * n_cols, n_cols, HEAD_DIM)[kind]
        slot = lax.rem(step, 2)
        out = []
        for n in range(2 * n_cols // wide):
            group = (step - (0, n_o, n_oa)[kind]) * (2 * n_cols // wide) + n
            col = (group * wide, group * heads * HEAD_DIM, (group + 1) * heads * HEAD_DIM - HEAD_DIM)[kind]
            dst = (wo_out, wq_out, wq_out)[kind].at[own_rows, pl.ds(pl.multiple_of(col, HEAD_DIM), wide)]
            src = tile.at[slot, :, pl.ds(n * wide, wide)]
            out.append((pltpu.make_async_copy(src, dst, t_sems.at[slot]), send(src, dst, x_sems, step, near.sib)))
        return out

    def start_tile(step):
        for kind, (low, high) in enumerate(((0, n_o), (n_o, n_oa), (n_oa, n_all))):
            @pl.when(jnp.logical_and(step >= low, step < high))
            def _():
                for keep, give in pieces(kind, step):
                    keep.start()
                    give.start()

    def whole_tile(step):
        slot = lax.rem(step, 2)
        dst = wo_out.at[own_rows, pl.ds(0, 2 * n_cols)]
        return pltpu.make_async_copy(tile.at[slot], dst, t_sems.at[slot]), send(tile.at[slot], dst, x_sems, step, near.sib)

    def wait_tile(step):
        keep, give = whole_tile(step)
        keep.wait()
        give.wait_send()

    def result_part():
        cols = b_buf.shape[2]

        def w_load(n):
            slot = lax.rem(n, 2)
            return pltpu.make_async_copy(wo_ref.at[:, pl.ds(pl.multiple_of(n * cols, cols), cols)], b_buf.at[slot, pl.ds(0, wo_ref.shape[0]), :],
                                         b_sems.at[slot, 0])

        w_load(jnp.int32(0)).start()
        ot_load.wait()

        @pl.loop(0, ot_v.shape[0] // BLK)
        def _(r):
            at = pl.ds(pl.multiple_of(r * BLK, BLK), BLK)
            o_v[:, at] = ot_v[at, :].T

        x_load.wait()

        @pl.loop(0, n_o)
        def _(n):
            w_load(n).wait()

            @pl.when(n + 1 < n_o)
            def _():
                w_load(n + 1).start()

            at = pl.ds(pl.multiple_of(n * cols, cols), cols)
            x_v[:, at] = (x_v[:, at].astype(F32) + dot(o_v[...], b_buf[lax.rem(n, 2), :wo_ref.shape[0], :])).astype(BF16)

        res_store.start()

    def hidden_parts(kind):
        count = own.shape[0] // (2 if kind == 1 else 1)

        def own_load(r, g):
            source = (qa_all, qb_all, kv_all)[kind]
            device, col = (2 * r + g, 0) if kind == 1 else (near.across(r), g * HEAD_DIM)
            at = pl.ds(pl.multiple_of(device * seq_len + near.me * rows, rows), rows)
            return pltpu.make_async_copy(source.at[at, pl.ds(col, HEAD_DIM)], own.at[r, :, pl.ds(g * HEAD_DIM, HEAD_DIM)], own_sems.at[r, g])

        def w_load(r, g):
            source = (wk_ref, wv_ref)[g] if kind == 2 else wq_ref
            col = near.across(r) if kind == 2 else heads * near.across(r) + g if kind == 0 else heads * (2 * r + g + 1) - 1
            slot = lax.rem(r, 2)
            return pltpu.make_async_copy(source.at[:, pl.ds(pl.multiple_of(col * HEAD_DIM, HEAD_DIM), HEAD_DIM)],
                                         w_v.at[slot, :, pl.ds(g * HEAD_DIM, HEAD_DIM)], w_sems.at[slot, g])

        return count, own_load, w_load

    def hidden_start(kind, low=0, high=None):
        count, own_load, w_load = hidden_parts(kind)
        for g in range(2):
            if low == 0:
                w_load(jnp.int32(0), g).start()

            @pl.loop(low, high or count)
            def _(r):
                own_load(r, g).start()

    def hidden_add(kind, low=0, high=None):
        count, own_load, w_load = hidden_parts(kind)

        @pl.loop(low, high or count)
        def _(r):
            for g in range(2):
                w_load(r, g).wait()
                own_load(r, g).wait()

            @pl.when(r + 1 < count)
            def _():
                for g in range(2):
                    w_load(r + 1, g).start()

            prod = dot(own[r], w_v[lax.rem(r, 2)], COLS_COLS)
            if kind == 0:
                @pl.when(r == 0)
                def _():
                    acc[...] = prod

                @pl.when(r > 0)
                def _():
                    acc[...] += prod
            else:
                acc[...] += prod

    others = near.others()
    near.meet(others)
    for c in range(CHUNKS):
        gathers[0].start(c)
    a_load(ot_ref).start()
    start_b(jnp.int32(0))
    stage_in(0).start()
    ot_load.start()
    x_load.start()
    a_load(ot_ref).wait()

    @pl.loop(0, n_all)
    def _(step):
        slot = lax.rem(step, 2)
        for g in range(2):
            b_loads(dy_ref, 0, slot, g)[0].wait()

        @pl.when(jnp.logical_and(step != n_o - 1, step != n_oa - 1))
        def _():
            start_b(step + 1)

        @pl.when(step >= 2)
        def _():
            wait_tile(step - 2)

        @pl.when(step == n_o)
        def _():
            a_load(ht_ref).wait()

        tile[slot] = dot(a_buf[...], b_buf[slot])
        start_tile(step)

        @pl.when(step == n_o - 2)
        def _():
            copy_own(0)
            gathers[0].middle()

        @pl.when(step == n_o - 1)
        def _():
            a_load(ht_ref).start()
            gathers[0].late()
            for c in range(CHUNKS):
                gathers[1].start(c)
            stage_out(0).wait()
            stage_in(1).start()
            result_part()
            gathers[0].end()
            start_b(step + 1)
            hidden_start(0)

        @pl.when(step == n_oa - 3)
        def _():
            copy_own(1)
            gathers[1].middle()

        @pl.when(step == n_oa - 2)
        def _():
            gathers[1].late()
            for c in range(CHUNKS):
                gathers[2].start(c)
            stage_out(1).wait()
            stage_in(2).start()

        @pl.when(step == n_oa - 1)
        def _():
            res_store.wait()
            x_load.start()
            dy_load.start()
            gathers[1].end()
            start_b(step + 1)
            hidden_add(0)
            hidden_start(1)

    hidden_add(1)
    copy_own(2)
    gathers[2].middle()
    gathers[2].late()
    stage_out(2).wait()
    gathers[2].end_near()
    near_count = own.shape[0] * 3 // 4
    hidden_start(2, 0, near_count)
    for step in (n_all - 2, n_all - 1):
        wait_tile(jnp.int32(step))
    hidden_add(2, 0, near_count)
    gathers[2].end_far()
    hidden_start(2, near_count)
    hidden_add(2, near_count)

    gain = gain_ref[...].astype(F32)
    gg_v[...] = jnp.zeros_like(gg_v)
    x_load.wait()
    dy_load.wait()

    @pl.loop(0, rows // 32)
    def _(r):
        at = pl.ds(pl.multiple_of(r * 32, 32), 32)
        x_f = x_v[at, :].astype(F32)
        inv_rms = lax.rsqrt(jnp.mean(x_f * x_f, axis=-1, keepdims=True) + NORM_EPS)
        normed = x_f * inv_rms
        d_hid = acc[at, :]
        both = d_hid * normed
        gg_v[...] += jnp.sum(both.reshape(4, 8, width), axis=0)
        mean = jnp.mean(both * gain, axis=-1, keepdims=True)
        o_v[at, :] = (o_v[at, :].astype(F32) + inv_rms * (d_hid * gain - normed * mean)).astype(BF16)

    gg_all[near.me] = gg_v[...]
    parts = [send(gg_v, gg_all.at[near.me], gg_sems, r, peer) for r, peer in enumerate(others)]
    for copy in parts:
        copy.start()
    gx_store.start()

    @pl.loop(0, n_all)
    def _(step):
        whole_tile(step)[1].wait_recv()

    for copy in parts:
        copy.wait()
    gg_ref[...] = jnp.sum(jnp.sum(gg_all[...], axis=0), axis=0, keepdims=True)
    gx_store.wait()


def products(ot_all, ht, d_out, d_kv, d_qa, d_qb, x, grad_out, gain, w_o, w_k, w_v, w_q, sp_size, heads):
    width, seq_len = ht.shape
    half = width // 2
    cols = 2 * d_kv.shape[1]
    n_all = width // cols + sp_size * (d_qa.shape[1] + d_qb.shape[1]) // cols
    any_spec = pl.BlockSpec(memory_space=pl.ANY)
    vmem = pl.BlockSpec(memory_space=pltpu.VMEM)
    dma = pltpu.SemaphoreType.DMA
    gathered = [jax.ShapeDtypeStruct((sp_size * seq_len, d.shape[1]), BF16) for d in (d_kv, d_qa, d_qb)]
    return pl.pallas_call(
        functools.partial(products_kernel, heads),
        in_specs=[any_spec] * 8 + [vmem] + [any_spec] * 4,
        out_specs=[any_spec] * 7 + [vmem],
        out_shape=[jax.ShapeDtypeStruct((ot_all.shape[0], width), F32), jax.ShapeDtypeStruct(w_q.shape, F32)] + gathered
        + [jax.ShapeDtypeStruct(x.shape, BF16), jax.ShapeDtypeStruct(x.shape, BF16), jax.ShapeDtypeStruct((1, width), F32)],
        scratch_shapes=[pltpu.VMEM((half, seq_len), BF16), pltpu.VMEM((2, seq_len, cols), BF16), pltpu.VMEM((2, half, cols), F32),
                        dma, dma((2, 2)), dma((2,)), dma((2, n_all)), pltpu.VMEM(d_kv.shape, BF16), dma((2,)),
                        pltpu.VMEM((ot_all.shape[0], x.shape[0]), BF16), pltpu.VMEM((x.shape[0], ot_all.shape[0]), BF16), pltpu.VMEM(x.shape, BF16),
                        dma((4,)), pltpu.VMEM((sp_size, x.shape[0], 2 * HEAD_DIM), BF16), dma((sp_size, 2)),
                        pltpu.VMEM((2, width, 2 * HEAD_DIM), BF16), dma((2, 2)), pltpu.VMEM(x.shape, F32),
                        pltpu.VMEM((8, width), F32), pltpu.VMEM((sp_size, 8, width), F32), dma((2, 7)), SEMS, SEMS, SEMS],
        compiler_params=pltpu.CompilerParams(vmem_limit_bytes=VMEM_LIMIT, collective_id=1, has_side_effects=True),
        cost_estimate=pl.CostEstimate(flops=2 * half * cols * seq_len * n_all, bytes_accessed=8 * half * cols * n_all, transcendentals=0),
        name="products",
    )(ot_all, ht, d_out, d_kv, d_qa, d_qb, x, grad_out, gain, w_o, w_k, w_v, w_q)


def finish_kernel(ht_ref, d_ref, gx_in, res_in, gg_in, wo_in, wq_in, wk_ref, wv_ref, wq_ref, wo_ref, gx_ref, res_ref, gg_ref, d_v, d_sems, ring, ring_sems):
    step = pl.program_id(0) * pl.num_programs(1) + pl.program_id(1)
    high = ring.shape[2]
    every = [(src, dst, r) for src, dst in ((wo_in, wo_ref), (wq_in, wq_ref)) for r in range(src.shape[0] // high)]
    groups = [every[g:g + RING] for g in range(0, len(every), RING)]

    def ins(g):
        return [pltpu.make_async_copy(src.at[pl.ds(r * high, high), :], ring.at[g % DEPTH, n], ring_sems.at[0, g % DEPTH, n])
                for n, (src, dst, r) in enumerate(groups[g])]

    def outs(g):
        return [pltpu.make_async_copy(ring.at[g % DEPTH, n], dst.at[pl.ds(r * high, high), :], ring_sems.at[1, g % DEPTH, n])
                for n, (src, dst, r) in enumerate(groups[g])]

    def pair_load(p):
        at = pl.ds(2 * p, 2)
        return pltpu.make_async_copy(d_ref.at[at], d_v.at[at], d_sems.at[p])

    @pl.when(step == 0)
    def _():
        for p in range(d_v.shape[0] // 2):
            pair_load(p).start()

    for g in range(len(groups) + DEPTH):
        @pl.when(step == g)
        def _():
            if g >= DEPTH:
                for copy in outs(g - DEPTH):
                    copy.wait()
            if g < len(groups):
                for copy in ins(g):
                    copy.start()
            if 2 <= g < len(groups) + 2:
                for copy in ins(g - 2):
                    copy.wait()
                for copy in outs(g - 2):
                    copy.start()

    for p in range(d_v.shape[0] // 2):
        @pl.when(step == p)
        def _():
            pair_load(p).wait()

    ht = ht_ref[...]
    pair = 2 * pl.program_id(1)
    wk_ref[...] = dot(ht, lanes(d_v[pair, :, :HEAD_DIM], d_v[pair + 1, :, :HEAD_DIM]))
    wv_ref[...] = dot(ht, lanes(d_v[pair, :, HEAD_DIM:], d_v[pair + 1, :, HEAD_DIM:]))

    @pl.when(step == 0)
    def _():
        gg_ref[...] = gg_in[...]

    @pl.when(step < ROW_STEPS)
    def _():
        gx_ref[...] = gx_in[...]
        res_ref[...] = res_in[...]


def finish(ht, d_kv, w_o_grad, w_q_grad, grad_x, result, grad_gain):
    width, seq_len = ht.shape
    groups = d_kv.shape[0]
    n_j = groups // 2
    steps = (width // MROWS) * n_j
    high = width // COPY_ROWS
    assert -(-(w_o_grad.shape[0] + w_q_grad.shape[0]) // (high * RING)) + DEPTH <= steps
    any_spec = pl.BlockSpec(memory_space=pl.ANY)
    rows = pl.BlockSpec((grad_x.shape[0] // ROW_STEPS, width), lambda m, j: (jnp.minimum(m * n_j + j, ROW_STEPS - 1), 0))
    whole = pl.BlockSpec((1, width), lambda m, j: (0, 0))
    kv_out = pl.BlockSpec((MROWS, 2 * HEAD_DIM), lambda m, j: (m, j))
    out = lambda cols: jax.ShapeDtypeStruct((width, cols), F32)
    like = lambda val: jax.ShapeDtypeStruct(val.shape, val.dtype)
    return pl.pallas_call(
        finish_kernel,
        grid=(width // MROWS, n_j),
        in_specs=[pl.BlockSpec((MROWS, seq_len), lambda m, j: (m, 0)), any_spec, rows, rows, whole, any_spec, any_spec],
        out_specs=[kv_out, kv_out, any_spec, any_spec, rows, rows, whole],
        out_shape=[out(groups * HEAD_DIM), out(groups * HEAD_DIM), like(w_q_grad), like(w_o_grad), like(grad_x), like(result), like(grad_gain)],
        scratch_shapes=[pltpu.VMEM(d_kv.shape, BF16), pltpu.SemaphoreType.DMA((groups // 2,)),
                        pltpu.VMEM((DEPTH, RING, high, width), F32), pltpu.SemaphoreType.DMA((2, DEPTH, RING))],
        compiler_params=params(2),
        cost_estimate=pl.CostEstimate(flops=4 * width * seq_len * groups * HEAD_DIM, bytes_accessed=2 * width * seq_len, transcendentals=0),
        name="finish",
    )(ht, d_kv, grad_x, result, grad_gain, w_o_grad, w_q_grad)


def solution(mesh):
    sp_size = mesh.shape['sp']
    seq_spec = P(('dp', 'sp'), None)
    pos_spec = P(('dp', 'sp'))
    replicated = P(None, None)
    part_rows = P('dp', None)

    def local_step(x, grad_out, positions, gain, w_q, w_k, w_v, w_o):
        n_heads = w_q.shape[1] // HEAD_DIM
        heads = n_heads // sp_size
        _, d_out, ot_all, ht, *grads = attention(x, gain, positions, grad_out, w_q, w_k, w_v, w_o, sp_size, heads)
        gain = gain.reshape(1, -1)
        w_o_grad, w_q_grad, kv_all, _, _, result, grad_x, grad_gain = products(ot_all, ht, d_out, *grads, x, grad_out, gain, w_o, w_k, w_v, w_q,
                                                                               sp_size, heads)
        grad_wk, grad_wv, grad_wq, grad_wo, grad_x, result, grad_gain = finish(
            ht, kv_all.reshape(sp_size, -1, 2 * HEAD_DIM), w_o_grad, w_q_grad, grad_x, result, grad_gain)
        return result, grad_x, grad_wq, grad_wk, grad_wv, grad_wo, grad_gain.reshape(-1)

    return jax.shard_map(local_step, mesh=mesh,
                         in_specs=(seq_spec, seq_spec, pos_spec, P(None), replicated, replicated, replicated, replicated),
                         out_specs=(seq_spec, seq_spec, part_rows, part_rows, part_rows, part_rows, P('dp')),
                         check_vma=False)
```

```python
import functools

import jax
import jax.numpy as jnp
import numpy as np
from jax import lax
from jax.experimental import pallas as pl
from jax.experimental.pallas import tpu as pltpu
from jax.sharding import PartitionSpec as P

HEAD_DIM = 128
HALF = HEAD_DIM // 2
ROPE_THETA = 1000000.0
NORM_EPS = 1e-05
NEG_LARGE = -1e30
LOG2E = 1.4426950408889634
BLK = 512
CHUNKS = 4
FWD_MIDDLE, FWD_LATE, BWD_MIDDLE, BWD_LATE = 6, 7, 5, 6
MROWS = 768
RING = 4
DEPTH = 3
COPY_ROWS = 24
ROW_STEPS = 8
F32 = jnp.float32
BF16 = jnp.bfloat16
ROWS_ROWS = (((0,), (0,)), ((), ()))
COLS_COLS = (((1,), (1,)), ((), ()))
ROWS_COLS = (((0,), (1,)), ((), ()))
VMEM_LIMIT = 63 * 1024 * 1024


def dot(a, b, dims=(((1,), (0,)), ((), ()))):
    return lax.dot_general(a, b, dims, preferred_element_type=F32)


def params(axes=1):
    return pltpu.CompilerParams(dimension_semantics=("arbitrary",) * axes, vmem_limit_bytes=VMEM_LIMIT)


class Neighbours:
    def __init__(self):
        self.me = lax.axis_index('sp')
        core, col, row = lax.rem(self.me, 2), lax.rem(self.me // 2, 2), self.me // 4
        self.sib = self.me + 1 - 2 * core
        self.xn = self.me + 2 - 4 * col
        self.yn = self.me + 4 - 8 * row
        self.diag = self.xn + self.yn - self.me

    def meet(self, peers):
        barrier = pltpu.get_barrier_semaphore()
        for peer in peers:
            pl.semaphore_signal(barrier, inc=1, device_id={'sp': peer}, device_id_type=pl.DeviceIdType.MESH)
        pl.semaphore_wait(barrier, len(peers))

    def across(self, r):
        core, col, row = lax.rem(self.me, 2), lax.rem(self.me // 2, 2), self.me // 4
        return (self.me + lax.rem(r, 2) * (1 - 2 * core) + lax.rem(r // 2, 2) * (2 - 4 * col) + (r // 4) * (4 - 8 * row))

    def others(self):
        flip = lambda dev: dev + 1 - 2 * lax.rem(dev, 2)
        return [self.sib, self.xn, flip(self.xn), self.yn, flip(self.yn), self.diag, flip(self.diag)]


def send(src, dst, sems, index, peer):
    return pltpu.make_async_remote_copy(src_ref=src, dst_ref=dst, send_sem=sems.at[0, index], recv_sem=sems.at[1, index],
                                        device_id={'sp': peer}, device_id_type=pl.DeviceIdType.MESH)


class Gather:
    COPIES = 22

    def __init__(self, near, own, dst, rows, sems):
        self.near, self.own, self.dst, self.rows, self.sems = near, own, dst, rows, sems

    def block(self, dev, chunk, count=1):
        size = self.rows // CHUNKS
        return self.dst.at[pl.ds(pl.multiple_of(dev * self.rows + chunk * size, size), count * size), :]

    def first(self, chunk, kind):
        peer = (self.near.xn, self.near.yn, self.near.sib)[kind]
        return send(self.own(chunk), self.block(self.near.me, chunk), self.sems, kind * CHUNKS + chunk, peer)

    def onward(self, chunk):
        over_y = chunk < CHUNKS // 2
        rows = self.block(self.near.xn if over_y else self.near.yn, chunk)
        return send(rows, rows, self.sems, 12 + chunk, self.near.yn if over_y else self.near.xn)

    def share(self, kind):
        rows = self.block((self.near.xn, self.near.yn)[kind], 0, CHUNKS)
        return send(rows, rows, self.sems, 16 + kind, self.near.sib)

    def share_diag(self, chunk):
        rows = self.block(self.near.diag, chunk)
        return send(rows, rows, self.sems, 18 + chunk, self.near.sib)

    def begin(self):
        self.near.meet([self.near.sib, self.near.xn, self.near.yn])
        for chunk in range(CHUNKS):
            self.start(chunk)

    def start(self, chunk):
        for kind in range(3):
            self.first(chunk, kind).start()

    def middle(self):
        for chunk in (0, 1):
            self.first(chunk, 0).wait_recv()
            self.onward(chunk).start()
        self.first(2, 1).wait_recv()
        self.onward(2).start()

    def late(self):
        self.first(3, 1).wait_recv()
        self.onward(3).start()
        for chunk in (2, 3):
            self.first(chunk, 0).wait_recv()
        self.share(0).start()
        for chunk in (0, 1):
            self.first(chunk, 1).wait_recv()
        self.share(1).start()

    def end_near(self):
        for chunk in range(CHUNKS):
            self.first(chunk, 2).wait_recv()
        for kind in range(2):
            self.share(kind).wait_recv()

    def end_far(self):
        for chunk in (0, 2, 1, 3):
            self.onward(chunk).wait_recv()
            self.share_diag(chunk).start()
        for chunk in range(CHUNKS):
            for kind in range(3):
                self.first(chunk, kind).wait_send()
            self.onward(chunk).wait_send()
        for kind in range(2):
            self.share(kind).wait_send()
        for chunk in range(CHUNKS):
            self.share_diag(chunk).wait()

    def end(self):
        self.end_near()
        self.end_far()


SEMS = pltpu.SemaphoreType.DMA((2, Gather.COPIES))


def masked(scores):
    key = lax.broadcasted_iota(jnp.int32, scores.shape, 0)
    query = lax.broadcasted_iota(jnp.int32, scores.shape, 1)
    return jnp.where(key <= query, scores, NEG_LARGE)


def unrotate(val, cos_t, sin_t):
    return (val * cos_t - pltpu.roll(val, HALF, 1) * sin_t).astype(BF16)


def attention_kernel(heads, x_ref, gain_ref, pos_ref, freq_ref, dy_ref, wq_ref, wk_ref, wv_ref, wo_ref,
                     h_all, dy_all, o_all, ht_ref, dkv_ref, dq_a_ref, dq_b_ref,
                     x_v, h_v, x_sems, own_sems, pos_all, pos_sems, cos_s, sin_s, w_v, wo_v, w_sems, blk, blk_sems, ht_v, ht_sems,
                     q_s, k_s, v_s, vt, kt, ot_s, lse_s, acc, do_s, dk_acc, dv_acc, dq_v, dq_sems, dkv_v, h_sems, dy_sems, o_sems):
    near = Neighbours()
    rows, width = x_ref.shape
    n_blocks = k_s.shape[0]
    q_cols = heads * HEAD_DIM
    size = rows // CHUNKS
    qk_scale = HEAD_DIM ** -0.5
    to_log2 = qk_scale * LOG2E
    cols = [slice(a * HEAD_DIM, (a + 1) * HEAD_DIM) for a in range(heads)]
    part = lambda ref, chunk, count=size: ref.at[pl.ds(chunk * count, count), :]
    gather_h = Gather(near, lambda chunk: part(h_v, chunk), h_all, rows, h_sems)
    gather_dy = Gather(near, lambda chunk: part(dy_ref, chunk), dy_all, rows, dy_sems)
    gather_o = Gather(near, lambda chunk: part(ot_s, chunk, q_cols // CHUNKS), o_all, q_cols, o_sems)

    loads = [pltpu.make_async_copy(part(x_ref, chunk), part(x_v, chunk), x_sems.at[chunk]) for chunk in range(CHUNKS)]
    for load in loads:
        load.start()
    others = near.others()
    near.meet(others)
    pos_all[near.me] = jnp.broadcast_to(pos_ref[...], pos_all.shape[1:])
    positions = [send(pos_ref, pos_all.at[near.me, pl.ds(0, 1), :], pos_sems, r, peer) for r, peer in enumerate(others)]
    gain = gain_ref[...].astype(F32)
    for chunk in range(CHUNKS):
        loads[chunk].wait()

        @pl.loop(0, size // 32)
        def _(r):
            at = pl.ds(pl.multiple_of(chunk * size + r * 32, 32), 32)
            x_f = x_v[at, :].astype(F32)
            normed = x_f * lax.rsqrt(jnp.mean(x_f * x_f, axis=-1, keepdims=True) + NORM_EPS)
            h_v[at, :] = (normed * gain).astype(BF16)

        gather_h.start(chunk)
    for copy in positions:
        copy.start()
    own_h = pltpu.make_async_copy(h_v, gather_h.block(near.me, 0, CHUNKS), own_sems.at[0])
    own_h.start()
    w_loads, col = [], 0
    for n, (ref, count) in enumerate(((wq_ref, q_cols), (wk_ref, HEAD_DIM), (wv_ref, HEAD_DIM))):
        at = pl.ds(pl.multiple_of(near.me * count, HEAD_DIM), count)
        w_loads.append(pltpu.make_async_copy(ref.at[:, at], w_v.at[:, pl.ds(col, count)], w_sems.at[n]))
        col += count
    w_loads.append(pltpu.make_async_copy(wo_ref.at[pl.ds(pl.multiple_of(near.me * q_cols, q_cols), q_cols), :], wo_v, w_sems.at[3]))
    stage_in = pltpu.make_async_copy(dy_ref, x_v, own_sems.at[1])
    stage_out = pltpu.make_async_copy(x_v, gather_dy.block(near.me, 0, CHUNKS), own_sems.at[2])
    for load in w_loads + [stage_in]:
        load.start()
    for copy in positions:
        copy.wait()
    sign = jnp.where(lax.broadcasted_iota(jnp.int32, (1, HEAD_DIM), 1) < HALF, -1.0, 1.0)

    @pl.loop(0, n_blocks)
    def _(b):
        pos = jnp.broadcast_to(pos_all[b, 0:1, :].astype(F32), (HEAD_DIM, rows)).T
        angles = pos * freq_ref[...]
        cos_s[b] = jnp.cos(angles)
        sin_s[b] = jnp.sin(angles) * sign

    gather_h.middle()
    gather_h.late()
    for chunk in range(CHUNKS):
        gather_dy.start(chunk)
    for load in w_loads + [stage_in]:
        load.wait()
    stage_out.start()
    own_h.wait()
    gather_h.end()

    def block_load(ref, block, slot):
        return pltpu.make_async_copy(ref.at[pl.ds(pl.multiple_of(block * rows, rows), rows), :], blk.at[slot], blk_sems.at[slot])

    def fwd_chunk(i, c, carry, diagonal):
        k_c, vt_c = k_s[c], vt[c]
        scores = [dot(k_c, q_s[i, :, cols[a]], COLS_COLS) * to_log2 for a in range(heads)]
        out = []
        for a in range(heads):
            s = masked(scores[a]) if diagonal else scores[a]
            m_old, l_old = carry[a]
            m_new = jnp.maximum(m_old, jnp.max(s, axis=0, keepdims=True))
            alpha = jnp.exp2(m_old - m_new)
            p = jnp.exp2(s - m_new)
            l_new = l_old * alpha + jnp.sum(p, axis=0, keepdims=True)
            acc[a] = acc[a] * alpha + dot(vt_c, p.astype(BF16))
            out.append((m_new, l_new))
        return tuple(out)

    def ht_store(i):
        at = pl.ds(pl.multiple_of(i * rows, rows), rows)
        return pltpu.make_async_copy(ht_v.at[lax.rem(i, 2)], ht_ref.at[:, at], ht_sems.at[lax.rem(i, 2)])

    block_load(h_all, 0, 0).start()

    @pl.loop(0, n_blocks)
    def _(i):
        slot = lax.rem(i, 2)
        block_load(h_all, i, slot).wait()

        @pl.when(i + 1 < n_blocks)
        def _():
            block_load(h_all, i + 1, 1 - slot).start()

        @pl.when(i >= 2)
        def _():
            ht_store(i - 2).wait()

        ht_v[slot] = blk[slot].T
        ht_store(i).start()
        prod = dot(blk[slot], w_v[...])
        cos_t, sin_t = cos_s[i], sin_s[i]
        for a in range(heads + 1):
            val = prod[:, a * HEAD_DIM:(a + 1) * HEAD_DIM]
            rot = (val * cos_t + pltpu.roll(val, HALF, 1) * sin_t).astype(BF16)
            if a < heads:
                q_s[i, :, cols[a]] = rot
            else:
                k_s[i] = rot
                kt[i] = rot.T
        v_i = prod[:, q_cols + HEAD_DIM:].astype(BF16)
        v_s[i] = v_i
        vt[i] = v_i.T
        acc[...] = jnp.zeros_like(acc)
        start = tuple((jnp.full((1, rows), NEG_LARGE, F32), jnp.zeros((1, rows), F32)) for _ in range(heads))
        carry = lax.fori_loop(0, i, lambda c, carry: fwd_chunk(i, c, carry, False), start)
        carry = fwd_chunk(i, i, carry, True)
        at = pl.ds(pl.multiple_of(i * rows, rows), rows)
        for a in range(heads):
            m_a, l_a = carry[a]
            ot_s[cols[a], at] = (acc[a] / l_a).astype(BF16)
            lse_s[i, a:a + 1, :] = m_a + jnp.log2(l_a)

        @pl.when(i == FWD_MIDDLE)
        def _():
            gather_dy.middle()

        @pl.when(i == FWD_LATE)
        def _():
            gather_dy.late()

    for chunk in range(CHUNKS):
        gather_o.start(chunk)
    own_o = pltpu.make_async_copy(ot_s, gather_o.block(near.me, 0, CHUNKS), own_sems.at[0])
    own_o.start()

    def d_o_blocks(low, high):
        block_load(dy_all, near.across(low), 0).start()

        @pl.loop(low, high)
        def _(r):
            slot = lax.rem(r - low, 2)
            block_load(dy_all, 0, slot).wait()

            @pl.when(r + 1 < high)
            def _():
                block_load(dy_all, near.across(r + 1), 1 - slot).start()

            do_s[near.across(r)] = dot(blk[slot], wo_v[...], COLS_COLS).astype(BF16)

    stage_out.wait()
    gather_dy.end_near()
    d_o_blocks(0, n_blocks * 3 // 4)
    gather_dy.end_far()
    d_o_blocks(n_blocks * 3 // 4, n_blocks)

    def bwd_chunk(i, c, delta, diagonal):
        k_c, v_c, kt_c = k_s[c], v_s[c], kt[c]
        dk_c = dv_c = None
        for a in range(heads):
            q_a, do_a = q_s[i, :, cols[a]], do_s[i, :, cols[a]]
            s = dot(k_c, q_a, COLS_COLS) * to_log2
            if diagonal:
                s = masked(s)
            p = jnp.exp2(s - lse_s[i, a:a + 1, :])
            d_p = dot(v_c, do_a, COLS_COLS)
            d_s = (p * (d_p - delta[a])).astype(BF16)
            dv_a = dot(p.astype(BF16), do_a)
            dk_a = dot(d_s, q_a)
            dv_c = dv_a if dv_c is None else dv_c + dv_a
            dk_c = dk_a if dk_c is None else dk_c + dk_a
            acc[a] += dot(kt_c, d_s)
        if diagonal:
            dk_acc[c] = dk_c
            dv_acc[c] = dv_c
        else:
            dk_acc[c] += dk_c
            dv_acc[c] += dv_c

    def dq_stores(i):
        slot = lax.rem(i, 2)
        at = pl.ds(pl.multiple_of(i * rows, rows), rows)
        last = q_cols - HEAD_DIM
        return [pltpu.make_async_copy(dq_v.at[slot, :, pl.ds(0, last)], dq_a_ref.at[at, :], dq_sems.at[slot, 0]),
                pltpu.make_async_copy(dq_v.at[slot, :, pl.ds(last, HEAD_DIM)], dq_b_ref.at[at, :], dq_sems.at[slot, 1])]

    for i in (n_blocks - 2, n_blocks - 1):
        ht_store(i).wait()

    @pl.loop(0, n_blocks)
    def _(i):
        at = pl.ds(pl.multiple_of(i * rows, rows), rows)
        acc[...] = jnp.zeros_like(acc)
        delta = [jnp.sum(ot_s[cols[a], at].astype(F32) * do_s[i, :, cols[a]].T.astype(F32), axis=0, keepdims=True) for a in range(heads)]

        @pl.loop(0, i)
        def _(c):
            bwd_chunk(i, c, delta, False)

        bwd_chunk(i, i, delta, True)

        @pl.when(i >= 2)
        def _():
            for store in dq_stores(i - 2):
                store.wait()

        for a in range(heads):
            dq_v[lax.rem(i, 2), :, cols[a]] = unrotate(acc[a].T * qk_scale, cos_s[i], sin_s[i])
        for store in dq_stores(i):
            store.start()

        @pl.when(i == BWD_MIDDLE)
        def _():
            gather_o.middle()

        @pl.when(i == BWD_LATE)
        def _():
            gather_o.late()

    @pl.loop(0, n_blocks)
    def _(c):
        at = pl.ds(pl.multiple_of(c * rows, rows), rows)
        dkv_v[at, :HEAD_DIM] = unrotate(dk_acc[c] * qk_scale, cos_s[c], sin_s[c])
        dkv_v[at, HEAD_DIM:] = dv_acc[c].astype(BF16)

    dkv_store = pltpu.make_async_copy(dkv_v, dkv_ref, own_sems.at[1])
    dkv_store.start()
    own_o.wait()
    gather_o.end()
    for i in (n_blocks - 2, n_blocks - 1):
        for store in dq_stores(i):
            store.wait()
    dkv_store.wait()


def attention(x, gain, positions, grad_out, w_q, w_k, w_v, w_o, sp_size, heads):
    rows, width = x.shape
    seq_len = rows * sp_size
    q_cols = heads * HEAD_DIM
    any_spec = pl.BlockSpec(memory_space=pl.ANY)
    vmem = pl.BlockSpec(memory_space=pltpu.VMEM)
    dma = pltpu.SemaphoreType.DMA
    inv_freq = ROPE_THETA ** (-np.arange(0, HEAD_DIM, 2) / HEAD_DIM)
    freq = jnp.asarray(np.concatenate([inv_freq, inv_freq])[None, :], F32)
    pairs = heads * seq_len * (seq_len + rows) // 2
    out = lambda *shape: jax.ShapeDtypeStruct(shape, BF16)
    blocks = lambda *shape, dtype=BF16: pltpu.VMEM((sp_size,) + shape, dtype)
    return pl.pallas_call(
        functools.partial(attention_kernel, heads),
        in_specs=[any_spec, vmem, vmem, vmem] + [any_spec] * 5,
        out_specs=[any_spec] * 7,
        out_shape=[out(seq_len, width), out(seq_len, width), out(q_cols * sp_size, seq_len), out(width, seq_len), out(seq_len, 2 * HEAD_DIM),
                   out(seq_len, q_cols - HEAD_DIM), out(seq_len, HEAD_DIM)],
        scratch_shapes=[pltpu.VMEM((rows, width), BF16), pltpu.VMEM((rows, width), BF16), dma((CHUNKS,)), dma((3,)),
                        blocks(8, rows, dtype=jnp.int32), dma((2, 7)), blocks(rows, HEAD_DIM, dtype=F32), blocks(rows, HEAD_DIM, dtype=F32),
                        pltpu.VMEM((width, q_cols + 2 * HEAD_DIM), BF16), pltpu.VMEM((q_cols, width), BF16), dma((4,)),
                        pltpu.VMEM((2, rows, width), BF16), dma((2,)), pltpu.VMEM((2, width, rows), BF16), dma((2,)),
                        blocks(rows, q_cols), blocks(rows, HEAD_DIM), blocks(rows, HEAD_DIM), blocks(HEAD_DIM, rows), blocks(HEAD_DIM, rows),
                        pltpu.VMEM((q_cols, seq_len), BF16), blocks(8, rows, dtype=F32), pltpu.VMEM((heads, HEAD_DIM, rows), F32),
                        blocks(rows, q_cols), blocks(rows, HEAD_DIM, dtype=F32), blocks(rows, HEAD_DIM, dtype=F32),
                        pltpu.VMEM((2, rows, q_cols), BF16), dma((2, 2)), pltpu.VMEM((seq_len, 2 * HEAD_DIM), BF16), SEMS, SEMS, SEMS],
        compiler_params=pltpu.CompilerParams(vmem_limit_bytes=VMEM_LIMIT, collective_id=0, has_side_effects=True),
        cost_estimate=pl.CostEstimate(flops=28 * pairs * HEAD_DIM, bytes_accessed=20 * seq_len * width, transcendentals=2 * pairs),
        name="attention",
    )(x, gain.reshape(1, -1), positions.reshape(1, -1), freq, grad_out, w_q, w_k, w_v, w_o)


def lanes(*parts):
    return jnp.concatenate(parts, axis=1)


def products_kernel(heads, ot_ref, ht_ref, dy_ref, d_kv_ref, d_qa_ref, d_qb_ref, x_ref, own_dy_ref, gain_ref, wo_ref, wk_ref, wv_ref, wq_ref,
                    wo_out, wq_out, kv_all, qa_all, qb_all, res_ref, gx_ref, gg_ref,
                    a_buf, b_buf, tile, a_sem, b_sems, t_sems, x_sems, stage, stage_sems, ot_v, o_v, x_v, io_sems, own, own_sems, w_v, w_sems, acc,
                    gg_v, gg_row, gg_all, gg_sems, kv_sems, qa_sems, qb_sems):
    near = Neighbours()
    core = lax.rem(near.me, 2)
    half = a_buf.shape[0]
    seq_len = d_kv_ref.shape[0]
    rows, width = x_ref.shape
    chunk = seq_len // CHUNKS
    n_cols = d_kv_ref.shape[1]
    n_o, n_all = width // (2 * n_cols), x_sems.shape[1]
    n_oa = n_o + (n_all - n_o) * 2 // 3

    def gather_of(src, dst, sems):
        return Gather(near, lambda c: src.at[pl.ds(c * chunk, chunk), :], dst, seq_len, sems)

    local = (d_qa_ref, d_qb_ref, d_kv_ref)
    gathers = [gather_of(d_qa_ref, qa_all, qa_sems), gather_of(d_qb_ref, qb_all, qb_sems), gather_of(d_kv_ref, kv_all, kv_sems)]

    def stage_in(n):
        return pltpu.make_async_copy(local[n], stage.at[:, pl.ds(0, local[n].shape[1])], stage_sems.at[0])

    def stage_out(n):
        return pltpu.make_async_copy(stage.at[:, pl.ds(0, local[n].shape[1])], gathers[n].block(near.me, 0, CHUNKS), stage_sems.at[1])

    def copy_own(n):
        stage_in(n).wait()
        stage_out(n).start()

    own_rows = pl.ds(pl.multiple_of(core * half, half), half)
    tokens = pl.ds(pl.multiple_of(near.me * rows, rows), rows)
    ot_load = pltpu.make_async_copy(ot_ref.at[:, tokens], ot_v, io_sems.at[0])
    x_load = pltpu.make_async_copy(x_ref, x_v, io_sems.at[1])
    res_store = pltpu.make_async_copy(x_v, res_ref, io_sems.at[2])
    dy_load = pltpu.make_async_copy(own_dy_ref, o_v, io_sems.at[3])
    gx_store = pltpu.make_async_copy(o_v, gx_ref, io_sems.at[0])

    def a_load(ref):
        return pltpu.make_async_copy(ref.at[own_rows, :], a_buf, a_sem)

    def b_loads(source, p, slot, g):
        if source is dy_ref:
            srcs = [dy_ref.at[:, pl.ds(pl.multiple_of((2 * p + g) * n_cols, n_cols), n_cols)]]
        else:
            per = n_cols // source.shape[1]
            srcs = [source.at[pl.ds(pl.multiple_of(((2 * p + g) * per + n) * seq_len, seq_len), seq_len), :] for n in range(per)]
        return [pltpu.make_async_copy(src, b_buf.at[slot, :, pl.ds(g * n_cols + n * src.shape[1], src.shape[1])], b_sems.at[slot, g])
                for n, src in enumerate(srcs)]

    def start_b(step):
        slot = lax.rem(step, 2)
        for source, low, high in ((dy_ref, 0, n_o), (qa_all, n_o, n_oa), (qb_all, n_oa, n_all)):
            @pl.when(jnp.logical_and(step >= low, step < high))
            def _():
                for g in range(2):
                    for load in b_loads(source, step - low, slot, g):
                        load.start()

    def pieces(kind, step):
        wide = (2 * n_cols, n_cols, HEAD_DIM)[kind]
        slot = lax.rem(step, 2)
        out = []
        for n in range(2 * n_cols // wide):
            group = (step - (0, n_o, n_oa)[kind]) * (2 * n_cols // wide) + n
            col = (group * wide, group * heads * HEAD_DIM, (group + 1) * heads * HEAD_DIM - HEAD_DIM)[kind]
            dst = (wo_out, wq_out, wq_out)[kind].at[own_rows, pl.ds(pl.multiple_of(col, HEAD_DIM), wide)]
            src = tile.at[slot, :, pl.ds(n * wide, wide)]
            out.append((pltpu.make_async_copy(src, dst, t_sems.at[slot]), send(src, dst, x_sems, step, near.sib)))
        return out

    def start_tile(step):
        for kind, (low, high) in enumerate(((0, n_o), (n_o, n_oa), (n_oa, n_all))):
            @pl.when(jnp.logical_and(step >= low, step < high))
            def _():
                for keep, give in pieces(kind, step):
                    keep.start()
                    give.start()

    def whole_tile(step):
        slot = lax.rem(step, 2)
        dst = wo_out.at[own_rows, pl.ds(0, 2 * n_cols)]
        return pltpu.make_async_copy(tile.at[slot], dst, t_sems.at[slot]), send(tile.at[slot], dst, x_sems, step, near.sib)

    def wait_tile(step):
        keep, give = whole_tile(step)
        keep.wait()
        give.wait_send()

    def result_part():
        cols = b_buf.shape[2]

        def w_load(n):
            slot = lax.rem(n, 2)
            return pltpu.make_async_copy(wo_ref.at[:, pl.ds(pl.multiple_of(n * cols, cols), cols)], b_buf.at[slot, pl.ds(0, wo_ref.shape[0]), :],
                                         b_sems.at[slot, 0])

        w_load(jnp.int32(0)).start()
        ot_load.wait()

        @pl.loop(0, ot_v.shape[0] // BLK)
        def _(r):
            at = pl.ds(pl.multiple_of(r * BLK, BLK), BLK)
            o_v[:, at] = ot_v[at, :].T

        x_load.wait()

        @pl.loop(0, n_o)
        def _(n):
            w_load(n).wait()

            @pl.when(n + 1 < n_o)
            def _():
                w_load(n + 1).start()

            at = pl.ds(pl.multiple_of(n * cols, cols), cols)
            x_v[:, at] = (x_v[:, at].astype(F32) + dot(o_v[...], b_buf[lax.rem(n, 2), :wo_ref.shape[0], :])).astype(BF16)

        res_store.start()

    def hidden_parts(kind):
        count = own.shape[0] // (2 if kind == 1 else 1)

        def own_load(r, g):
            source = (qa_all, qb_all, kv_all)[kind]
            device, col = (2 * r + g, 0) if kind == 1 else (near.across(r), g * HEAD_DIM)
            at = pl.ds(pl.multiple_of(device * seq_len + near.me * rows, rows), rows)
            return pltpu.make_async_copy(source.at[at, pl.ds(col, HEAD_DIM)], own.at[r, :, pl.ds(g * HEAD_DIM, HEAD_DIM)], own_sems.at[r, g])

        def w_load(r, g):
            source = (wk_ref, wv_ref)[g] if kind == 2 else wq_ref
            col = near.across(r) if kind == 2 else heads * near.across(r) + g if kind == 0 else heads * (2 * r + g + 1) - 1
            slot = lax.rem(r, 2)
            return pltpu.make_async_copy(source.at[:, pl.ds(pl.multiple_of(col * HEAD_DIM, HEAD_DIM), HEAD_DIM)],
                                         w_v.at[slot, :, pl.ds(g * HEAD_DIM, HEAD_DIM)], w_sems.at[slot, g])

        return count, own_load, w_load

    def hidden_start(kind, low=0, high=None):
        count, own_load, w_load = hidden_parts(kind)
        for g in range(2):
            if low == 0:
                w_load(jnp.int32(0), g).start()

            @pl.loop(low, high or count)
            def _(r):
                own_load(r, g).start()

    def hidden_add(kind, low=0, high=None):
        count, own_load, w_load = hidden_parts(kind)

        @pl.loop(low, high or count)
        def _(r):
            for g in range(2):
                w_load(r, g).wait()
                own_load(r, g).wait()

            @pl.when(r + 1 < count)
            def _():
                for g in range(2):
                    w_load(r + 1, g).start()

            prod = dot(own[r], w_v[lax.rem(r, 2)], COLS_COLS)
            if kind == 0:
                @pl.when(r == 0)
                def _():
                    acc[...] = prod

                @pl.when(r > 0)
                def _():
                    acc[...] += prod
            else:
                acc[...] += prod

    others = near.others()
    near.meet(others)
    for c in range(CHUNKS):
        gathers[0].start(c)
    a_load(ot_ref).start()
    start_b(jnp.int32(0))
    stage_in(0).start()
    ot_load.start()
    x_load.start()
    a_load(ot_ref).wait()

    @pl.loop(0, n_all)
    def _(step):
        slot = lax.rem(step, 2)
        for g in range(2):
            b_loads(dy_ref, 0, slot, g)[0].wait()

        @pl.when(jnp.logical_and(step != n_o - 1, step != n_oa - 1))
        def _():
            start_b(step + 1)

        @pl.when(step >= 2)
        def _():
            wait_tile(step - 2)

        @pl.when(step == n_o)
        def _():
            a_load(ht_ref).wait()

        tile[slot] = dot(a_buf[...], b_buf[slot])
        start_tile(step)

        @pl.when(step == n_o - 2)
        def _():
            copy_own(0)
            gathers[0].middle()

        @pl.when(step == n_o - 1)
        def _():
            a_load(ht_ref).start()
            gathers[0].late()
            for c in range(CHUNKS):
                gathers[1].start(c)
            stage_out(0).wait()
            stage_in(1).start()
            result_part()
            gathers[0].end()
            start_b(step + 1)
            hidden_start(0)

        @pl.when(step == n_oa - 3)
        def _():
            copy_own(1)
            gathers[1].middle()

        @pl.when(step == n_oa - 2)
        def _():
            gathers[1].late()
            for c in range(CHUNKS):
                gathers[2].start(c)
            stage_out(1).wait()
            stage_in(2).start()

        @pl.when(step == n_oa - 1)
        def _():
            res_store.wait()
            x_load.start()
            dy_load.start()
            gathers[1].end()
            start_b(step + 1)
            hidden_add(0)
            hidden_start(1)

    hidden_add(1)
    copy_own(2)
    gathers[2].middle()
    gathers[2].late()
    stage_out(2).wait()
    gathers[2].end_near()
    near_count = own.shape[0] * 3 // 4
    hidden_start(2, 0, near_count)
    for step in (n_all - 2, n_all - 1):
        wait_tile(jnp.int32(step))
    hidden_add(2, 0, near_count)
    gathers[2].end_far()
    hidden_start(2, near_count)
    hidden_add(2, near_count)

    gain = gain_ref[...].astype(F32)
    gg_v[...] = jnp.zeros_like(gg_v)
    x_load.wait()
    dy_load.wait()

    @pl.loop(0, rows // 32)
    def _(r):
        at = pl.ds(pl.multiple_of(r * 32, 32), 32)
        x_f = x_v[at, :].astype(F32)
        inv_rms = lax.rsqrt(jnp.mean(x_f * x_f, axis=-1, keepdims=True) + NORM_EPS)
        normed = x_f * inv_rms
        d_hid = acc[at, :]
        both = d_hid * normed
        gg_v[...] += jnp.sum(both.reshape(4, 8, width), axis=0)
        mean = jnp.mean(both * gain, axis=-1, keepdims=True)
        o_v[at, :] = (o_v[at, :].astype(F32) + inv_rms * (d_hid * gain - normed * mean)).astype(BF16)

    gg_row[...] = jnp.sum(gg_v[...], axis=0, keepdims=True)
    gg_all[near.me] = gg_row[...]
    parts = [send(gg_row, gg_all.at[near.me], gg_sems, r, peer) for r, peer in enumerate(others)]
    for copy in parts:
        copy.start()
    gx_store.start()

    @pl.loop(0, n_all)
    def _(step):
        whole_tile(step)[1].wait_recv()

    for copy in parts:
        copy.wait()
    gg_ref[...] = jnp.sum(gg_all[...], axis=0)
    gx_store.wait()


def products(ot_all, ht, d_out, d_kv, d_qa, d_qb, x, grad_out, gain, w_o, w_k, w_v, w_q, sp_size, heads):
    width, seq_len = ht.shape
    half = width // 2
    cols = 2 * d_kv.shape[1]
    n_all = width // cols + sp_size * (d_qa.shape[1] + d_qb.shape[1]) // cols
    any_spec = pl.BlockSpec(memory_space=pl.ANY)
    vmem = pl.BlockSpec(memory_space=pltpu.VMEM)
    dma = pltpu.SemaphoreType.DMA
    gathered = [jax.ShapeDtypeStruct((sp_size * seq_len, d.shape[1]), BF16) for d in (d_kv, d_qa, d_qb)]
    return pl.pallas_call(
        functools.partial(products_kernel, heads),
        in_specs=[any_spec] * 8 + [vmem] + [any_spec] * 4,
        out_specs=[any_spec] * 7 + [vmem],
        out_shape=[jax.ShapeDtypeStruct((ot_all.shape[0], width), F32), jax.ShapeDtypeStruct(w_q.shape, F32)] + gathered
        + [jax.ShapeDtypeStruct(x.shape, BF16), jax.ShapeDtypeStruct(x.shape, BF16), jax.ShapeDtypeStruct((1, width), F32)],
        scratch_shapes=[pltpu.VMEM((half, seq_len), BF16), pltpu.VMEM((2, seq_len, cols), BF16), pltpu.VMEM((2, half, cols), F32),
                        dma, dma((2, 2)), dma((2,)), dma((2, n_all)), pltpu.VMEM(d_kv.shape, BF16), dma((2,)),
                        pltpu.VMEM((ot_all.shape[0], x.shape[0]), BF16), pltpu.VMEM((x.shape[0], ot_all.shape[0]), BF16), pltpu.VMEM(x.shape, BF16),
                        dma((4,)), pltpu.VMEM((sp_size, x.shape[0], 2 * HEAD_DIM), BF16), dma((sp_size, 2)),
                        pltpu.VMEM((2, width, 2 * HEAD_DIM), BF16), dma((2, 2)), pltpu.VMEM(x.shape, F32),
                        pltpu.VMEM((8, width), F32), pltpu.VMEM((1, width), F32), pltpu.VMEM((sp_size, 1, width), F32), dma((2, 7)), SEMS, SEMS, SEMS],
        compiler_params=pltpu.CompilerParams(vmem_limit_bytes=VMEM_LIMIT, collective_id=1, has_side_effects=True),
        cost_estimate=pl.CostEstimate(flops=2 * half * cols * seq_len * n_all, bytes_accessed=8 * half * cols * n_all, transcendentals=0),
        name="products",
    )(ot_all, ht, d_out, d_kv, d_qa, d_qb, x, grad_out, gain, w_o, w_k, w_v, w_q)


def finish_kernel(ht_ref, d_ref, gx_in, res_in, gg_in, wo_in, wq_in, wk_ref, wv_ref, wq_ref, wo_ref, gx_ref, res_ref, gg_ref, d_v, d_sems, ring, ring_sems):
    step = pl.program_id(0) * pl.num_programs(1) + pl.program_id(1)
    high = ring.shape[2]
    per_array = wo_in.shape[0] // (high * RING)
    count = 2 * per_array

    def copy_in(src, g, n):
        at = pl.ds(pl.multiple_of((lax.rem(g, per_array) * RING + n) * high, high), high)
        return pltpu.make_async_copy(src.at[at, :], ring.at[lax.rem(g, DEPTH), n], ring_sems.at[0, lax.rem(g, DEPTH), n])

    def copy_out(dst, g, n):
        at = pl.ds(pl.multiple_of((lax.rem(g, per_array) * RING + n) * high, high), high)
        return pltpu.make_async_copy(ring.at[lax.rem(g, DEPTH), n], dst.at[at, :], ring_sems.at[1, lax.rem(g, DEPTH), n])

    def start(copy, first, second, g):
        for ref, mine in ((first, g < per_array), (second, g >= per_array)):
            @pl.when(mine)
            def _():
                for n in range(RING):
                    copy(ref, g, n).start()

    def pair_load(p):
        at = pl.ds(2 * p, 2)
        return pltpu.make_async_copy(d_ref.at[at], d_v.at[at], d_sems.at[p])

    @pl.when(step == 0)
    def _():
        for p in range(d_v.shape[0] // 2):
            pair_load(p).start()

    @pl.when(jnp.logical_and(step >= DEPTH, step < count + DEPTH))
    def _():
        for n in range(RING):
            copy_out(wo_ref, step - DEPTH, n).wait()

    @pl.when(step < count)
    def _():
        start(copy_in, wo_in, wq_in, step)

    @pl.when(jnp.logical_and(step >= 1, step < count + 1))
    def _():
        for n in range(RING):
            copy_in(wo_in, step - 1, n).wait()
        start(copy_out, wo_ref, wq_ref, step - 1)

    for p in range(d_v.shape[0] // 2):
        @pl.when(step == p)
        def _():
            pair_load(p).wait()

    ht = ht_ref[...]
    pair = 2 * pl.program_id(1)
    wk_ref[...] = dot(ht, lanes(d_v[pair, :, :HEAD_DIM], d_v[pair + 1, :, :HEAD_DIM]))
    wv_ref[...] = dot(ht, lanes(d_v[pair, :, HEAD_DIM:], d_v[pair + 1, :, HEAD_DIM:]))

    @pl.when(step == 0)
    def _():
        gg_ref[...] = gg_in[...]

    @pl.when(step < ROW_STEPS)
    def _():
        gx_ref[...] = gx_in[...]
        res_ref[...] = res_in[...]


def finish(ht, d_kv, w_o_grad, w_q_grad, grad_x, result, grad_gain):
    width, seq_len = ht.shape
    groups = d_kv.shape[0]
    n_j = groups // 2
    steps = (width // MROWS) * n_j
    high = width // COPY_ROWS
    assert -(-(w_o_grad.shape[0] + w_q_grad.shape[0]) // (high * RING)) + DEPTH <= steps
    any_spec = pl.BlockSpec(memory_space=pl.ANY)
    rows = pl.BlockSpec((grad_x.shape[0] // ROW_STEPS, width), lambda m, j: (jnp.minimum(m * n_j + j, ROW_STEPS - 1), 0))
    whole = pl.BlockSpec((1, width), lambda m, j: (0, 0))
    kv_out = pl.BlockSpec((MROWS, 2 * HEAD_DIM), lambda m, j: (m, j))
    out = lambda cols: jax.ShapeDtypeStruct((width, cols), F32)
    like = lambda val: jax.ShapeDtypeStruct(val.shape, val.dtype)
    return pl.pallas_call(
        finish_kernel,
        grid=(width // MROWS, n_j),
        in_specs=[pl.BlockSpec((MROWS, seq_len), lambda m, j: (m, 0)), any_spec, rows, rows, whole, any_spec, any_spec],
        out_specs=[kv_out, kv_out, any_spec, any_spec, rows, rows, whole],
        out_shape=[out(groups * HEAD_DIM), out(groups * HEAD_DIM), like(w_q_grad), like(w_o_grad), like(grad_x), like(result), like(grad_gain)],
        scratch_shapes=[pltpu.VMEM(d_kv.shape, BF16), pltpu.SemaphoreType.DMA((groups // 2,)),
                        pltpu.VMEM((DEPTH, RING, high, width), F32), pltpu.SemaphoreType.DMA((2, DEPTH, RING))],
        compiler_params=params(2),
        cost_estimate=pl.CostEstimate(flops=4 * width * seq_len * groups * HEAD_DIM, bytes_accessed=2 * width * seq_len, transcendentals=0),
        name="finish",
    )(ht, d_kv, grad_x, result, grad_gain, w_o_grad, w_q_grad)


def solution(mesh):
    sp_size = mesh.shape['sp']
    seq_spec = P(('dp', 'sp'), None)
    pos_spec = P(('dp', 'sp'))
    replicated = P(None, None)
    part_rows = P('dp', None)

    def local_step(x, grad_out, positions, gain, w_q, w_k, w_v, w_o):
        n_heads = w_q.shape[1] // HEAD_DIM
        heads = n_heads // sp_size
        _, d_out, ot_all, ht, *grads = attention(x, gain, positions, grad_out, w_q, w_k, w_v, w_o, sp_size, heads)
        gain = gain.reshape(1, -1)
        w_o_grad, w_q_grad, kv_all, _, _, result, grad_x, grad_gain = products(ot_all, ht, d_out, *grads, x, grad_out, gain, w_o, w_k, w_v, w_q,
                                                                               sp_size, heads)
        grad_wk, grad_wv, grad_wq, grad_wo, grad_x, result, grad_gain = finish(
            ht, kv_all.reshape(sp_size, -1, 2 * HEAD_DIM), w_o_grad, w_q_grad, grad_x, result, grad_gain)
        return result, grad_x, grad_wq, grad_wk, grad_wv, grad_wo, grad_gain.reshape(-1)

    return jax.shard_map(local_step, mesh=mesh,
                         in_specs=(seq_spec, seq_spec, pos_spec, P(None), replicated, replicated, replicated, replicated),
                         out_specs=(seq_spec, seq_spec, part_rows, part_rows, part_rows, part_rows, P('dp')),
                         check_vma=False)
```

```python
import functools

import jax
import jax.numpy as jnp
import numpy as np
from jax import lax
from jax.experimental import pallas as pl
from jax.experimental.pallas import tpu as pltpu
from jax.sharding import PartitionSpec as P

HEAD_DIM = 128
HALF = HEAD_DIM // 2
ROPE_THETA = 1000000.0
NORM_EPS = 1e-05
NEG_LARGE = -1e30
LOG2E = 1.4426950408889634
BLK = 512
CHUNKS = 4
FWD_MIDDLE, FWD_LATE, BWD_MIDDLE, BWD_LATE = 6, 7, 5, 6
MROWS = 768
RING = 3
DEPTH = 3
COPY_ROWS = 24
PARTS = 3
ROW_STEPS = 8
F32 = jnp.float32
BF16 = jnp.bfloat16
ROWS_ROWS = (((0,), (0,)), ((), ()))
COLS_COLS = (((1,), (1,)), ((), ()))
ROWS_COLS = (((0,), (1,)), ((), ()))
VMEM_LIMIT = 63 * 1024 * 1024


def dot(a, b, dims=(((1,), (0,)), ((), ()))):
    return lax.dot_general(a, b, dims, preferred_element_type=F32)


def params(axes=1):
    return pltpu.CompilerParams(dimension_semantics=("arbitrary",) * axes, vmem_limit_bytes=VMEM_LIMIT)


class Neighbours:
    def __init__(self):
        self.me = lax.axis_index('sp')
        core, col, row = lax.rem(self.me, 2), lax.rem(self.me // 2, 2), self.me // 4
        self.sib = self.me + 1 - 2 * core
        self.xn = self.me + 2 - 4 * col
        self.yn = self.me + 4 - 8 * row
        self.diag = self.xn + self.yn - self.me

    def meet(self, peers):
        barrier = pltpu.get_barrier_semaphore()
        for peer in peers:
            pl.semaphore_signal(barrier, inc=1, device_id={'sp': peer}, device_id_type=pl.DeviceIdType.MESH)
        pl.semaphore_wait(barrier, len(peers))

    def across(self, r):
        core, col, row = lax.rem(self.me, 2), lax.rem(self.me // 2, 2), self.me // 4
        return (self.me + lax.rem(r, 2) * (1 - 2 * core) + lax.rem(r // 2, 2) * (2 - 4 * col) + (r // 4) * (4 - 8 * row))

    def others(self):
        flip = lambda dev: dev + 1 - 2 * lax.rem(dev, 2)
        return [self.sib, self.xn, flip(self.xn), self.yn, flip(self.yn), self.diag, flip(self.diag)]


def send(src, dst, sems, index, peer):
    return pltpu.make_async_remote_copy(src_ref=src, dst_ref=dst, send_sem=sems.at[0, index], recv_sem=sems.at[1, index],
                                        device_id={'sp': peer}, device_id_type=pl.DeviceIdType.MESH)


class Gather:
    COPIES = 22

    def __init__(self, near, own, dst, rows, sems):
        self.near, self.own, self.dst, self.rows, self.sems = near, own, dst, rows, sems

    def block(self, dev, chunk, count=1):
        size = self.rows // CHUNKS
        return self.dst.at[pl.ds(pl.multiple_of(dev * self.rows + chunk * size, size), count * size), :]

    def first(self, chunk, kind):
        peer = (self.near.xn, self.near.yn, self.near.sib)[kind]
        return send(self.own(chunk), self.block(self.near.me, chunk), self.sems, kind * CHUNKS + chunk, peer)

    def onward(self, chunk):
        over_y = chunk < CHUNKS // 2
        rows = self.block(self.near.xn if over_y else self.near.yn, chunk)
        return send(rows, rows, self.sems, 12 + chunk, self.near.yn if over_y else self.near.xn)

    def share(self, kind):
        rows = self.block((self.near.xn, self.near.yn)[kind], 0, CHUNKS)
        return send(rows, rows, self.sems, 16 + kind, self.near.sib)

    def share_diag(self, chunk):
        rows = self.block(self.near.diag, chunk)
        return send(rows, rows, self.sems, 18 + chunk, self.near.sib)

    def begin(self):
        self.near.meet([self.near.sib, self.near.xn, self.near.yn])
        for chunk in range(CHUNKS):
            self.start(chunk)

    def start(self, chunk):
        for kind in range(3):
            self.first(chunk, kind).start()

    def middle(self):
        for chunk in (0, 1):
            self.first(chunk, 0).wait_recv()
            self.onward(chunk).start()
        self.first(2, 1).wait_recv()
        self.onward(2).start()

    def late(self):
        self.first(3, 1).wait_recv()
        self.onward(3).start()
        for chunk in (2, 3):
            self.first(chunk, 0).wait_recv()
        self.share(0).start()
        for chunk in (0, 1):
            self.first(chunk, 1).wait_recv()
        self.share(1).start()

    def end_near(self):
        for chunk in range(CHUNKS):
            self.first(chunk, 2).wait_recv()
        for kind in range(2):
            self.share(kind).wait_recv()

    def end_far(self):
        for chunk in (0, 2, 1, 3):
            self.onward(chunk).wait_recv()
            self.share_diag(chunk).start()
        for chunk in range(CHUNKS):
            for kind in range(3):
                self.first(chunk, kind).wait_send()
            self.onward(chunk).wait_send()
        for kind in range(2):
            self.share(kind).wait_send()
        for chunk in range(CHUNKS):
            self.share_diag(chunk).wait()

    def end(self):
        self.end_near()
        self.end_far()


SEMS = pltpu.SemaphoreType.DMA((2, Gather.COPIES))


def masked(scores):
    key = lax.broadcasted_iota(jnp.int32, scores.shape, 0)
    query = lax.broadcasted_iota(jnp.int32, scores.shape, 1)
    return jnp.where(key <= query, scores, NEG_LARGE)


def unrotate(val, cos_t, sin_t):
    return (val * cos_t - pltpu.roll(val, HALF, 1) * sin_t).astype(BF16)


def attention_part(heads, near, gather_next, x_ref, gain_ref, pos_ref, freq_ref, dy_ref, wq_ref, wk_ref, wv_ref, wo_ref,
                   h_all, dy_all, o_all, ht_ref, dkv_ref, dq_a_ref, dq_b_ref, pos_all, pos_sems, h_sems, dy_sems, o_sems,
                   x_v, h_v, x_sems, own_sems, cos_s, sin_s, w_v, wo_v, w_sems, blk, blk_sems, ht_v, ht_sems,
                   q_s, k_s, v_s, vt, kt, ot_s, lse_s, acc, do_s, dk_acc, dv_acc, dq_v, dq_sems, dkv_v):
    rows, width = x_ref.shape
    n_blocks = k_s.shape[0]
    q_cols = heads * HEAD_DIM
    size = rows // CHUNKS
    qk_scale = HEAD_DIM ** -0.5
    to_log2 = qk_scale * LOG2E
    cols = [slice(a * HEAD_DIM, (a + 1) * HEAD_DIM) for a in range(heads)]
    part = lambda ref, chunk, count=size: ref.at[pl.ds(chunk * count, count), :]
    gather_h = Gather(near, lambda chunk: part(h_v, chunk), h_all, rows, h_sems)
    gather_dy = Gather(near, lambda chunk: part(dy_ref, chunk), dy_all, rows, dy_sems)
    gather_o = Gather(near, lambda chunk: part(ot_s, chunk, q_cols // CHUNKS), o_all, q_cols, o_sems)

    loads = [pltpu.make_async_copy(part(x_ref, chunk), part(x_v, chunk), x_sems.at[chunk]) for chunk in range(CHUNKS)]
    for load in loads:
        load.start()
    others = near.others()
    near.meet(others)
    pos_all[near.me] = jnp.broadcast_to(pos_ref[...], pos_all.shape[1:])
    positions = [send(pos_ref, pos_all.at[near.me, pl.ds(0, 1), :], pos_sems, r, peer) for r, peer in enumerate(others)]
    gain = gain_ref[...].astype(F32)
    for chunk in range(CHUNKS):
        loads[chunk].wait()

        @pl.loop(0, size // 32)
        def _(r):
            at = pl.ds(pl.multiple_of(chunk * size + r * 32, 32), 32)
            x_f = x_v[at, :].astype(F32)
            normed = x_f * lax.rsqrt(jnp.mean(x_f * x_f, axis=-1, keepdims=True) + NORM_EPS)
            h_v[at, :] = (normed * gain).astype(BF16)

        gather_h.start(chunk)
    for copy in positions:
        copy.start()
    own_h = pltpu.make_async_copy(h_v, gather_h.block(near.me, 0, CHUNKS), own_sems.at[0])
    own_h.start()
    w_loads, col = [], 0
    for n, (ref, count) in enumerate(((wq_ref, q_cols), (wk_ref, HEAD_DIM), (wv_ref, HEAD_DIM))):
        at = pl.ds(pl.multiple_of(near.me * count, HEAD_DIM), count)
        w_loads.append(pltpu.make_async_copy(ref.at[:, at], w_v.at[:, pl.ds(col, count)], w_sems.at[n]))
        col += count
    w_loads.append(pltpu.make_async_copy(wo_ref.at[pl.ds(pl.multiple_of(near.me * q_cols, q_cols), q_cols), :], wo_v, w_sems.at[3]))
    stage_in = pltpu.make_async_copy(dy_ref, x_v, own_sems.at[1])
    stage_out = pltpu.make_async_copy(x_v, gather_dy.block(near.me, 0, CHUNKS), own_sems.at[2])
    for load in w_loads + [stage_in]:
        load.start()
    for copy in positions:
        copy.wait()
    sign = jnp.where(lax.broadcasted_iota(jnp.int32, (1, HEAD_DIM), 1) < HALF, -1.0, 1.0)

    @pl.loop(0, n_blocks)
    def _(b):
        pos = jnp.broadcast_to(pos_all[b, 0:1, :].astype(F32), (HEAD_DIM, rows)).T
        angles = pos * freq_ref[...]
        cos_s[b] = jnp.cos(angles)
        sin_s[b] = jnp.sin(angles) * sign

    gather_h.middle()
    gather_h.late()
    for chunk in range(CHUNKS):
        gather_dy.start(chunk)
    for load in w_loads + [stage_in]:
        load.wait()
    stage_out.start()
    own_h.wait()
    gather_h.end()

    def block_load(ref, block, slot):
        return pltpu.make_async_copy(ref.at[pl.ds(pl.multiple_of(block * rows, rows), rows), :], blk.at[slot], blk_sems.at[slot])

    def fwd_chunk(i, c, carry, diagonal):
        k_c, vt_c = k_s[c], vt[c]
        scores = [dot(k_c, q_s[i, :, cols[a]], COLS_COLS) * to_log2 for a in range(heads)]
        out = []
        for a in range(heads):
            s = masked(scores[a]) if diagonal else scores[a]
            m_old, l_old = carry[a]
            m_new = jnp.maximum(m_old, jnp.max(s, axis=0, keepdims=True))
            alpha = jnp.exp2(m_old - m_new)
            p = jnp.exp2(s - m_new)
            l_new = l_old * alpha + jnp.sum(p, axis=0, keepdims=True)
            acc[a] = acc[a] * alpha + dot(vt_c, p.astype(BF16))
            out.append((m_new, l_new))
        return tuple(out)

    def ht_store(i):
        at = pl.ds(pl.multiple_of(i * rows, rows), rows)
        return pltpu.make_async_copy(ht_v.at[lax.rem(i, 2)], ht_ref.at[:, at], ht_sems.at[lax.rem(i, 2)])

    block_load(h_all, 0, 0).start()

    @pl.loop(0, n_blocks)
    def _(i):
        slot = lax.rem(i, 2)
        block_load(h_all, i, slot).wait()

        @pl.when(i + 1 < n_blocks)
        def _():
            block_load(h_all, i + 1, 1 - slot).start()

        @pl.when(i >= 2)
        def _():
            ht_store(i - 2).wait()

        ht_v[slot] = blk[slot].T
        ht_store(i).start()
        prod = dot(blk[slot], w_v[...])
        cos_t, sin_t = cos_s[i], sin_s[i]
        for a in range(heads + 1):
            val = prod[:, a * HEAD_DIM:(a + 1) * HEAD_DIM]
            rot = (val * cos_t + pltpu.roll(val, HALF, 1) * sin_t).astype(BF16)
            if a < heads:
                q_s[i, :, cols[a]] = rot
            else:
                k_s[i] = rot
                kt[i] = rot.T
        v_i = prod[:, q_cols + HEAD_DIM:].astype(BF16)
        v_s[i] = v_i
        vt[i] = v_i.T
        acc[...] = jnp.zeros_like(acc)
        start = tuple((jnp.full((1, rows), NEG_LARGE, F32), jnp.zeros((1, rows), F32)) for _ in range(heads))
        carry = lax.fori_loop(0, i, lambda c, carry: fwd_chunk(i, c, carry, False), start)
        carry = fwd_chunk(i, i, carry, True)
        at = pl.ds(pl.multiple_of(i * rows, rows), rows)
        for a in range(heads):
            m_a, l_a = carry[a]
            ot_s[cols[a], at] = (acc[a] / l_a).astype(BF16)
            lse_s[i, a:a + 1, :] = m_a + jnp.log2(l_a)

        @pl.when(i == FWD_MIDDLE)
        def _():
            gather_dy.middle()

        @pl.when(i == FWD_LATE)
        def _():
            gather_dy.late()

    for chunk in range(CHUNKS):
        gather_o.start(chunk)
    own_o = pltpu.make_async_copy(ot_s, gather_o.block(near.me, 0, CHUNKS), own_sems.at[0])
    own_o.start()

    def d_o_blocks(low, high):
        block_load(dy_all, near.across(low), 0).start()

        @pl.loop(low, high)
        def _(r):
            slot = lax.rem(r - low, 2)
            block_load(dy_all, 0, slot).wait()

            @pl.when(r + 1 < high)
            def _():
                block_load(dy_all, near.across(r + 1), 1 - slot).start()

            do_s[near.across(r)] = dot(blk[slot], wo_v[...], COLS_COLS).astype(BF16)

    stage_out.wait()
    gather_dy.end_near()
    d_o_blocks(0, n_blocks * 3 // 4)
    gather_dy.end_far()
    d_o_blocks(n_blocks * 3 // 4, n_blocks)

    def bwd_chunk(i, c, delta, diagonal):
        k_c, v_c, kt_c = k_s[c], v_s[c], kt[c]
        dk_c = dv_c = None
        for a in range(heads):
            q_a, do_a = q_s[i, :, cols[a]], do_s[i, :, cols[a]]
            s = dot(k_c, q_a, COLS_COLS) * to_log2
            if diagonal:
                s = masked(s)
            p = jnp.exp2(s - lse_s[i, a:a + 1, :])
            d_p = dot(v_c, do_a, COLS_COLS)
            d_s = (p * (d_p - delta[a])).astype(BF16)
            dv_a = dot(p.astype(BF16), do_a)
            dk_a = dot(d_s, q_a)
            dv_c = dv_a if dv_c is None else dv_c + dv_a
            dk_c = dk_a if dk_c is None else dk_c + dk_a
            acc[a] += dot(kt_c, d_s)
        if diagonal:
            dk_acc[c] = dk_c
            dv_acc[c] = dv_c
        else:
            dk_acc[c] += dk_c
            dv_acc[c] += dv_c

    def dq_stores(i):
        slot = lax.rem(i, 2)
        at = pl.ds(pl.multiple_of(i * rows, rows), rows)
        last = q_cols - HEAD_DIM
        return [pltpu.make_async_copy(dq_v.at[slot, :, pl.ds(0, last)], dq_a_ref.at[at, :], dq_sems.at[slot, 0]),
                pltpu.make_async_copy(dq_v.at[slot, :, pl.ds(last, HEAD_DIM)], dq_b_ref.at[at, :], dq_sems.at[slot, 1])]

    for i in (n_blocks - 2, n_blocks - 1):
        ht_store(i).wait()

    @pl.loop(0, n_blocks)
    def _(i):
        at = pl.ds(pl.multiple_of(i * rows, rows), rows)
        acc[...] = jnp.zeros_like(acc)
        delta = [jnp.sum(ot_s[cols[a], at].astype(F32) * do_s[i, :, cols[a]].T.astype(F32), axis=0, keepdims=True) for a in range(heads)]

        @pl.loop(0, i)
        def _(c):
            bwd_chunk(i, c, delta, False)

        bwd_chunk(i, i, delta, True)

        @pl.when(i >= 2)
        def _():
            for store in dq_stores(i - 2):
                store.wait()

        for a in range(heads):
            dq_v[lax.rem(i, 2), :, cols[a]] = unrotate(acc[a].T * qk_scale, cos_s[i], sin_s[i])
        for store in dq_stores(i):
            store.start()

        @pl.when(i == BWD_MIDDLE)
        def _():
            gather_o.middle()

        @pl.when(i == BWD_LATE)
        def _():
            gather_o.late()

    for i in (n_blocks - 2, n_blocks - 1):
        for store in dq_stores(i):
            store.wait()
    for chunk in range(CHUNKS):
        gather_next.start(chunk)

    @pl.loop(0, n_blocks)
    def _(c):
        at = pl.ds(pl.multiple_of(c * rows, rows), rows)
        dkv_v[at, :HEAD_DIM] = unrotate(dk_acc[c] * qk_scale, cos_s[c], sin_s[c])
        dkv_v[at, HEAD_DIM:] = dv_acc[c].astype(BF16)

    dkv_store = pltpu.make_async_copy(dkv_v, dkv_ref, own_sems.at[1])
    dkv_store.start()
    own_o.wait()
    gather_o.end()
    dkv_store.wait()


def lanes(*parts):
    return jnp.concatenate(parts, axis=1)


def products_part(heads, near, gathers, ot_ref, ht_ref, dy_ref, d_kv_ref, d_qa_ref, d_qb_ref, x_ref, own_dy_ref, gain_ref, wo_ref, wk_ref, wv_ref, wq_ref,
                  wo_out, wq_out, kv_all, qa_all, qb_all, res_ref, gx_ref, gg_ref, gg_row, gg_all, gg_sems, x_sems,
                  a_buf, b_buf, tile, a_sem, b_sems, t_sems, stage, stage_sems, ot_v, o_v, x_v, io_sems, own, own_sems, w_v, w_sems, acc,
                  gg_v):
    core = lax.rem(near.me, 2)
    half = a_buf.shape[0]
    seq_len = d_kv_ref.shape[0]
    rows, width = x_ref.shape
    n_cols = d_kv_ref.shape[1]
    n_o, n_all = width // (2 * n_cols), x_sems.shape[1]
    n_oa = n_o + (n_all - n_o) * 2 // 3

    local = (d_qa_ref, d_qb_ref, d_kv_ref)

    def stage_in(n):
        return pltpu.make_async_copy(local[n], stage.at[:, pl.ds(0, local[n].shape[1])], stage_sems.at[0])

    def stage_out(n):
        return pltpu.make_async_copy(stage.at[:, pl.ds(0, local[n].shape[1])], gathers[n].block(near.me, 0, CHUNKS), stage_sems.at[1])

    def copy_own(n):
        stage_in(n).wait()
        stage_out(n).start()

    own_rows = pl.ds(pl.multiple_of(core * half, half), half)
    tokens = pl.ds(pl.multiple_of(near.me * rows, rows), rows)
    ot_load = pltpu.make_async_copy(ot_ref.at[:, tokens], ot_v, io_sems.at[0])
    x_load = pltpu.make_async_copy(x_ref, x_v, io_sems.at[1])
    res_store = pltpu.make_async_copy(x_v, res_ref, io_sems.at[2])
    dy_load = pltpu.make_async_copy(own_dy_ref, o_v, io_sems.at[3])
    gx_store = pltpu.make_async_copy(o_v, gx_ref, io_sems.at[0])

    def a_load(ref):
        return pltpu.make_async_copy(ref.at[own_rows, :], a_buf, a_sem)

    def b_loads(source, p, slot, g):
        if source is dy_ref:
            srcs = [dy_ref.at[:, pl.ds(pl.multiple_of((2 * p + g) * n_cols, n_cols), n_cols)]]
        else:
            per = n_cols // source.shape[1]
            srcs = [source.at[pl.ds(pl.multiple_of(((2 * p + g) * per + n) * seq_len, seq_len), seq_len), :] for n in range(per)]
        return [pltpu.make_async_copy(src, b_buf.at[slot, :, pl.ds(g * n_cols + n * src.shape[1], src.shape[1])], b_sems.at[slot, g])
                for n, src in enumerate(srcs)]

    def start_b(step):
        slot = lax.rem(step, 2)
        for source, low, high in ((dy_ref, 0, n_o), (qa_all, n_o, n_oa), (qb_all, n_oa, n_all)):
            @pl.when(jnp.logical_and(step >= low, step < high))
            def _():
                for g in range(2):
                    for load in b_loads(source, step - low, slot, g):
                        load.start()

    def pieces(kind, step):
        wide = (2 * n_cols, n_cols, HEAD_DIM)[kind]
        slot = lax.rem(step, 2)
        out = []
        for n in range(2 * n_cols // wide):
            group = (step - (0, n_o, n_oa)[kind]) * (2 * n_cols // wide) + n
            col = (group * wide, group * heads * HEAD_DIM, (group + 1) * heads * HEAD_DIM - HEAD_DIM)[kind]
            dst = (wo_out, wq_out, wq_out)[kind].at[own_rows, pl.ds(pl.multiple_of(col, HEAD_DIM), wide)]
            src = tile.at[slot, :, pl.ds(n * wide, wide)]
            out.append((pltpu.make_async_copy(src, dst, t_sems.at[slot]), send(src, dst, x_sems, step, near.sib)))
        return out

    def start_tile(step):
        for kind, (low, high) in enumerate(((0, n_o), (n_o, n_oa), (n_oa, n_all))):
            @pl.when(jnp.logical_and(step >= low, step < high))
            def _():
                for keep, give in pieces(kind, step):
                    keep.start()
                    give.start()

    def whole_tile(step):
        slot = lax.rem(step, 2)
        dst = wo_out.at[own_rows, pl.ds(0, 2 * n_cols)]
        return pltpu.make_async_copy(tile.at[slot], dst, t_sems.at[slot]), send(tile.at[slot], dst, x_sems, step, near.sib)

    def wait_tile(step):
        keep, give = whole_tile(step)
        keep.wait()
        give.wait_send()

    def result_part():
        cols = b_buf.shape[2]

        def w_load(n):
            slot = lax.rem(n, 2)
            return pltpu.make_async_copy(wo_ref.at[:, pl.ds(pl.multiple_of(n * cols, cols), cols)], b_buf.at[slot, pl.ds(0, wo_ref.shape[0]), :],
                                         b_sems.at[slot, 0])

        w_load(jnp.int32(0)).start()
        ot_load.wait()

        @pl.loop(0, ot_v.shape[0] // BLK)
        def _(r):
            at = pl.ds(pl.multiple_of(r * BLK, BLK), BLK)
            o_v[:, at] = ot_v[at, :].T

        x_load.wait()

        @pl.loop(0, n_o)
        def _(n):
            w_load(n).wait()

            @pl.when(n + 1 < n_o)
            def _():
                w_load(n + 1).start()

            at = pl.ds(pl.multiple_of(n * cols, cols), cols)
            x_v[:, at] = (x_v[:, at].astype(F32) + dot(o_v[...], b_buf[lax.rem(n, 2), :wo_ref.shape[0], :])).astype(BF16)

        res_store.start()

    def hidden_parts(kind):
        count = own.shape[0] // (2 if kind == 1 else 1)

        def own_load(r, g):
            source = (qa_all, qb_all, kv_all)[kind]
            device, col = (2 * r + g, 0) if kind == 1 else (near.across(r), g * HEAD_DIM)
            at = pl.ds(pl.multiple_of(device * seq_len + near.me * rows, rows), rows)
            return pltpu.make_async_copy(source.at[at, pl.ds(col, HEAD_DIM)], own.at[r, :, pl.ds(g * HEAD_DIM, HEAD_DIM)], own_sems.at[r, g])

        def w_load(r, g):
            source = (wk_ref, wv_ref)[g] if kind == 2 else wq_ref
            col = near.across(r) if kind == 2 else heads * near.across(r) + g if kind == 0 else heads * (2 * r + g + 1) - 1
            slot = lax.rem(r, 2)
            return pltpu.make_async_copy(source.at[:, pl.ds(pl.multiple_of(col * HEAD_DIM, HEAD_DIM), HEAD_DIM)],
                                         w_v.at[slot, :, pl.ds(g * HEAD_DIM, HEAD_DIM)], w_sems.at[slot, g])

        return count, own_load, w_load

    def hidden_start(kind, low=0, high=None):
        count, own_load, w_load = hidden_parts(kind)
        for g in range(2):
            if low == 0:
                w_load(jnp.int32(0), g).start()

            @pl.loop(low, high or count)
            def _(r):
                own_load(r, g).start()

    def hidden_add(kind, low=0, high=None):
        count, own_load, w_load = hidden_parts(kind)

        @pl.loop(low, high or count)
        def _(r):
            for g in range(2):
                w_load(r, g).wait()
                own_load(r, g).wait()

            @pl.when(r + 1 < count)
            def _():
                for g in range(2):
                    w_load(r + 1, g).start()

            for col in range(0, width, width // PARTS):
                at = slice(col, col + width // PARTS)
                acc[:, at] += dot(own[r], w_v[lax.rem(r, 2), at, :], COLS_COLS)

    a_load(ot_ref).start()
    start_b(jnp.int32(0))
    stage_in(0).start()
    ot_load.start()
    x_load.start()
    a_load(ot_ref).wait()

    @pl.loop(0, n_all)
    def _(step):
        slot = lax.rem(step, 2)
        for g in range(2):
            b_loads(dy_ref, 0, slot, g)[0].wait()

        @pl.when(jnp.logical_and(step != n_o - 1, step != n_oa - 1))
        def _():
            start_b(step + 1)

        @pl.when(step >= 2)
        def _():
            wait_tile(step - 2)

        @pl.when(step == n_o)
        def _():
            a_load(ht_ref).wait()

        for r in range(0, half, half // PARTS):
            tile[slot, r:r + half // PARTS, :] = dot(a_buf[r:r + half // PARTS, :], b_buf[slot])
        start_tile(step)

        @pl.when(step == n_o - 3)
        def _():
            acc[...] = jnp.zeros_like(acc)
            copy_own(0)
            gathers[0].middle()

        @pl.when(step == n_o - 1)
        def _():
            a_load(ht_ref).start()
            gathers[0].late()
            for c in range(CHUNKS):
                gathers[1].start(c)
            stage_out(0).wait()
            stage_in(1).start()
            result_part()
            gathers[0].end()
            start_b(step + 1)
            hidden_start(0)

        @pl.when(step == n_oa - 3)
        def _():
            copy_own(1)
            gathers[1].middle()

        @pl.when(step == n_oa - 2)
        def _():
            gathers[1].late()
            for c in range(CHUNKS):
                gathers[2].start(c)
            stage_out(1).wait()
            stage_in(2).start()

        @pl.when(step == n_oa - 1)
        def _():
            res_store.wait()
            x_load.start()
            dy_load.start()
            gathers[1].end()
            start_b(step + 1)
            hidden_add(0)
            hidden_start(1)

    hidden_add(1)
    copy_own(2)
    gathers[2].middle()
    gathers[2].late()
    stage_out(2).wait()
    gathers[2].end_near()
    near_count = own.shape[0] * 3 // 4
    hidden_start(2, 0, near_count)
    for step in (n_all - 2, n_all - 1):
        wait_tile(jnp.int32(step))
    hidden_add(2, 0, near_count)
    gathers[2].end_far()
    hidden_start(2, near_count)
    hidden_add(2, near_count)

    gain = gain_ref[...].astype(F32)
    gg_v[...] = jnp.zeros_like(gg_v)
    x_load.wait()
    dy_load.wait()

    @pl.loop(0, rows // 32)
    def _(r):
        at = pl.ds(pl.multiple_of(r * 32, 32), 32)
        x_f = x_v[at, :].astype(F32)
        inv_rms = lax.rsqrt(jnp.mean(x_f * x_f, axis=-1, keepdims=True) + NORM_EPS)
        normed = x_f * inv_rms
        d_hid = acc[at, :]
        both = d_hid * normed
        gg_v[...] += jnp.sum(both.reshape(4, 8, width), axis=0)
        mean = jnp.mean(both * gain, axis=-1, keepdims=True)
        o_v[at, :] = (o_v[at, :].astype(F32) + inv_rms * (d_hid * gain - normed * mean)).astype(BF16)

    gg_row[...] = jnp.sum(gg_v[...], axis=0, keepdims=True)
    gg_all[near.me] = gg_row[...]
    parts = [send(gg_row, gg_all.at[near.me], gg_sems, r, peer) for r, peer in enumerate(near.others())]
    for copy in parts:
        copy.start()
    gx_store.start()

    @pl.loop(0, n_all)
    def _(step):
        whole_tile(step)[1].wait_recv()

    for copy in parts:
        copy.wait()
    gg_ref[...] = jnp.sum(gg_all[...], axis=0)
    gx_store.wait()


def step_kernel(heads, first_scratch, second_scratch, x_ref, gain_ref, pos_ref, freq_ref, dy_ref, wq_ref, wk_ref, wv_ref, wo_ref,
                h_all, dy_all, o_all, ht, d_kv, d_qa, d_qb, wo_out, wq_out, kv_all, qa_all, qb_all, res, gx, gg,
                pos_all, pos_sems, gg_row, gg_all, gg_sems, x_sems, h_sems, dy_sems, o_sems, kv_sems, qa_sems, qb_sems):
    near = Neighbours()
    seq_len = d_kv.shape[0]

    def gather_of(src, dst, sems):
        return Gather(near, lambda c: src.at[pl.ds(c * (seq_len // CHUNKS), seq_len // CHUNKS), :], dst, seq_len, sems)

    gathers = [gather_of(d_qa, qa_all, qa_sems), gather_of(d_qb, qb_all, qb_sems), gather_of(d_kv, kv_all, kv_sems)]

    def first(*scratch):
        attention_part(heads, near, gathers[0], x_ref, gain_ref, pos_ref, freq_ref, dy_ref, wq_ref, wk_ref, wv_ref, wo_ref,
                       h_all, dy_all, o_all, ht, d_kv, d_qa, d_qb, pos_all, pos_sems, h_sems, dy_sems, o_sems, *scratch)

    def second(*scratch):
        products_part(heads, near, gathers, o_all, ht, dy_all, d_kv, d_qa, d_qb, x_ref, dy_ref, gain_ref, wo_ref, wk_ref, wv_ref, wq_ref,
                      wo_out, wq_out, kv_all, qa_all, qb_all, res, gx, gg, gg_row, gg_all, gg_sems, x_sems, *scratch)

    pl.run_scoped(first, *first_scratch)
    pl.run_scoped(second, *second_scratch)


def step(x, gain, positions, grad_out, w_q, w_k, w_v, w_o, sp_size, heads):
    rows, width = x.shape
    seq_len = rows * sp_size
    q_cols = heads * HEAD_DIM
    all_cols = q_cols * sp_size
    half = width // 2
    cols = 4 * HEAD_DIM
    n_all = (width + all_cols) // cols
    any_spec = pl.BlockSpec(memory_space=pl.ANY)
    vmem = pl.BlockSpec(memory_space=pltpu.VMEM)
    dma = pltpu.SemaphoreType.DMA
    inv_freq = ROPE_THETA ** (-np.arange(0, HEAD_DIM, 2) / HEAD_DIM)
    freq = jnp.asarray(np.concatenate([inv_freq, inv_freq])[None, :], F32)
    pairs = heads * seq_len * (seq_len + rows) // 2
    out = lambda *shape, dtype=BF16: jax.ShapeDtypeStruct(shape, dtype)
    array = lambda *shape, dtype=BF16: pltpu.VMEM(shape, dtype)
    blocks = lambda *shape, dtype=BF16: pltpu.VMEM((sp_size,) + shape, dtype)
    first_scratch = [array(rows, width), array(rows, width), dma((CHUNKS,)), dma((3,)), blocks(rows, HEAD_DIM, dtype=F32),
                     blocks(rows, HEAD_DIM, dtype=F32), array(width, q_cols + 2 * HEAD_DIM), array(q_cols, width), dma((4,)),
                     array(2, rows, width), dma((2,)), array(2, width, rows), dma((2,)),
                     blocks(rows, q_cols), blocks(rows, HEAD_DIM), blocks(rows, HEAD_DIM), blocks(HEAD_DIM, rows), blocks(HEAD_DIM, rows),
                     array(q_cols, seq_len), blocks(8, rows, dtype=F32), array(heads, HEAD_DIM, rows, dtype=F32),
                     blocks(rows, q_cols), blocks(rows, HEAD_DIM, dtype=F32), blocks(rows, HEAD_DIM, dtype=F32),
                     array(2, rows, q_cols), dma((2, 2)), array(seq_len, 2 * HEAD_DIM)]
    second_scratch = [array(half, seq_len), array(2, seq_len, cols), array(2, half, cols, dtype=F32), dma, dma((2, 2)), dma((2,)),
                      array(seq_len, 2 * HEAD_DIM), dma((2,)), array(all_cols, rows), array(rows, all_cols), array(rows, width),
                      dma((4,)), blocks(rows, 2 * HEAD_DIM), dma((sp_size, 2)), array(2, width, 2 * HEAD_DIM), dma((2, 2)),
                      array(rows, width, dtype=F32), array(8, width, dtype=F32)]
    return pl.pallas_call(
        functools.partial(step_kernel, heads, first_scratch, second_scratch),
        in_specs=[any_spec, vmem, vmem, vmem] + [any_spec] * 5,
        out_specs=[any_spec] * 14 + [vmem],
        out_shape=[out(seq_len, width), out(seq_len, width), out(all_cols, seq_len), out(width, seq_len), out(seq_len, 2 * HEAD_DIM),
                   out(seq_len, q_cols - HEAD_DIM), out(seq_len, HEAD_DIM), out(all_cols, width, dtype=F32), out(width, all_cols, dtype=F32),
                   out(sp_size * seq_len, 2 * HEAD_DIM), out(sp_size * seq_len, q_cols - HEAD_DIM), out(sp_size * seq_len, HEAD_DIM),
                   out(rows, width), out(rows, width), out(1, width, dtype=F32)],
        scratch_shapes=[blocks(8, rows, dtype=jnp.int32), dma((2, 7)), array(1, width, dtype=F32), blocks(1, width, dtype=F32), dma((2, 7)),
                        dma((2, n_all))] + [SEMS] * 6,
        compiler_params=pltpu.CompilerParams(vmem_limit_bytes=VMEM_LIMIT, collective_id=0, has_side_effects=True),
        cost_estimate=pl.CostEstimate(flops=28 * pairs * HEAD_DIM + 2 * half * cols * seq_len * n_all, bytes_accessed=20 * seq_len * width,
                                      transcendentals=2 * pairs),
        name="step",
    )(x, gain, positions.reshape(1, -1), freq, grad_out, w_q, w_k, w_v, w_o)


def finish_kernel(ht_ref, d_ref, gx_in, res_in, gg_in, wo_in, wq_in, wk_ref, wv_ref, wq_ref, wo_ref, gx_ref, res_ref, gg_ref, d_v, d_sems, ring, ring_sems):
    step = pl.program_id(0) * pl.num_programs(1) + pl.program_id(1)
    high = ring.shape[2]
    per_array = wo_in.shape[0] // (high * RING)

    def copy_in(src, g, n):
        at = pl.ds(pl.multiple_of((lax.rem(g, per_array) * RING + n) * high, high), high)
        return pltpu.make_async_copy(src.at[at, :], ring.at[lax.rem(g, DEPTH), n], ring_sems.at[0, lax.rem(g, DEPTH), n])

    def copy_out(dst, g, n):
        at = pl.ds(pl.multiple_of((lax.rem(g, per_array) * RING + n) * high, high), high)
        return pltpu.make_async_copy(ring.at[lax.rem(g, DEPTH), n], dst.at[at, :], ring_sems.at[1, lax.rem(g, DEPTH), n])

    def start(copy, first, second, g):
        for ref, mine in ((first, g < per_array), (second, g >= per_array)):
            @pl.when(mine)
            def _():
                for n in range(RING):
                    copy(ref, g, n).start()

    def pair_load(p):
        at = pl.ds(2 * p, 2)
        return pltpu.make_async_copy(d_ref.at[at], d_v.at[at], d_sems.at[p])

    @pl.when(step == 0)
    def _():
        for p in range(d_v.shape[0] // 2):
            pair_load(p).start()

    last = pl.num_programs(0) * pl.num_programs(1) - 1

    def free(g):
        for n in range(RING):
            copy_out(wo_ref, g, n).wait()

    def pass_on(g):
        for n in range(RING):
            copy_in(wo_in, g, n).wait()
        start(copy_out, wo_ref, wq_ref, g)

    @pl.when(step >= DEPTH)
    def _():
        free(step - DEPTH)

    start(copy_in, wo_in, wq_in, step)

    @pl.when(step >= 1)
    def _():
        pass_on(step - 1)

    for p in range(d_v.shape[0] // 2):
        @pl.when(step == p)
        def _():
            pair_load(p).wait()

    ht = ht_ref[...]
    pair = 2 * pl.program_id(1)
    wk_ref[...] = dot(ht, lanes(d_v[pair, :, :HEAD_DIM], d_v[pair + 1, :, :HEAD_DIM]))
    wv_ref[...] = dot(ht, lanes(d_v[pair, :, HEAD_DIM:], d_v[pair + 1, :, HEAD_DIM:]))

    @pl.when(step == 0)
    def _():
        gg_ref[...] = gg_in[...]

    @pl.when(step == last)
    def _():
        pass_on(last)
        for back in range(DEPTH):
            free(last - back)

    @pl.when(step < ROW_STEPS)
    def _():
        gx_ref[...] = gx_in[...]
        res_ref[...] = res_in[...]


def finish(ht, d_kv, w_o_grad, w_q_grad, grad_x, result, grad_gain):
    width, seq_len = ht.shape
    groups = d_kv.shape[0]
    n_j = groups // 2
    steps = (width // MROWS) * n_j
    high = width // COPY_ROWS
    assert w_o_grad.shape[0] + w_q_grad.shape[0] == high * RING * steps
    any_spec = pl.BlockSpec(memory_space=pl.ANY)
    rows = pl.BlockSpec((grad_x.shape[0] // ROW_STEPS, width), lambda m, j: (jnp.minimum(m * n_j + j, ROW_STEPS - 1), 0))
    whole = pl.BlockSpec((1, width), lambda m, j: (0, 0))
    kv_out = pl.BlockSpec((MROWS, 2 * HEAD_DIM), lambda m, j: (m, j))
    out = lambda cols: jax.ShapeDtypeStruct((width, cols), F32)
    like = lambda val: jax.ShapeDtypeStruct(val.shape, val.dtype)
    return pl.pallas_call(
        finish_kernel,
        grid=(width // MROWS, n_j),
        in_specs=[pl.BlockSpec((MROWS, seq_len), lambda m, j: (m, 0)), any_spec, rows, rows, whole, any_spec, any_spec],
        out_specs=[kv_out, kv_out, any_spec, any_spec, rows, rows, whole],
        out_shape=[out(groups * HEAD_DIM), out(groups * HEAD_DIM), like(w_q_grad), like(w_o_grad), like(grad_x), like(result), like(grad_gain)],
        scratch_shapes=[pltpu.VMEM(d_kv.shape, BF16), pltpu.SemaphoreType.DMA((groups // 2,)),
                        pltpu.VMEM((DEPTH, RING, high, width), F32), pltpu.SemaphoreType.DMA((2, DEPTH, RING))],
        compiler_params=params(2),
        cost_estimate=pl.CostEstimate(flops=4 * width * seq_len * groups * HEAD_DIM, bytes_accessed=2 * width * seq_len, transcendentals=0),
        name="finish",
    )(ht, d_kv, grad_x, result, grad_gain, w_o_grad, w_q_grad)


def solution(mesh):
    sp_size = mesh.shape['sp']
    seq_spec = P(('dp', 'sp'), None)
    pos_spec = P(('dp', 'sp'))
    replicated = P(None, None)
    part_rows = P('dp', None)

    def local_step(x, grad_out, positions, gain, w_q, w_k, w_v, w_o):
        n_heads = w_q.shape[1] // HEAD_DIM
        heads = n_heads // sp_size
        _, _, _, ht, _, _, _, w_o_grad, w_q_grad, kv_all, _, _, result, grad_x, grad_gain = step(
            x, gain.reshape(1, -1), positions, grad_out, w_q, w_k, w_v, w_o, sp_size, heads)
        grad_wk, grad_wv, grad_wq, grad_wo, grad_x, result, grad_gain = finish(
            ht, kv_all.reshape(sp_size, -1, 2 * HEAD_DIM), w_o_grad, w_q_grad, grad_x, result, grad_gain)
        return result, grad_x, grad_wq, grad_wk, grad_wv, grad_wo, grad_gain.reshape(-1)

    return jax.shard_map(local_step, mesh=mesh,
                         in_specs=(seq_spec, seq_spec, pos_spec, P(None), replicated, replicated, replicated, replicated),
                         out_specs=(seq_spec, seq_spec, part_rows, part_rows, part_rows, part_rows, P('dp')),
                         check_vma=False)
```

```python
import functools

import jax
import jax.numpy as jnp
import numpy as np
from jax import lax
from jax.experimental import pallas as pl
from jax.experimental.pallas import tpu as pltpu
from jax.sharding import PartitionSpec as P

HEAD_DIM = 128
HALF = HEAD_DIM // 2
ROPE_THETA = 1000000.0
NORM_EPS = 1e-05
NEG_LARGE = -1e30
LOG2E = 1.4426950408889634
BLK = 512
CHUNKS = 4
FWD_MIDDLE, FWD_LATE, BWD_MIDDLE = 6, 7, 31
MROWS = 768
RING = 3
DEPTH = 3
COPY_ROWS = 24
PARTS = 3
ROW_STEPS = 8
F32 = jnp.float32
BF16 = jnp.bfloat16
ROWS_ROWS = (((0,), (0,)), ((), ()))
COLS_COLS = (((1,), (1,)), ((), ()))
ROWS_COLS = (((0,), (1,)), ((), ()))
VMEM_LIMIT = 63 * 1024 * 1024


def dot(a, b, dims=(((1,), (0,)), ((), ()))):
    return lax.dot_general(a, b, dims, preferred_element_type=F32)


def params(axes=1):
    return pltpu.CompilerParams(dimension_semantics=("arbitrary",) * axes, vmem_limit_bytes=VMEM_LIMIT)


class Neighbours:
    def __init__(self):
        self.me = lax.axis_index('sp')
        core, col, row = lax.rem(self.me, 2), lax.rem(self.me // 2, 2), self.me // 4
        self.sib = self.me + 1 - 2 * core
        self.xn = self.me + 2 - 4 * col
        self.yn = self.me + 4 - 8 * row
        self.diag = self.xn + self.yn - self.me

    def meet(self, peers):
        barrier = pltpu.get_barrier_semaphore()
        for peer in peers:
            pl.semaphore_signal(barrier, inc=1, device_id={'sp': peer}, device_id_type=pl.DeviceIdType.MESH)
        pl.semaphore_wait(barrier, len(peers))

    def across(self, r):
        core, col, row = lax.rem(self.me, 2), lax.rem(self.me // 2, 2), self.me // 4
        return (self.me + lax.rem(r, 2) * (1 - 2 * core) + lax.rem(r // 2, 2) * (2 - 4 * col) + (r // 4) * (4 - 8 * row))

    def others(self):
        flip = lambda dev: dev + 1 - 2 * lax.rem(dev, 2)
        return [self.sib, self.xn, flip(self.xn), self.yn, flip(self.yn), self.diag, flip(self.diag)]


def send(src, dst, sems, index, peer):
    return pltpu.make_async_remote_copy(src_ref=src, dst_ref=dst, send_sem=sems.at[0, index], recv_sem=sems.at[1, index],
                                        device_id={'sp': peer}, device_id_type=pl.DeviceIdType.MESH)


class Gather:
    COPIES = 22

    def __init__(self, near, own, dst, rows, sems):
        self.near, self.own, self.dst, self.rows, self.sems = near, own, dst, rows, sems

    def block(self, dev, chunk, count=1):
        size = self.rows // CHUNKS
        return self.dst.at[pl.ds(pl.multiple_of(dev * self.rows + chunk * size, size), count * size), :]

    def first(self, chunk, kind):
        peer = (self.near.xn, self.near.yn, self.near.sib)[kind]
        return send(self.own(chunk), self.block(self.near.me, chunk), self.sems, kind * CHUNKS + chunk, peer)

    def onward(self, chunk):
        over_y = chunk < CHUNKS // 2
        rows = self.block(self.near.xn if over_y else self.near.yn, chunk)
        return send(rows, rows, self.sems, 12 + chunk, self.near.yn if over_y else self.near.xn)

    def share(self, kind):
        rows = self.block((self.near.xn, self.near.yn)[kind], 0, CHUNKS)
        return send(rows, rows, self.sems, 16 + kind, self.near.sib)

    def share_diag(self, chunk):
        rows = self.block(self.near.diag, chunk)
        return send(rows, rows, self.sems, 18 + chunk, self.near.sib)

    def begin(self):
        self.near.meet([self.near.sib, self.near.xn, self.near.yn])
        for chunk in range(CHUNKS):
            self.start(chunk)

    def start(self, chunk):
        for kind in range(3):
            self.first(chunk, kind).start()

    def middle(self):
        for chunk in (0, 1):
            self.first(chunk, 0).wait_recv()
            self.onward(chunk).start()
        self.first(2, 1).wait_recv()
        self.onward(2).start()

    def late(self):
        self.first(3, 1).wait_recv()
        self.onward(3).start()
        for chunk in (2, 3):
            self.first(chunk, 0).wait_recv()
        self.share(0).start()
        for chunk in (0, 1):
            self.first(chunk, 1).wait_recv()
        self.share(1).start()

    def end_sib(self):
        for chunk in range(CHUNKS):
            self.first(chunk, 2).wait_recv()

    def end_near(self):
        for kind in range(2):
            self.share(kind).wait_recv()

    def end_far(self):
        for chunk in (0, 2, 1, 3):
            self.onward(chunk).wait_recv()
            self.share_diag(chunk).start()
        for chunk in range(CHUNKS):
            for kind in range(3):
                self.first(chunk, kind).wait_send()
            self.onward(chunk).wait_send()
        for kind in range(2):
            self.share(kind).wait_send()
        for chunk in range(CHUNKS):
            self.share_diag(chunk).wait()

    def end(self):
        self.end_sib()
        self.end_near()
        self.end_far()


SEMS = pltpu.SemaphoreType.DMA((2, Gather.COPIES))


def masked(scores):
    key = lax.broadcasted_iota(jnp.int32, scores.shape, 0)
    query = lax.broadcasted_iota(jnp.int32, scores.shape, 1)
    return jnp.where(key <= query, scores, NEG_LARGE)


def unrotate(val, cos_t, sin_t):
    return (val * cos_t - pltpu.roll(val, HALF, 1) * sin_t).astype(BF16)


def attention_part(heads, near, gather_next, x_ref, gain_ref, pos_ref, freq_ref, dy_ref, wq_ref, wk_ref, wv_ref, wo_ref,
                   h_all, dy_all, o_all, ht_ref, dkv_ref, dq_a_ref, dq_b_ref, pos_all, pos_sems, h_sems, dy_sems, o_sems,
                   x_v, h_v, x_sems, own_sems, cos_s, sin_s, w_v, wo_v, w_sems, blk, blk_sems, ht_v, ht_sems,
                   q_s, k_s, v_s, vt, kt, ot_s, lse_s, acc, do_s, dk_acc, dv_acc, dq_v, dq_sems, dkv_v):
    rows, width = x_ref.shape
    n_blocks = k_s.shape[0]
    q_cols = heads * HEAD_DIM
    size = rows // CHUNKS
    qk_scale = HEAD_DIM ** -0.5
    to_log2 = qk_scale * LOG2E
    cols = [slice(a * HEAD_DIM, (a + 1) * HEAD_DIM) for a in range(heads)]
    part = lambda ref, chunk, count=size: ref.at[pl.ds(chunk * count, count), :]
    gather_h = Gather(near, lambda chunk: part(h_v, chunk), h_all, rows, h_sems)
    gather_dy = Gather(near, lambda chunk: part(dy_ref, chunk), dy_all, rows, dy_sems)
    gather_o = Gather(near, lambda chunk: part(ot_s, chunk, q_cols // CHUNKS), o_all, q_cols, o_sems)

    loads = [pltpu.make_async_copy(part(x_ref, chunk), part(x_v, chunk), x_sems.at[chunk]) for chunk in range(CHUNKS)]
    for load in loads:
        load.start()
    others = near.others()
    near.meet(others)
    pos_all[near.me] = jnp.broadcast_to(pos_ref[...], pos_all.shape[1:])
    positions = [send(pos_ref, pos_all.at[near.me, pl.ds(0, 1), :], pos_sems, r, peer) for r, peer in enumerate(others)]
    gain = gain_ref[...].astype(F32)
    for chunk in range(CHUNKS):
        loads[chunk].wait()

        @pl.loop(0, size // 32)
        def _(r):
            at = pl.ds(pl.multiple_of(chunk * size + r * 32, 32), 32)
            x_f = x_v[at, :].astype(F32)
            normed = x_f * lax.rsqrt(jnp.mean(x_f * x_f, axis=-1, keepdims=True) + NORM_EPS)
            h_v[at, :] = (normed * gain).astype(BF16)

        gather_h.start(chunk)
    for copy in positions:
        copy.start()
    own_h = pltpu.make_async_copy(h_v, gather_h.block(near.me, 0, CHUNKS), own_sems.at[0])
    own_h.start()
    w_loads, col = [], 0
    for n, (ref, count) in enumerate(((wq_ref, q_cols), (wk_ref, HEAD_DIM), (wv_ref, HEAD_DIM))):
        at = pl.ds(pl.multiple_of(near.me * count, HEAD_DIM), count)
        w_loads.append(pltpu.make_async_copy(ref.at[:, at], w_v.at[:, pl.ds(col, count)], w_sems.at[n]))
        col += count
    w_loads.append(pltpu.make_async_copy(wo_ref.at[pl.ds(pl.multiple_of(near.me * q_cols, q_cols), q_cols), :], wo_v, w_sems.at[3]))
    stage_in = pltpu.make_async_copy(dy_ref, x_v, own_sems.at[1])
    stage_out = pltpu.make_async_copy(x_v, gather_dy.block(near.me, 0, CHUNKS), own_sems.at[2])
    for load in w_loads + [stage_in]:
        load.start()
    for copy in positions:
        copy.wait()
    sign = jnp.where(lax.broadcasted_iota(jnp.int32, (1, HEAD_DIM), 1) < HALF, -1.0, 1.0)

    @pl.loop(0, n_blocks)
    def _(b):
        pos = jnp.broadcast_to(pos_all[b, 0:1, :].astype(F32), (HEAD_DIM, rows)).T
        angles = pos * freq_ref[...]
        cos_s[b] = jnp.cos(angles)
        sin_s[b] = jnp.sin(angles) * sign

    gather_h.middle()
    gather_h.late()
    for chunk in range(CHUNKS):
        gather_dy.start(chunk)
    for load in w_loads + [stage_in]:
        load.wait()
    stage_out.start()
    own_h.wait()
    gather_h.end()

    def block_load(ref, block, slot):
        return pltpu.make_async_copy(ref.at[pl.ds(pl.multiple_of(block * rows, rows), rows), :], blk.at[slot], blk_sems.at[slot])

    def fwd_chunk(i, c, carry, diagonal):
        k_c, vt_c = k_s[c], vt[c]
        scores = [dot(k_c, q_s[i, :, cols[a]], COLS_COLS) * to_log2 for a in range(heads)]
        out = []
        for a in range(heads):
            s = masked(scores[a]) if diagonal else scores[a]
            m_old, l_old = carry[a]
            m_new = jnp.maximum(m_old, jnp.max(s, axis=0, keepdims=True))
            alpha = jnp.exp2(m_old - m_new)
            p = jnp.exp2(s - m_new)
            l_new = l_old * alpha + jnp.sum(p, axis=0, keepdims=True)
            acc[a] = acc[a] * alpha + dot(vt_c, p.astype(BF16))
            out.append((m_new, l_new))
        return tuple(out)

    def ht_store(i):
        at = pl.ds(pl.multiple_of(i * rows, rows), rows)
        return pltpu.make_async_copy(ht_v.at[lax.rem(i, 2)], ht_ref.at[:, at], ht_sems.at[lax.rem(i, 2)])

    block_load(h_all, 0, 0).start()

    @pl.loop(0, n_blocks)
    def _(i):
        slot = lax.rem(i, 2)
        block_load(h_all, i, slot).wait()

        @pl.when(i + 1 < n_blocks)
        def _():
            block_load(h_all, i + 1, 1 - slot).start()

        @pl.when(i >= 2)
        def _():
            ht_store(i - 2).wait()

        ht_v[slot] = blk[slot].T
        ht_store(i).start()
        prod = dot(blk[slot], w_v[...])
        cos_t, sin_t = cos_s[i], sin_s[i]
        for a in range(heads + 1):
            val = prod[:, a * HEAD_DIM:(a + 1) * HEAD_DIM]
            rot = (val * cos_t + pltpu.roll(val, HALF, 1) * sin_t).astype(BF16)
            if a < heads:
                q_s[i, :, cols[a]] = rot
            else:
                k_s[i] = rot
                kt[i] = rot.T
        v_i = prod[:, q_cols + HEAD_DIM:].astype(BF16)
        v_s[i] = v_i
        vt[i] = v_i.T
        acc[...] = jnp.zeros_like(acc)
        start = tuple((jnp.full((1, rows), NEG_LARGE, F32), jnp.zeros((1, rows), F32)) for _ in range(heads))
        carry = lax.fori_loop(0, i, lambda c, carry: fwd_chunk(i, c, carry, False), start)
        carry = fwd_chunk(i, i, carry, True)
        at = pl.ds(pl.multiple_of(i * rows, rows), rows)
        for a in range(heads):
            m_a, l_a = carry[a]
            ot_s[cols[a], at] = (acc[a] / l_a).astype(BF16)
            lse_s[i, a:a + 1, :] = m_a + jnp.log2(l_a)

        @pl.when(i == FWD_MIDDLE)
        def _():
            gather_dy.middle()

        @pl.when(i == FWD_LATE)
        def _():
            gather_dy.late()

    for chunk in range(CHUNKS):
        gather_o.start(chunk)
    own_o = pltpu.make_async_copy(ot_s, gather_o.block(near.me, 0, CHUNKS), own_sems.at[0])
    own_o.start()

    def bwd_chunk(i, c, delta, diagonal):
        k_c, v_c, kt_c = k_s[c], v_s[c], kt[c]
        dk_c = dv_c = None
        for a in range(heads):
            q_a, do_a = q_s[i, :, cols[a]], do_s[i, :, cols[a]]
            s = dot(k_c, q_a, COLS_COLS) * to_log2
            if diagonal:
                s = masked(s)
            p = jnp.exp2(s - lse_s[i, a:a + 1, :])
            d_p = dot(v_c, do_a, COLS_COLS)
            d_s = (p * (d_p - delta[a])).astype(BF16)
            dv_a = dot(p.astype(BF16), do_a)
            dk_a = dot(d_s, q_a)
            dv_c = dv_a if dv_c is None else dv_c + dv_a
            dk_c = dk_a if dk_c is None else dk_c + dk_a
            acc[a] += dot(kt_c, d_s)
        dk_acc[c] += dk_c
        dv_acc[c] += dv_c

    def dq_stores(r):
        slot = lax.rem(r, 2)
        at = pl.ds(pl.multiple_of(near.across(r) * rows, rows), rows)
        last = q_cols - HEAD_DIM
        return [pltpu.make_async_copy(dq_v.at[slot, :, pl.ds(0, last)], dq_a_ref.at[at, :], dq_sems.at[slot, 0]),
                pltpu.make_async_copy(dq_v.at[slot, :, pl.ds(last, HEAD_DIM)], dq_b_ref.at[at, :], dq_sems.at[slot, 1])]

    def pass_on(done):
        @pl.when(done == BWD_MIDDLE)
        def _():
            gather_o.middle()

    for i in (n_blocks - 2, n_blocks - 1):
        ht_store(i).wait()
    dk_acc[...] = jnp.zeros_like(dk_acc)
    dv_acc[...] = jnp.zeros_like(dv_acc)
    stage_out.wait()
    block_load(dy_all, near.me, 0).start()

    def bwd_block(r, done):
        i = near.across(r)
        slot = lax.rem(r, 2)
        at = pl.ds(pl.multiple_of(i * rows, rows), rows)

        @pl.when(r == 1)
        def _():
            gather_dy.end_sib()

        @pl.when(r == 2)
        def _():
            gather_dy.end_near()

        @pl.when(r == n_blocks * 3 // 4)
        def _():
            gather_dy.end_far()

        waits = [r == first for first in (1, 2, n_blocks * 3 // 4)]
        @pl.when(functools.reduce(jnp.logical_or, waits))
        def _():
            block_load(dy_all, i, slot).start()

        block_load(dy_all, 0, slot).wait()

        @pl.when(functools.reduce(jnp.logical_and, [r + 1 != first for first in (1, 2, n_blocks * 3 // 4, n_blocks)]))
        def _():
            block_load(dy_all, near.across(r + 1), 1 - slot).start()

        do_s[i] = dot(blk[slot], wo_v[...], COLS_COLS).astype(BF16)
        acc[...] = jnp.zeros_like(acc)
        delta = [jnp.sum(ot_s[cols[a], at].astype(F32) * do_s[i, :, cols[a]].T.astype(F32), axis=0, keepdims=True) for a in range(heads)]

        @pl.loop(0, i)
        def _(c):
            bwd_chunk(i, c, delta, False)
            pass_on(done + c)

        bwd_chunk(i, i, delta, True)
        pass_on(done + i)

        @pl.when(r >= 2)
        def _():
            for store in dq_stores(r - 2):
                store.wait()

        for a in range(heads):
            dq_v[slot, :, cols[a]] = unrotate(acc[a].T * qk_scale, cos_s[i], sin_s[i])
        for store in dq_stores(r):
            store.start()
        return done + i + 1

    lax.fori_loop(0, n_blocks, bwd_block, jnp.int32(0))
    gather_o.late()
    for r in (n_blocks - 2, n_blocks - 1):
        for store in dq_stores(r):
            store.wait()
    for chunk in range(CHUNKS):
        gather_next.start(chunk)

    @pl.loop(0, n_blocks)
    def _(c):
        at = pl.ds(pl.multiple_of(c * rows, rows), rows)
        dkv_v[at, :HEAD_DIM] = unrotate(dk_acc[c] * qk_scale, cos_s[c], sin_s[c])
        dkv_v[at, HEAD_DIM:] = dv_acc[c].astype(BF16)

    dkv_store = pltpu.make_async_copy(dkv_v, dkv_ref, own_sems.at[1])
    dkv_store.start()
    own_o.wait()
    gather_o.end()
    dkv_store.wait()


def lanes(*parts):
    return jnp.concatenate(parts, axis=1)


def products_part(heads, near, gathers, ot_ref, ht_ref, dy_ref, d_kv_ref, d_qa_ref, d_qb_ref, x_ref, own_dy_ref, gain_ref, wo_ref, wk_ref, wv_ref, wq_ref,
                  wo_out, wq_out, kv_all, qa_all, qb_all, res_ref, gx_ref, gg_ref, gg_row, gg_all, gg_sems, x_sems,
                  a_buf, b_buf, tile, a_sem, b_sems, t_sems, stage, stage_sems, ot_v, o_v, x_v, io_sems, own, own_sems, w_v, w_sems, acc,
                  gg_v):
    core = lax.rem(near.me, 2)
    half = a_buf.shape[0]
    seq_len = d_kv_ref.shape[0]
    rows, width = x_ref.shape
    n_cols = d_kv_ref.shape[1]
    n_o, n_all = width // (2 * n_cols), x_sems.shape[1]
    n_oa = n_o + (n_all - n_o) * 2 // 3

    local = (d_qa_ref, d_qb_ref, d_kv_ref)

    def stage_in(n):
        return pltpu.make_async_copy(local[n], stage.at[:, pl.ds(0, local[n].shape[1])], stage_sems.at[0])

    def stage_out(n):
        return pltpu.make_async_copy(stage.at[:, pl.ds(0, local[n].shape[1])], gathers[n].block(near.me, 0, CHUNKS), stage_sems.at[1])

    def copy_own(n):
        stage_in(n).wait()
        stage_out(n).start()

    own_rows = pl.ds(pl.multiple_of(core * half, half), half)
    tokens = pl.ds(pl.multiple_of(near.me * rows, rows), rows)
    ot_load = pltpu.make_async_copy(ot_ref.at[:, tokens], ot_v, io_sems.at[0])
    x_load = pltpu.make_async_copy(x_ref, x_v, io_sems.at[1])
    res_store = pltpu.make_async_copy(x_v, res_ref, io_sems.at[2])
    dy_load = pltpu.make_async_copy(own_dy_ref, o_v, io_sems.at[3])
    gx_store = pltpu.make_async_copy(o_v, gx_ref, io_sems.at[0])

    def a_load(ref):
        return pltpu.make_async_copy(ref.at[own_rows, :], a_buf, a_sem)

    def b_loads(source, p, slot, g):
        if source is dy_ref:
            srcs = [dy_ref.at[:, pl.ds(pl.multiple_of((2 * p + g) * n_cols, n_cols), n_cols)]]
        else:
            per = n_cols // source.shape[1]
            srcs = [source.at[pl.ds(pl.multiple_of(((2 * p + g) * per + n) * seq_len, seq_len), seq_len), :] for n in range(per)]
        return [pltpu.make_async_copy(src, b_buf.at[slot, :, pl.ds(g * n_cols + n * src.shape[1], src.shape[1])], b_sems.at[slot, g])
                for n, src in enumerate(srcs)]

    def start_b(step):
        slot = lax.rem(step, 2)
        for source, low, high in ((dy_ref, 0, n_o), (qa_all, n_o, n_oa), (qb_all, n_oa, n_all)):
            @pl.when(jnp.logical_and(step >= low, step < high))
            def _():
                for g in range(2):
                    for load in b_loads(source, step - low, slot, g):
                        load.start()

    def pieces(kind, step):
        wide = (2 * n_cols, n_cols, HEAD_DIM)[kind]
        slot = lax.rem(step, 2)
        out = []
        for n in range(2 * n_cols // wide):
            group = (step - (0, n_o, n_oa)[kind]) * (2 * n_cols // wide) + n
            col = (group * wide, group * heads * HEAD_DIM, (group + 1) * heads * HEAD_DIM - HEAD_DIM)[kind]
            dst = (wo_out, wq_out, wq_out)[kind].at[own_rows, pl.ds(pl.multiple_of(col, HEAD_DIM), wide)]
            src = tile.at[slot, :, pl.ds(n * wide, wide)]
            out.append((pltpu.make_async_copy(src, dst, t_sems.at[slot]), send(src, dst, x_sems, step, near.sib)))
        return out

    def start_tile(step):
        for kind, (low, high) in enumerate(((0, n_o), (n_o, n_oa), (n_oa, n_all))):
            @pl.when(jnp.logical_and(step >= low, step < high))
            def _():
                for keep, give in pieces(kind, step):
                    keep.start()
                    give.start()

    def whole_tile(step):
        slot = lax.rem(step, 2)
        dst = wo_out.at[own_rows, pl.ds(0, 2 * n_cols)]
        return pltpu.make_async_copy(tile.at[slot], dst, t_sems.at[slot]), send(tile.at[slot], dst, x_sems, step, near.sib)

    def wait_tile(step):
        keep, give = whole_tile(step)
        keep.wait()
        give.wait_send()

    def result_part():
        cols = b_buf.shape[2]

        def w_load(n):
            slot = lax.rem(n, 2)
            return pltpu.make_async_copy(wo_ref.at[:, pl.ds(pl.multiple_of(n * cols, cols), cols)], b_buf.at[slot, pl.ds(0, wo_ref.shape[0]), :],
                                         b_sems.at[slot, 0])

        w_load(jnp.int32(0)).start()
        ot_load.wait()

        @pl.loop(0, ot_v.shape[0] // BLK)
        def _(r):
            at = pl.ds(pl.multiple_of(r * BLK, BLK), BLK)
            o_v[:, at] = ot_v[at, :].T

        x_load.wait()

        @pl.loop(0, n_o)
        def _(n):
            w_load(n).wait()

            @pl.when(n + 1 < n_o)
            def _():
                w_load(n + 1).start()

            at = pl.ds(pl.multiple_of(n * cols, cols), cols)
            x_v[:, at] = (x_v[:, at].astype(F32) + dot(o_v[...], b_buf[lax.rem(n, 2), :wo_ref.shape[0], :])).astype(BF16)

        res_store.start()

    def hidden_parts(kind):
        count = own.shape[0] // (2 if kind == 1 else 1)

        def own_load(r, g):
            source = (qa_all, qb_all, kv_all)[kind]
            device, col = (2 * r + g, 0) if kind == 1 else (near.across(r), g * HEAD_DIM)
            at = pl.ds(pl.multiple_of(device * seq_len + near.me * rows, rows), rows)
            return pltpu.make_async_copy(source.at[at, pl.ds(col, HEAD_DIM)], own.at[r, :, pl.ds(g * HEAD_DIM, HEAD_DIM)], own_sems.at[r, g])

        def w_load(r, g):
            source = (wk_ref, wv_ref)[g] if kind == 2 else wq_ref
            col = near.across(r) if kind == 2 else heads * near.across(r) + g if kind == 0 else heads * (2 * r + g + 1) - 1
            slot = lax.rem(r, 2)
            return pltpu.make_async_copy(source.at[:, pl.ds(pl.multiple_of(col * HEAD_DIM, HEAD_DIM), HEAD_DIM)],
                                         w_v.at[slot, :, pl.ds(g * HEAD_DIM, HEAD_DIM)], w_sems.at[slot, g])

        return count, own_load, w_load

    def hidden_start(kind, low=0, high=None):
        count, own_load, w_load = hidden_parts(kind)
        for g in range(2):
            if low == 0:
                w_load(jnp.int32(0), g).start()

            @pl.loop(low, high or count)
            def _(r):
                own_load(r, g).start()

    def hidden_add(kind, low=0, high=None):
        count, own_load, w_load = hidden_parts(kind)

        @pl.loop(low, high or count)
        def _(r):
            for g in range(2):
                w_load(r, g).wait()
                own_load(r, g).wait()

            @pl.when(r + 1 < count)
            def _():
                for g in range(2):
                    w_load(r + 1, g).start()

            for col in range(0, width, width // PARTS):
                at = slice(col, col + width // PARTS)
                acc[:, at] += dot(own[r], w_v[lax.rem(r, 2), at, :], COLS_COLS)

    a_load(ot_ref).start()
    start_b(jnp.int32(0))
    stage_in(0).start()
    ot_load.start()
    x_load.start()
    a_load(ot_ref).wait()

    @pl.loop(0, n_all)
    def _(step):
        slot = lax.rem(step, 2)
        for g in range(2):
            b_loads(dy_ref, 0, slot, g)[0].wait()

        @pl.when(jnp.logical_and(step != n_o - 1, step != n_oa - 1))
        def _():
            start_b(step + 1)

        @pl.when(step >= 2)
        def _():
            wait_tile(step - 2)

        @pl.when(step == n_o)
        def _():
            a_load(ht_ref).wait()

        for r in range(0, half, half // PARTS):
            tile[slot, r:r + half // PARTS, :] = dot(a_buf[r:r + half // PARTS, :], b_buf[slot])
        start_tile(step)

        @pl.when(step == n_o - 3)
        def _():
            acc[...] = jnp.zeros_like(acc)
            copy_own(0)
            gathers[0].middle()

        @pl.when(step == n_o - 1)
        def _():
            a_load(ht_ref).start()
            gathers[0].late()
            for c in range(CHUNKS):
                gathers[1].start(c)
            stage_out(0).wait()
            stage_in(1).start()
            result_part()
            gathers[0].end()
            start_b(step + 1)
            hidden_start(0)

        @pl.when(step == n_oa - 3)
        def _():
            copy_own(1)
            gathers[1].middle()

        @pl.when(step == n_oa - 2)
        def _():
            gathers[1].late()
            for c in range(CHUNKS):
                gathers[2].start(c)
            stage_out(1).wait()
            stage_in(2).start()

        @pl.when(step == n_oa - 1)
        def _():
            res_store.wait()
            x_load.start()
            dy_load.start()
            gathers[1].end()
            start_b(step + 1)
            hidden_add(0)
            hidden_start(1)

    hidden_add(1)
    copy_own(2)
    gathers[2].middle()
    gathers[2].late()
    stage_out(2).wait()
    gathers[2].end_sib()
    gathers[2].end_near()
    near_count = own.shape[0] * 3 // 4
    hidden_start(2, 0, near_count)
    for step in (n_all - 2, n_all - 1):
        wait_tile(jnp.int32(step))
    hidden_add(2, 0, near_count)
    gathers[2].end_far()
    hidden_start(2, near_count)
    hidden_add(2, near_count)

    gain = gain_ref[...].astype(F32)
    gg_v[...] = jnp.zeros_like(gg_v)
    x_load.wait()
    dy_load.wait()

    @pl.loop(0, rows // 32)
    def _(r):
        at = pl.ds(pl.multiple_of(r * 32, 32), 32)
        x_f = x_v[at, :].astype(F32)
        inv_rms = lax.rsqrt(jnp.mean(x_f * x_f, axis=-1, keepdims=True) + NORM_EPS)
        normed = x_f * inv_rms
        d_hid = acc[at, :]
        both = d_hid * normed
        gg_v[...] += jnp.sum(both.reshape(4, 8, width), axis=0)
        mean = jnp.mean(both * gain, axis=-1, keepdims=True)
        o_v[at, :] = (o_v[at, :].astype(F32) + inv_rms * (d_hid * gain - normed * mean)).astype(BF16)

    gg_row[...] = jnp.sum(gg_v[...], axis=0, keepdims=True)
    gg_all[near.me] = gg_row[...]
    parts = [send(gg_row, gg_all.at[near.me], gg_sems, r, peer) for r, peer in enumerate(near.others())]
    for copy in parts:
        copy.start()
    gx_store.start()

    @pl.loop(0, n_all)
    def _(step):
        whole_tile(step)[1].wait_recv()

    for copy in parts:
        copy.wait()
    gg_ref[...] = jnp.sum(gg_all[...], axis=0)
    gx_store.wait()


def step_kernel(heads, first_scratch, second_scratch, x_ref, gain_ref, pos_ref, freq_ref, dy_ref, wq_ref, wk_ref, wv_ref, wo_ref,
                h_all, dy_all, o_all, ht, d_kv, d_qa, d_qb, wo_out, wq_out, kv_all, qa_all, qb_all, res, gx, gg,
                pos_all, pos_sems, gg_row, gg_all, gg_sems, x_sems, h_sems, dy_sems, o_sems, kv_sems, qa_sems, qb_sems):
    near = Neighbours()
    seq_len = d_kv.shape[0]

    def gather_of(src, dst, sems):
        return Gather(near, lambda c: src.at[pl.ds(c * (seq_len // CHUNKS), seq_len // CHUNKS), :], dst, seq_len, sems)

    gathers = [gather_of(d_qa, qa_all, qa_sems), gather_of(d_qb, qb_all, qb_sems), gather_of(d_kv, kv_all, kv_sems)]

    def first(*scratch):
        attention_part(heads, near, gathers[0], x_ref, gain_ref, pos_ref, freq_ref, dy_ref, wq_ref, wk_ref, wv_ref, wo_ref,
                       h_all, dy_all, o_all, ht, d_kv, d_qa, d_qb, pos_all, pos_sems, h_sems, dy_sems, o_sems, *scratch)

    def second(*scratch):
        products_part(heads, near, gathers, o_all, ht, dy_all, d_kv, d_qa, d_qb, x_ref, dy_ref, gain_ref, wo_ref, wk_ref, wv_ref, wq_ref,
                      wo_out, wq_out, kv_all, qa_all, qb_all, res, gx, gg, gg_row, gg_all, gg_sems, x_sems, *scratch)

    pl.run_scoped(first, *first_scratch)
    pl.run_scoped(second, *second_scratch)


def step(x, gain, positions, grad_out, w_q, w_k, w_v, w_o, sp_size, heads):
    rows, width = x.shape
    seq_len = rows * sp_size
    q_cols = heads * HEAD_DIM
    all_cols = q_cols * sp_size
    half = width // 2
    cols = 4 * HEAD_DIM
    n_all = (width + all_cols) // cols
    any_spec = pl.BlockSpec(memory_space=pl.ANY)
    vmem = pl.BlockSpec(memory_space=pltpu.VMEM)
    dma = pltpu.SemaphoreType.DMA
    inv_freq = ROPE_THETA ** (-np.arange(0, HEAD_DIM, 2) / HEAD_DIM)
    freq = jnp.asarray(np.concatenate([inv_freq, inv_freq])[None, :], F32)
    pairs = heads * seq_len * (seq_len + rows) // 2
    out = lambda *shape, dtype=BF16: jax.ShapeDtypeStruct(shape, dtype)
    array = lambda *shape, dtype=BF16: pltpu.VMEM(shape, dtype)
    blocks = lambda *shape, dtype=BF16: pltpu.VMEM((sp_size,) + shape, dtype)
    first_scratch = [array(rows, width), array(rows, width), dma((CHUNKS,)), dma((3,)), blocks(rows, HEAD_DIM, dtype=F32),
                     blocks(rows, HEAD_DIM, dtype=F32), array(width, q_cols + 2 * HEAD_DIM), array(q_cols, width), dma((4,)),
                     array(2, rows, width), dma((2,)), array(2, width, rows), dma((2,)),
                     blocks(rows, q_cols), blocks(rows, HEAD_DIM), blocks(rows, HEAD_DIM), blocks(HEAD_DIM, rows), blocks(HEAD_DIM, rows),
                     array(q_cols, seq_len), blocks(8, rows, dtype=F32), array(heads, HEAD_DIM, rows, dtype=F32),
                     blocks(rows, q_cols), blocks(rows, HEAD_DIM, dtype=F32), blocks(rows, HEAD_DIM, dtype=F32),
                     array(2, rows, q_cols), dma((2, 2)), array(seq_len, 2 * HEAD_DIM)]
    second_scratch = [array(half, seq_len), array(2, seq_len, cols), array(2, half, cols, dtype=F32), dma, dma((2, 2)), dma((2,)),
                      array(seq_len, 2 * HEAD_DIM), dma((2,)), array(all_cols, rows), array(rows, all_cols), array(rows, width),
                      dma((4,)), blocks(rows, 2 * HEAD_DIM), dma((sp_size, 2)), array(2, width, 2 * HEAD_DIM), dma((2, 2)),
                      array(rows, width, dtype=F32), array(8, width, dtype=F32)]
    return pl.pallas_call(
        functools.partial(step_kernel, heads, first_scratch, second_scratch),
        in_specs=[any_spec, vmem, vmem, vmem] + [any_spec] * 5,
        out_specs=[any_spec] * 14 + [vmem],
        out_shape=[out(seq_len, width), out(seq_len, width), out(all_cols, seq_len), out(width, seq_len), out(seq_len, 2 * HEAD_DIM),
                   out(seq_len, q_cols - HEAD_DIM), out(seq_len, HEAD_DIM), out(all_cols, width, dtype=F32), out(width, all_cols, dtype=F32),
                   out(sp_size * seq_len, 2 * HEAD_DIM), out(sp_size * seq_len, q_cols - HEAD_DIM), out(sp_size * seq_len, HEAD_DIM),
                   out(rows, width), out(rows, width), out(1, width, dtype=F32)],
        scratch_shapes=[blocks(8, rows, dtype=jnp.int32), dma((2, 7)), array(1, width, dtype=F32), blocks(1, width, dtype=F32), dma((2, 7)),
                        dma((2, n_all))] + [SEMS] * 6,
        compiler_params=pltpu.CompilerParams(vmem_limit_bytes=VMEM_LIMIT, collective_id=0, has_side_effects=True),
        cost_estimate=pl.CostEstimate(flops=28 * pairs * HEAD_DIM + 2 * half * cols * seq_len * n_all, bytes_accessed=20 * seq_len * width,
                                      transcendentals=2 * pairs),
        name="step",
    )(x, gain, positions.reshape(1, -1), freq, grad_out, w_q, w_k, w_v, w_o)


def finish_kernel(ht_ref, d_ref, gx_in, res_in, gg_in, wo_in, wq_in, wk_ref, wv_ref, wq_ref, wo_ref, gx_ref, res_ref, gg_ref, d_v, d_sems, ring, ring_sems):
    step = pl.program_id(0) * pl.num_programs(1) + pl.program_id(1)
    high = ring.shape[2]
    per_array = wo_in.shape[0] // (high * RING)

    def copy_in(src, g, n):
        at = pl.ds(pl.multiple_of((lax.rem(g, per_array) * RING + n) * high, high), high)
        return pltpu.make_async_copy(src.at[at, :], ring.at[lax.rem(g, DEPTH), n], ring_sems.at[0, lax.rem(g, DEPTH), n])

    def copy_out(dst, g, n):
        at = pl.ds(pl.multiple_of((lax.rem(g, per_array) * RING + n) * high, high), high)
        return pltpu.make_async_copy(ring.at[lax.rem(g, DEPTH), n], dst.at[at, :], ring_sems.at[1, lax.rem(g, DEPTH), n])

    def start(copy, first, second, g):
        for ref, mine in ((first, g < per_array), (second, g >= per_array)):
            @pl.when(mine)
            def _():
                for n in range(RING):
                    copy(ref, g, n).start()

    def pair_load(p):
        at = pl.ds(2 * p, 2)
        return pltpu.make_async_copy(d_ref.at[at], d_v.at[at], d_sems.at[p])

    @pl.when(step == 0)
    def _():
        for p in range(d_v.shape[0] // 2):
            pair_load(p).start()

    last = pl.num_programs(0) * pl.num_programs(1) - 1

    def free(g):
        for n in range(RING):
            copy_out(wo_ref, g, n).wait()

    def pass_on(g):
        for n in range(RING):
            copy_in(wo_in, g, n).wait()
        start(copy_out, wo_ref, wq_ref, g)

    @pl.when(step >= DEPTH)
    def _():
        free(step - DEPTH)

    start(copy_in, wo_in, wq_in, step)

    @pl.when(step >= 1)
    def _():
        pass_on(step - 1)

    for p in range(d_v.shape[0] // 2):
        @pl.when(step == p)
        def _():
            pair_load(p).wait()

    ht = ht_ref[...]
    pair = 2 * pl.program_id(1)
    wk_ref[...] = dot(ht, lanes(d_v[pair, :, :HEAD_DIM], d_v[pair + 1, :, :HEAD_DIM]))
    wv_ref[...] = dot(ht, lanes(d_v[pair, :, HEAD_DIM:], d_v[pair + 1, :, HEAD_DIM:]))

    @pl.when(step == 0)
    def _():
        gg_ref[...] = gg_in[...]

    @pl.when(step == last)
    def _():
        pass_on(last)
        for back in range(DEPTH):
            free(last - back)

    @pl.when(step < ROW_STEPS)
    def _():
        gx_ref[...] = gx_in[...]
        res_ref[...] = res_in[...]


def finish(ht, d_kv, w_o_grad, w_q_grad, grad_x, result, grad_gain):
    width, seq_len = ht.shape
    groups = d_kv.shape[0]
    n_j = groups // 2
    steps = (width // MROWS) * n_j
    high = width // COPY_ROWS
    assert w_o_grad.shape[0] + w_q_grad.shape[0] == high * RING * steps
    any_spec = pl.BlockSpec(memory_space=pl.ANY)
    rows = pl.BlockSpec((grad_x.shape[0] // ROW_STEPS, width), lambda m, j: (jnp.minimum(m * n_j + j, ROW_STEPS - 1), 0))
    whole = pl.BlockSpec((1, width), lambda m, j: (0, 0))
    kv_out = pl.BlockSpec((MROWS, 2 * HEAD_DIM), lambda m, j: (m, j))
    out = lambda cols: jax.ShapeDtypeStruct((width, cols), F32)
    like = lambda val: jax.ShapeDtypeStruct(val.shape, val.dtype)
    return pl.pallas_call(
        finish_kernel,
        grid=(width // MROWS, n_j),
        in_specs=[pl.BlockSpec((MROWS, seq_len), lambda m, j: (m, 0)), any_spec, rows, rows, whole, any_spec, any_spec],
        out_specs=[kv_out, kv_out, any_spec, any_spec, rows, rows, whole],
        out_shape=[out(groups * HEAD_DIM), out(groups * HEAD_DIM), like(w_q_grad), like(w_o_grad), like(grad_x), like(result), like(grad_gain)],
        scratch_shapes=[pltpu.VMEM(d_kv.shape, BF16), pltpu.SemaphoreType.DMA((groups // 2,)),
                        pltpu.VMEM((DEPTH, RING, high, width), F32), pltpu.SemaphoreType.DMA((2, DEPTH, RING))],
        compiler_params=params(2),
        cost_estimate=pl.CostEstimate(flops=4 * width * seq_len * groups * HEAD_DIM, bytes_accessed=2 * width * seq_len, transcendentals=0),
        name="finish",
    )(ht, d_kv, grad_x, result, grad_gain, w_o_grad, w_q_grad)


def solution(mesh):
    sp_size = mesh.shape['sp']
    seq_spec = P(('dp', 'sp'), None)
    pos_spec = P(('dp', 'sp'))
    replicated = P(None, None)
    part_rows = P('dp', None)

    def local_step(x, grad_out, positions, gain, w_q, w_k, w_v, w_o):
        n_heads = w_q.shape[1] // HEAD_DIM
        heads = n_heads // sp_size
        _, _, _, ht, _, _, _, w_o_grad, w_q_grad, kv_all, _, _, result, grad_x, grad_gain = step(
            x, gain.reshape(1, -1), positions, grad_out, w_q, w_k, w_v, w_o, sp_size, heads)
        grad_wk, grad_wv, grad_wq, grad_wo, grad_x, result, grad_gain = finish(
            ht, kv_all.reshape(sp_size, -1, 2 * HEAD_DIM), w_o_grad, w_q_grad, grad_x, result, grad_gain)
        return result, grad_x, grad_wq, grad_wk, grad_wv, grad_wo, grad_gain.reshape(-1)

    return jax.shard_map(local_step, mesh=mesh,
                         in_specs=(seq_spec, seq_spec, pos_spec, P(None), replicated, replicated, replicated, replicated),
                         out_specs=(seq_spec, seq_spec, part_rows, part_rows, part_rows, part_rows, P('dp')),
                         check_vma=False)
```

```python
import functools

import jax
import jax.numpy as jnp
import numpy as np
from jax import lax
from jax.experimental import pallas as pl
from jax.experimental.pallas import tpu as pltpu
from jax.sharding import PartitionSpec as P

HEAD_DIM = 128
HALF = HEAD_DIM // 2
ROPE_THETA = 1000000.0
NORM_EPS = 1e-05
NEG_LARGE = -1e30
LOG2E = 1.4426950408889634
BLK = 512
CHUNKS = 4
FWD_MIDDLE, BWD_MIDDLE = 5, 27
MROWS = 768
RING = 3
DEPTH = 3
COPY_ROWS = 24
PARTS = 3
ROW_STEPS = 8
F32 = jnp.float32
BF16 = jnp.bfloat16
ROWS_ROWS = (((0,), (0,)), ((), ()))
COLS_COLS = (((1,), (1,)), ((), ()))
ROWS_COLS = (((0,), (1,)), ((), ()))
VMEM_LIMIT = 63 * 1024 * 1024


def dot(a, b, dims=(((1,), (0,)), ((), ()))):
    return lax.dot_general(a, b, dims, preferred_element_type=F32)


def params(axes=1):
    return pltpu.CompilerParams(dimension_semantics=("arbitrary",) * axes, vmem_limit_bytes=VMEM_LIMIT)


class Neighbours:
    def __init__(self):
        self.me = lax.axis_index('sp')
        core, col, row = lax.rem(self.me, 2), lax.rem(self.me // 2, 2), self.me // 4
        self.sib = self.me + 1 - 2 * core
        self.xn = self.me + 2 - 4 * col
        self.yn = self.me + 4 - 8 * row
        self.diag = self.xn + self.yn - self.me

    def meet(self, peers):
        barrier = pltpu.get_barrier_semaphore()
        for peer in peers:
            pl.semaphore_signal(barrier, inc=1, device_id={'sp': peer}, device_id_type=pl.DeviceIdType.MESH)
        pl.semaphore_wait(barrier, len(peers))

    def across(self, r):
        core, col, row = lax.rem(self.me, 2), lax.rem(self.me // 2, 2), self.me // 4
        return (self.me + lax.rem(r, 2) * (1 - 2 * core) + lax.rem(r // 2, 2) * (2 - 4 * col) + (r // 4) * (4 - 8 * row))

    def others(self):
        flip = lambda dev: dev + 1 - 2 * lax.rem(dev, 2)
        return [self.sib, self.xn, flip(self.xn), self.yn, flip(self.yn), self.diag, flip(self.diag)]


def send(src, dst, sems, index, peer):
    return pltpu.make_async_remote_copy(src_ref=src, dst_ref=dst, send_sem=sems.at[0, index], recv_sem=sems.at[1, index],
                                        device_id={'sp': peer}, device_id_type=pl.DeviceIdType.MESH)


class Gather:
    COPIES = 22

    def __init__(self, near, own, dst, rows, sems):
        self.near, self.own, self.dst, self.rows, self.sems = near, own, dst, rows, sems

    def block(self, dev, chunk, count=1):
        size = self.rows // CHUNKS
        return self.dst.at[pl.ds(pl.multiple_of(dev * self.rows + chunk * size, size), count * size), :]

    def first(self, chunk, kind):
        peer = (self.near.xn, self.near.yn, self.near.sib)[kind]
        return send(self.own(chunk), self.block(self.near.me, chunk), self.sems, kind * CHUNKS + chunk, peer)

    def onward(self, chunk):
        over_y = chunk < CHUNKS // 2
        rows = self.block(self.near.xn if over_y else self.near.yn, chunk)
        return send(rows, rows, self.sems, 12 + chunk, self.near.yn if over_y else self.near.xn)

    def share(self, kind):
        rows = self.block((self.near.xn, self.near.yn)[kind], 0, CHUNKS)
        return send(rows, rows, self.sems, 16 + kind, self.near.sib)

    def share_diag(self, chunk):
        rows = self.block(self.near.diag, chunk)
        return send(rows, rows, self.sems, 18 + chunk, self.near.sib)

    def start(self):
        for chunk in range(CHUNKS):
            for kind in (0, 1):
                self.send_first(chunk, kind)
            self.first(chunk, 2).start()

    def send_first(self, turn, kind):
        self.first(turn if kind == 0 else (turn + CHUNKS // 2) % CHUNKS, kind).start()

    def middle(self):
        for chunk in (0, 2, 1, 3):
            self.first(chunk, 0 if chunk < CHUNKS // 2 else 1).wait_recv()
            self.onward(chunk).start()

    def late(self):
        for chunk in (2, 3):
            self.first(chunk, 0).wait_recv()
        self.share(0).start()
        for chunk in (0, 1):
            self.first(chunk, 1).wait_recv()
        self.share(1).start()

    def end_sib(self):
        for chunk in range(CHUNKS):
            self.first(chunk, 2).wait_recv()

    def end_near(self):
        for kind in range(2):
            self.share(kind).wait_recv()

    def end_far(self, between=None):
        for chunk in (0, 2, 1, 3):
            self.onward(chunk).wait_recv()
            self.share_diag(chunk).start()
            if chunk == 2 and between:
                between()
        for chunk in range(CHUNKS):
            for kind in range(3):
                self.first(chunk, kind).wait_send()
            self.onward(chunk).wait_send()
        for kind in range(2):
            self.share(kind).wait_send()
        for chunk in range(CHUNKS):
            self.share_diag(chunk).wait()

    def end(self, between=None):
        self.end_sib()
        self.end_near()
        self.end_far(between)


SEMS = pltpu.SemaphoreType.DMA((2, Gather.COPIES))


def masked(scores):
    key = lax.broadcasted_iota(jnp.int32, scores.shape, 0)
    query = lax.broadcasted_iota(jnp.int32, scores.shape, 1)
    return jnp.where(key <= query, scores, NEG_LARGE)


def unrotate(val, cos_t, sin_t):
    return (val * cos_t - pltpu.roll(val, HALF, 1) * sin_t).astype(BF16)


def attention_part(heads, near, gather_next, x_ref, gain_ref, pos_ref, freq_ref, dy_ref, wq_ref, wk_ref, wv_ref, wo_ref,
                   h_all, dy_all, o_all, ht_ref, dkv_ref, dq_a_ref, dq_b_ref, pos_all, pos_sems, h_sems, dy_sems, o_sems,
                   x_v, h_v, x_sems, own_sems, cos_s, sin_s, w_v, wo_v, w_sems, blk, blk_sems, ht_v, ht_sems,
                   q_s, k_s, v_s, vt, kt, ot_s, lse_s, acc, do_s, dk_acc, dv_acc, dq_v, dq_sems, dkv_v):
    rows, width = x_ref.shape
    n_blocks = k_s.shape[0]
    q_cols = heads * HEAD_DIM
    size = rows // CHUNKS
    qk_scale = HEAD_DIM ** -0.5
    to_log2 = qk_scale * LOG2E
    cols = [slice(a * HEAD_DIM, (a + 1) * HEAD_DIM) for a in range(heads)]
    part = lambda ref, chunk, count=size: ref.at[pl.ds(chunk * count, count), :]
    gather_h = Gather(near, lambda chunk: part(h_v, chunk), h_all, rows, h_sems)
    gather_dy = Gather(near, lambda chunk: part(dy_ref, chunk), dy_all, rows, dy_sems)
    gather_o = Gather(near, lambda chunk: part(ot_s, chunk, q_cols // CHUNKS), o_all, q_cols, o_sems)

    loads = [pltpu.make_async_copy(part(x_ref, chunk), part(x_v, chunk), x_sems.at[chunk]) for chunk in range(CHUNKS)]
    for load in loads:
        load.start()
    others = near.others()
    near.meet(others)
    pos_all[near.me] = jnp.broadcast_to(pos_ref[...], pos_all.shape[1:])
    positions = [send(pos_ref, pos_all.at[near.me, pl.ds(0, 1), :], pos_sems, r, peer) for r, peer in enumerate(others)]
    gain = gain_ref[...].astype(F32)
    for turn, chunk in enumerate((0, 2, 1, 3)):
        loads[chunk].wait()

        @pl.loop(0, size // 32)
        def _(r):
            at = pl.ds(pl.multiple_of(chunk * size + r * 32, 32), 32)
            x_f = x_v[at, :].astype(F32)
            normed = x_f * lax.rsqrt(jnp.mean(x_f * x_f, axis=-1, keepdims=True) + NORM_EPS)
            h_v[at, :] = (normed * gain).astype(BF16)

        gather_h.send_first(turn // 2, turn % 2)
        gather_h.first(chunk, 2).start()
    for turn in (2, 3):
        for kind in (0, 1):
            gather_h.send_first(turn, kind)
    for copy in positions:
        copy.start()
    own_h = pltpu.make_async_copy(h_v, gather_h.block(near.me, 0, CHUNKS), own_sems.at[0])
    own_h.start()
    w_loads, col = [], 0
    for n, (ref, count) in enumerate(((wq_ref, q_cols), (wk_ref, HEAD_DIM), (wv_ref, HEAD_DIM))):
        at = pl.ds(pl.multiple_of(near.me * count, HEAD_DIM), count)
        w_loads.append(pltpu.make_async_copy(ref.at[:, at], w_v.at[:, pl.ds(col, count)], w_sems.at[n]))
        col += count
    w_loads.append(pltpu.make_async_copy(wo_ref.at[pl.ds(pl.multiple_of(near.me * q_cols, q_cols), q_cols), :], wo_v, w_sems.at[3]))
    stage_in = pltpu.make_async_copy(dy_ref, x_v, own_sems.at[1])
    stage_out = pltpu.make_async_copy(x_v, gather_dy.block(near.me, 0, CHUNKS), own_sems.at[2])
    for load in w_loads + [stage_in]:
        load.start()
    for copy in positions:
        copy.wait()
    sign = jnp.where(lax.broadcasted_iota(jnp.int32, (1, HEAD_DIM), 1) < HALF, -1.0, 1.0)

    @pl.loop(0, n_blocks)
    def _(b):
        pos = jnp.broadcast_to(pos_all[b, 0:1, :].astype(F32), (HEAD_DIM, rows)).T
        angles = pos * freq_ref[...]
        cos_s[b] = jnp.cos(angles)
        sin_s[b] = jnp.sin(angles) * sign

    gather_h.middle()
    gather_h.late()
    for load in w_loads + [stage_in]:
        load.wait()
    stage_out.start()
    own_h.wait()
    gather_h.end(gather_dy.start)

    def block_load(ref, block, slot):
        return pltpu.make_async_copy(ref.at[pl.ds(pl.multiple_of(block * rows, rows), rows), :], blk.at[slot], blk_sems.at[slot])

    def fwd_chunk(i, c, carry, diagonal):
        k_c, vt_c = k_s[c], vt[c]
        scores = [dot(k_c, q_s[i, :, cols[a]], COLS_COLS) * to_log2 for a in range(heads)]
        out = []
        for a in range(heads):
            s = masked(scores[a]) if diagonal else scores[a]
            m_old, l_old = carry[a]
            m_new = jnp.maximum(m_old, jnp.max(s, axis=0, keepdims=True))
            alpha = jnp.exp2(m_old - m_new)
            p = jnp.exp2(s - m_new)
            l_new = l_old * alpha + jnp.sum(p, axis=0, keepdims=True)
            acc[a] = acc[a] * alpha + dot(vt_c, p.astype(BF16))
            out.append((m_new, l_new))
        return tuple(out)

    def ht_store(i):
        at = pl.ds(pl.multiple_of(i * rows, rows), rows)
        return pltpu.make_async_copy(ht_v.at[lax.rem(i, 2)], ht_ref.at[:, at], ht_sems.at[lax.rem(i, 2)])

    block_load(h_all, 0, 0).start()

    @pl.loop(0, n_blocks)
    def _(i):
        slot = lax.rem(i, 2)
        block_load(h_all, i, slot).wait()

        @pl.when(i + 1 < n_blocks)
        def _():
            block_load(h_all, i + 1, 1 - slot).start()

        @pl.when(i >= 2)
        def _():
            ht_store(i - 2).wait()

        ht_v[slot] = blk[slot].T
        ht_store(i).start()
        prod = dot(blk[slot], w_v[...])
        cos_t, sin_t = cos_s[i], sin_s[i]
        for a in range(heads + 1):
            val = prod[:, a * HEAD_DIM:(a + 1) * HEAD_DIM]
            rot = (val * cos_t + pltpu.roll(val, HALF, 1) * sin_t).astype(BF16)
            if a < heads:
                q_s[i, :, cols[a]] = rot
            else:
                k_s[i] = rot
                kt[i] = rot.T
        v_i = prod[:, q_cols + HEAD_DIM:].astype(BF16)
        v_s[i] = v_i
        vt[i] = v_i.T
        acc[...] = jnp.zeros_like(acc)
        start = tuple((jnp.full((1, rows), NEG_LARGE, F32), jnp.zeros((1, rows), F32)) for _ in range(heads))
        carry = lax.fori_loop(0, i, lambda c, carry: fwd_chunk(i, c, carry, False), start)
        carry = fwd_chunk(i, i, carry, True)
        at = pl.ds(pl.multiple_of(i * rows, rows), rows)
        for a in range(heads):
            m_a, l_a = carry[a]
            ot_s[cols[a], at] = (acc[a] / l_a).astype(BF16)
            lse_s[i, a:a + 1, :] = m_a + jnp.log2(l_a)

        @pl.when(i == FWD_MIDDLE)
        def _():
            gather_dy.middle()

    gather_dy.late()
    gather_o.start()
    own_o = pltpu.make_async_copy(ot_s, gather_o.block(near.me, 0, CHUNKS), own_sems.at[0])
    own_o.start()

    def bwd_chunk(i, c, delta, diagonal):
        k_c, v_c, kt_c = k_s[c], v_s[c], kt[c]
        dk_c = dv_c = None
        for a in range(heads):
            q_a, do_a = q_s[i, :, cols[a]], do_s[i, :, cols[a]]
            s = dot(k_c, q_a, COLS_COLS) * to_log2
            if diagonal:
                s = masked(s)
            p = jnp.exp2(s - lse_s[i, a:a + 1, :])
            d_p = dot(v_c, do_a, COLS_COLS)
            d_s = (p * (d_p - delta[a])).astype(BF16)
            dv_a = dot(p.astype(BF16), do_a)
            dk_a = dot(d_s, q_a)
            dv_c = dv_a if dv_c is None else dv_c + dv_a
            dk_c = dk_a if dk_c is None else dk_c + dk_a
            acc[a] += dot(kt_c, d_s)
        dk_acc[c] += dk_c
        dv_acc[c] += dv_c

    def dq_stores(r):
        slot = lax.rem(r, 2)
        at = pl.ds(pl.multiple_of(near.across(r) * rows, rows), rows)
        last = q_cols - HEAD_DIM
        return [pltpu.make_async_copy(dq_v.at[slot, :, pl.ds(0, last)], dq_a_ref.at[at, :], dq_sems.at[slot, 0]),
                pltpu.make_async_copy(dq_v.at[slot, :, pl.ds(last, HEAD_DIM)], dq_b_ref.at[at, :], dq_sems.at[slot, 1])]

    def pass_on(done):
        @pl.when(done == BWD_MIDDLE)
        def _():
            gather_o.middle()

    for i in (n_blocks - 2, n_blocks - 1):
        ht_store(i).wait()
    dk_acc[...] = jnp.zeros_like(dk_acc)
    dv_acc[...] = jnp.zeros_like(dv_acc)
    stage_out.wait()
    block_load(dy_all, near.me, 0).start()

    def bwd_block(r, done):
        i = near.across(r)
        slot = lax.rem(r, 2)
        at = pl.ds(pl.multiple_of(i * rows, rows), rows)

        @pl.when(r == 1)
        def _():
            gather_dy.end_sib()

        @pl.when(r == 2)
        def _():
            gather_dy.end_near()

        @pl.when(r == n_blocks * 3 // 4)
        def _():
            gather_dy.end_far()

        waits = [r == first for first in (1, 2, n_blocks * 3 // 4)]
        @pl.when(functools.reduce(jnp.logical_or, waits))
        def _():
            block_load(dy_all, i, slot).start()

        block_load(dy_all, 0, slot).wait()

        @pl.when(functools.reduce(jnp.logical_and, [r + 1 != first for first in (1, 2, n_blocks * 3 // 4, n_blocks)]))
        def _():
            block_load(dy_all, near.across(r + 1), 1 - slot).start()

        do_s[i] = dot(blk[slot], wo_v[...], COLS_COLS).astype(BF16)
        acc[...] = jnp.zeros_like(acc)
        delta = [jnp.sum(ot_s[cols[a], at].astype(F32) * do_s[i, :, cols[a]].T.astype(F32), axis=0, keepdims=True) for a in range(heads)]

        @pl.loop(0, i)
        def _(c):
            bwd_chunk(i, c, delta, False)
            pass_on(done + c)

        bwd_chunk(i, i, delta, True)
        pass_on(done + i)

        @pl.when(r >= 2)
        def _():
            for store in dq_stores(r - 2):
                store.wait()

        for a in range(heads):
            dq_v[slot, :, cols[a]] = unrotate(acc[a].T * qk_scale, cos_s[i], sin_s[i])
        for store in dq_stores(r):
            store.start()
        return done + i + 1

    lax.fori_loop(0, n_blocks, bwd_block, jnp.int32(0))
    gather_o.late()
    for r in (n_blocks - 2, n_blocks - 1):
        for store in dq_stores(r):
            store.wait()
    gather_next.start()

    @pl.loop(0, n_blocks)
    def _(c):
        at = pl.ds(pl.multiple_of(c * rows, rows), rows)
        dkv_v[at, :HEAD_DIM] = unrotate(dk_acc[c] * qk_scale, cos_s[c], sin_s[c])
        dkv_v[at, HEAD_DIM:] = dv_acc[c].astype(BF16)

    dkv_store = pltpu.make_async_copy(dkv_v, dkv_ref, own_sems.at[1])
    dkv_store.start()
    own_o.wait()
    gather_o.end()
    dkv_store.wait()


def lanes(*parts):
    return jnp.concatenate(parts, axis=1)


def products_part(heads, near, gathers, ot_ref, ht_ref, dy_ref, d_kv_ref, d_qa_ref, d_qb_ref, x_ref, own_dy_ref, gain_ref, wo_ref, wk_ref, wv_ref, wq_ref,
                  wo_out, wq_out, kv_all, qa_all, qb_all, res_ref, gx_ref, gg_ref, gg_row, gg_all, gg_sems, x_sems,
                  a_buf, b_buf, tile, a_sem, b_sems, t_sems, stage, stage_sems, ot_v, o_v, x_v, io_sems, own, own_sems, w_v, w_sems, acc,
                  gg_v):
    core = lax.rem(near.me, 2)
    half = a_buf.shape[0]
    seq_len = d_kv_ref.shape[0]
    rows, width = x_ref.shape
    n_cols = d_kv_ref.shape[1]
    n_o, n_all = width // (2 * n_cols), x_sems.shape[1]
    n_oa = n_o + (n_all - n_o) * 2 // 3

    local = (d_qa_ref, d_qb_ref, d_kv_ref)

    def stage_in(n):
        return pltpu.make_async_copy(local[n], stage.at[:, pl.ds(0, local[n].shape[1])], stage_sems.at[0])

    def stage_out(n):
        return pltpu.make_async_copy(stage.at[:, pl.ds(0, local[n].shape[1])], gathers[n].block(near.me, 0, CHUNKS), stage_sems.at[1])

    def copy_own(n):
        stage_in(n).wait()
        stage_out(n).start()

    own_rows = pl.ds(pl.multiple_of(core * half, half), half)
    tokens = pl.ds(pl.multiple_of(near.me * rows, rows), rows)
    ot_load = pltpu.make_async_copy(ot_ref.at[:, tokens], ot_v, io_sems.at[0])
    x_load = pltpu.make_async_copy(x_ref, x_v, io_sems.at[1])
    res_store = pltpu.make_async_copy(x_v, res_ref, io_sems.at[2])
    dy_load = pltpu.make_async_copy(own_dy_ref, o_v, io_sems.at[3])
    gx_store = pltpu.make_async_copy(o_v, gx_ref, io_sems.at[0])

    def a_load(ref):
        return pltpu.make_async_copy(ref.at[own_rows, :], a_buf, a_sem)

    def b_loads(source, p, slot, g):
        if source is dy_ref:
            srcs = [dy_ref.at[:, pl.ds(pl.multiple_of((2 * p + g) * n_cols, n_cols), n_cols)]]
        else:
            per = n_cols // source.shape[1]
            srcs = [source.at[pl.ds(pl.multiple_of(((2 * p + g) * per + n) * seq_len, seq_len), seq_len), :] for n in range(per)]
        return [pltpu.make_async_copy(src, b_buf.at[slot, :, pl.ds(g * n_cols + n * src.shape[1], src.shape[1])], b_sems.at[slot, g])
                for n, src in enumerate(srcs)]

    def start_b(step):
        slot = lax.rem(step, 2)
        for source, low, high in ((dy_ref, 0, n_o), (qa_all, n_o, n_oa), (qb_all, n_oa, n_all)):
            @pl.when(jnp.logical_and(step >= low, step < high))
            def _():
                for g in range(2):
                    for load in b_loads(source, step - low, slot, g):
                        load.start()

    def pieces(kind, step):
        wide = (2 * n_cols, n_cols, HEAD_DIM)[kind]
        slot = lax.rem(step, 2)
        out = []
        for n in range(2 * n_cols // wide):
            group = (step - (0, n_o, n_oa)[kind]) * (2 * n_cols // wide) + n
            col = (group * wide, group * heads * HEAD_DIM, (group + 1) * heads * HEAD_DIM - HEAD_DIM)[kind]
            dst = (wo_out, wq_out, wq_out)[kind].at[own_rows, pl.ds(pl.multiple_of(col, HEAD_DIM), wide)]
            src = tile.at[slot, :, pl.ds(n * wide, wide)]
            out.append((pltpu.make_async_copy(src, dst, t_sems.at[slot]), send(src, dst, x_sems, step, near.sib)))
        return out

    def start_tile(step):
        for kind, (low, high) in enumerate(((0, n_o), (n_o, n_oa), (n_oa, n_all))):
            @pl.when(jnp.logical_and(step >= low, step < high))
            def _():
                for keep, give in pieces(kind, step):
                    keep.start()
                    give.start()

    def whole_tile(step):
        slot = lax.rem(step, 2)
        dst = wo_out.at[own_rows, pl.ds(0, 2 * n_cols)]
        return pltpu.make_async_copy(tile.at[slot], dst, t_sems.at[slot]), send(tile.at[slot], dst, x_sems, step, near.sib)

    def wait_tile(step):
        keep, give = whole_tile(step)
        keep.wait()
        give.wait_send()

    def result_part():
        cols = b_buf.shape[2]

        def w_load(n):
            slot = lax.rem(n, 2)
            return pltpu.make_async_copy(wo_ref.at[:, pl.ds(pl.multiple_of(n * cols, cols), cols)], b_buf.at[slot, pl.ds(0, wo_ref.shape[0]), :],
                                         b_sems.at[slot, 0])

        w_load(jnp.int32(0)).start()
        ot_load.wait()

        @pl.loop(0, ot_v.shape[0] // BLK)
        def _(r):
            at = pl.ds(pl.multiple_of(r * BLK, BLK), BLK)
            o_v[:, at] = ot_v[at, :].T

        x_load.wait()

        @pl.loop(0, n_o)
        def _(n):
            w_load(n).wait()

            @pl.when(n + 1 < n_o)
            def _():
                w_load(n + 1).start()

            at = pl.ds(pl.multiple_of(n * cols, cols), cols)
            x_v[:, at] = (x_v[:, at].astype(F32) + dot(o_v[...], b_buf[lax.rem(n, 2), :wo_ref.shape[0], :])).astype(BF16)

        res_store.start()

    def hidden_parts(kind):
        count = own.shape[0] // (2 if kind == 1 else 1)

        def own_load(r, g):
            source = (qa_all, qb_all, kv_all)[kind]
            device, col = (2 * r + g, 0) if kind == 1 else (near.across(r), g * HEAD_DIM)
            at = pl.ds(pl.multiple_of(device * seq_len + near.me * rows, rows), rows)
            return pltpu.make_async_copy(source.at[at, pl.ds(col, HEAD_DIM)], own.at[r, :, pl.ds(g * HEAD_DIM, HEAD_DIM)], own_sems.at[r, g])

        def w_load(r, g):
            source = (wk_ref, wv_ref)[g] if kind == 2 else wq_ref
            col = near.across(r) if kind == 2 else heads * near.across(r) + g if kind == 0 else heads * (2 * r + g + 1) - 1
            slot = lax.rem(r, 2)
            return pltpu.make_async_copy(source.at[:, pl.ds(pl.multiple_of(col * HEAD_DIM, HEAD_DIM), HEAD_DIM)],
                                         w_v.at[slot, :, pl.ds(g * HEAD_DIM, HEAD_DIM)], w_sems.at[slot, g])

        return count, own_load, w_load

    def hidden_start(kind, low=0, high=None):
        count, own_load, w_load = hidden_parts(kind)
        for g in range(2):
            if low == 0:
                w_load(jnp.int32(0), g).start()

            @pl.loop(low, high or count)
            def _(r):
                own_load(r, g).start()

    def hidden_add(kind, low=0, high=None):
        count, own_load, w_load = hidden_parts(kind)

        @pl.loop(low, high or count)
        def _(r):
            for g in range(2):
                w_load(r, g).wait()
                own_load(r, g).wait()

            @pl.when(r + 1 < count)
            def _():
                for g in range(2):
                    w_load(r + 1, g).start()

            for col in range(0, width, width // PARTS):
                at = slice(col, col + width // PARTS)
                acc[:, at] += dot(own[r], w_v[lax.rem(r, 2), at, :], COLS_COLS)

    a_load(ot_ref).start()
    start_b(jnp.int32(0))
    stage_in(0).start()
    ot_load.start()
    x_load.start()
    a_load(ot_ref).wait()

    @pl.loop(0, n_all)
    def _(step):
        slot = lax.rem(step, 2)
        for g in range(2):
            b_loads(dy_ref, 0, slot, g)[0].wait()

        @pl.when(jnp.logical_and(step != n_o - 1, step != n_oa - 1))
        def _():
            start_b(step + 1)

        @pl.when(step >= 2)
        def _():
            wait_tile(step - 2)

        @pl.when(step == n_o)
        def _():
            a_load(ht_ref).wait()

        for r in range(0, half, half // PARTS):
            tile[slot, r:r + half // PARTS, :] = dot(a_buf[r:r + half // PARTS, :], b_buf[slot])
        start_tile(step)

        @pl.when(step == n_o - 4)
        def _():
            acc[...] = jnp.zeros_like(acc)
            copy_own(0)
            gathers[0].middle()

        @pl.when(step == n_o - 1)
        def _():
            a_load(ht_ref).start()
            gathers[0].late()
            gathers[1].start()
            stage_out(0).wait()
            stage_in(1).start()
            result_part()
            gathers[0].end()
            start_b(step + 1)
            hidden_start(0)

        @pl.when(step == n_oa - 4)
        def _():
            copy_own(1)
            gathers[1].middle()

        @pl.when(step == n_oa - 2)
        def _():
            gathers[1].late()
            gathers[2].start()
            stage_out(1).wait()
            stage_in(2).start()

        @pl.when(step == n_oa - 1)
        def _():
            res_store.wait()
            x_load.start()
            dy_load.start()
            gathers[1].end()
            start_b(step + 1)
            hidden_add(0)
            hidden_start(1)

    copy_own(2)
    gathers[2].middle()
    hidden_add(1)
    gathers[2].late()
    stage_out(2).wait()
    gathers[2].end_sib()
    gathers[2].end_near()
    near_count = own.shape[0] * 3 // 4
    hidden_start(2, 0, near_count)
    for step in (n_all - 2, n_all - 1):
        wait_tile(jnp.int32(step))
    hidden_add(2, 0, near_count)
    gathers[2].end_far()
    hidden_start(2, near_count)
    hidden_add(2, near_count)

    gain = gain_ref[...].astype(F32)
    gg_v[...] = jnp.zeros_like(gg_v)
    x_load.wait()
    dy_load.wait()

    @pl.loop(0, rows // 32)
    def _(r):
        at = pl.ds(pl.multiple_of(r * 32, 32), 32)
        x_f = x_v[at, :].astype(F32)
        inv_rms = lax.rsqrt(jnp.mean(x_f * x_f, axis=-1, keepdims=True) + NORM_EPS)
        normed = x_f * inv_rms
        d_hid = acc[at, :]
        both = d_hid * normed
        gg_v[...] += jnp.sum(both.reshape(4, 8, width), axis=0)
        mean = jnp.mean(both * gain, axis=-1, keepdims=True)
        o_v[at, :] = (o_v[at, :].astype(F32) + inv_rms * (d_hid * gain - normed * mean)).astype(BF16)

    gg_row[...] = jnp.sum(gg_v[...], axis=0, keepdims=True)
    gg_all[near.me] = gg_row[...]
    parts = [send(gg_row, gg_all.at[near.me], gg_sems, r, peer) for r, peer in enumerate(near.others())]
    for copy in parts:
        copy.start()
    gx_store.start()

    @pl.loop(0, n_all)
    def _(step):
        whole_tile(step)[1].wait_recv()

    for copy in parts:
        copy.wait()
    gg_ref[...] = jnp.sum(gg_all[...], axis=0)
    gx_store.wait()


def step_kernel(heads, first_scratch, second_scratch, x_ref, gain_ref, pos_ref, freq_ref, dy_ref, wq_ref, wk_ref, wv_ref, wo_ref,
                h_all, dy_all, o_all, ht, d_kv, d_qa, d_qb, wo_out, wq_out, kv_all, qa_all, qb_all, res, gx, gg,
                pos_all, pos_sems, gg_row, gg_all, gg_sems, x_sems, h_sems, dy_sems, o_sems, kv_sems, qa_sems, qb_sems):
    near = Neighbours()
    seq_len = d_kv.shape[0]

    def gather_of(src, dst, sems):
        return Gather(near, lambda c: src.at[pl.ds(c * (seq_len // CHUNKS), seq_len // CHUNKS), :], dst, seq_len, sems)

    gathers = [gather_of(d_qa, qa_all, qa_sems), gather_of(d_qb, qb_all, qb_sems), gather_of(d_kv, kv_all, kv_sems)]

    def first(*scratch):
        attention_part(heads, near, gathers[0], x_ref, gain_ref, pos_ref, freq_ref, dy_ref, wq_ref, wk_ref, wv_ref, wo_ref,
                       h_all, dy_all, o_all, ht, d_kv, d_qa, d_qb, pos_all, pos_sems, h_sems, dy_sems, o_sems, *scratch)

    def second(*scratch):
        products_part(heads, near, gathers, o_all, ht, dy_all, d_kv, d_qa, d_qb, x_ref, dy_ref, gain_ref, wo_ref, wk_ref, wv_ref, wq_ref,
                      wo_out, wq_out, kv_all, qa_all, qb_all, res, gx, gg, gg_row, gg_all, gg_sems, x_sems, *scratch)

    pl.run_scoped(first, *first_scratch)
    pl.run_scoped(second, *second_scratch)


def step(x, gain, positions, grad_out, w_q, w_k, w_v, w_o, sp_size, heads):
    rows, width = x.shape
    seq_len = rows * sp_size
    q_cols = heads * HEAD_DIM
    all_cols = q_cols * sp_size
    half = width // 2
    cols = 4 * HEAD_DIM
    n_all = (width + all_cols) // cols
    any_spec = pl.BlockSpec(memory_space=pl.ANY)
    vmem = pl.BlockSpec(memory_space=pltpu.VMEM)
    dma = pltpu.SemaphoreType.DMA
    inv_freq = ROPE_THETA ** (-np.arange(0, HEAD_DIM, 2) / HEAD_DIM)
    freq = jnp.asarray(np.concatenate([inv_freq, inv_freq])[None, :], F32)
    pairs = heads * seq_len * (seq_len + rows) // 2
    out = lambda *shape, dtype=BF16: jax.ShapeDtypeStruct(shape, dtype)
    array = lambda *shape, dtype=BF16: pltpu.VMEM(shape, dtype)
    blocks = lambda *shape, dtype=BF16: pltpu.VMEM((sp_size,) + shape, dtype)
    first_scratch = [array(rows, width), array(rows, width), dma((CHUNKS,)), dma((3,)), blocks(rows, HEAD_DIM, dtype=F32),
                     blocks(rows, HEAD_DIM, dtype=F32), array(width, q_cols + 2 * HEAD_DIM), array(q_cols, width), dma((4,)),
                     array(2, rows, width), dma((2,)), array(2, width, rows), dma((2,)),
                     blocks(rows, q_cols), blocks(rows, HEAD_DIM), blocks(rows, HEAD_DIM), blocks(HEAD_DIM, rows), blocks(HEAD_DIM, rows),
                     array(q_cols, seq_len), blocks(8, rows, dtype=F32), array(heads, HEAD_DIM, rows, dtype=F32),
                     blocks(rows, q_cols), blocks(rows, HEAD_DIM, dtype=F32), blocks(rows, HEAD_DIM, dtype=F32),
                     array(2, rows, q_cols), dma((2, 2)), array(seq_len, 2 * HEAD_DIM)]
    second_scratch = [array(half, seq_len), array(2, seq_len, cols), array(2, half, cols, dtype=F32), dma, dma((2, 2)), dma((2,)),
                      array(seq_len, 2 * HEAD_DIM), dma((2,)), array(all_cols, rows), array(rows, all_cols), array(rows, width),
                      dma((4,)), blocks(rows, 2 * HEAD_DIM), dma((sp_size, 2)), array(2, width, 2 * HEAD_DIM), dma((2, 2)),
                      array(rows, width, dtype=F32), array(8, width, dtype=F32)]
    return pl.pallas_call(
        functools.partial(step_kernel, heads, first_scratch, second_scratch),
        in_specs=[any_spec, vmem, vmem, vmem] + [any_spec] * 5,
        out_specs=[any_spec] * 14 + [vmem],
        out_shape=[out(seq_len, width), out(seq_len, width), out(all_cols, seq_len), out(width, seq_len), out(seq_len, 2 * HEAD_DIM),
                   out(seq_len, q_cols - HEAD_DIM), out(seq_len, HEAD_DIM), out(all_cols, width, dtype=F32), out(width, all_cols, dtype=F32),
                   out(sp_size * seq_len, 2 * HEAD_DIM), out(sp_size * seq_len, q_cols - HEAD_DIM), out(sp_size * seq_len, HEAD_DIM),
                   out(rows, width), out(rows, width), out(1, width, dtype=F32)],
        scratch_shapes=[blocks(8, rows, dtype=jnp.int32), dma((2, 7)), array(1, width, dtype=F32), blocks(1, width, dtype=F32), dma((2, 7)),
                        dma((2, n_all))] + [SEMS] * 6,
        compiler_params=pltpu.CompilerParams(vmem_limit_bytes=VMEM_LIMIT, collective_id=0, has_side_effects=True),
        cost_estimate=pl.CostEstimate(flops=28 * pairs * HEAD_DIM + 2 * half * cols * seq_len * n_all, bytes_accessed=20 * seq_len * width,
                                      transcendentals=2 * pairs),
        name="step",
    )(x, gain, positions.reshape(1, -1), freq, grad_out, w_q, w_k, w_v, w_o)


def finish_kernel(ht_ref, d_ref, gx_in, res_in, gg_in, wo_in, wq_in, wk_ref, wv_ref, wq_ref, wo_ref, gx_ref, res_ref, gg_ref, d_v, d_sems, ring, ring_sems):
    step = pl.program_id(0) * pl.num_programs(1) + pl.program_id(1)
    high = ring.shape[2]
    per_array = wo_in.shape[0] // (high * RING)

    def copy_in(src, g, n):
        at = pl.ds(pl.multiple_of((lax.rem(g, per_array) * RING + n) * high, high), high)
        return pltpu.make_async_copy(src.at[at, :], ring.at[lax.rem(g, DEPTH), n], ring_sems.at[0, lax.rem(g, DEPTH), n])

    def copy_out(dst, g, n):
        at = pl.ds(pl.multiple_of((lax.rem(g, per_array) * RING + n) * high, high), high)
        return pltpu.make_async_copy(ring.at[lax.rem(g, DEPTH), n], dst.at[at, :], ring_sems.at[1, lax.rem(g, DEPTH), n])

    def start(copy, first, second, g):
        for ref, mine in ((first, g < per_array), (second, g >= per_array)):
            @pl.when(mine)
            def _():
                for n in range(RING):
                    copy(ref, g, n).start()

    def pair_load(p):
        at = pl.ds(2 * p, 2)
        return pltpu.make_async_copy(d_ref.at[at], d_v.at[at], d_sems.at[p])

    @pl.when(step == 0)
    def _():
        for p in range(d_v.shape[0] // 2):
            pair_load(p).start()

    last = pl.num_programs(0) * pl.num_programs(1) - 1

    def free(g):
        for n in range(RING):
            copy_out(wo_ref, g, n).wait()

    def pass_on(g):
        for n in range(RING):
            copy_in(wo_in, g, n).wait()
        start(copy_out, wo_ref, wq_ref, g)

    @pl.when(step >= DEPTH)
    def _():
        free(step - DEPTH)

    start(copy_in, wo_in, wq_in, step)

    @pl.when(step >= 1)
    def _():
        pass_on(step - 1)

    for p in range(d_v.shape[0] // 2):
        @pl.when(step == p)
        def _():
            pair_load(p).wait()

    ht = ht_ref[...]
    pair = 2 * pl.program_id(1)
    wk_ref[...] = dot(ht, lanes(d_v[pair, :, :HEAD_DIM], d_v[pair + 1, :, :HEAD_DIM]))
    wv_ref[...] = dot(ht, lanes(d_v[pair, :, HEAD_DIM:], d_v[pair + 1, :, HEAD_DIM:]))

    @pl.when(step == 0)
    def _():
        gg_ref[...] = gg_in[...]

    @pl.when(step == last)
    def _():
        pass_on(last)
        for back in range(DEPTH):
            free(last - back)

    @pl.when(step < ROW_STEPS)
    def _():
        gx_ref[...] = gx_in[...]
        res_ref[...] = res_in[...]


def finish(ht, d_kv, w_o_grad, w_q_grad, grad_x, result, grad_gain):
    width, seq_len = ht.shape
    groups = d_kv.shape[0]
    n_j = groups // 2
    steps = (width // MROWS) * n_j
    high = width // COPY_ROWS
    assert w_o_grad.shape[0] + w_q_grad.shape[0] == high * RING * steps
    any_spec = pl.BlockSpec(memory_space=pl.ANY)
    rows = pl.BlockSpec((grad_x.shape[0] // ROW_STEPS, width), lambda m, j: (jnp.minimum(m * n_j + j, ROW_STEPS - 1), 0))
    whole = pl.BlockSpec((1, width), lambda m, j: (0, 0))
    kv_out = pl.BlockSpec((MROWS, 2 * HEAD_DIM), lambda m, j: (m, j))
    out = lambda cols: jax.ShapeDtypeStruct((width, cols), F32)
    like = lambda val: jax.ShapeDtypeStruct(val.shape, val.dtype)
    return pl.pallas_call(
        finish_kernel,
        grid=(width // MROWS, n_j),
        in_specs=[pl.BlockSpec((MROWS, seq_len), lambda m, j: (m, 0)), any_spec, rows, rows, whole, any_spec, any_spec],
        out_specs=[kv_out, kv_out, any_spec, any_spec, rows, rows, whole],
        out_shape=[out(groups * HEAD_DIM), out(groups * HEAD_DIM), like(w_q_grad), like(w_o_grad), like(grad_x), like(result), like(grad_gain)],
        scratch_shapes=[pltpu.VMEM(d_kv.shape, BF16), pltpu.SemaphoreType.DMA((groups // 2,)),
                        pltpu.VMEM((DEPTH, RING, high, width), F32), pltpu.SemaphoreType.DMA((2, DEPTH, RING))],
        compiler_params=params(2),
        cost_estimate=pl.CostEstimate(flops=4 * width * seq_len * groups * HEAD_DIM, bytes_accessed=2 * width * seq_len, transcendentals=0),
        name="finish",
    )(ht, d_kv, grad_x, result, grad_gain, w_o_grad, w_q_grad)


def solution(mesh):
    sp_size = mesh.shape['sp']
    seq_spec = P(('dp', 'sp'), None)
    pos_spec = P(('dp', 'sp'))
    replicated = P(None, None)
    part_rows = P('dp', None)

    def local_step(x, grad_out, positions, gain, w_q, w_k, w_v, w_o):
        n_heads = w_q.shape[1] // HEAD_DIM
        heads = n_heads // sp_size
        _, _, _, ht, _, _, _, w_o_grad, w_q_grad, kv_all, _, _, result, grad_x, grad_gain = step(
            x, gain.reshape(1, -1), positions, grad_out, w_q, w_k, w_v, w_o, sp_size, heads)
        grad_wk, grad_wv, grad_wq, grad_wo, grad_x, result, grad_gain = finish(
            ht, kv_all.reshape(sp_size, -1, 2 * HEAD_DIM), w_o_grad, w_q_grad, grad_x, result, grad_gain)
        return result, grad_x, grad_wq, grad_wk, grad_wv, grad_wo, grad_gain.reshape(-1)

    return jax.shard_map(local_step, mesh=mesh,
                         in_specs=(seq_spec, seq_spec, pos_spec, P(None), replicated, replicated, replicated, replicated),
                         out_specs=(seq_spec, seq_spec, part_rows, part_rows, part_rows, part_rows, P('dp')),
                         check_vma=False)
```

```python
import functools

import jax
import jax.numpy as jnp
import numpy as np
from jax import lax
from jax.experimental import pallas as pl
from jax.experimental.pallas import tpu as pltpu
from jax.sharding import PartitionSpec as P

HEAD_DIM = 128
HALF = HEAD_DIM // 2
ROPE_THETA = 1000000.0
NORM_EPS = 1e-05
NEG_LARGE = -1e30
LOG2E = 1.4426950408889634
BLK = 512
CHUNKS = 4
FWD_MIDDLE, BWD_MIDDLE = 5, 27
MROWS = 768
RING = 3
DEPTH = 3
COPY_ROWS = 24
PARTS = 3
ROW_STEPS = 8
F32 = jnp.float32
BF16 = jnp.bfloat16
ROWS_ROWS = (((0,), (0,)), ((), ()))
COLS_COLS = (((1,), (1,)), ((), ()))
ROWS_COLS = (((0,), (1,)), ((), ()))
VMEM_LIMIT = 63 * 1024 * 1024


def dot(a, b, dims=(((1,), (0,)), ((), ()))):
    return lax.dot_general(a, b, dims, preferred_element_type=F32)


def params(axes=1):
    return pltpu.CompilerParams(dimension_semantics=("arbitrary",) * axes, vmem_limit_bytes=VMEM_LIMIT)


class Neighbours:
    def __init__(self):
        self.me = lax.axis_index('sp')
        core, col, row = lax.rem(self.me, 2), lax.rem(self.me // 2, 2), self.me // 4
        self.sib = self.me + 1 - 2 * core
        self.xn = self.me + 2 - 4 * col
        self.yn = self.me + 4 - 8 * row
        self.diag = self.xn + self.yn - self.me

    def meet(self, peers):
        barrier = pltpu.get_barrier_semaphore()
        for peer in peers:
            pl.semaphore_signal(barrier, inc=1, device_id={'sp': peer}, device_id_type=pl.DeviceIdType.MESH)
        pl.semaphore_wait(barrier, len(peers))

    def across(self, r):
        core, col, row = lax.rem(self.me, 2), lax.rem(self.me // 2, 2), self.me // 4
        return (self.me + lax.rem(r, 2) * (1 - 2 * core) + lax.rem(r // 2, 2) * (2 - 4 * col) + (r // 4) * (4 - 8 * row))

    def others(self):
        flip = lambda dev: dev + 1 - 2 * lax.rem(dev, 2)
        return [self.sib, self.xn, flip(self.xn), self.yn, flip(self.yn), self.diag, flip(self.diag)]


def send(src, dst, sems, index, peer):
    return pltpu.make_async_remote_copy(src_ref=src, dst_ref=dst, send_sem=sems.at[0, index], recv_sem=sems.at[1, index],
                                        device_id={'sp': peer}, device_id_type=pl.DeviceIdType.MESH)


class Gather:
    COPIES = 22

    def __init__(self, near, own, dst, rows, sems):
        self.near, self.own, self.dst, self.rows, self.sems = near, own, dst, rows, sems

    def block(self, dev, chunk, count=1):
        size = self.rows // CHUNKS
        return self.dst.at[pl.ds(pl.multiple_of(dev * self.rows + chunk * size, size), count * size), :]

    def first(self, chunk, kind):
        peer = (self.near.xn, self.near.yn, self.near.sib)[kind]
        return send(self.own(chunk), self.block(self.near.me, chunk), self.sems, kind * CHUNKS + chunk, peer)

    def onward(self, chunk):
        over_y = chunk < CHUNKS // 2
        rows = self.block(self.near.xn if over_y else self.near.yn, chunk)
        return send(rows, rows, self.sems, 12 + chunk, self.near.yn if over_y else self.near.xn)

    def share(self, kind):
        rows = self.block((self.near.xn, self.near.yn)[kind], 0, CHUNKS)
        return send(rows, rows, self.sems, 16 + kind, self.near.sib)

    def share_diag(self, chunk):
        rows = self.block(self.near.diag, chunk)
        return send(rows, rows, self.sems, 18 + chunk, self.near.sib)

    def start(self):
        for chunk in range(CHUNKS):
            for kind in (0, 1):
                self.send_first(chunk, kind)
            self.first(chunk, 2).start()

    def send_first(self, turn, kind):
        self.first(turn if kind == 0 else (turn + CHUNKS // 2) % CHUNKS, kind).start()

    def middle(self):
        for chunk in (0, 2, 1, 3):
            self.first(chunk, 0 if chunk < CHUNKS // 2 else 1).wait_recv()
            self.onward(chunk).start()

    def late(self):
        for chunk in (2, 3):
            self.first(chunk, 0).wait_recv()
        self.share(0).start()
        for chunk in (0, 1):
            self.first(chunk, 1).wait_recv()
        self.share(1).start()

    def end_sib(self):
        for chunk in range(CHUNKS):
            self.first(chunk, 2).wait_recv()

    def end_near(self):
        for kind in range(2):
            self.share(kind).wait_recv()

    def end_far(self, between=None):
        for chunk in (0, 2, 1, 3):
            self.onward(chunk).wait_recv()
            self.share_diag(chunk).start()
            if chunk == 2 and between:
                between()
        for chunk in range(CHUNKS):
            for kind in range(3):
                self.first(chunk, kind).wait_send()
            self.onward(chunk).wait_send()
        for kind in range(2):
            self.share(kind).wait_send()
        for chunk in range(CHUNKS):
            self.share_diag(chunk).wait()

    def end(self, between=None):
        self.end_sib()
        self.end_near()
        self.end_far(between)


SEMS = pltpu.SemaphoreType.DMA((2, Gather.COPIES))


def masked(scores):
    key = lax.broadcasted_iota(jnp.int32, scores.shape, 0)
    query = lax.broadcasted_iota(jnp.int32, scores.shape, 1)
    return jnp.where(key <= query, scores, NEG_LARGE)


def unrotate(val, cos_t, sin_t):
    return (val * cos_t - pltpu.roll(val, HALF, 1) * sin_t).astype(BF16)


def attention_part(heads, near, gather_next, x_ref, gain_ref, pos_ref, freq_ref, dy_ref, wq_ref, wk_ref, wv_ref, wo_ref,
                   h_all, dy_all, o_all, ht_ref, dkv_ref, dq_a_ref, dq_b_ref, pos_all, pos_sems, h_sems, dy_sems, o_sems,
                   x_v, h_v, x_sems, own_sems, cos_s, sin_s, w_v, wo_v, w_sems, blk, blk_sems, ht_v, ht_sems,
                   q_s, k_s, v_s, vt, kt, ot_s, lse_s, acc, do_s, dk_acc, dv_acc, dq_v, dq_sems, dkv_v):
    rows, width = x_ref.shape
    n_blocks = k_s.shape[0]
    q_cols = heads * HEAD_DIM
    size = rows // CHUNKS
    qk_scale = HEAD_DIM ** -0.5
    to_log2 = qk_scale * LOG2E
    cols = [slice(a * HEAD_DIM, (a + 1) * HEAD_DIM) for a in range(heads)]
    part = lambda ref, chunk, count=size: ref.at[pl.ds(chunk * count, count), :]
    gather_h = Gather(near, lambda chunk: part(h_v, chunk), h_all, rows, h_sems)
    gather_dy = Gather(near, lambda chunk: part(dy_ref, chunk), dy_all, rows, dy_sems)
    gather_o = Gather(near, lambda chunk: part(ot_s, chunk, q_cols // CHUNKS), o_all, q_cols, o_sems)

    loads = [pltpu.make_async_copy(part(x_ref, chunk), part(x_v, chunk), x_sems.at[chunk]) for chunk in range(CHUNKS)]
    for load in loads:
        load.start()
    others = near.others()
    near.meet(others)
    pos_all[near.me] = jnp.broadcast_to(pos_ref[...], pos_all.shape[1:])
    positions = [send(pos_ref, pos_all.at[near.me, pl.ds(0, 1), :], pos_sems, r, peer) for r, peer in enumerate(others)]
    gain = gain_ref[...].astype(F32)
    for turn, chunk in enumerate((0, 2, 1, 3)):
        loads[chunk].wait()

        @pl.loop(0, size // 32)
        def _(r):
            at = pl.ds(pl.multiple_of(chunk * size + r * 32, 32), 32)
            x_f = x_v[at, :].astype(F32)
            normed = x_f * lax.rsqrt(jnp.mean(x_f * x_f, axis=-1, keepdims=True) + NORM_EPS)
            h_v[at, :] = (normed * gain).astype(BF16)

        gather_h.send_first(turn // 2, turn % 2)
        gather_h.first(chunk, 2).start()
    for turn in (2, 3):
        for kind in (0, 1):
            gather_h.send_first(turn, kind)
    for copy in positions:
        copy.start()
    own_h = pltpu.make_async_copy(h_v, gather_h.block(near.me, 0, CHUNKS), own_sems.at[0])
    own_h.start()
    w_loads, col = [], 0
    for n, (ref, count) in enumerate(((wq_ref, q_cols), (wk_ref, HEAD_DIM), (wv_ref, HEAD_DIM))):
        at = pl.ds(pl.multiple_of(near.me * count, HEAD_DIM), count)
        w_loads.append(pltpu.make_async_copy(ref.at[:, at], w_v.at[:, pl.ds(col, count)], w_sems.at[n]))
        col += count
    w_loads.append(pltpu.make_async_copy(wo_ref.at[pl.ds(pl.multiple_of(near.me * q_cols, q_cols), q_cols), :], wo_v, w_sems.at[3]))
    stage_in = pltpu.make_async_copy(dy_ref, x_v, own_sems.at[1])
    stage_out = pltpu.make_async_copy(x_v, gather_dy.block(near.me, 0, CHUNKS), own_sems.at[2])
    for load in w_loads + [stage_in]:
        load.start()
    for copy in positions:
        copy.wait()
    sign = jnp.where(lax.broadcasted_iota(jnp.int32, (1, HEAD_DIM), 1) < HALF, -1.0, 1.0)

    @pl.loop(0, n_blocks)
    def _(b):
        pos = jnp.broadcast_to(pos_all[b, 0:1, :].astype(F32), (HEAD_DIM, rows)).T
        angles = pos * freq_ref[...]
        cos_s[b] = jnp.cos(angles)
        sin_s[b] = jnp.sin(angles) * sign

    gather_h.middle()
    for load in w_loads + [stage_in]:
        load.wait()
    stage_out.start()
    own_h.wait()

    def block_load(ref, block, slot):
        return pltpu.make_async_copy(ref.at[pl.ds(pl.multiple_of(block * rows, rows), rows), :], blk.at[slot], blk_sems.at[slot])

    far = n_blocks * 3 // 4

    def arrive(r, ref, gather, before_near=None, between=None):
        slot = lax.rem(r, 2)

        @pl.when(r == 1)
        def _():
            gather.end_sib()

        @pl.when(r == 2)
        def _():
            if before_near:
                before_near()
            gather.end_near()

        @pl.when(r == far)
        def _():
            gather.end_far(between)

        @pl.when(functools.reduce(jnp.logical_or, [r == first for first in (0, 1, 2, far)]))
        def _():
            block_load(ref, near.across(r), slot).start()

        block_load(ref, 0, slot).wait()

        @pl.when(functools.reduce(jnp.logical_and, [r + 1 != first for first in (1, 2, far, n_blocks)]))
        def _():
            block_load(ref, near.across(r + 1), 1 - slot).start()

    def ht_store(r):
        at = pl.ds(pl.multiple_of(near.across(r) * rows, rows), rows)
        return pltpu.make_async_copy(ht_v.at[lax.rem(r, 2)], ht_ref.at[:, at], ht_sems.at[lax.rem(r, 2)])

    @pl.loop(0, n_blocks)
    def _(r):
        i = near.across(r)
        slot = lax.rem(r, 2)
        arrive(r, h_all, gather_h, gather_h.late, gather_dy.start)

        @pl.when(r >= 2)
        def _():
            ht_store(r - 2).wait()

        ht_v[slot] = blk[slot].T
        ht_store(r).start()
        prod = dot(blk[slot], w_v[...])
        cos_t, sin_t = cos_s[i], sin_s[i]
        for a in range(heads + 1):
            val = prod[:, a * HEAD_DIM:(a + 1) * HEAD_DIM]
            rot = (val * cos_t + pltpu.roll(val, HALF, 1) * sin_t).astype(BF16)
            if a < heads:
                q_s[i, :, cols[a]] = rot
            else:
                k_s[i] = rot
                kt[i] = rot.T
        v_i = prod[:, q_cols + HEAD_DIM:].astype(BF16)
        v_s[i] = v_i
        vt[i] = v_i.T

    def fwd_chunk(i, c, carry, diagonal):
        k_c, vt_c = k_s[c], vt[c]
        scores = [dot(k_c, q_s[i, :, cols[a]], COLS_COLS) * to_log2 for a in range(heads)]
        out = []
        for a in range(heads):
            s = masked(scores[a]) if diagonal else scores[a]
            m_old, l_old = carry[a]
            m_new = jnp.maximum(m_old, jnp.max(s, axis=0, keepdims=True))
            alpha = jnp.exp2(m_old - m_new)
            p = jnp.exp2(s - m_new)
            l_new = l_old * alpha + jnp.sum(p, axis=0, keepdims=True)
            acc[a] = acc[a] * alpha + dot(vt_c, p.astype(BF16))
            out.append((m_new, l_new))
        return tuple(out)

    @pl.loop(0, n_blocks)
    def _(i):
        acc[...] = jnp.zeros_like(acc)
        start = tuple((jnp.full((1, rows), NEG_LARGE, F32), jnp.zeros((1, rows), F32)) for _ in range(heads))
        carry = lax.fori_loop(0, i, lambda c, carry: fwd_chunk(i, c, carry, False), start)
        carry = fwd_chunk(i, i, carry, True)
        at = pl.ds(pl.multiple_of(i * rows, rows), rows)
        for a in range(heads):
            m_a, l_a = carry[a]
            ot_s[cols[a], at] = (acc[a] / l_a).astype(BF16)
            lse_s[i, a:a + 1, :] = m_a + jnp.log2(l_a)

        @pl.when(i == FWD_MIDDLE)
        def _():
            gather_dy.middle()

    gather_dy.late()
    gather_o.start()
    own_o = pltpu.make_async_copy(ot_s, gather_o.block(near.me, 0, CHUNKS), own_sems.at[0])
    own_o.start()

    def bwd_chunk(i, c, delta, diagonal):
        k_c, v_c, kt_c = k_s[c], v_s[c], kt[c]
        dk_c = dv_c = None
        for a in range(heads):
            q_a, do_a = q_s[i, :, cols[a]], do_s[i, :, cols[a]]
            s = dot(k_c, q_a, COLS_COLS) * to_log2
            if diagonal:
                s = masked(s)
            p = jnp.exp2(s - lse_s[i, a:a + 1, :])
            d_p = dot(v_c, do_a, COLS_COLS)
            d_s = (p * (d_p - delta[a])).astype(BF16)
            dv_a = dot(p.astype(BF16), do_a)
            dk_a = dot(d_s, q_a)
            dv_c = dv_a if dv_c is None else dv_c + dv_a
            dk_c = dk_a if dk_c is None else dk_c + dk_a
            acc[a] += dot(kt_c, d_s)
        dk_acc[c] += dk_c
        dv_acc[c] += dv_c

    def dq_stores(r):
        slot = lax.rem(r, 2)
        at = pl.ds(pl.multiple_of(near.across(r) * rows, rows), rows)
        last = q_cols - HEAD_DIM
        return [pltpu.make_async_copy(dq_v.at[slot, :, pl.ds(0, last)], dq_a_ref.at[at, :], dq_sems.at[slot, 0]),
                pltpu.make_async_copy(dq_v.at[slot, :, pl.ds(last, HEAD_DIM)], dq_b_ref.at[at, :], dq_sems.at[slot, 1])]

    def pass_on(done):
        @pl.when(done == BWD_MIDDLE)
        def _():
            gather_o.middle()

    for r in (n_blocks - 2, n_blocks - 1):
        ht_store(jnp.int32(r)).wait()
    dk_acc[...] = jnp.zeros_like(dk_acc)
    dv_acc[...] = jnp.zeros_like(dv_acc)
    stage_out.wait()

    def bwd_block(r, done):
        i = near.across(r)
        slot = lax.rem(r, 2)
        at = pl.ds(pl.multiple_of(i * rows, rows), rows)

        arrive(r, dy_all, gather_dy)
        do_s[i] = dot(blk[slot], wo_v[...], COLS_COLS).astype(BF16)
        acc[...] = jnp.zeros_like(acc)
        delta = [jnp.sum(ot_s[cols[a], at].astype(F32) * do_s[i, :, cols[a]].T.astype(F32), axis=0, keepdims=True) for a in range(heads)]

        @pl.loop(0, i)
        def _(c):
            bwd_chunk(i, c, delta, False)
            pass_on(done + c)

        bwd_chunk(i, i, delta, True)
        pass_on(done + i)

        @pl.when(r >= 2)
        def _():
            for store in dq_stores(r - 2):
                store.wait()

        for a in range(heads):
            dq_v[slot, :, cols[a]] = unrotate(acc[a].T * qk_scale, cos_s[i], sin_s[i])
        for store in dq_stores(r):
            store.start()
        return done + i + 1

    lax.fori_loop(0, n_blocks, bwd_block, jnp.int32(0))
    gather_o.late()
    for r in (n_blocks - 2, n_blocks - 1):
        for store in dq_stores(r):
            store.wait()
    gather_next.start()

    @pl.loop(0, n_blocks)
    def _(c):
        at = pl.ds(pl.multiple_of(c * rows, rows), rows)
        dkv_v[at, :HEAD_DIM] = unrotate(dk_acc[c] * qk_scale, cos_s[c], sin_s[c])
        dkv_v[at, HEAD_DIM:] = dv_acc[c].astype(BF16)

    dkv_store = pltpu.make_async_copy(dkv_v, dkv_ref, own_sems.at[1])
    dkv_store.start()
    own_o.wait()
    gather_o.end()
    dkv_store.wait()


def lanes(*parts):
    return jnp.concatenate(parts, axis=1)


def products_part(heads, near, gathers, ot_ref, ht_ref, dy_ref, d_kv_ref, d_qa_ref, d_qb_ref, x_ref, own_dy_ref, gain_ref, wo_ref, wk_ref, wv_ref, wq_ref,
                  wo_out, wq_out, kv_all, qa_all, qb_all, res_ref, gx_ref, gg_ref, gg_row, gg_all, gg_sems, x_sems,
                  a_buf, b_buf, tile, a_sem, b_sems, t_sems, stage, stage_sems, ot_v, o_v, x_v, io_sems, own, own_sems, w_v, w_sems, acc,
                  gg_v):
    core = lax.rem(near.me, 2)
    half = a_buf.shape[0]
    seq_len = d_kv_ref.shape[0]
    rows, width = x_ref.shape
    n_cols = d_kv_ref.shape[1]
    n_o, n_all = width // (2 * n_cols), x_sems.shape[1]
    n_oa = n_o + (n_all - n_o) * 2 // 3

    local = (d_qa_ref, d_qb_ref, d_kv_ref)

    def stage_in(n):
        return pltpu.make_async_copy(local[n], stage.at[:, pl.ds(0, local[n].shape[1])], stage_sems.at[0])

    def stage_out(n):
        return pltpu.make_async_copy(stage.at[:, pl.ds(0, local[n].shape[1])], gathers[n].block(near.me, 0, CHUNKS), stage_sems.at[1])

    def copy_own(n):
        stage_in(n).wait()
        stage_out(n).start()

    own_rows = pl.ds(pl.multiple_of(core * half, half), half)
    tokens = pl.ds(pl.multiple_of(near.me * rows, rows), rows)
    ot_load = pltpu.make_async_copy(ot_ref.at[:, tokens], ot_v, io_sems.at[0])
    x_load = pltpu.make_async_copy(x_ref, x_v, io_sems.at[1])
    res_store = pltpu.make_async_copy(x_v, res_ref, io_sems.at[2])
    dy_load = pltpu.make_async_copy(own_dy_ref, o_v, io_sems.at[3])
    gx_store = pltpu.make_async_copy(o_v, gx_ref, io_sems.at[0])

    def a_load(ref):
        return pltpu.make_async_copy(ref.at[own_rows, :], a_buf, a_sem)

    def b_loads(source, p, slot, g):
        if source is dy_ref:
            srcs = [dy_ref.at[:, pl.ds(pl.multiple_of((2 * p + g) * n_cols, n_cols), n_cols)]]
        else:
            per = n_cols // source.shape[1]
            srcs = [source.at[pl.ds(pl.multiple_of(((2 * p + g) * per + n) * seq_len, seq_len), seq_len), :] for n in range(per)]
        return [pltpu.make_async_copy(src, b_buf.at[slot, :, pl.ds(g * n_cols + n * src.shape[1], src.shape[1])], b_sems.at[slot, g])
                for n, src in enumerate(srcs)]

    def start_b(step):
        slot = lax.rem(step, 2)
        for source, low, high in ((dy_ref, 0, n_o), (qa_all, n_o, n_oa), (qb_all, n_oa, n_all)):
            @pl.when(jnp.logical_and(step >= low, step < high))
            def _():
                for g in range(2):
                    for load in b_loads(source, step - low, slot, g):
                        load.start()

    def pieces(kind, step):
        wide = (2 * n_cols, n_cols, HEAD_DIM)[kind]
        slot = lax.rem(step, 2)
        out = []
        for n in range(2 * n_cols // wide):
            group = (step - (0, n_o, n_oa)[kind]) * (2 * n_cols // wide) + n
            col = (group * wide, group * heads * HEAD_DIM, (group + 1) * heads * HEAD_DIM - HEAD_DIM)[kind]
            dst = (wo_out, wq_out, wq_out)[kind].at[own_rows, pl.ds(pl.multiple_of(col, HEAD_DIM), wide)]
            src = tile.at[slot, :, pl.ds(n * wide, wide)]
            out.append((pltpu.make_async_copy(src, dst, t_sems.at[slot]), send(src, dst, x_sems, step, near.sib)))
        return out

    def start_tile(step):
        for kind, (low, high) in enumerate(((0, n_o), (n_o, n_oa), (n_oa, n_all))):
            @pl.when(jnp.logical_and(step >= low, step < high))
            def _():
                for keep, give in pieces(kind, step):
                    keep.start()
                    give.start()

    def whole_tile(step):
        slot = lax.rem(step, 2)
        dst = wo_out.at[own_rows, pl.ds(0, 2 * n_cols)]
        return pltpu.make_async_copy(tile.at[slot], dst, t_sems.at[slot]), send(tile.at[slot], dst, x_sems, step, near.sib)

    def wait_tile(step):
        keep, give = whole_tile(step)
        keep.wait()
        give.wait_send()

    def result_part():
        cols = b_buf.shape[2]

        def w_load(n):
            slot = lax.rem(n, 2)
            return pltpu.make_async_copy(wo_ref.at[:, pl.ds(pl.multiple_of(n * cols, cols), cols)], b_buf.at[slot, pl.ds(0, wo_ref.shape[0]), :],
                                         b_sems.at[slot, 0])

        w_load(jnp.int32(0)).start()
        ot_load.wait()

        @pl.loop(0, ot_v.shape[0] // BLK)
        def _(r):
            at = pl.ds(pl.multiple_of(r * BLK, BLK), BLK)
            o_v[:, at] = ot_v[at, :].T

        x_load.wait()

        @pl.loop(0, n_o)
        def _(n):
            w_load(n).wait()

            @pl.when(n + 1 < n_o)
            def _():
                w_load(n + 1).start()

            at = pl.ds(pl.multiple_of(n * cols, cols), cols)
            x_v[:, at] = (x_v[:, at].astype(F32) + dot(o_v[...], b_buf[lax.rem(n, 2), :wo_ref.shape[0], :])).astype(BF16)

        res_store.start()

    def hidden_parts(kind):
        count = own.shape[0] // (2 if kind == 1 else 1)

        def own_load(r, g):
            source = (qa_all, qb_all, kv_all)[kind]
            device, col = (2 * r + g, 0) if kind == 1 else (near.across(r), g * HEAD_DIM)
            at = pl.ds(pl.multiple_of(device * seq_len + near.me * rows, rows), rows)
            return pltpu.make_async_copy(source.at[at, pl.ds(col, HEAD_DIM)], own.at[r, :, pl.ds(g * HEAD_DIM, HEAD_DIM)], own_sems.at[r, g])

        def w_load(r, g):
            source = (wk_ref, wv_ref)[g] if kind == 2 else wq_ref
            col = near.across(r) if kind == 2 else heads * near.across(r) + g if kind == 0 else heads * (2 * r + g + 1) - 1
            slot = lax.rem(r, 2)
            return pltpu.make_async_copy(source.at[:, pl.ds(pl.multiple_of(col * HEAD_DIM, HEAD_DIM), HEAD_DIM)],
                                         w_v.at[slot, :, pl.ds(g * HEAD_DIM, HEAD_DIM)], w_sems.at[slot, g])

        return count, own_load, w_load

    def hidden_start(kind, low=0, high=None):
        count, own_load, w_load = hidden_parts(kind)
        for g in range(2):
            if low == 0:
                w_load(jnp.int32(0), g).start()

            @pl.loop(low, high or count)
            def _(r):
                own_load(r, g).start()

    def hidden_add(kind, low=0, high=None):
        count, own_load, w_load = hidden_parts(kind)

        @pl.loop(low, high or count)
        def _(r):
            for g in range(2):
                w_load(r, g).wait()
                own_load(r, g).wait()

            @pl.when(r + 1 < count)
            def _():
                for g in range(2):
                    w_load(r + 1, g).start()

            for col in range(0, width, width // PARTS):
                at = slice(col, col + width // PARTS)
                acc[:, at] += dot(own[r], w_v[lax.rem(r, 2), at, :], COLS_COLS)

    a_load(ot_ref).start()
    start_b(jnp.int32(0))
    stage_in(0).start()
    ot_load.start()
    x_load.start()
    a_load(ot_ref).wait()

    @pl.loop(0, n_all)
    def _(step):
        slot = lax.rem(step, 2)
        for g in range(2):
            b_loads(dy_ref, 0, slot, g)[0].wait()

        @pl.when(jnp.logical_and(step != n_o - 1, step != n_oa - 1))
        def _():
            start_b(step + 1)

        @pl.when(step >= 2)
        def _():
            wait_tile(step - 2)

        @pl.when(step == n_o)
        def _():
            a_load(ht_ref).wait()

        for r in range(0, half, half // PARTS):
            tile[slot, r:r + half // PARTS, :] = dot(a_buf[r:r + half // PARTS, :], b_buf[slot])
        start_tile(step)

        @pl.when(step == n_o - 4)
        def _():
            acc[...] = jnp.zeros_like(acc)
            copy_own(0)
            gathers[0].middle()

        @pl.when(step == n_o - 1)
        def _():
            a_load(ht_ref).start()
            gathers[0].late()
            gathers[1].start()
            stage_out(0).wait()
            stage_in(1).start()
            result_part()
            gathers[0].end()
            start_b(step + 1)
            hidden_start(0)

        @pl.when(step == n_oa - 4)
        def _():
            copy_own(1)
            gathers[1].middle()

        @pl.when(step == n_oa - 2)
        def _():
            gathers[1].late()
            gathers[2].start()
            stage_out(1).wait()
            stage_in(2).start()

        @pl.when(step == n_oa - 1)
        def _():
            res_store.wait()
            x_load.start()
            dy_load.start()
            gathers[1].end()
            start_b(step + 1)
            hidden_add(0)
            hidden_start(1)

    copy_own(2)
    gathers[2].middle()
    hidden_add(1)
    gathers[2].late()
    stage_out(2).wait()
    gathers[2].end_sib()
    gathers[2].end_near()
    near_count = own.shape[0] * 3 // 4
    hidden_start(2, 0, near_count)
    for step in (n_all - 2, n_all - 1):
        wait_tile(jnp.int32(step))
    hidden_add(2, 0, near_count)
    gathers[2].end_far()
    hidden_start(2, near_count)
    hidden_add(2, near_count)

    gain = gain_ref[...].astype(F32)
    gg_v[...] = jnp.zeros_like(gg_v)
    x_load.wait()
    dy_load.wait()

    @pl.loop(0, rows // 32)
    def _(r):
        at = pl.ds(pl.multiple_of(r * 32, 32), 32)
        x_f = x_v[at, :].astype(F32)
        inv_rms = lax.rsqrt(jnp.mean(x_f * x_f, axis=-1, keepdims=True) + NORM_EPS)
        normed = x_f * inv_rms
        d_hid = acc[at, :]
        both = d_hid * normed
        gg_v[...] += jnp.sum(both.reshape(4, 8, width), axis=0)
        mean = jnp.mean(both * gain, axis=-1, keepdims=True)
        o_v[at, :] = (o_v[at, :].astype(F32) + inv_rms * (d_hid * gain - normed * mean)).astype(BF16)

    gg_row[...] = jnp.sum(gg_v[...], axis=0, keepdims=True)
    gg_all[near.me] = gg_row[...]
    parts = [send(gg_row, gg_all.at[near.me], gg_sems, r, peer) for r, peer in enumerate(near.others())]
    for copy in parts:
        copy.start()
    gx_store.start()

    @pl.loop(0, n_all)
    def _(step):
        whole_tile(step)[1].wait_recv()

    for copy in parts:
        copy.wait()
    gg_ref[...] = jnp.sum(gg_all[...], axis=0)
    gx_store.wait()


def step_kernel(heads, first_scratch, second_scratch, x_ref, gain_ref, pos_ref, freq_ref, dy_ref, wq_ref, wk_ref, wv_ref, wo_ref,
                h_all, dy_all, o_all, ht, d_kv, d_qa, d_qb, wo_out, wq_out, kv_all, qa_all, qb_all, res, gx, gg,
                pos_all, pos_sems, gg_row, gg_all, gg_sems, x_sems, h_sems, dy_sems, o_sems, kv_sems, qa_sems, qb_sems):
    near = Neighbours()
    seq_len = d_kv.shape[0]

    def gather_of(src, dst, sems):
        return Gather(near, lambda c: src.at[pl.ds(c * (seq_len // CHUNKS), seq_len // CHUNKS), :], dst, seq_len, sems)

    gathers = [gather_of(d_qa, qa_all, qa_sems), gather_of(d_qb, qb_all, qb_sems), gather_of(d_kv, kv_all, kv_sems)]

    def first(*scratch):
        attention_part(heads, near, gathers[0], x_ref, gain_ref, pos_ref, freq_ref, dy_ref, wq_ref, wk_ref, wv_ref, wo_ref,
                       h_all, dy_all, o_all, ht, d_kv, d_qa, d_qb, pos_all, pos_sems, h_sems, dy_sems, o_sems, *scratch)

    def second(*scratch):
        products_part(heads, near, gathers, o_all, ht, dy_all, d_kv, d_qa, d_qb, x_ref, dy_ref, gain_ref, wo_ref, wk_ref, wv_ref, wq_ref,
                      wo_out, wq_out, kv_all, qa_all, qb_all, res, gx, gg, gg_row, gg_all, gg_sems, x_sems, *scratch)

    pl.run_scoped(first, *first_scratch)
    pl.run_scoped(second, *second_scratch)


def step(x, gain, positions, grad_out, w_q, w_k, w_v, w_o, sp_size, heads):
    rows, width = x.shape
    seq_len = rows * sp_size
    q_cols = heads * HEAD_DIM
    all_cols = q_cols * sp_size
    half = width // 2
    cols = 4 * HEAD_DIM
    n_all = (width + all_cols) // cols
    any_spec = pl.BlockSpec(memory_space=pl.ANY)
    vmem = pl.BlockSpec(memory_space=pltpu.VMEM)
    dma = pltpu.SemaphoreType.DMA
    inv_freq = ROPE_THETA ** (-np.arange(0, HEAD_DIM, 2) / HEAD_DIM)
    freq = jnp.asarray(np.concatenate([inv_freq, inv_freq])[None, :], F32)
    pairs = heads * seq_len * (seq_len + rows) // 2
    out = lambda *shape, dtype=BF16: jax.ShapeDtypeStruct(shape, dtype)
    array = lambda *shape, dtype=BF16: pltpu.VMEM(shape, dtype)
    blocks = lambda *shape, dtype=BF16: pltpu.VMEM((sp_size,) + shape, dtype)
    first_scratch = [array(rows, width), array(rows, width), dma((CHUNKS,)), dma((3,)), blocks(rows, HEAD_DIM, dtype=F32),
                     blocks(rows, HEAD_DIM, dtype=F32), array(width, q_cols + 2 * HEAD_DIM), array(q_cols, width), dma((4,)),
                     array(2, rows, width), dma((2,)), array(2, width, rows), dma((2,)),
                     blocks(rows, q_cols), blocks(rows, HEAD_DIM), blocks(rows, HEAD_DIM), blocks(HEAD_DIM, rows), blocks(HEAD_DIM, rows),
                     array(q_cols, seq_len), blocks(8, rows, dtype=F32), array(heads, HEAD_DIM, rows, dtype=F32),
                     blocks(rows, q_cols), blocks(rows, HEAD_DIM, dtype=F32), blocks(rows, HEAD_DIM, dtype=F32),
                     array(2, rows, q_cols), dma((2, 2)), array(seq_len, 2 * HEAD_DIM)]
    second_scratch = [array(half, seq_len), array(2, seq_len, cols), array(2, half, cols, dtype=F32), dma, dma((2, 2)), dma((2,)),
                      array(seq_len, 2 * HEAD_DIM), dma((2,)), array(all_cols, rows), array(rows, all_cols), array(rows, width),
                      dma((4,)), blocks(rows, 2 * HEAD_DIM), dma((sp_size, 2)), array(2, width, 2 * HEAD_DIM), dma((2, 2)),
                      array(rows, width, dtype=F32), array(8, width, dtype=F32)]
    return pl.pallas_call(
        functools.partial(step_kernel, heads, first_scratch, second_scratch),
        in_specs=[any_spec, vmem, vmem, vmem] + [any_spec] * 5,
        out_specs=[any_spec] * 14 + [vmem],
        out_shape=[out(seq_len, width), out(seq_len, width), out(all_cols, seq_len), out(width, seq_len), out(seq_len, 2 * HEAD_DIM),
                   out(seq_len, q_cols - HEAD_DIM), out(seq_len, HEAD_DIM), out(all_cols, width, dtype=F32), out(width, all_cols, dtype=F32),
                   out(sp_size * seq_len, 2 * HEAD_DIM), out(sp_size * seq_len, q_cols - HEAD_DIM), out(sp_size * seq_len, HEAD_DIM),
                   out(rows, width), out(rows, width), out(1, width, dtype=F32)],
        scratch_shapes=[blocks(8, rows, dtype=jnp.int32), dma((2, 7)), array(1, width, dtype=F32), blocks(1, width, dtype=F32), dma((2, 7)),
                        dma((2, n_all))] + [SEMS] * 6,
        compiler_params=pltpu.CompilerParams(vmem_limit_bytes=VMEM_LIMIT, collective_id=0, has_side_effects=True),
        cost_estimate=pl.CostEstimate(flops=28 * pairs * HEAD_DIM + 2 * half * cols * seq_len * n_all, bytes_accessed=20 * seq_len * width,
                                      transcendentals=2 * pairs),
        name="step",
    )(x, gain, positions.reshape(1, -1), freq, grad_out, w_q, w_k, w_v, w_o)


def finish_kernel(ht_ref, d_ref, gx_in, res_in, gg_in, wo_in, wq_in, wk_ref, wv_ref, wq_ref, wo_ref, gx_ref, res_ref, gg_ref, d_v, d_sems, ring, ring_sems):
    step = pl.program_id(0) * pl.num_programs(1) + pl.program_id(1)
    high = ring.shape[2]
    per_array = wo_in.shape[0] // (high * RING)

    def copy_in(src, g, n):
        at = pl.ds(pl.multiple_of((lax.rem(g, per_array) * RING + n) * high, high), high)
        return pltpu.make_async_copy(src.at[at, :], ring.at[lax.rem(g, DEPTH), n], ring_sems.at[0, lax.rem(g, DEPTH), n])

    def copy_out(dst, g, n):
        at = pl.ds(pl.multiple_of((lax.rem(g, per_array) * RING + n) * high, high), high)
        return pltpu.make_async_copy(ring.at[lax.rem(g, DEPTH), n], dst.at[at, :], ring_sems.at[1, lax.rem(g, DEPTH), n])

    def start(copy, first, second, g):
        for ref, mine in ((first, g < per_array), (second, g >= per_array)):
            @pl.when(mine)
            def _():
                for n in range(RING):
                    copy(ref, g, n).start()

    def pair_load(p):
        at = pl.ds(2 * p, 2)
        return pltpu.make_async_copy(d_ref.at[at], d_v.at[at], d_sems.at[p])

    @pl.when(step == 0)
    def _():
        for p in range(d_v.shape[0] // 2):
            pair_load(p).start()

    last = pl.num_programs(0) * pl.num_programs(1) - 1

    def free(g):
        for n in range(RING):
            copy_out(wo_ref, g, n).wait()

    def pass_on(g):
        for n in range(RING):
            copy_in(wo_in, g, n).wait()
        start(copy_out, wo_ref, wq_ref, g)

    @pl.when(step >= DEPTH)
    def _():
        free(step - DEPTH)

    start(copy_in, wo_in, wq_in, step)

    @pl.when(step >= 1)
    def _():
        pass_on(step - 1)

    for p in range(d_v.shape[0] // 2):
        @pl.when(step == p)
        def _():
            pair_load(p).wait()

    ht = ht_ref[...]
    pair = 2 * pl.program_id(1)
    wk_ref[...] = dot(ht, lanes(d_v[pair, :, :HEAD_DIM], d_v[pair + 1, :, :HEAD_DIM]))
    wv_ref[...] = dot(ht, lanes(d_v[pair, :, HEAD_DIM:], d_v[pair + 1, :, HEAD_DIM:]))

    @pl.when(step == 0)
    def _():
        gg_ref[...] = gg_in[...]

    @pl.when(step == last)
    def _():
        pass_on(last)
        for back in range(DEPTH):
            free(last - back)

    @pl.when(step < ROW_STEPS)
    def _():
        gx_ref[...] = gx_in[...]
        res_ref[...] = res_in[...]


def finish(ht, d_kv, w_o_grad, w_q_grad, grad_x, result, grad_gain):
    width, seq_len = ht.shape
    groups = d_kv.shape[0]
    n_j = groups // 2
    steps = (width // MROWS) * n_j
    high = width // COPY_ROWS
    assert w_o_grad.shape[0] + w_q_grad.shape[0] == high * RING * steps
    any_spec = pl.BlockSpec(memory_space=pl.ANY)
    rows = pl.BlockSpec((grad_x.shape[0] // ROW_STEPS, width), lambda m, j: (jnp.minimum(m * n_j + j, ROW_STEPS - 1), 0))
    whole = pl.BlockSpec((1, width), lambda m, j: (0, 0))
    kv_out = pl.BlockSpec((MROWS, 2 * HEAD_DIM), lambda m, j: (m, j))
    out = lambda cols: jax.ShapeDtypeStruct((width, cols), F32)
    like = lambda val: jax.ShapeDtypeStruct(val.shape, val.dtype)
    return pl.pallas_call(
        finish_kernel,
        grid=(width // MROWS, n_j),
        in_specs=[pl.BlockSpec((MROWS, seq_len), lambda m, j: (m, 0)), any_spec, rows, rows, whole, any_spec, any_spec],
        out_specs=[kv_out, kv_out, any_spec, any_spec, rows, rows, whole],
        out_shape=[out(groups * HEAD_DIM), out(groups * HEAD_DIM), like(w_q_grad), like(w_o_grad), like(grad_x), like(result), like(grad_gain)],
        scratch_shapes=[pltpu.VMEM(d_kv.shape, BF16), pltpu.SemaphoreType.DMA((groups // 2,)),
                        pltpu.VMEM((DEPTH, RING, high, width), F32), pltpu.SemaphoreType.DMA((2, DEPTH, RING))],
        compiler_params=params(2),
        cost_estimate=pl.CostEstimate(flops=4 * width * seq_len * groups * HEAD_DIM, bytes_accessed=2 * width * seq_len, transcendentals=0),
        name="finish",
    )(ht, d_kv, grad_x, result, grad_gain, w_o_grad, w_q_grad)


def solution(mesh):
    sp_size = mesh.shape['sp']
    seq_spec = P(('dp', 'sp'), None)
    pos_spec = P(('dp', 'sp'))
    replicated = P(None, None)
    part_rows = P('dp', None)

    def local_step(x, grad_out, positions, gain, w_q, w_k, w_v, w_o):
        n_heads = w_q.shape[1] // HEAD_DIM
        heads = n_heads // sp_size
        _, _, _, ht, _, _, _, w_o_grad, w_q_grad, kv_all, _, _, result, grad_x, grad_gain = step(
            x, gain.reshape(1, -1), positions, grad_out, w_q, w_k, w_v, w_o, sp_size, heads)
        grad_wk, grad_wv, grad_wq, grad_wo, grad_x, result, grad_gain = finish(
            ht, kv_all.reshape(sp_size, -1, 2 * HEAD_DIM), w_o_grad, w_q_grad, grad_x, result, grad_gain)
        return result, grad_x, grad_wq, grad_wk, grad_wv, grad_wo, grad_gain.reshape(-1)

    return jax.shard_map(local_step, mesh=mesh,
                         in_specs=(seq_spec, seq_spec, pos_spec, P(None), replicated, replicated, replicated, replicated),
                         out_specs=(seq_spec, seq_spec, part_rows, part_rows, part_rows, part_rows, P('dp')),
                         check_vma=False)
```

```python
import functools

import jax
import jax.numpy as jnp
import numpy as np
from jax import lax
from jax.experimental import pallas as pl
from jax.experimental.pallas import tpu as pltpu
from jax.sharding import PartitionSpec as P

HEAD_DIM = 128
HALF = HEAD_DIM // 2
ROPE_THETA = 1000000.0
NORM_EPS = 1e-05
NEG_LARGE = -1e30
LOG2E = 1.4426950408889634
BLK = 512
CHUNKS = 4
FWD_MIDDLE, BWD_MIDDLE = 5, 27
MROWS = 768
RING = 3
DEPTH = 4
COPY_ROWS = 24
PARTS = 3
ROW_STEPS = 8
F32 = jnp.float32
BF16 = jnp.bfloat16
ROWS_ROWS = (((0,), (0,)), ((), ()))
COLS_COLS = (((1,), (1,)), ((), ()))
ROWS_COLS = (((0,), (1,)), ((), ()))
VMEM_LIMIT = 63 * 1024 * 1024


def dot(a, b, dims=(((1,), (0,)), ((), ()))):
    return lax.dot_general(a, b, dims, preferred_element_type=F32)


def params(axes=1):
    return pltpu.CompilerParams(dimension_semantics=("arbitrary",) * axes, vmem_limit_bytes=VMEM_LIMIT)


class Neighbours:
    def __init__(self):
        self.me = lax.axis_index('sp')
        core, col, row = lax.rem(self.me, 2), lax.rem(self.me // 2, 2), self.me // 4
        self.sib = self.me + 1 - 2 * core
        self.xn = self.me + 2 - 4 * col
        self.yn = self.me + 4 - 8 * row
        self.diag = self.xn + self.yn - self.me

    def meet(self, peers):
        barrier = pltpu.get_barrier_semaphore()
        for peer in peers:
            pl.semaphore_signal(barrier, inc=1, device_id={'sp': peer}, device_id_type=pl.DeviceIdType.MESH)
        pl.semaphore_wait(barrier, len(peers))

    def across(self, r):
        core, col, row = lax.rem(self.me, 2), lax.rem(self.me // 2, 2), self.me // 4
        return (self.me + lax.rem(r, 2) * (1 - 2 * core) + lax.rem(r // 2, 2) * (2 - 4 * col) + (r // 4) * (4 - 8 * row))

    def others(self):
        flip = lambda dev: dev + 1 - 2 * lax.rem(dev, 2)
        return [self.sib, self.xn, flip(self.xn), self.yn, flip(self.yn), self.diag, flip(self.diag)]


def send(src, dst, sems, index, peer):
    return pltpu.make_async_remote_copy(src_ref=src, dst_ref=dst, send_sem=sems.at[0, index], recv_sem=sems.at[1, index],
                                        device_id={'sp': peer}, device_id_type=pl.DeviceIdType.MESH)


class Gather:
    COPIES = 22

    def __init__(self, near, own, dst, rows, sems):
        self.near, self.own, self.dst, self.rows, self.sems = near, own, dst, rows, sems

    def block(self, dev, chunk, count=1):
        size = self.rows // CHUNKS
        return self.dst.at[pl.ds(pl.multiple_of(dev * self.rows + chunk * size, size), count * size), :]

    def first(self, chunk, kind):
        peer = (self.near.xn, self.near.yn, self.near.sib)[kind]
        return send(self.own(chunk), self.block(self.near.me, chunk), self.sems, kind * CHUNKS + chunk, peer)

    def onward(self, chunk):
        over_y = chunk < CHUNKS // 2
        rows = self.block(self.near.xn if over_y else self.near.yn, chunk)
        return send(rows, rows, self.sems, 12 + chunk, self.near.yn if over_y else self.near.xn)

    def share(self, kind):
        rows = self.block((self.near.xn, self.near.yn)[kind], 0, CHUNKS)
        return send(rows, rows, self.sems, 16 + kind, self.near.sib)

    def share_diag(self, chunk):
        rows = self.block(self.near.diag, chunk)
        return send(rows, rows, self.sems, 18 + chunk, self.near.sib)

    def start(self):
        for chunk in range(CHUNKS):
            for kind in (0, 1):
                self.send_first(chunk, kind)
            self.first(chunk, 2).start()

    def send_first(self, turn, kind):
        self.first(turn if kind == 0 else (turn + CHUNKS // 2) % CHUNKS, kind).start()

    def middle(self):
        for chunk in (0, 2, 1, 3):
            self.first(chunk, 0 if chunk < CHUNKS // 2 else 1).wait_recv()
            self.onward(chunk).start()

    def late(self):
        for chunk in (2, 3):
            self.first(chunk, 0).wait_recv()
        self.share(0).start()
        for chunk in (0, 1):
            self.first(chunk, 1).wait_recv()
        self.share(1).start()

    def end_sib(self):
        for chunk in range(CHUNKS):
            self.first(chunk, 2).wait_recv()

    def end_near(self):
        for kind in range(2):
            self.share(kind).wait_recv()

    def end_far(self, between=None):
        for chunk in (0, 2, 1, 3):
            self.onward(chunk).wait_recv()
            self.share_diag(chunk).start()
            if chunk == 2 and between:
                between()
        for chunk in range(CHUNKS):
            for kind in range(3):
                self.first(chunk, kind).wait_send()
            self.onward(chunk).wait_send()
        for kind in range(2):
            self.share(kind).wait_send()
        for chunk in range(CHUNKS):
            self.share_diag(chunk).wait()

    def end(self, between=None):
        self.end_sib()
        self.end_near()
        self.end_far(between)


SEMS = pltpu.SemaphoreType.DMA((2, Gather.COPIES))


def masked(scores):
    key = lax.broadcasted_iota(jnp.int32, scores.shape, 0)
    query = lax.broadcasted_iota(jnp.int32, scores.shape, 1)
    return jnp.where(key <= query, scores, NEG_LARGE)


def unrotate(val, cos_t, sin_t):
    return (val * cos_t - pltpu.roll(val, HALF, 1) * sin_t).astype(BF16)


def attention_part(heads, near, gather_next, x_ref, gain_ref, pos_ref, freq_ref, dy_ref, wq_ref, wk_ref, wv_ref, wo_ref,
                   h_all, dy_all, o_all, ht_ref, dkv_ref, dq_a_ref, dq_b_ref, pos_all, pos_sems, h_sems, dy_sems, o_sems,
                   x_v, h_v, x_sems, own_sems, cos_s, sin_s, w_v, wo_v, w_sems, blk, blk_sems, ht_v, ht_sems,
                   q_s, k_s, v_s, vt, kt, ot_s, lse_s, acc, do_s, dk_acc, dv_acc, dq_v, dq_sems, dkv_v):
    rows, width = x_ref.shape
    n_blocks = k_s.shape[0]
    q_cols = heads * HEAD_DIM
    size = rows // CHUNKS
    qk_scale = HEAD_DIM ** -0.5
    to_log2 = qk_scale * LOG2E
    cols = [slice(a * HEAD_DIM, (a + 1) * HEAD_DIM) for a in range(heads)]
    part = lambda ref, chunk, count=size: ref.at[pl.ds(chunk * count, count), :]
    gather_h = Gather(near, lambda chunk: part(h_v, chunk), h_all, rows, h_sems)
    gather_dy = Gather(near, lambda chunk: part(dy_ref, chunk), dy_all, rows, dy_sems)
    gather_o = Gather(near, lambda chunk: part(ot_s, chunk, q_cols // CHUNKS), o_all, q_cols, o_sems)

    loads = [pltpu.make_async_copy(part(x_ref, chunk), part(x_v, chunk), x_sems.at[chunk]) for chunk in range(CHUNKS)]
    for load in loads:
        load.start()
    others = near.others()
    near.meet(others)
    pos_all[near.me] = jnp.broadcast_to(pos_ref[...], pos_all.shape[1:])
    positions = [send(pos_ref, pos_all.at[near.me, pl.ds(0, 1), :], pos_sems, r, peer) for r, peer in enumerate(others)]
    gain = gain_ref[...].astype(F32)
    for turn, chunk in enumerate((0, 2, 1, 3)):
        loads[chunk].wait()

        @pl.loop(0, size // 32)
        def _(r):
            at = pl.ds(pl.multiple_of(chunk * size + r * 32, 32), 32)
            x_f = x_v[at, :].astype(F32)
            normed = x_f * lax.rsqrt(jnp.mean(x_f * x_f, axis=-1, keepdims=True) + NORM_EPS)
            h_v[at, :] = (normed * gain).astype(BF16)

        gather_h.send_first(turn // 2, turn % 2)
        gather_h.first(chunk, 2).start()
    for turn in (2, 3):
        for kind in (0, 1):
            gather_h.send_first(turn, kind)
    for copy in positions:
        copy.start()
    own_h = pltpu.make_async_copy(h_v, gather_h.block(near.me, 0, CHUNKS), own_sems.at[0])
    own_h.start()
    w_loads, col = [], 0
    for n, (ref, count) in enumerate(((wq_ref, q_cols), (wk_ref, HEAD_DIM), (wv_ref, HEAD_DIM))):
        at = pl.ds(pl.multiple_of(near.me * count, HEAD_DIM), count)
        w_loads.append(pltpu.make_async_copy(ref.at[:, at], w_v.at[:, pl.ds(col, count)], w_sems.at[n]))
        col += count
    w_loads.append(pltpu.make_async_copy(wo_ref.at[pl.ds(pl.multiple_of(near.me * q_cols, q_cols), q_cols), :], wo_v, w_sems.at[3]))
    stage_in = pltpu.make_async_copy(dy_ref, x_v, own_sems.at[1])
    stage_out = pltpu.make_async_copy(x_v, gather_dy.block(near.me, 0, CHUNKS), own_sems.at[2])
    for load in w_loads + [stage_in]:
        load.start()
    for copy in positions:
        copy.wait()
    sign = jnp.where(lax.broadcasted_iota(jnp.int32, (1, HEAD_DIM), 1) < HALF, -1.0, 1.0)

    @pl.loop(0, n_blocks)
    def _(b):
        pos = jnp.broadcast_to(pos_all[b, 0:1, :].astype(F32), (HEAD_DIM, rows)).T
        angles = pos * freq_ref[...]
        cos_s[b] = jnp.cos(angles)
        sin_s[b] = jnp.sin(angles) * sign

    gather_h.middle()
    for load in w_loads + [stage_in]:
        load.wait()
    stage_out.start()
    own_h.wait()

    def block_load(ref, block, slot):
        return pltpu.make_async_copy(ref.at[pl.ds(pl.multiple_of(block * rows, rows), rows), :], blk.at[slot], blk_sems.at[slot])

    far = n_blocks * 3 // 4

    def arrive(r, ref, gather, before_near=None, between=None):
        slot = lax.rem(r, 2)

        @pl.when(r == 1)
        def _():
            gather.end_sib()

        @pl.when(r == 2)
        def _():
            if before_near:
                before_near()
            gather.end_near()

        @pl.when(r == far)
        def _():
            gather.end_far(between)

        @pl.when(functools.reduce(jnp.logical_or, [r == first for first in (0, 1, 2, far)]))
        def _():
            block_load(ref, near.across(r), slot).start()

        block_load(ref, 0, slot).wait()

        @pl.when(functools.reduce(jnp.logical_and, [r + 1 != first for first in (1, 2, far, n_blocks)]))
        def _():
            block_load(ref, near.across(r + 1), 1 - slot).start()

    def ht_store(r):
        at = pl.ds(pl.multiple_of(near.across(r) * rows, rows), rows)
        return pltpu.make_async_copy(ht_v.at[lax.rem(r, 2)], ht_ref.at[:, at], ht_sems.at[lax.rem(r, 2)])

    @pl.loop(0, n_blocks)
    def _(r):
        i = near.across(r)
        slot = lax.rem(r, 2)
        arrive(r, h_all, gather_h, gather_h.late, gather_dy.start)

        @pl.when(r >= 2)
        def _():
            ht_store(r - 2).wait()

        ht_v[slot] = blk[slot].T
        ht_store(r).start()
        prod = dot(blk[slot], w_v[...])
        cos_t, sin_t = cos_s[i], sin_s[i]
        for a in range(heads + 1):
            val = prod[:, a * HEAD_DIM:(a + 1) * HEAD_DIM]
            rot = (val * cos_t + pltpu.roll(val, HALF, 1) * sin_t).astype(BF16)
            if a < heads:
                q_s[i, :, cols[a]] = rot
            else:
                k_s[i] = rot
                kt[i] = rot.T
        v_i = prod[:, q_cols + HEAD_DIM:].astype(BF16)
        v_s[i] = v_i
        vt[i] = v_i.T

    def fwd_chunk(i, c, carry, diagonal):
        k_c, vt_c = k_s[c], vt[c]
        scores = [dot(k_c, q_s[i, :, cols[a]], COLS_COLS) * to_log2 for a in range(heads)]
        out = []
        for a in range(heads):
            s = masked(scores[a]) if diagonal else scores[a]
            m_old, l_old = carry[a]
            m_new = jnp.maximum(m_old, jnp.max(s, axis=0, keepdims=True))
            alpha = jnp.exp2(m_old - m_new)
            p = jnp.exp2(s - m_new)
            l_new = l_old * alpha + jnp.sum(p, axis=0, keepdims=True)
            acc[a] = acc[a] * alpha + dot(vt_c, p.astype(BF16))
            out.append((m_new, l_new))
        return tuple(out)

    @pl.loop(0, n_blocks)
    def _(i):
        acc[...] = jnp.zeros_like(acc)
        start = tuple((jnp.full((1, rows), NEG_LARGE, F32), jnp.zeros((1, rows), F32)) for _ in range(heads))
        carry = lax.fori_loop(0, i, lambda c, carry: fwd_chunk(i, c, carry, False), start)
        carry = fwd_chunk(i, i, carry, True)
        at = pl.ds(pl.multiple_of(i * rows, rows), rows)
        for a in range(heads):
            m_a, l_a = carry[a]
            ot_s[cols[a], at] = (acc[a] / l_a).astype(BF16)
            lse_s[i, a:a + 1, :] = m_a + jnp.log2(l_a)

        @pl.when(i == FWD_MIDDLE)
        def _():
            gather_dy.middle()

    gather_dy.late()
    gather_o.start()
    own_o = pltpu.make_async_copy(ot_s, gather_o.block(near.me, 0, CHUNKS), own_sems.at[0])
    own_o.start()

    def bwd_chunk(i, c, delta, diagonal):
        k_c, v_c, kt_c = k_s[c], v_s[c], kt[c]
        dk_c = dv_c = None
        for a in range(heads):
            q_a, do_a = q_s[i, :, cols[a]], do_s[i, :, cols[a]]
            s = dot(k_c, q_a, COLS_COLS) * to_log2
            if diagonal:
                s = masked(s)
            p = jnp.exp2(s - lse_s[i, a:a + 1, :])
            d_p = dot(v_c, do_a, COLS_COLS)
            d_s = (p * (d_p - delta[a])).astype(BF16)
            dv_a = dot(p.astype(BF16), do_a)
            dk_a = dot(d_s, q_a)
            dv_c = dv_a if dv_c is None else dv_c + dv_a
            dk_c = dk_a if dk_c is None else dk_c + dk_a
            acc[a] += dot(kt_c, d_s)
        dk_acc[c] += dk_c
        dv_acc[c] += dv_c

    def dq_stores(r):
        slot = lax.rem(r, 2)
        at = pl.ds(pl.multiple_of(near.across(r) * rows, rows), rows)
        last = q_cols - HEAD_DIM
        return [pltpu.make_async_copy(dq_v.at[slot, :, pl.ds(0, last)], dq_a_ref.at[at, :], dq_sems.at[slot, 0]),
                pltpu.make_async_copy(dq_v.at[slot, :, pl.ds(last, HEAD_DIM)], dq_b_ref.at[at, :], dq_sems.at[slot, 1])]

    def pass_on(done):
        @pl.when(done == BWD_MIDDLE)
        def _():
            gather_o.middle()

    for r in (n_blocks - 2, n_blocks - 1):
        ht_store(jnp.int32(r)).wait()
    dk_acc[...] = jnp.zeros_like(dk_acc)
    dv_acc[...] = jnp.zeros_like(dv_acc)
    stage_out.wait()

    def bwd_block(r, done):
        i = near.across(r)
        slot = lax.rem(r, 2)
        at = pl.ds(pl.multiple_of(i * rows, rows), rows)

        arrive(r, dy_all, gather_dy)
        do_s[i] = dot(blk[slot], wo_v[...], COLS_COLS).astype(BF16)
        acc[...] = jnp.zeros_like(acc)
        delta = [jnp.sum(ot_s[cols[a], at].astype(F32) * do_s[i, :, cols[a]].T.astype(F32), axis=0, keepdims=True) for a in range(heads)]

        @pl.loop(0, i)
        def _(c):
            bwd_chunk(i, c, delta, False)
            pass_on(done + c)

        bwd_chunk(i, i, delta, True)
        pass_on(done + i)

        @pl.when(r >= 2)
        def _():
            for store in dq_stores(r - 2):
                store.wait()

        for a in range(heads):
            dq_v[slot, :, cols[a]] = unrotate(acc[a].T * qk_scale, cos_s[i], sin_s[i])
        for store in dq_stores(r):
            store.start()
        return done + i + 1

    lax.fori_loop(0, n_blocks, bwd_block, jnp.int32(0))
    gather_o.late()
    for r in (n_blocks - 2, n_blocks - 1):
        for store in dq_stores(r):
            store.wait()
    gather_next.start()

    @pl.loop(0, n_blocks)
    def _(c):
        at = pl.ds(pl.multiple_of(c * rows, rows), rows)
        dkv_v[at, :HEAD_DIM] = unrotate(dk_acc[c] * qk_scale, cos_s[c], sin_s[c])
        dkv_v[at, HEAD_DIM:] = dv_acc[c].astype(BF16)

    dkv_store = pltpu.make_async_copy(dkv_v, dkv_ref, own_sems.at[1])
    dkv_store.start()
    own_o.wait()
    gather_o.end()
    dkv_store.wait()


def lanes(*parts):
    return jnp.concatenate(parts, axis=1)


def products_part(heads, near, gathers, ot_ref, ht_ref, dy_ref, d_kv_ref, d_qa_ref, d_qb_ref, x_ref, own_dy_ref, gain_ref, wo_ref, wk_ref, wv_ref, wq_ref,
                  wo_out, wq_out, kv_all, qa_all, qb_all, res_ref, gx_ref, gg_ref, gg_row, gg_all, gg_sems, x_sems,
                  a_buf, b_buf, tile, a_sem, b_sems, t_sems, stage, stage_sems, ot_v, o_v, x_v, io_sems, own, own_sems, w_v, w_sems, acc,
                  gg_v):
    core = lax.rem(near.me, 2)
    half = a_buf.shape[0]
    seq_len = d_kv_ref.shape[0]
    rows, width = x_ref.shape
    n_cols = d_kv_ref.shape[1]
    n_o, n_all = width // (2 * n_cols), x_sems.shape[1]
    n_oa = n_o + (n_all - n_o) * 2 // 3

    local = (d_qa_ref, d_qb_ref, d_kv_ref)

    def stage_in(n):
        return pltpu.make_async_copy(local[n], stage.at[:, pl.ds(0, local[n].shape[1])], stage_sems.at[0])

    def stage_out(n):
        return pltpu.make_async_copy(stage.at[:, pl.ds(0, local[n].shape[1])], gathers[n].block(near.me, 0, CHUNKS), stage_sems.at[1])

    def copy_own(n):
        stage_in(n).wait()
        stage_out(n).start()

    own_rows = pl.ds(pl.multiple_of(core * half, half), half)
    tokens = pl.ds(pl.multiple_of(near.me * rows, rows), rows)
    ot_load = pltpu.make_async_copy(ot_ref.at[:, tokens], ot_v, io_sems.at[0])
    x_load = pltpu.make_async_copy(x_ref, x_v, io_sems.at[1])
    res_store = pltpu.make_async_copy(x_v, res_ref, io_sems.at[2])
    dy_load = pltpu.make_async_copy(own_dy_ref, o_v, io_sems.at[3])
    gx_store = pltpu.make_async_copy(o_v, gx_ref, io_sems.at[0])

    def a_load(ref):
        return pltpu.make_async_copy(ref.at[own_rows, :], a_buf, a_sem)

    def b_loads(source, p, slot, g):
        if source is dy_ref:
            srcs = [dy_ref.at[:, pl.ds(pl.multiple_of((2 * p + g) * n_cols, n_cols), n_cols)]]
        else:
            per = n_cols // source.shape[1]
            srcs = [source.at[pl.ds(pl.multiple_of(((2 * p + g) * per + n) * seq_len, seq_len), seq_len), :] for n in range(per)]
        return [pltpu.make_async_copy(src, b_buf.at[slot, :, pl.ds(g * n_cols + n * src.shape[1], src.shape[1])], b_sems.at[slot, g])
                for n, src in enumerate(srcs)]

    def start_b(step):
        slot = lax.rem(step, 2)
        for source, low, high in ((dy_ref, 0, n_o), (qa_all, n_o, n_oa), (qb_all, n_oa, n_all)):
            @pl.when(jnp.logical_and(step >= low, step < high))
            def _():
                for g in range(2):
                    for load in b_loads(source, step - low, slot, g):
                        load.start()

    def pieces(kind, step):
        wide = (2 * n_cols, n_cols, HEAD_DIM)[kind]
        slot = lax.rem(step, 2)
        out = []
        for n in range(2 * n_cols // wide):
            group = (step - (0, n_o, n_oa)[kind]) * (2 * n_cols // wide) + n
            col = (group * wide, group * heads * HEAD_DIM, (group + 1) * heads * HEAD_DIM - HEAD_DIM)[kind]
            dst = (wo_out, wq_out, wq_out)[kind].at[own_rows, pl.ds(pl.multiple_of(col, HEAD_DIM), wide)]
            src = tile.at[slot, :, pl.ds(n * wide, wide)]
            out.append((pltpu.make_async_copy(src, dst, t_sems.at[slot]), send(src, dst, x_sems, step, near.sib)))
        return out

    def start_tile(step):
        for kind, (low, high) in enumerate(((0, n_o), (n_o, n_oa), (n_oa, n_all))):
            @pl.when(jnp.logical_and(step >= low, step < high))
            def _():
                for keep, give in pieces(kind, step):
                    keep.start()
                    give.start()

    def whole_tile(step):
        slot = lax.rem(step, 2)
        dst = wo_out.at[own_rows, pl.ds(0, 2 * n_cols)]
        return pltpu.make_async_copy(tile.at[slot], dst, t_sems.at[slot]), send(tile.at[slot], dst, x_sems, step, near.sib)

    def wait_tile(step):
        keep, give = whole_tile(step)
        keep.wait()
        give.wait_send()

    def result_part():
        cols = b_buf.shape[2]

        def w_load(n):
            slot = lax.rem(n, 2)
            return pltpu.make_async_copy(wo_ref.at[:, pl.ds(pl.multiple_of(n * cols, cols), cols)], b_buf.at[slot, pl.ds(0, wo_ref.shape[0]), :],
                                         b_sems.at[slot, 0])

        w_load(jnp.int32(0)).start()
        ot_load.wait()

        @pl.loop(0, ot_v.shape[0] // BLK)
        def _(r):
            at = pl.ds(pl.multiple_of(r * BLK, BLK), BLK)
            o_v[:, at] = ot_v[at, :].T

        x_load.wait()

        @pl.loop(0, n_o)
        def _(n):
            w_load(n).wait()

            @pl.when(n + 1 < n_o)
            def _():
                w_load(n + 1).start()

            at = pl.ds(pl.multiple_of(n * cols, cols), cols)
            x_v[:, at] = (x_v[:, at].astype(F32) + dot(o_v[...], b_buf[lax.rem(n, 2), :wo_ref.shape[0], :])).astype(BF16)

        res_store.start()

    def hidden_parts(kind):
        count = own.shape[0] // (2 if kind == 1 else 1)

        def own_load(r, g):
            source = (qa_all, qb_all, kv_all)[kind]
            device, col = (2 * r + g, 0) if kind == 1 else (near.across(r), g * HEAD_DIM)
            at = pl.ds(pl.multiple_of(device * seq_len + near.me * rows, rows), rows)
            return pltpu.make_async_copy(source.at[at, pl.ds(col, HEAD_DIM)], own.at[r, :, pl.ds(g * HEAD_DIM, HEAD_DIM)], own_sems.at[r, g])

        def w_load(r, g):
            source = (wk_ref, wv_ref)[g] if kind == 2 else wq_ref
            col = near.across(r) if kind == 2 else heads * near.across(r) + g if kind == 0 else heads * (2 * r + g + 1) - 1
            slot = lax.rem(r, 2)
            return pltpu.make_async_copy(source.at[:, pl.ds(pl.multiple_of(col * HEAD_DIM, HEAD_DIM), HEAD_DIM)],
                                         w_v.at[slot, :, pl.ds(g * HEAD_DIM, HEAD_DIM)], w_sems.at[slot, g])

        return count, own_load, w_load

    def hidden_start(kind, low=0, high=None):
        count, own_load, w_load = hidden_parts(kind)
        for g in range(2):
            if low == 0:
                w_load(jnp.int32(0), g).start()

            @pl.loop(low, high or count)
            def _(r):
                own_load(r, g).start()

    def hidden_add(kind, low=0, high=None):
        count, own_load, w_load = hidden_parts(kind)

        @pl.loop(low, high or count)
        def _(r):
            for g in range(2):
                w_load(r, g).wait()
                own_load(r, g).wait()

            @pl.when(r + 1 < count)
            def _():
                for g in range(2):
                    w_load(r + 1, g).start()

            for col in range(0, width, width // PARTS):
                at = slice(col, col + width // PARTS)
                acc[:, at] += dot(own[r], w_v[lax.rem(r, 2), at, :], COLS_COLS)

    a_load(ot_ref).start()
    start_b(jnp.int32(0))
    stage_in(0).start()
    ot_load.start()
    x_load.start()
    a_load(ot_ref).wait()

    @pl.loop(0, n_all)
    def _(step):
        slot = lax.rem(step, 2)
        for g in range(2):
            b_loads(dy_ref, 0, slot, g)[0].wait()

        @pl.when(jnp.logical_and(step != n_o - 1, step != n_oa - 1))
        def _():
            start_b(step + 1)

        @pl.when(step >= 2)
        def _():
            wait_tile(step - 2)

        @pl.when(step == n_o)
        def _():
            a_load(ht_ref).wait()

        for r in range(0, half, half // PARTS):
            tile[slot, r:r + half // PARTS, :] = dot(a_buf[r:r + half // PARTS, :], b_buf[slot])
        start_tile(step)

        @pl.when(step == n_o - 4)
        def _():
            acc[...] = jnp.zeros_like(acc)
            copy_own(0)
            gathers[0].middle()

        @pl.when(step == n_o - 1)
        def _():
            a_load(ht_ref).start()
            gathers[0].late()
            gathers[1].start()
            stage_out(0).wait()
            stage_in(1).start()
            result_part()
            gathers[0].end()
            start_b(step + 1)
            hidden_start(0)

        @pl.when(step == n_oa - 4)
        def _():
            copy_own(1)
            gathers[1].middle()

        @pl.when(step == n_oa - 2)
        def _():
            gathers[1].late()
            gathers[2].start()
            stage_out(1).wait()
            stage_in(2).start()

        @pl.when(step == n_oa - 1)
        def _():
            res_store.wait()
            x_load.start()
            dy_load.start()
            gathers[1].end()
            start_b(step + 1)

    hidden_add(0)
    copy_own(2)
    gathers[2].middle()
    hidden_start(1)
    hidden_add(1)
    gathers[2].late()
    stage_out(2).wait()
    gathers[2].end_sib()
    gathers[2].end_near()
    near_count = own.shape[0] * 3 // 4
    hidden_start(2, 0, near_count)
    for step in (n_all - 2, n_all - 1):
        wait_tile(jnp.int32(step))
    hidden_add(2, 0, near_count)
    gathers[2].end_far()
    hidden_start(2, near_count)
    hidden_add(2, near_count)

    gain = gain_ref[...].astype(F32)
    gg_v[...] = jnp.zeros_like(gg_v)
    x_load.wait()
    dy_load.wait()

    @pl.loop(0, rows // 32)
    def _(r):
        at = pl.ds(pl.multiple_of(r * 32, 32), 32)
        x_f = x_v[at, :].astype(F32)
        inv_rms = lax.rsqrt(jnp.mean(x_f * x_f, axis=-1, keepdims=True) + NORM_EPS)
        normed = x_f * inv_rms
        d_hid = acc[at, :]
        both = d_hid * normed
        gg_v[...] += jnp.sum(both.reshape(4, 8, width), axis=0)
        mean = jnp.mean(both * gain, axis=-1, keepdims=True)
        o_v[at, :] = (o_v[at, :].astype(F32) + inv_rms * (d_hid * gain - normed * mean)).astype(BF16)

    gg_row[...] = jnp.sum(gg_v[...], axis=0, keepdims=True)
    gg_all[near.me] = gg_row[...]
    parts = [send(gg_row, gg_all.at[near.me], gg_sems, r, peer) for r, peer in enumerate(near.others())]
    for copy in parts:
        copy.start()
    gx_store.start()

    @pl.loop(0, n_all)
    def _(step):
        whole_tile(step)[1].wait_recv()

    for copy in parts:
        copy.wait()
    gg_ref[...] = jnp.sum(gg_all[...], axis=0)
    gx_store.wait()


def step_kernel(heads, first_scratch, second_scratch, x_ref, gain_ref, pos_ref, freq_ref, dy_ref, wq_ref, wk_ref, wv_ref, wo_ref,
                h_all, dy_all, o_all, ht, d_kv, d_qa, d_qb, wo_out, wq_out, kv_all, qa_all, qb_all, res, gx, gg,
                pos_all, pos_sems, gg_row, gg_all, gg_sems, x_sems, h_sems, dy_sems, o_sems, kv_sems, qa_sems, qb_sems):
    near = Neighbours()
    seq_len = d_kv.shape[0]

    def gather_of(src, dst, sems):
        return Gather(near, lambda c: src.at[pl.ds(c * (seq_len // CHUNKS), seq_len // CHUNKS), :], dst, seq_len, sems)

    gathers = [gather_of(d_qa, qa_all, qa_sems), gather_of(d_qb, qb_all, qb_sems), gather_of(d_kv, kv_all, kv_sems)]

    def first(*scratch):
        attention_part(heads, near, gathers[0], x_ref, gain_ref, pos_ref, freq_ref, dy_ref, wq_ref, wk_ref, wv_ref, wo_ref,
                       h_all, dy_all, o_all, ht, d_kv, d_qa, d_qb, pos_all, pos_sems, h_sems, dy_sems, o_sems, *scratch)

    def second(*scratch):
        products_part(heads, near, gathers, o_all, ht, dy_all, d_kv, d_qa, d_qb, x_ref, dy_ref, gain_ref, wo_ref, wk_ref, wv_ref, wq_ref,
                      wo_out, wq_out, kv_all, qa_all, qb_all, res, gx, gg, gg_row, gg_all, gg_sems, x_sems, *scratch)

    pl.run_scoped(first, *first_scratch)
    pl.run_scoped(second, *second_scratch)


def step(x, gain, positions, grad_out, w_q, w_k, w_v, w_o, sp_size, heads):
    rows, width = x.shape
    seq_len = rows * sp_size
    q_cols = heads * HEAD_DIM
    all_cols = q_cols * sp_size
    half = width // 2
    cols = 4 * HEAD_DIM
    n_all = (width + all_cols) // cols
    any_spec = pl.BlockSpec(memory_space=pl.ANY)
    vmem = pl.BlockSpec(memory_space=pltpu.VMEM)
    dma = pltpu.SemaphoreType.DMA
    inv_freq = ROPE_THETA ** (-np.arange(0, HEAD_DIM, 2) / HEAD_DIM)
    freq = jnp.asarray(np.concatenate([inv_freq, inv_freq])[None, :], F32)
    pairs = heads * seq_len * (seq_len + rows) // 2
    out = lambda *shape, dtype=BF16: jax.ShapeDtypeStruct(shape, dtype)
    array = lambda *shape, dtype=BF16: pltpu.VMEM(shape, dtype)
    blocks = lambda *shape, dtype=BF16: pltpu.VMEM((sp_size,) + shape, dtype)
    first_scratch = [array(rows, width), array(rows, width), dma((CHUNKS,)), dma((3,)), blocks(rows, HEAD_DIM, dtype=F32),
                     blocks(rows, HEAD_DIM, dtype=F32), array(width, q_cols + 2 * HEAD_DIM), array(q_cols, width), dma((4,)),
                     array(2, rows, width), dma((2,)), array(2, width, rows), dma((2,)),
                     blocks(rows, q_cols), blocks(rows, HEAD_DIM), blocks(rows, HEAD_DIM), blocks(HEAD_DIM, rows), blocks(HEAD_DIM, rows),
                     array(q_cols, seq_len), blocks(8, rows, dtype=F32), array(heads, HEAD_DIM, rows, dtype=F32),
                     blocks(rows, q_cols), blocks(rows, HEAD_DIM, dtype=F32), blocks(rows, HEAD_DIM, dtype=F32),
                     array(2, rows, q_cols), dma((2, 2)), array(seq_len, 2 * HEAD_DIM)]
    second_scratch = [array(half, seq_len), array(2, seq_len, cols), array(2, half, cols, dtype=F32), dma, dma((2, 2)), dma((2,)),
                      array(seq_len, 2 * HEAD_DIM), dma((2,)), array(all_cols, rows), array(rows, all_cols), array(rows, width),
                      dma((4,)), blocks(rows, 2 * HEAD_DIM), dma((sp_size, 2)), array(2, width, 2 * HEAD_DIM), dma((2, 2)),
                      array(rows, width, dtype=F32), array(8, width, dtype=F32)]
    return pl.pallas_call(
        functools.partial(step_kernel, heads, first_scratch, second_scratch),
        in_specs=[any_spec, vmem, vmem, vmem] + [any_spec] * 5,
        out_specs=[any_spec] * 14 + [vmem],
        out_shape=[out(seq_len, width), out(seq_len, width), out(all_cols, seq_len), out(width, seq_len), out(seq_len, 2 * HEAD_DIM),
                   out(seq_len, q_cols - HEAD_DIM), out(seq_len, HEAD_DIM), out(all_cols, width, dtype=F32), out(width, all_cols, dtype=F32),
                   out(sp_size * seq_len, 2 * HEAD_DIM), out(sp_size * seq_len, q_cols - HEAD_DIM), out(sp_size * seq_len, HEAD_DIM),
                   out(rows, width), out(rows, width), out(1, width, dtype=F32)],
        scratch_shapes=[blocks(8, rows, dtype=jnp.int32), dma((2, 7)), array(1, width, dtype=F32), blocks(1, width, dtype=F32), dma((2, 7)),
                        dma((2, n_all))] + [SEMS] * 6,
        compiler_params=pltpu.CompilerParams(vmem_limit_bytes=VMEM_LIMIT, collective_id=0, has_side_effects=True),
        cost_estimate=pl.CostEstimate(flops=28 * pairs * HEAD_DIM + 2 * half * cols * seq_len * n_all, bytes_accessed=20 * seq_len * width,
                                      transcendentals=2 * pairs),
        name="step",
    )(x, gain, positions.reshape(1, -1), freq, grad_out, w_q, w_k, w_v, w_o)


def finish_kernel(ht_ref, d_ref, gx_in, res_in, gg_in, wo_in, wq_in, wk_ref, wv_ref, wq_ref, wo_ref, gx_ref, res_ref, gg_ref, d_v, d_sems, ring, ring_sems):
    step = pl.program_id(0) * pl.num_programs(1) + pl.program_id(1)
    high = ring.shape[2]
    per_array = wo_in.shape[0] // (high * RING)

    def copy_in(src, g, n):
        at = pl.ds(pl.multiple_of((lax.rem(g, per_array) * RING + n) * high, high), high)
        return pltpu.make_async_copy(src.at[at, :], ring.at[lax.rem(g, DEPTH), n], ring_sems.at[0, lax.rem(g, DEPTH), n])

    def copy_out(dst, g, n):
        at = pl.ds(pl.multiple_of((lax.rem(g, per_array) * RING + n) * high, high), high)
        return pltpu.make_async_copy(ring.at[lax.rem(g, DEPTH), n], dst.at[at, :], ring_sems.at[1, lax.rem(g, DEPTH), n])

    def start(copy, first, second, g):
        for ref, mine in ((first, g < per_array), (second, g >= per_array)):
            @pl.when(mine)
            def _():
                for n in range(RING):
                    copy(ref, g, n).start()

    def pair_load(p):
        at = pl.ds(2 * p, 2)
        return pltpu.make_async_copy(d_ref.at[at], d_v.at[at], d_sems.at[p])

    @pl.when(step == 0)
    def _():
        for p in range(d_v.shape[0] // 2):
            pair_load(p).start()

    last = pl.num_programs(0) * pl.num_programs(1) - 1

    def free(g):
        for n in range(RING):
            copy_out(wo_ref, g, n).wait()

    def pass_on(g):
        for n in range(RING):
            copy_in(wo_in, g, n).wait()
        start(copy_out, wo_ref, wq_ref, g)

    @pl.when(step == 0)
    def _():
        start(copy_in, wo_in, wq_in, step)

    @pl.when(step >= DEPTH - 1)
    def _():
        free(step + 1 - DEPTH)

    @pl.when(step < last)
    def _():
        start(copy_in, wo_in, wq_in, step + 1)

    @pl.when(step >= 1)
    def _():
        pass_on(step - 1)

    for p in range(d_v.shape[0] // 2):
        @pl.when(step == p)
        def _():
            pair_load(p).wait()

    ht = ht_ref[...]
    pair = 2 * pl.program_id(1)
    wk_ref[...] = dot(ht, lanes(d_v[pair, :, :HEAD_DIM], d_v[pair + 1, :, :HEAD_DIM]))
    wv_ref[...] = dot(ht, lanes(d_v[pair, :, HEAD_DIM:], d_v[pair + 1, :, HEAD_DIM:]))

    @pl.when(step == 0)
    def _():
        gg_ref[...] = gg_in[...]

    @pl.when(step == last)
    def _():
        pass_on(last)
        for back in range(DEPTH - 1):
            free(last - back)

    @pl.when(step < ROW_STEPS)
    def _():
        gx_ref[...] = gx_in[...]
        res_ref[...] = res_in[...]


def finish(ht, d_kv, w_o_grad, w_q_grad, grad_x, result, grad_gain):
    width, seq_len = ht.shape
    groups = d_kv.shape[0]
    n_j = groups // 2
    steps = (width // MROWS) * n_j
    high = width // COPY_ROWS
    assert w_o_grad.shape[0] + w_q_grad.shape[0] == high * RING * steps
    any_spec = pl.BlockSpec(memory_space=pl.ANY)
    rows = pl.BlockSpec((grad_x.shape[0] // ROW_STEPS, width), lambda m, j: (jnp.minimum(m * n_j + j, ROW_STEPS - 1), 0))
    whole = pl.BlockSpec((1, width), lambda m, j: (0, 0))
    kv_out = pl.BlockSpec((MROWS, 2 * HEAD_DIM), lambda m, j: (m, j))
    out = lambda cols: jax.ShapeDtypeStruct((width, cols), F32)
    like = lambda val: jax.ShapeDtypeStruct(val.shape, val.dtype)
    return pl.pallas_call(
        finish_kernel,
        grid=(width // MROWS, n_j),
        in_specs=[pl.BlockSpec((MROWS, seq_len), lambda m, j: (m, 0)), any_spec, rows, rows, whole, any_spec, any_spec],
        out_specs=[kv_out, kv_out, any_spec, any_spec, rows, rows, whole],
        out_shape=[out(groups * HEAD_DIM), out(groups * HEAD_DIM), like(w_q_grad), like(w_o_grad), like(grad_x), like(result), like(grad_gain)],
        scratch_shapes=[pltpu.VMEM(d_kv.shape, BF16), pltpu.SemaphoreType.DMA((groups // 2,)),
                        pltpu.VMEM((DEPTH, RING, high, width), F32), pltpu.SemaphoreType.DMA((2, DEPTH, RING))],
        compiler_params=params(2),
        cost_estimate=pl.CostEstimate(flops=4 * width * seq_len * groups * HEAD_DIM, bytes_accessed=2 * width * seq_len, transcendentals=0),
        name="finish",
    )(ht, d_kv, grad_x, result, grad_gain, w_o_grad, w_q_grad)


def solution(mesh):
    sp_size = mesh.shape['sp']
    seq_spec = P(('dp', 'sp'), None)
    pos_spec = P(('dp', 'sp'))
    replicated = P(None, None)
    part_rows = P('dp', None)

    def local_step(x, grad_out, positions, gain, w_q, w_k, w_v, w_o):
        n_heads = w_q.shape[1] // HEAD_DIM
        heads = n_heads // sp_size
        _, _, _, ht, _, _, _, w_o_grad, w_q_grad, kv_all, _, _, result, grad_x, grad_gain = step(
            x, gain.reshape(1, -1), positions, grad_out, w_q, w_k, w_v, w_o, sp_size, heads)
        grad_wk, grad_wv, grad_wq, grad_wo, grad_x, result, grad_gain = finish(
            ht, kv_all.reshape(sp_size, -1, 2 * HEAD_DIM), w_o_grad, w_q_grad, grad_x, result, grad_gain)
        return result, grad_x, grad_wq, grad_wk, grad_wv, grad_wo, grad_gain.reshape(-1)

    return jax.shard_map(local_step, mesh=mesh,
                         in_specs=(seq_spec, seq_spec, pos_spec, P(None), replicated, replicated, replicated, replicated),
                         out_specs=(seq_spec, seq_spec, part_rows, part_rows, part_rows, part_rows, P('dp')),
                         check_vma=False)
```

```python
import functools

import jax
import jax.numpy as jnp
import numpy as np
from jax import lax
from jax.experimental import pallas as pl
from jax.experimental.pallas import tpu as pltpu
from jax.sharding import PartitionSpec as P

HEAD_DIM = 128
HALF = HEAD_DIM // 2
ROPE_THETA = 1000000.0
NORM_EPS = 1e-05
NEG_LARGE = -1e30
LOG2E = 1.4426950408889634
BLK = 512
CHUNKS = 2
FWD_MIDDLE, BWD_MIDDLE = 5, 27
MROWS = 768
RING = 3
DEPTH = 4
COPY_ROWS = 24
PARTS = 3
ROW_STEPS = 8
F32 = jnp.float32
BF16 = jnp.bfloat16
ROWS_ROWS = (((0,), (0,)), ((), ()))
COLS_COLS = (((1,), (1,)), ((), ()))
ROWS_COLS = (((0,), (1,)), ((), ()))
VMEM_LIMIT = 63 * 1024 * 1024


def dot(a, b, dims=(((1,), (0,)), ((), ()))):
    return lax.dot_general(a, b, dims, preferred_element_type=F32)


def params(axes=1):
    return pltpu.CompilerParams(dimension_semantics=("arbitrary",) * axes, vmem_limit_bytes=VMEM_LIMIT)


class Neighbours:
    def __init__(self):
        self.me = lax.axis_index('sp')
        core, col, row = lax.rem(self.me, 2), lax.rem(self.me // 2, 2), self.me // 4
        self.sib = self.me + 1 - 2 * core
        self.xn = self.me + 2 - 4 * col
        self.yn = self.me + 4 - 8 * row
        self.diag = self.xn + self.yn - self.me

    def meet(self, peers):
        barrier = pltpu.get_barrier_semaphore()
        for peer in peers:
            pl.semaphore_signal(barrier, inc=1, device_id={'sp': peer}, device_id_type=pl.DeviceIdType.MESH)
        pl.semaphore_wait(barrier, len(peers))

    def across(self, r):
        core, col, row = lax.rem(self.me, 2), lax.rem(self.me // 2, 2), self.me // 4
        return (self.me + lax.rem(r, 2) * (1 - 2 * core) + lax.rem(r // 2, 2) * (2 - 4 * col) + (r // 4) * (4 - 8 * row))

    def others(self):
        flip = lambda dev: dev + 1 - 2 * lax.rem(dev, 2)
        return [self.sib, self.xn, flip(self.xn), self.yn, flip(self.yn), self.diag, flip(self.diag)]


def send(src, dst, sems, index, peer):
    return pltpu.make_async_remote_copy(src_ref=src, dst_ref=dst, send_sem=sems.at[0, index], recv_sem=sems.at[1, index],
                                        device_id={'sp': peer}, device_id_type=pl.DeviceIdType.MESH)


class Gather:
    COPIES = 5 * CHUNKS + 2
    HALF_CHUNKS = CHUNKS // 2
    ORDER = [chunk + half * (CHUNKS // 2) for chunk in range(CHUNKS // 2) for half in range(2)]

    def __init__(self, near, own, dst, rows, sems):
        self.near, self.own, self.dst, self.rows, self.sems = near, own, dst, rows, sems

    def block(self, dev, chunk, count=1):
        size = self.rows // CHUNKS
        return self.dst.at[pl.ds(pl.multiple_of(dev * self.rows + chunk * size, size), count * size), :]

    def first(self, chunk, kind):
        peer = (self.near.xn, self.near.yn, self.near.sib)[kind]
        return send(self.own(chunk), self.block(self.near.me, chunk), self.sems, kind * CHUNKS + chunk, peer)

    def onward(self, chunk):
        over_y = chunk < self.HALF_CHUNKS
        rows = self.block(self.near.xn if over_y else self.near.yn, chunk)
        return send(rows, rows, self.sems, 3 * CHUNKS + chunk, self.near.yn if over_y else self.near.xn)

    def share(self, kind):
        rows = self.block((self.near.xn, self.near.yn)[kind], 0, CHUNKS)
        return send(rows, rows, self.sems, 4 * CHUNKS + kind, self.near.sib)

    def share_diag(self, chunk):
        rows = self.block(self.near.diag, chunk)
        return send(rows, rows, self.sems, 4 * CHUNKS + 2 + chunk, self.near.sib)

    def start(self):
        for chunk in range(CHUNKS):
            for kind in (0, 1):
                self.send_first(chunk, kind)
            self.first(chunk, 2).start()

    def send_first(self, turn, kind):
        self.first(turn if kind == 0 else (turn + self.HALF_CHUNKS) % CHUNKS, kind).start()

    def middle(self):
        for chunk in self.ORDER:
            self.first(chunk, 0 if chunk < self.HALF_CHUNKS else 1).wait_recv()
            self.onward(chunk).start()

    def late(self):
        for chunk in range(self.HALF_CHUNKS, CHUNKS):
            self.first(chunk, 0).wait_recv()
        self.share(0).start()
        for chunk in range(self.HALF_CHUNKS):
            self.first(chunk, 1).wait_recv()
        self.share(1).start()

    def end_sib(self):
        for chunk in range(CHUNKS):
            self.first(chunk, 2).wait_recv()

    def end_near(self):
        for kind in range(2):
            self.share(kind).wait_recv()

    def end_far(self):
        for chunk in self.ORDER:
            self.onward(chunk).wait_recv()
            self.share_diag(chunk).start()
        for chunk in range(CHUNKS):
            for kind in range(3):
                self.first(chunk, kind).wait_send()
            self.onward(chunk).wait_send()
        for kind in range(2):
            self.share(kind).wait_send()
        for chunk in range(CHUNKS):
            self.share_diag(chunk).wait()

    def end(self):
        self.end_sib()
        self.end_near()
        self.end_far()


SEMS = pltpu.SemaphoreType.DMA((2, Gather.COPIES))


def masked(scores):
    key = lax.broadcasted_iota(jnp.int32, scores.shape, 0)
    query = lax.broadcasted_iota(jnp.int32, scores.shape, 1)
    return jnp.where(key <= query, scores, NEG_LARGE)


def unrotate(val, cos_t, sin_t):
    return (val * cos_t - pltpu.roll(val, HALF, 1) * sin_t).astype(BF16)


def attention_part(heads, near, gather_next, x_ref, gain_ref, pos_ref, freq_ref, dy_ref, wq_ref, wk_ref, wv_ref, wo_ref,
                   h_all, dy_all, o_all, ht_ref, dkv_ref, dq_a_ref, dq_b_ref, pos_all, pos_sems, h_sems, dy_sems, o_sems,
                   x_v, h_v, x_sems, own_sems, cos_s, sin_s, w_v, wo_v, w_sems, blk, blk_sems, ht_v, ht_sems,
                   q_s, k_s, v_s, vt, kt, ot_s, lse_s, acc, do_s, dk_acc, dv_acc, dq_v, dq_sems, dkv_v):
    rows, width = x_ref.shape
    n_blocks = k_s.shape[0]
    q_cols = heads * HEAD_DIM
    size = rows // CHUNKS
    qk_scale = HEAD_DIM ** -0.5
    to_log2 = qk_scale * LOG2E
    cols = [slice(a * HEAD_DIM, (a + 1) * HEAD_DIM) for a in range(heads)]
    part = lambda ref, chunk, count=size: ref.at[pl.ds(chunk * count, count), :]
    gather_h = Gather(near, lambda chunk: part(h_v, chunk), h_all, rows, h_sems)
    gather_dy = Gather(near, lambda chunk: part(dy_ref, chunk), dy_all, rows, dy_sems)
    gather_o = Gather(near, lambda chunk: part(ot_s, chunk, q_cols // CHUNKS), o_all, q_cols, o_sems)

    loads = [pltpu.make_async_copy(part(x_ref, chunk), part(x_v, chunk), x_sems.at[chunk]) for chunk in range(CHUNKS)]
    for load in loads:
        load.start()
    others = near.others()
    near.meet(others)
    pos_all[near.me] = jnp.broadcast_to(pos_ref[...], pos_all.shape[1:])
    positions = [send(pos_ref, pos_all.at[near.me, pl.ds(0, 1), :], pos_sems, r, peer) for r, peer in enumerate(others)]
    gain = gain_ref[...].astype(F32)
    for turn, chunk in enumerate(Gather.ORDER):
        loads[chunk].wait()

        @pl.loop(0, size // 32)
        def _(r):
            at = pl.ds(pl.multiple_of(chunk * size + r * 32, 32), 32)
            x_f = x_v[at, :].astype(F32)
            normed = x_f * lax.rsqrt(jnp.mean(x_f * x_f, axis=-1, keepdims=True) + NORM_EPS)
            h_v[at, :] = (normed * gain).astype(BF16)

        gather_h.send_first(turn // 2, turn % 2)
        gather_h.first(chunk, 2).start()
    for turn in range(Gather.HALF_CHUNKS, CHUNKS):
        for kind in (0, 1):
            gather_h.send_first(turn, kind)
    for copy in positions:
        copy.start()
    own_h = pltpu.make_async_copy(h_v, gather_h.block(near.me, 0, CHUNKS), own_sems.at[0])
    own_h.start()
    w_loads, col = [], 0
    for n, (ref, count) in enumerate(((wq_ref, q_cols), (wk_ref, HEAD_DIM), (wv_ref, HEAD_DIM))):
        at = pl.ds(pl.multiple_of(near.me * count, HEAD_DIM), count)
        w_loads.append(pltpu.make_async_copy(ref.at[:, at], w_v.at[:, pl.ds(col, count)], w_sems.at[n]))
        col += count
    w_loads.append(pltpu.make_async_copy(wo_ref.at[pl.ds(pl.multiple_of(near.me * q_cols, q_cols), q_cols), :], wo_v, w_sems.at[3]))
    stage_in = pltpu.make_async_copy(dy_ref, x_v, own_sems.at[1])
    stage_out = pltpu.make_async_copy(x_v, gather_dy.block(near.me, 0, CHUNKS), own_sems.at[2])
    for load in w_loads + [stage_in]:
        load.start()
    for copy in positions:
        copy.wait()
    sign = jnp.where(lax.broadcasted_iota(jnp.int32, (1, HEAD_DIM), 1) < HALF, -1.0, 1.0)

    @pl.loop(0, n_blocks)
    def _(b):
        pos = jnp.broadcast_to(pos_all[b, 0:1, :].astype(F32), (HEAD_DIM, rows)).T
        angles = pos * freq_ref[...]
        cos_s[b] = jnp.cos(angles)
        sin_s[b] = jnp.sin(angles) * sign

    gather_h.middle()
    for load in w_loads + [stage_in]:
        load.wait()
    stage_out.start()
    own_h.wait()

    def block_load(ref, block, slot):
        return pltpu.make_async_copy(ref.at[pl.ds(pl.multiple_of(block * rows, rows), rows), :], blk.at[slot], blk_sems.at[slot])

    far = n_blocks * 3 // 4

    def arrive(r, ref, gather, before_near=None, before_far=None):
        slot = lax.rem(r, 2)

        @pl.when(r == 1)
        def _():
            gather.end_sib()

        @pl.when(r == 2)
        def _():
            if before_near:
                before_near()
            gather.end_near()

        @pl.when(r == far)
        def _():
            if before_far:
                before_far()
            gather.end_far()

        @pl.when(functools.reduce(jnp.logical_or, [r == first for first in (0, 1, 2, far)]))
        def _():
            block_load(ref, near.across(r), slot).start()

        block_load(ref, 0, slot).wait()

        @pl.when(functools.reduce(jnp.logical_and, [r + 1 != first for first in (1, 2, far, n_blocks)]))
        def _():
            block_load(ref, near.across(r + 1), 1 - slot).start()

    def ht_store(r):
        at = pl.ds(pl.multiple_of(near.across(r) * rows, rows), rows)
        return pltpu.make_async_copy(ht_v.at[lax.rem(r, 2)], ht_ref.at[:, at], ht_sems.at[lax.rem(r, 2)])

    @pl.loop(0, n_blocks)
    def _(r):
        i = near.across(r)
        slot = lax.rem(r, 2)
        arrive(r, h_all, gather_h, gather_h.late, gather_dy.start)

        @pl.when(r >= 2)
        def _():
            ht_store(r - 2).wait()

        ht_v[slot] = blk[slot].T
        ht_store(r).start()
        prod = dot(blk[slot], w_v[...])
        cos_t, sin_t = cos_s[i], sin_s[i]
        for a in range(heads + 1):
            val = prod[:, a * HEAD_DIM:(a + 1) * HEAD_DIM]
            rot = (val * cos_t + pltpu.roll(val, HALF, 1) * sin_t).astype(BF16)
            if a < heads:
                q_s[i, :, cols[a]] = rot
            else:
                k_s[i] = rot
                kt[i] = rot.T
        v_i = prod[:, q_cols + HEAD_DIM:].astype(BF16)
        v_s[i] = v_i
        vt[i] = v_i.T

    def fwd_chunk(i, c, carry, diagonal):
        k_c, vt_c = k_s[c], vt[c]
        scores = [dot(k_c, q_s[i, :, cols[a]], COLS_COLS) * to_log2 for a in range(heads)]
        out = []
        for a in range(heads):
            s = masked(scores[a]) if diagonal else scores[a]
            m_old, l_old = carry[a]
            m_new = jnp.maximum(m_old, jnp.max(s, axis=0, keepdims=True))
            alpha = jnp.exp2(m_old - m_new)
            p = jnp.exp2(s - m_new)
            l_new = l_old * alpha + jnp.sum(p, axis=0, keepdims=True)
            acc[a] = acc[a] * alpha + dot(vt_c, p.astype(BF16))
            out.append((m_new, l_new))
        return tuple(out)

    @pl.loop(0, n_blocks)
    def _(i):
        acc[...] = jnp.zeros_like(acc)
        start = tuple((jnp.full((1, rows), NEG_LARGE, F32), jnp.zeros((1, rows), F32)) for _ in range(heads))
        carry = lax.fori_loop(0, i, lambda c, carry: fwd_chunk(i, c, carry, False), start)
        carry = fwd_chunk(i, i, carry, True)
        at = pl.ds(pl.multiple_of(i * rows, rows), rows)
        for a in range(heads):
            m_a, l_a = carry[a]
            ot_s[cols[a], at] = (acc[a] / l_a).astype(BF16)
            lse_s[i, a:a + 1, :] = m_a + jnp.log2(l_a)

        @pl.when(i == FWD_MIDDLE)
        def _():
            gather_dy.middle()

    gather_dy.late()
    gather_o.start()
    own_o = pltpu.make_async_copy(ot_s, gather_o.block(near.me, 0, CHUNKS), own_sems.at[0])
    own_o.start()

    def bwd_chunk(i, c, delta, diagonal):
        k_c, v_c, kt_c = k_s[c], v_s[c], kt[c]
        dk_c = dv_c = None
        for a in range(heads):
            q_a, do_a = q_s[i, :, cols[a]], do_s[i, :, cols[a]]
            s = dot(k_c, q_a, COLS_COLS) * to_log2
            if diagonal:
                s = masked(s)
            p = jnp.exp2(s - lse_s[i, a:a + 1, :])
            d_p = dot(v_c, do_a, COLS_COLS)
            d_s = (p * (d_p - delta[a])).astype(BF16)
            dv_a = dot(p.astype(BF16), do_a)
            dk_a = dot(d_s, q_a)
            dv_c = dv_a if dv_c is None else dv_c + dv_a
            dk_c = dk_a if dk_c is None else dk_c + dk_a
            acc[a] += dot(kt_c, d_s)
        dk_acc[c] += dk_c
        dv_acc[c] += dv_c

    def dq_stores(r):
        slot = lax.rem(r, 2)
        at = pl.ds(pl.multiple_of(near.across(r) * rows, rows), rows)
        last = q_cols - HEAD_DIM
        return [pltpu.make_async_copy(dq_v.at[slot, :, pl.ds(0, last)], dq_a_ref.at[at, :], dq_sems.at[slot, 0]),
                pltpu.make_async_copy(dq_v.at[slot, :, pl.ds(last, HEAD_DIM)], dq_b_ref.at[at, :], dq_sems.at[slot, 1])]

    def pass_on(done):
        @pl.when(done == BWD_MIDDLE)
        def _():
            gather_o.middle()

    for r in (n_blocks - 2, n_blocks - 1):
        ht_store(jnp.int32(r)).wait()
    dk_acc[...] = jnp.zeros_like(dk_acc)
    dv_acc[...] = jnp.zeros_like(dv_acc)
    stage_out.wait()

    def bwd_block(r, done):
        i = near.across(r)
        slot = lax.rem(r, 2)
        at = pl.ds(pl.multiple_of(i * rows, rows), rows)

        arrive(r, dy_all, gather_dy)
        do_s[i] = dot(blk[slot], wo_v[...], COLS_COLS).astype(BF16)
        acc[...] = jnp.zeros_like(acc)
        delta = [jnp.sum(ot_s[cols[a], at].astype(F32) * do_s[i, :, cols[a]].T.astype(F32), axis=0, keepdims=True) for a in range(heads)]

        @pl.loop(0, i)
        def _(c):
            bwd_chunk(i, c, delta, False)
            pass_on(done + c)

        bwd_chunk(i, i, delta, True)
        pass_on(done + i)

        @pl.when(r >= 2)
        def _():
            for store in dq_stores(r - 2):
                store.wait()

        for a in range(heads):
            dq_v[slot, :, cols[a]] = unrotate(acc[a].T * qk_scale, cos_s[i], sin_s[i])
        for store in dq_stores(r):
            store.start()
        return done + i + 1

    lax.fori_loop(0, n_blocks, bwd_block, jnp.int32(0))
    gather_o.late()
    for r in (n_blocks - 2, n_blocks - 1):
        for store in dq_stores(r):
            store.wait()
    gather_next.start()

    @pl.loop(0, n_blocks)
    def _(c):
        at = pl.ds(pl.multiple_of(c * rows, rows), rows)
        dkv_v[at, :HEAD_DIM] = unrotate(dk_acc[c] * qk_scale, cos_s[c], sin_s[c])
        dkv_v[at, HEAD_DIM:] = dv_acc[c].astype(BF16)

    dkv_store = pltpu.make_async_copy(dkv_v, dkv_ref, own_sems.at[1])
    dkv_store.start()
    own_o.wait()
    gather_o.end()
    dkv_store.wait()


def lanes(*parts):
    return jnp.concatenate(parts, axis=1)


def products_part(heads, near, gathers, ot_ref, ht_ref, dy_ref, d_kv_ref, d_qa_ref, d_qb_ref, x_ref, own_dy_ref, gain_ref, wo_ref, wk_ref, wv_ref, wq_ref,
                  wo_out, wq_out, kv_all, qa_all, qb_all, res_ref, gx_ref, gg_ref, gg_row, gg_all, gg_sems, x_sems,
                  a_buf, b_buf, tile, a_sem, b_sems, t_sems, stage, stage_sems, ot_v, o_v, x_v, io_sems, own, own_sems, w_v, w_sems, acc,
                  gg_v):
    core = lax.rem(near.me, 2)
    half = a_buf.shape[0]
    seq_len = d_kv_ref.shape[0]
    rows, width = x_ref.shape
    n_cols = d_kv_ref.shape[1]
    n_o, n_all = width // (2 * n_cols), x_sems.shape[1]
    n_oa = n_o + (n_all - n_o) * 2 // 3

    local = (d_qa_ref, d_qb_ref, d_kv_ref)

    def stage_in(n):
        return pltpu.make_async_copy(local[n], stage.at[:, pl.ds(0, local[n].shape[1])], stage_sems.at[0])

    def stage_out(n):
        return pltpu.make_async_copy(stage.at[:, pl.ds(0, local[n].shape[1])], gathers[n].block(near.me, 0, CHUNKS), stage_sems.at[1])

    def copy_own(n):
        stage_in(n).wait()
        stage_out(n).start()

    own_rows = pl.ds(pl.multiple_of(core * half, half), half)
    tokens = pl.ds(pl.multiple_of(near.me * rows, rows), rows)
    ot_load = pltpu.make_async_copy(ot_ref.at[:, tokens], ot_v, io_sems.at[0])
    x_load = pltpu.make_async_copy(x_ref, x_v, io_sems.at[1])
    res_store = pltpu.make_async_copy(x_v, res_ref, io_sems.at[2])
    dy_load = pltpu.make_async_copy(own_dy_ref, o_v, io_sems.at[3])
    gx_store = pltpu.make_async_copy(o_v, gx_ref, io_sems.at[0])

    def a_load(ref):
        return pltpu.make_async_copy(ref.at[own_rows, :], a_buf, a_sem)

    def b_loads(source, p, slot, g):
        if source is dy_ref:
            srcs = [dy_ref.at[:, pl.ds(pl.multiple_of((2 * p + g) * n_cols, n_cols), n_cols)]]
        else:
            per = n_cols // source.shape[1]
            srcs = [source.at[pl.ds(pl.multiple_of(((2 * p + g) * per + n) * seq_len, seq_len), seq_len), :] for n in range(per)]
        return [pltpu.make_async_copy(src, b_buf.at[slot, :, pl.ds(g * n_cols + n * src.shape[1], src.shape[1])], b_sems.at[slot, g])
                for n, src in enumerate(srcs)]

    def start_b(step):
        slot = lax.rem(step, 2)
        for source, low, high in ((dy_ref, 0, n_o), (qa_all, n_o, n_oa), (qb_all, n_oa, n_all)):
            @pl.when(jnp.logical_and(step >= low, step < high))
            def _():
                for g in range(2):
                    for load in b_loads(source, step - low, slot, g):
                        load.start()

    def pieces(kind, step):
        wide = (2 * n_cols, n_cols, HEAD_DIM)[kind]
        slot = lax.rem(step, 2)
        out = []
        for n in range(2 * n_cols // wide):
            group = (step - (0, n_o, n_oa)[kind]) * (2 * n_cols // wide) + n
            col = (group * wide, group * heads * HEAD_DIM, (group + 1) * heads * HEAD_DIM - HEAD_DIM)[kind]
            dst = (wo_out, wq_out, wq_out)[kind].at[own_rows, pl.ds(pl.multiple_of(col, HEAD_DIM), wide)]
            src = tile.at[slot, :, pl.ds(n * wide, wide)]
            out.append((pltpu.make_async_copy(src, dst, t_sems.at[slot]), send(src, dst, x_sems, step, near.sib)))
        return out

    def start_tile(step):
        for kind, (low, high) in enumerate(((0, n_o), (n_o, n_oa), (n_oa, n_all))):
            @pl.when(jnp.logical_and(step >= low, step < high))
            def _():
                for keep, give in pieces(kind, step):
                    keep.start()
                    give.start()

    def whole_tile(step):
        slot = lax.rem(step, 2)
        dst = wo_out.at[own_rows, pl.ds(0, 2 * n_cols)]
        return pltpu.make_async_copy(tile.at[slot], dst, t_sems.at[slot]), send(tile.at[slot], dst, x_sems, step, near.sib)

    def wait_tile(step):
        keep, give = whole_tile(step)
        keep.wait()
        give.wait_send()

    def result_part():
        cols = b_buf.shape[2]

        def w_load(n):
            slot = lax.rem(n, 2)
            return pltpu.make_async_copy(wo_ref.at[:, pl.ds(pl.multiple_of(n * cols, cols), cols)], b_buf.at[slot, pl.ds(0, wo_ref.shape[0]), :],
                                         b_sems.at[slot, 0])

        w_load(jnp.int32(0)).start()
        ot_load.wait()

        @pl.loop(0, ot_v.shape[0] // BLK)
        def _(r):
            at = pl.ds(pl.multiple_of(r * BLK, BLK), BLK)
            o_v[:, at] = ot_v[at, :].T

        x_load.wait()

        @pl.loop(0, n_o)
        def _(n):
            w_load(n).wait()

            @pl.when(n + 1 < n_o)
            def _():
                w_load(n + 1).start()

            at = pl.ds(pl.multiple_of(n * cols, cols), cols)
            x_v[:, at] = (x_v[:, at].astype(F32) + dot(o_v[...], b_buf[lax.rem(n, 2), :wo_ref.shape[0], :])).astype(BF16)

        res_store.start()

    def hidden_parts(kind):
        count = own.shape[0] // (2 if kind == 1 else 1)

        def own_load(r, g):
            source = (qa_all, qb_all, kv_all)[kind]
            device, col = (2 * r + g, 0) if kind == 1 else (near.across(r), g * HEAD_DIM)
            at = pl.ds(pl.multiple_of(device * seq_len + near.me * rows, rows), rows)
            return pltpu.make_async_copy(source.at[at, pl.ds(col, HEAD_DIM)], own.at[r, :, pl.ds(g * HEAD_DIM, HEAD_DIM)], own_sems.at[r, g])

        def w_load(r, g):
            source = (wk_ref, wv_ref)[g] if kind == 2 else wq_ref
            col = near.across(r) if kind == 2 else heads * near.across(r) + g if kind == 0 else heads * (2 * r + g + 1) - 1
            slot = lax.rem(r, 2)
            return pltpu.make_async_copy(source.at[:, pl.ds(pl.multiple_of(col * HEAD_DIM, HEAD_DIM), HEAD_DIM)],
                                         w_v.at[slot, :, pl.ds(g * HEAD_DIM, HEAD_DIM)], w_sems.at[slot, g])

        return count, own_load, w_load

    def hidden_start(kind, low=0, high=None):
        count, own_load, w_load = hidden_parts(kind)
        for g in range(2):
            if low == 0:
                w_load(jnp.int32(0), g).start()

            @pl.loop(low, high or count)
            def _(r):
                own_load(r, g).start()

    def hidden_add(kind, low=0, high=None):
        count, own_load, w_load = hidden_parts(kind)

        @pl.loop(low, high or count)
        def _(r):
            for g in range(2):
                w_load(r, g).wait()
                own_load(r, g).wait()

            @pl.when(r + 1 < count)
            def _():
                for g in range(2):
                    w_load(r + 1, g).start()

            for col in range(0, width, width // PARTS):
                at = slice(col, col + width // PARTS)
                acc[:, at] += dot(own[r], w_v[lax.rem(r, 2), at, :], COLS_COLS)

    a_load(ot_ref).start()
    start_b(jnp.int32(0))
    stage_in(0).start()
    ot_load.start()
    x_load.start()
    a_load(ot_ref).wait()

    @pl.loop(0, n_all)
    def _(step):
        slot = lax.rem(step, 2)
        for g in range(2):
            b_loads(dy_ref, 0, slot, g)[0].wait()

        @pl.when(jnp.logical_and(step != n_o - 1, step != n_oa - 1))
        def _():
            start_b(step + 1)

        @pl.when(step >= 2)
        def _():
            wait_tile(step - 2)

        @pl.when(step == n_o)
        def _():
            a_load(ht_ref).wait()

        for r in range(0, half, half // PARTS):
            tile[slot, r:r + half // PARTS, :] = dot(a_buf[r:r + half // PARTS, :], b_buf[slot])
        start_tile(step)

        @pl.when(step == n_o - 4)
        def _():
            acc[...] = jnp.zeros_like(acc)
            copy_own(0)
            gathers[0].middle()

        @pl.when(step == n_o - 1)
        def _():
            a_load(ht_ref).start()
            gathers[0].late()
            gathers[1].start()
            stage_out(0).wait()
            stage_in(1).start()
            result_part()
            gathers[0].end()
            start_b(step + 1)
            hidden_start(0)

        @pl.when(step == n_oa - 4)
        def _():
            copy_own(1)
            gathers[1].middle()

        @pl.when(step == n_oa - 2)
        def _():
            gathers[1].late()
            gathers[2].start()
            stage_out(1).wait()
            stage_in(2).start()

        @pl.when(step == n_oa - 1)
        def _():
            res_store.wait()
            x_load.start()
            dy_load.start()
            gathers[1].end()
            start_b(step + 1)

    hidden_add(0)
    copy_own(2)
    gathers[2].middle()
    hidden_start(1)
    hidden_add(1)
    gathers[2].late()
    stage_out(2).wait()
    gathers[2].end_sib()
    gathers[2].end_near()
    near_count = own.shape[0] * 3 // 4
    hidden_start(2, 0, near_count)
    for step in (n_all - 2, n_all - 1):
        wait_tile(jnp.int32(step))
    hidden_add(2, 0, near_count)
    gathers[2].end_far()
    hidden_start(2, near_count)
    hidden_add(2, near_count)

    gain = gain_ref[...].astype(F32)
    gg_v[...] = jnp.zeros_like(gg_v)
    x_load.wait()
    dy_load.wait()

    @pl.loop(0, rows // 32)
    def _(r):
        at = pl.ds(pl.multiple_of(r * 32, 32), 32)
        x_f = x_v[at, :].astype(F32)
        inv_rms = lax.rsqrt(jnp.mean(x_f * x_f, axis=-1, keepdims=True) + NORM_EPS)
        normed = x_f * inv_rms
        d_hid = acc[at, :]
        both = d_hid * normed
        gg_v[...] += jnp.sum(both.reshape(4, 8, width), axis=0)
        mean = jnp.mean(both * gain, axis=-1, keepdims=True)
        o_v[at, :] = (o_v[at, :].astype(F32) + inv_rms * (d_hid * gain - normed * mean)).astype(BF16)

    gg_row[...] = jnp.sum(gg_v[...], axis=0, keepdims=True)
    gg_all[near.me] = gg_row[...]
    parts = [send(gg_row, gg_all.at[near.me], gg_sems, r, peer) for r, peer in enumerate(near.others())]
    for copy in parts:
        copy.start()
    gx_store.start()

    @pl.loop(0, n_all)
    def _(step):
        whole_tile(step)[1].wait_recv()

    for copy in parts:
        copy.wait()
    gg_ref[...] = jnp.sum(gg_all[...], axis=0)
    gx_store.wait()


def step_kernel(heads, first_scratch, second_scratch, x_ref, gain_ref, pos_ref, freq_ref, dy_ref, wq_ref, wk_ref, wv_ref, wo_ref,
                h_all, dy_all, o_all, ht, d_kv, d_qa, d_qb, wo_out, wq_out, kv_all, qa_all, qb_all, res, gx, gg,
                pos_all, pos_sems, gg_row, gg_all, gg_sems, x_sems, h_sems, dy_sems, o_sems, kv_sems, qa_sems, qb_sems):
    near = Neighbours()
    seq_len = d_kv.shape[0]

    def gather_of(src, dst, sems):
        return Gather(near, lambda c: src.at[pl.ds(c * (seq_len // CHUNKS), seq_len // CHUNKS), :], dst, seq_len, sems)

    gathers = [gather_of(d_qa, qa_all, qa_sems), gather_of(d_qb, qb_all, qb_sems), gather_of(d_kv, kv_all, kv_sems)]

    def first(*scratch):
        attention_part(heads, near, gathers[0], x_ref, gain_ref, pos_ref, freq_ref, dy_ref, wq_ref, wk_ref, wv_ref, wo_ref,
                       h_all, dy_all, o_all, ht, d_kv, d_qa, d_qb, pos_all, pos_sems, h_sems, dy_sems, o_sems, *scratch)

    def second(*scratch):
        products_part(heads, near, gathers, o_all, ht, dy_all, d_kv, d_qa, d_qb, x_ref, dy_ref, gain_ref, wo_ref, wk_ref, wv_ref, wq_ref,
                      wo_out, wq_out, kv_all, qa_all, qb_all, res, gx, gg, gg_row, gg_all, gg_sems, x_sems, *scratch)

    pl.run_scoped(first, *first_scratch)
    pl.run_scoped(second, *second_scratch)


def step(x, gain, positions, grad_out, w_q, w_k, w_v, w_o, sp_size, heads):
    rows, width = x.shape
    seq_len = rows * sp_size
    q_cols = heads * HEAD_DIM
    all_cols = q_cols * sp_size
    half = width // 2
    cols = 4 * HEAD_DIM
    n_all = (width + all_cols) // cols
    any_spec = pl.BlockSpec(memory_space=pl.ANY)
    vmem = pl.BlockSpec(memory_space=pltpu.VMEM)
    dma = pltpu.SemaphoreType.DMA
    inv_freq = ROPE_THETA ** (-np.arange(0, HEAD_DIM, 2) / HEAD_DIM)
    freq = jnp.asarray(np.concatenate([inv_freq, inv_freq])[None, :], F32)
    pairs = heads * seq_len * (seq_len + rows) // 2
    out = lambda *shape, dtype=BF16: jax.ShapeDtypeStruct(shape, dtype)
    array = lambda *shape, dtype=BF16: pltpu.VMEM(shape, dtype)
    blocks = lambda *shape, dtype=BF16: pltpu.VMEM((sp_size,) + shape, dtype)
    first_scratch = [array(rows, width), array(rows, width), dma((CHUNKS,)), dma((3,)), blocks(rows, HEAD_DIM, dtype=F32),
                     blocks(rows, HEAD_DIM, dtype=F32), array(width, q_cols + 2 * HEAD_DIM), array(q_cols, width), dma((4,)),
                     array(2, rows, width), dma((2,)), array(2, width, rows), dma((2,)),
                     blocks(rows, q_cols), blocks(rows, HEAD_DIM), blocks(rows, HEAD_DIM), blocks(HEAD_DIM, rows), blocks(HEAD_DIM, rows),
                     array(q_cols, seq_len), blocks(8, rows, dtype=F32), array(heads, HEAD_DIM, rows, dtype=F32),
                     blocks(rows, q_cols), blocks(rows, HEAD_DIM, dtype=F32), blocks(rows, HEAD_DIM, dtype=F32),
                     array(2, rows, q_cols), dma((2, 2)), array(seq_len, 2 * HEAD_DIM)]
    second_scratch = [array(half, seq_len), array(2, seq_len, cols), array(2, half, cols, dtype=F32), dma, dma((2, 2)), dma((2,)),
                      array(seq_len, 2 * HEAD_DIM), dma((2,)), array(all_cols, rows), array(rows, all_cols), array(rows, width),
                      dma((4,)), blocks(rows, 2 * HEAD_DIM), dma((sp_size, 2)), array(2, width, 2 * HEAD_DIM), dma((2, 2)),
                      array(rows, width, dtype=F32), array(8, width, dtype=F32)]
    return pl.pallas_call(
        functools.partial(step_kernel, heads, first_scratch, second_scratch),
        in_specs=[any_spec, vmem, vmem, vmem] + [any_spec] * 5,
        out_specs=[any_spec] * 14 + [vmem],
        out_shape=[out(seq_len, width), out(seq_len, width), out(all_cols, seq_len), out(width, seq_len), out(seq_len, 2 * HEAD_DIM),
                   out(seq_len, q_cols - HEAD_DIM), out(seq_len, HEAD_DIM), out(all_cols, width, dtype=F32), out(width, all_cols, dtype=F32),
                   out(sp_size * seq_len, 2 * HEAD_DIM), out(sp_size * seq_len, q_cols - HEAD_DIM), out(sp_size * seq_len, HEAD_DIM),
                   out(rows, width), out(rows, width), out(1, width, dtype=F32)],
        scratch_shapes=[blocks(8, rows, dtype=jnp.int32), dma((2, 7)), array(1, width, dtype=F32), blocks(1, width, dtype=F32), dma((2, 7)),
                        dma((2, n_all))] + [SEMS] * 6,
        compiler_params=pltpu.CompilerParams(vmem_limit_bytes=VMEM_LIMIT, collective_id=0, has_side_effects=True),
        cost_estimate=pl.CostEstimate(flops=28 * pairs * HEAD_DIM + 2 * half * cols * seq_len * n_all, bytes_accessed=20 * seq_len * width,
                                      transcendentals=2 * pairs),
        name="step",
    )(x, gain, positions.reshape(1, -1), freq, grad_out, w_q, w_k, w_v, w_o)


def finish_kernel(ht_ref, d_ref, gx_in, res_in, gg_in, wo_in, wq_in, wk_ref, wv_ref, wq_ref, wo_ref, gx_ref, res_ref, gg_ref, d_v, d_sems, ring, ring_sems):
    step = pl.program_id(0) * pl.num_programs(1) + pl.program_id(1)
    high = ring.shape[2]
    per_array = wo_in.shape[0] // (high * RING)

    def copy_in(src, g, n):
        at = pl.ds(pl.multiple_of((lax.rem(g, per_array) * RING + n) * high, high), high)
        return pltpu.make_async_copy(src.at[at, :], ring.at[lax.rem(g, DEPTH), n], ring_sems.at[0, lax.rem(g, DEPTH), n])

    def copy_out(dst, g, n):
        at = pl.ds(pl.multiple_of((lax.rem(g, per_array) * RING + n) * high, high), high)
        return pltpu.make_async_copy(ring.at[lax.rem(g, DEPTH), n], dst.at[at, :], ring_sems.at[1, lax.rem(g, DEPTH), n])

    def start(copy, first, second, g):
        for ref, mine in ((first, g < per_array), (second, g >= per_array)):
            @pl.when(mine)
            def _():
                for n in range(RING):
                    copy(ref, g, n).start()

    def pair_load(p):
        at = pl.ds(2 * p, 2)
        return pltpu.make_async_copy(d_ref.at[at], d_v.at[at], d_sems.at[p])

    @pl.when(step == 0)
    def _():
        for p in range(d_v.shape[0] // 2):
            pair_load(p).start()

    last = pl.num_programs(0) * pl.num_programs(1) - 1

    def free(g):
        for n in range(RING):
            copy_out(wo_ref, g, n).wait()

    def pass_on(g):
        for n in range(RING):
            copy_in(wo_in, g, n).wait()
        start(copy_out, wo_ref, wq_ref, g)

    @pl.when(step == 0)
    def _():
        start(copy_in, wo_in, wq_in, step)

    @pl.when(step >= DEPTH - 1)
    def _():
        free(step + 1 - DEPTH)

    @pl.when(step < last)
    def _():
        start(copy_in, wo_in, wq_in, step + 1)

    @pl.when(step >= 1)
    def _():
        pass_on(step - 1)

    for p in range(d_v.shape[0] // 2):
        @pl.when(step == p)
        def _():
            pair_load(p).wait()

    ht = ht_ref[...]
    pair = 2 * pl.program_id(1)
    wk_ref[...] = dot(ht, lanes(d_v[pair, :, :HEAD_DIM], d_v[pair + 1, :, :HEAD_DIM]))
    wv_ref[...] = dot(ht, lanes(d_v[pair, :, HEAD_DIM:], d_v[pair + 1, :, HEAD_DIM:]))

    @pl.when(step == 0)
    def _():
        gg_ref[...] = gg_in[...]

    @pl.when(step == last)
    def _():
        pass_on(last)
        for back in range(DEPTH - 1):
            free(last - back)

    @pl.when(step < ROW_STEPS)
    def _():
        gx_ref[...] = gx_in[...]
        res_ref[...] = res_in[...]


def finish(ht, d_kv, w_o_grad, w_q_grad, grad_x, result, grad_gain):
    width, seq_len = ht.shape
    groups = d_kv.shape[0]
    n_j = groups // 2
    steps = (width // MROWS) * n_j
    high = width // COPY_ROWS
    assert w_o_grad.shape[0] + w_q_grad.shape[0] == high * RING * steps
    any_spec = pl.BlockSpec(memory_space=pl.ANY)
    rows = pl.BlockSpec((grad_x.shape[0] // ROW_STEPS, width), lambda m, j: (jnp.minimum(m * n_j + j, ROW_STEPS - 1), 0))
    whole = pl.BlockSpec((1, width), lambda m, j: (0, 0))
    kv_out = pl.BlockSpec((MROWS, 2 * HEAD_DIM), lambda m, j: (m, j))
    out = lambda cols: jax.ShapeDtypeStruct((width, cols), F32)
    like = lambda val: jax.ShapeDtypeStruct(val.shape, val.dtype)
    return pl.pallas_call(
        finish_kernel,
        grid=(width // MROWS, n_j),
        in_specs=[pl.BlockSpec((MROWS, seq_len), lambda m, j: (m, 0)), any_spec, rows, rows, whole, any_spec, any_spec],
        out_specs=[kv_out, kv_out, any_spec, any_spec, rows, rows, whole],
        out_shape=[out(groups * HEAD_DIM), out(groups * HEAD_DIM), like(w_q_grad), like(w_o_grad), like(grad_x), like(result), like(grad_gain)],
        scratch_shapes=[pltpu.VMEM(d_kv.shape, BF16), pltpu.SemaphoreType.DMA((groups // 2,)),
                        pltpu.VMEM((DEPTH, RING, high, width), F32), pltpu.SemaphoreType.DMA((2, DEPTH, RING))],
        compiler_params=params(2),
        cost_estimate=pl.CostEstimate(flops=4 * width * seq_len * groups * HEAD_DIM, bytes_accessed=2 * width * seq_len, transcendentals=0),
        name="finish",
    )(ht, d_kv, grad_x, result, grad_gain, w_o_grad, w_q_grad)


def solution(mesh):
    sp_size = mesh.shape['sp']
    seq_spec = P(('dp', 'sp'), None)
    pos_spec = P(('dp', 'sp'))
    replicated = P(None, None)
    part_rows = P('dp', None)

    def local_step(x, grad_out, positions, gain, w_q, w_k, w_v, w_o):
        n_heads = w_q.shape[1] // HEAD_DIM
        heads = n_heads // sp_size
        _, _, _, ht, _, _, _, w_o_grad, w_q_grad, kv_all, _, _, result, grad_x, grad_gain = step(
            x, gain.reshape(1, -1), positions, grad_out, w_q, w_k, w_v, w_o, sp_size, heads)
        grad_wk, grad_wv, grad_wq, grad_wo, grad_x, result, grad_gain = finish(
            ht, kv_all.reshape(sp_size, -1, 2 * HEAD_DIM), w_o_grad, w_q_grad, grad_x, result, grad_gain)
        return result, grad_x, grad_wq, grad_wk, grad_wv, grad_wo, grad_gain.reshape(-1)

    return jax.shard_map(local_step, mesh=mesh,
                         in_specs=(seq_spec, seq_spec, pos_spec, P(None), replicated, replicated, replicated, replicated),
                         out_specs=(seq_spec, seq_spec, part_rows, part_rows, part_rows, part_rows, P('dp')),
                         check_vma=False)
```

```python
import functools

import jax
import jax.numpy as jnp
import numpy as np
from jax import lax
from jax.experimental import pallas as pl
from jax.experimental.pallas import tpu as pltpu
from jax.sharding import PartitionSpec as P

HEAD_DIM = 128
HALF = HEAD_DIM // 2
ROPE_THETA = 1000000.0
NORM_EPS = 1e-05
NEG_LARGE = -1e30
LOG2E = 1.4426950408889634
BLK = 512
CHUNKS = 8
FWD_MIDDLE, BWD_MIDDLE = 5, 27
MROWS = 768
RING = 3
DEPTH = 4
COPY_ROWS = 24
PARTS = 3
ROW_STEPS = 8
F32 = jnp.float32
BF16 = jnp.bfloat16
ROWS_ROWS = (((0,), (0,)), ((), ()))
COLS_COLS = (((1,), (1,)), ((), ()))
ROWS_COLS = (((0,), (1,)), ((), ()))
VMEM_LIMIT = 63 * 1024 * 1024


def dot(a, b, dims=(((1,), (0,)), ((), ()))):
    return lax.dot_general(a, b, dims, preferred_element_type=F32)


def params(axes=1):
    return pltpu.CompilerParams(dimension_semantics=("arbitrary",) * axes, vmem_limit_bytes=VMEM_LIMIT)


class Neighbours:
    def __init__(self):
        self.me = lax.axis_index('sp')
        core, col, row = lax.rem(self.me, 2), lax.rem(self.me // 2, 2), self.me // 4
        self.sib = self.me + 1 - 2 * core
        self.xn = self.me + 2 - 4 * col
        self.yn = self.me + 4 - 8 * row
        self.diag = self.xn + self.yn - self.me

    def meet(self, peers):
        barrier = pltpu.get_barrier_semaphore()
        for peer in peers:
            pl.semaphore_signal(barrier, inc=1, device_id={'sp': peer}, device_id_type=pl.DeviceIdType.MESH)
        pl.semaphore_wait(barrier, len(peers))

    def across(self, r):
        core, col, row = lax.rem(self.me, 2), lax.rem(self.me // 2, 2), self.me // 4
        return (self.me + lax.rem(r, 2) * (1 - 2 * core) + lax.rem(r // 2, 2) * (2 - 4 * col) + (r // 4) * (4 - 8 * row))

    def others(self):
        flip = lambda dev: dev + 1 - 2 * lax.rem(dev, 2)
        return [self.sib, self.xn, flip(self.xn), self.yn, flip(self.yn), self.diag, flip(self.diag)]


def send(src, dst, sems, index, peer):
    return pltpu.make_async_remote_copy(src_ref=src, dst_ref=dst, send_sem=sems.at[0, index], recv_sem=sems.at[1, index],
                                        device_id={'sp': peer}, device_id_type=pl.DeviceIdType.MESH)


class Gather:
    COPIES = 5 * CHUNKS + 2
    HALF_CHUNKS = CHUNKS // 2
    ORDER = [chunk + half * (CHUNKS // 2) for chunk in range(CHUNKS // 2) for half in range(2)]

    def __init__(self, near, own, dst, rows, sems):
        self.near, self.own, self.dst, self.rows, self.sems = near, own, dst, rows, sems

    def block(self, dev, chunk, count=1):
        size = self.rows // CHUNKS
        return self.dst.at[pl.ds(pl.multiple_of(dev * self.rows + chunk * size, size), count * size), :]

    def first(self, chunk, kind):
        peer = (self.near.xn, self.near.yn, self.near.sib)[kind]
        return send(self.own(chunk), self.block(self.near.me, chunk), self.sems, kind * CHUNKS + chunk, peer)

    def onward(self, chunk):
        over_y = chunk < self.HALF_CHUNKS
        rows = self.block(self.near.xn if over_y else self.near.yn, chunk)
        return send(rows, rows, self.sems, 3 * CHUNKS + chunk, self.near.yn if over_y else self.near.xn)

    def share(self, kind):
        rows = self.block((self.near.xn, self.near.yn)[kind], 0, CHUNKS)
        return send(rows, rows, self.sems, 4 * CHUNKS + kind, self.near.sib)

    def share_diag(self, chunk):
        rows = self.block(self.near.diag, chunk)
        return send(rows, rows, self.sems, 4 * CHUNKS + 2 + chunk, self.near.sib)

    def start(self):
        for chunk in range(CHUNKS):
            for kind in (0, 1):
                self.send_first(chunk, kind)
            self.first(chunk, 2).start()

    def send_first(self, turn, kind):
        self.first(turn if kind == 0 else (turn + self.HALF_CHUNKS) % CHUNKS, kind).start()

    def middle(self):
        for chunk in self.ORDER:
            self.first(chunk, 0 if chunk < self.HALF_CHUNKS else 1).wait_recv()
            self.onward(chunk).start()

    def late(self):
        for chunk in range(self.HALF_CHUNKS, CHUNKS):
            self.first(chunk, 0).wait_recv()
        self.share(0).start()
        for chunk in range(self.HALF_CHUNKS):
            self.first(chunk, 1).wait_recv()
        self.share(1).start()

    def end_sib(self):
        for chunk in range(CHUNKS):
            self.first(chunk, 2).wait_recv()

    def end_near(self):
        for kind in range(2):
            self.share(kind).wait_recv()

    def end_far(self):
        for chunk in self.ORDER:
            self.onward(chunk).wait_recv()
            self.share_diag(chunk).start()
        for chunk in range(CHUNKS):
            for kind in range(3):
                self.first(chunk, kind).wait_send()
            self.onward(chunk).wait_send()
        for kind in range(2):
            self.share(kind).wait_send()
        for chunk in range(CHUNKS):
            self.share_diag(chunk).wait()

    def end(self):
        self.end_sib()
        self.end_near()
        self.end_far()


SEMS = pltpu.SemaphoreType.DMA((2, Gather.COPIES))


def masked(scores):
    key = lax.broadcasted_iota(jnp.int32, scores.shape, 0)
    query = lax.broadcasted_iota(jnp.int32, scores.shape, 1)
    return jnp.where(key <= query, scores, NEG_LARGE)


def unrotate(val, cos_t, sin_t):
    return (val * cos_t - pltpu.roll(val, HALF, 1) * sin_t).astype(BF16)


def attention_part(heads, near, gather_next, x_ref, gain_ref, pos_ref, freq_ref, dy_ref, wq_ref, wk_ref, wv_ref, wo_ref,
                   h_all, dy_all, o_all, ht_ref, dkv_ref, dq_a_ref, dq_b_ref, pos_all, pos_sems, h_sems, dy_sems, o_sems,
                   x_v, h_v, x_sems, own_sems, cos_s, sin_s, w_v, wo_v, w_sems, blk, blk_sems, ht_v, ht_sems,
                   q_s, k_s, v_s, vt, kt, ot_s, lse_s, acc, do_s, dk_acc, dv_acc, dq_v, dq_sems, dkv_v):
    rows, width = x_ref.shape
    n_blocks = k_s.shape[0]
    q_cols = heads * HEAD_DIM
    size = rows // CHUNKS
    qk_scale = HEAD_DIM ** -0.5
    to_log2 = qk_scale * LOG2E
    cols = [slice(a * HEAD_DIM, (a + 1) * HEAD_DIM) for a in range(heads)]
    part = lambda ref, chunk, count=size: ref.at[pl.ds(chunk * count, count), :]
    gather_h = Gather(near, lambda chunk: part(h_v, chunk), h_all, rows, h_sems)
    gather_dy = Gather(near, lambda chunk: part(dy_ref, chunk), dy_all, rows, dy_sems)
    gather_o = Gather(near, lambda chunk: part(ot_s, chunk, q_cols // CHUNKS), o_all, q_cols, o_sems)

    loads = [pltpu.make_async_copy(part(x_ref, chunk), part(x_v, chunk), x_sems.at[chunk]) for chunk in range(CHUNKS)]
    for load in loads:
        load.start()
    others = near.others()
    pos_all[near.me] = jnp.broadcast_to(pos_ref[...], pos_all.shape[1:])
    positions = [send(pos_ref, pos_all.at[near.me, pl.ds(0, 1), :], pos_sems, r, peer) for r, peer in enumerate(others)]
    gain = gain_ref[...].astype(F32).reshape(1, width)
    for turn, chunk in enumerate(Gather.ORDER):
        loads[chunk].wait()

        @pl.loop(0, size // 32)
        def _(r):
            at = pl.ds(pl.multiple_of(chunk * size + r * 32, 32), 32)
            x_f = x_v[at, :].astype(F32)
            normed = x_f * lax.rsqrt(jnp.mean(x_f * x_f, axis=-1, keepdims=True) + NORM_EPS)
            h_v[at, :] = (normed * gain).astype(BF16)

        if turn == 0:
            near.meet(others)
        gather_h.send_first(turn // 2, turn % 2)
        gather_h.first(chunk, 2).start()
    for turn in range(Gather.HALF_CHUNKS, CHUNKS):
        for kind in (0, 1):
            gather_h.send_first(turn, kind)
    for copy in positions:
        copy.start()
    own_h = pltpu.make_async_copy(h_v, gather_h.block(near.me, 0, CHUNKS), own_sems.at[0])
    own_h.start()
    w_loads, col = [], 0
    for n, (ref, count) in enumerate(((wq_ref, q_cols), (wk_ref, HEAD_DIM), (wv_ref, HEAD_DIM))):
        at = pl.ds(pl.multiple_of(near.me * count, HEAD_DIM), count)
        w_loads.append(pltpu.make_async_copy(ref.at[:, at], w_v.at[:, pl.ds(col, count)], w_sems.at[n]))
        col += count
    w_loads.append(pltpu.make_async_copy(wo_ref.at[pl.ds(pl.multiple_of(near.me * q_cols, q_cols), q_cols), :], wo_v, w_sems.at[3]))
    stage_in = pltpu.make_async_copy(dy_ref, x_v, own_sems.at[1])
    stage_out = pltpu.make_async_copy(x_v, gather_dy.block(near.me, 0, CHUNKS), own_sems.at[2])
    for load in w_loads + [stage_in]:
        load.start()
    for copy in positions:
        copy.wait()
    sign = jnp.where(lax.broadcasted_iota(jnp.int32, (1, HEAD_DIM), 1) < HALF, -1.0, 1.0)

    @pl.loop(0, n_blocks)
    def _(b):
        pos = jnp.broadcast_to(pos_all[b, 0:1, :].astype(F32), (HEAD_DIM, rows)).T
        angles = pos * freq_ref[...]
        cos_s[b] = jnp.cos(angles)
        sin_s[b] = jnp.sin(angles) * sign

    gather_h.middle()
    for load in w_loads + [stage_in]:
        load.wait()
    stage_out.start()
    own_h.wait()

    def block_load(ref, block, slot):
        return pltpu.make_async_copy(ref.at[pl.ds(pl.multiple_of(block * rows, rows), rows), :], blk.at[slot], blk_sems.at[slot])

    far = n_blocks * 3 // 4

    def arrive(r, ref, gather, before_near=None, before_far=None):
        slot = lax.rem(r, 2)

        @pl.when(r == 1)
        def _():
            gather.end_sib()

        @pl.when(r == 2)
        def _():
            if before_near:
                before_near()
            gather.end_near()

        @pl.when(r == far)
        def _():
            if before_far:
                before_far()
            gather.end_far()

        @pl.when(functools.reduce(jnp.logical_or, [r == first for first in (0, 1, 2, far)]))
        def _():
            block_load(ref, near.across(r), slot).start()

        block_load(ref, 0, slot).wait()

        @pl.when(functools.reduce(jnp.logical_and, [r + 1 != first for first in (1, 2, far, n_blocks)]))
        def _():
            block_load(ref, near.across(r + 1), 1 - slot).start()

    def ht_store(r):
        at = pl.ds(pl.multiple_of(near.across(r) * rows, rows), rows)
        return pltpu.make_async_copy(ht_v.at[lax.rem(r, 2)], ht_ref.at[:, at], ht_sems.at[lax.rem(r, 2)])

    @pl.loop(0, n_blocks)
    def _(r):
        i = near.across(r)
        slot = lax.rem(r, 2)
        arrive(r, h_all, gather_h, gather_h.late, gather_dy.start)

        @pl.when(r >= 2)
        def _():
            ht_store(r - 2).wait()

        ht_v[slot] = blk[slot].T
        ht_store(r).start()
        prod = dot(blk[slot], w_v[...])
        cos_t, sin_t = cos_s[i], sin_s[i]
        for a in range(heads + 1):
            val = prod[:, a * HEAD_DIM:(a + 1) * HEAD_DIM]
            rot = (val * cos_t + pltpu.roll(val, HALF, 1) * sin_t).astype(BF16)
            if a < heads:
                q_s[i, :, cols[a]] = rot
            else:
                k_s[i] = rot
                kt[i] = rot.T
        v_i = prod[:, q_cols + HEAD_DIM:].astype(BF16)
        v_s[i] = v_i
        vt[i] = v_i.T

    def fwd_chunk(i, c, carry, diagonal):
        k_c, vt_c = k_s[c], vt[c]
        scores = [dot(k_c, q_s[i, :, cols[a]], COLS_COLS) * to_log2 for a in range(heads)]
        out = []
        for a in range(heads):
            s = masked(scores[a]) if diagonal else scores[a]
            m_old, l_old = carry[a]
            m_new = jnp.maximum(m_old, jnp.max(s, axis=0, keepdims=True))
            alpha = jnp.exp2(m_old - m_new)
            p = jnp.exp2(s - m_new)
            l_new = l_old * alpha + jnp.sum(p, axis=0, keepdims=True)
            acc[a] = acc[a] * alpha + dot(vt_c, p.astype(BF16))
            out.append((m_new, l_new))
        return tuple(out)

    @pl.loop(0, n_blocks)
    def _(i):
        acc[...] = jnp.zeros_like(acc)
        start = tuple((jnp.full((1, rows), NEG_LARGE, F32), jnp.zeros((1, rows), F32)) for _ in range(heads))
        carry = lax.fori_loop(0, i, lambda c, carry: fwd_chunk(i, c, carry, False), start)
        carry = fwd_chunk(i, i, carry, True)
        at = pl.ds(pl.multiple_of(i * rows, rows), rows)
        for a in range(heads):
            m_a, l_a = carry[a]
            ot_s[cols[a], at] = (acc[a] / l_a).astype(BF16)
            lse_s[i, a:a + 1, :] = m_a + jnp.log2(l_a)

        @pl.when(i == FWD_MIDDLE)
        def _():
            gather_dy.middle()

    gather_dy.late()
    gather_o.start()
    own_o = pltpu.make_async_copy(ot_s, gather_o.block(near.me, 0, CHUNKS), own_sems.at[0])
    own_o.start()

    def bwd_chunk(i, c, delta, diagonal):
        k_c, v_c, kt_c = k_s[c], v_s[c], kt[c]
        dk_c = dv_c = None
        for a in range(heads):
            q_a, do_a = q_s[i, :, cols[a]], do_s[i, :, cols[a]]
            s = dot(k_c, q_a, COLS_COLS) * to_log2
            if diagonal:
                s = masked(s)
            p = jnp.exp2(s - lse_s[i, a:a + 1, :])
            d_p = dot(v_c, do_a, COLS_COLS)
            d_s = (p * (d_p - delta[a])).astype(BF16)
            dv_a = dot(p.astype(BF16), do_a)
            dk_a = dot(d_s, q_a)
            dv_c = dv_a if dv_c is None else dv_c + dv_a
            dk_c = dk_a if dk_c is None else dk_c + dk_a
            acc[a] += dot(kt_c, d_s)
        dk_acc[c] += dk_c
        dv_acc[c] += dv_c

    def dq_stores(r):
        slot = lax.rem(r, 2)
        at = pl.ds(pl.multiple_of(near.across(r) * rows, rows), rows)
        last = q_cols - HEAD_DIM
        return [pltpu.make_async_copy(dq_v.at[slot, :, pl.ds(0, last)], dq_a_ref.at[at, :], dq_sems.at[slot, 0]),
                pltpu.make_async_copy(dq_v.at[slot, :, pl.ds(last, HEAD_DIM)], dq_b_ref.at[at, :], dq_sems.at[slot, 1])]

    def pass_on(done):
        @pl.when(done == BWD_MIDDLE)
        def _():
            gather_o.middle()

    for r in (n_blocks - 2, n_blocks - 1):
        ht_store(jnp.int32(r)).wait()
    dk_acc[...] = jnp.zeros_like(dk_acc)
    dv_acc[...] = jnp.zeros_like(dv_acc)
    stage_out.wait()

    def bwd_block(r, done):
        i = near.across(r)
        slot = lax.rem(r, 2)
        at = pl.ds(pl.multiple_of(i * rows, rows), rows)

        arrive(r, dy_all, gather_dy)
        do_s[i] = dot(blk[slot], wo_v[...], COLS_COLS).astype(BF16)
        acc[...] = jnp.zeros_like(acc)
        delta = [jnp.sum(ot_s[cols[a], at].astype(F32) * do_s[i, :, cols[a]].T.astype(F32), axis=0, keepdims=True) for a in range(heads)]

        @pl.loop(0, i)
        def _(c):
            bwd_chunk(i, c, delta, False)
            pass_on(done + c)

        bwd_chunk(i, i, delta, True)
        pass_on(done + i)

        @pl.when(r >= 2)
        def _():
            for store in dq_stores(r - 2):
                store.wait()

        for a in range(heads):
            dq_v[slot, :, cols[a]] = unrotate(acc[a].T * qk_scale, cos_s[i], sin_s[i])
        for store in dq_stores(r):
            store.start()
        return done + i + 1

    lax.fori_loop(0, n_blocks, bwd_block, jnp.int32(0))
    gather_o.late()
    for r in (n_blocks - 2, n_blocks - 1):
        for store in dq_stores(r):
            store.wait()
    gather_next.start()

    @pl.loop(0, n_blocks)
    def _(c):
        at = pl.ds(pl.multiple_of(c * rows, rows), rows)
        dkv_v[at, :HEAD_DIM] = unrotate(dk_acc[c] * qk_scale, cos_s[c], sin_s[c])
        dkv_v[at, HEAD_DIM:] = dv_acc[c].astype(BF16)

    dkv_store = pltpu.make_async_copy(dkv_v, dkv_ref, own_sems.at[1])
    dkv_store.start()
    own_o.wait()
    gather_o.end()
    dkv_store.wait()


def lanes(*parts):
    return jnp.concatenate(parts, axis=1)


def products_part(heads, near, gathers, ot_ref, ht_ref, dy_ref, d_kv_ref, d_qa_ref, d_qb_ref, x_ref, own_dy_ref, gain_ref, wo_ref, wk_ref, wv_ref, wq_ref,
                  wo_out, wq_out, kv_all, qa_all, qb_all, res_ref, gx_ref, gg_ref, gg_row, gg_all, gg_sems, x_sems,
                  a_buf, b_buf, tile, a_sem, b_sems, t_sems, stage, stage_sems, ot_v, o_v, x_v, io_sems, own, own_sems, w_v, w_sems, acc,
                  gg_v):
    core = lax.rem(near.me, 2)
    half = a_buf.shape[0]
    seq_len = d_kv_ref.shape[0]
    rows, width = x_ref.shape
    n_cols = d_kv_ref.shape[1]
    n_o, n_all = width // (2 * n_cols), x_sems.shape[1]
    n_oa = n_o + (n_all - n_o) * 2 // 3

    local = (d_qa_ref, d_qb_ref, d_kv_ref)

    def stage_in(n):
        return pltpu.make_async_copy(local[n], stage.at[:, pl.ds(0, local[n].shape[1])], stage_sems.at[0])

    def stage_out(n):
        return pltpu.make_async_copy(stage.at[:, pl.ds(0, local[n].shape[1])], gathers[n].block(near.me, 0, CHUNKS), stage_sems.at[1])

    def copy_own(n):
        stage_in(n).wait()
        stage_out(n).start()

    own_rows = pl.ds(pl.multiple_of(core * half, half), half)
    tokens = pl.ds(pl.multiple_of(near.me * rows, rows), rows)
    ot_load = pltpu.make_async_copy(ot_ref.at[:, tokens], ot_v, io_sems.at[0])
    x_load = pltpu.make_async_copy(x_ref, x_v, io_sems.at[1])
    res_store = pltpu.make_async_copy(x_v, res_ref, io_sems.at[2])
    dy_load = pltpu.make_async_copy(own_dy_ref, o_v, io_sems.at[3])
    gx_store = pltpu.make_async_copy(o_v, gx_ref, io_sems.at[0])

    def a_load(ref):
        return pltpu.make_async_copy(ref.at[own_rows, :], a_buf, a_sem)

    def b_loads(source, p, slot, g):
        if source is dy_ref:
            srcs = [dy_ref.at[:, pl.ds(pl.multiple_of((2 * p + g) * n_cols, n_cols), n_cols)]]
        else:
            per = n_cols // source.shape[1]
            srcs = [source.at[pl.ds(pl.multiple_of(((2 * p + g) * per + n) * seq_len, seq_len), seq_len), :] for n in range(per)]
        return [pltpu.make_async_copy(src, b_buf.at[slot, :, pl.ds(g * n_cols + n * src.shape[1], src.shape[1])], b_sems.at[slot, g])
                for n, src in enumerate(srcs)]

    def start_b(step):
        slot = lax.rem(step, 2)
        for source, low, high in ((dy_ref, 0, n_o), (qa_all, n_o, n_oa), (qb_all, n_oa, n_all)):
            @pl.when(jnp.logical_and(step >= low, step < high))
            def _():
                for g in range(2):
                    for load in b_loads(source, step - low, slot, g):
                        load.start()

    def pieces(kind, step):
        wide = (2 * n_cols, n_cols, HEAD_DIM)[kind]
        slot = lax.rem(step, 2)
        out = []
        for n in range(2 * n_cols // wide):
            group = (step - (0, n_o, n_oa)[kind]) * (2 * n_cols // wide) + n
            col = (group * wide, group * heads * HEAD_DIM, (group + 1) * heads * HEAD_DIM - HEAD_DIM)[kind]
            dst = (wo_out, wq_out, wq_out)[kind].at[own_rows, pl.ds(pl.multiple_of(col, HEAD_DIM), wide)]
            src = tile.at[slot, :, pl.ds(n * wide, wide)]
            out.append((pltpu.make_async_copy(src, dst, t_sems.at[slot]), send(src, dst, x_sems, step, near.sib)))
        return out

    def start_tile(step):
        for kind, (low, high) in enumerate(((0, n_o), (n_o, n_oa), (n_oa, n_all))):
            @pl.when(jnp.logical_and(step >= low, step < high))
            def _():
                for keep, give in pieces(kind, step):
                    keep.start()
                    give.start()

    def whole_tile(step):
        slot = lax.rem(step, 2)
        dst = wo_out.at[own_rows, pl.ds(0, 2 * n_cols)]
        return pltpu.make_async_copy(tile.at[slot], dst, t_sems.at[slot]), send(tile.at[slot], dst, x_sems, step, near.sib)

    def wait_tile(step):
        keep, give = whole_tile(step)
        keep.wait()
        give.wait_send()

    def result_part():
        cols = b_buf.shape[2]

        def w_load(n):
            slot = lax.rem(n, 2)
            return pltpu.make_async_copy(wo_ref.at[:, pl.ds(pl.multiple_of(n * cols, cols), cols)], b_buf.at[slot, pl.ds(0, wo_ref.shape[0]), :],
                                         b_sems.at[slot, 0])

        w_load(jnp.int32(0)).start()
        ot_load.wait()

        @pl.loop(0, ot_v.shape[0] // BLK)
        def _(r):
            at = pl.ds(pl.multiple_of(r * BLK, BLK), BLK)
            o_v[:, at] = ot_v[at, :].T

        x_load.wait()

        @pl.loop(0, n_o)
        def _(n):
            w_load(n).wait()

            @pl.when(n + 1 < n_o)
            def _():
                w_load(n + 1).start()

            at = pl.ds(pl.multiple_of(n * cols, cols), cols)
            x_v[:, at] = (x_v[:, at].astype(F32) + dot(o_v[...], b_buf[lax.rem(n, 2), :wo_ref.shape[0], :])).astype(BF16)

        res_store.start()

    def hidden_parts(kind):
        count = own.shape[0] // (2 if kind == 1 else 1)

        def own_load(r, g):
            source = (qa_all, qb_all, kv_all)[kind]
            device, col = (2 * r + g, 0) if kind == 1 else (near.across(r), g * HEAD_DIM)
            at = pl.ds(pl.multiple_of(device * seq_len + near.me * rows, rows), rows)
            return pltpu.make_async_copy(source.at[at, pl.ds(col, HEAD_DIM)], own.at[r, :, pl.ds(g * HEAD_DIM, HEAD_DIM)], own_sems.at[r, g])

        def w_load(r, g):
            source = (wk_ref, wv_ref)[g] if kind == 2 else wq_ref
            col = near.across(r) if kind == 2 else heads * near.across(r) + g if kind == 0 else heads * (2 * r + g + 1) - 1
            slot = lax.rem(r, 2)
            return pltpu.make_async_copy(source.at[:, pl.ds(pl.multiple_of(col * HEAD_DIM, HEAD_DIM), HEAD_DIM)],
                                         w_v.at[slot, :, pl.ds(g * HEAD_DIM, HEAD_DIM)], w_sems.at[slot, g])

        return count, own_load, w_load

    def hidden_start(kind, low=0, high=None):
        count, own_load, w_load = hidden_parts(kind)
        for g in range(2):
            if low == 0:
                w_load(jnp.int32(0), g).start()

            @pl.loop(low, high or count)
            def _(r):
                own_load(r, g).start()

    def hidden_add(kind, low=0, high=None):
        count, own_load, w_load = hidden_parts(kind)

        @pl.loop(low, high or count)
        def _(r):
            for g in range(2):
                w_load(r, g).wait()
                own_load(r, g).wait()

            @pl.when(r + 1 < count)
            def _():
                for g in range(2):
                    w_load(r + 1, g).start()

            for col in range(0, width, width // PARTS):
                at = slice(col, col + width // PARTS)
                acc[:, at] += dot(own[r], w_v[lax.rem(r, 2), at, :], COLS_COLS)

    a_load(ot_ref).start()
    start_b(jnp.int32(0))
    stage_in(0).start()
    ot_load.start()
    x_load.start()
    a_load(ot_ref).wait()

    @pl.loop(0, n_all)
    def _(step):
        slot = lax.rem(step, 2)
        for g in range(2):
            b_loads(dy_ref, 0, slot, g)[0].wait()

        @pl.when(jnp.logical_and(step != n_o - 1, step != n_oa - 1))
        def _():
            start_b(step + 1)

        @pl.when(step >= 2)
        def _():
            wait_tile(step - 2)

        @pl.when(step == n_o)
        def _():
            a_load(ht_ref).wait()

        for r in range(0, half, half // PARTS):
            tile[slot, r:r + half // PARTS, :] = dot(a_buf[r:r + half // PARTS, :], b_buf[slot])
        start_tile(step)

        @pl.when(step == n_o - 4)
        def _():
            acc[...] = jnp.zeros_like(acc)
            copy_own(0)
            gathers[0].middle()

        @pl.when(step == n_o - 1)
        def _():
            a_load(ht_ref).start()
            gathers[0].late()
            gathers[1].start()
            stage_out(0).wait()
            stage_in(1).start()
            result_part()
            gathers[0].end()
            start_b(step + 1)
            hidden_start(0)

        @pl.when(step == n_oa - 4)
        def _():
            copy_own(1)
            gathers[1].middle()

        @pl.when(step == n_oa - 2)
        def _():
            gathers[1].late()
            gathers[2].start()
            stage_out(1).wait()
            stage_in(2).start()

        @pl.when(step == n_oa - 1)
        def _():
            res_store.wait()
            x_load.start()
            dy_load.start()
            gathers[1].end()
            start_b(step + 1)

    hidden_add(0)
    copy_own(2)
    gathers[2].middle()
    hidden_start(1)
    hidden_add(1)
    gathers[2].late()
    stage_out(2).wait()
    gathers[2].end_sib()
    gathers[2].end_near()
    near_count = own.shape[0] * 3 // 4
    hidden_start(2, 0, near_count)
    for step in (n_all - 2, n_all - 1):
        wait_tile(jnp.int32(step))
    hidden_add(2, 0, near_count)
    gathers[2].end_far()
    hidden_start(2, near_count)
    hidden_add(2, near_count)

    gain = gain_ref[...].astype(F32).reshape(1, width)
    gg_v[...] = jnp.zeros_like(gg_v)
    x_load.wait()
    dy_load.wait()

    @pl.loop(0, rows // 32)
    def _(r):
        at = pl.ds(pl.multiple_of(r * 32, 32), 32)
        x_f = x_v[at, :].astype(F32)
        inv_rms = lax.rsqrt(jnp.mean(x_f * x_f, axis=-1, keepdims=True) + NORM_EPS)
        normed = x_f * inv_rms
        d_hid = acc[at, :]
        both = d_hid * normed
        gg_v[...] += jnp.sum(both.reshape(4, 8, width), axis=0)
        mean = jnp.mean(both * gain, axis=-1, keepdims=True)
        o_v[at, :] = (o_v[at, :].astype(F32) + inv_rms * (d_hid * gain - normed * mean)).astype(BF16)

    gg_row[...] = jnp.sum(gg_v[...], axis=0, keepdims=True)
    gg_all[near.me] = gg_row[...]
    parts = [send(gg_row, gg_all.at[near.me], gg_sems, r, peer) for r, peer in enumerate(near.others())]
    for copy in parts:
        copy.start()
    gx_store.start()

    @pl.loop(0, n_all)
    def _(step):
        whole_tile(step)[1].wait_recv()

    for copy in parts:
        copy.wait()
    gg_ref[...] = jnp.sum(gg_all[...], axis=0)
    gx_store.wait()


def step_kernel(heads, first_scratch, second_scratch, x_ref, gain_ref, pos_ref, freq_ref, dy_ref, wq_ref, wk_ref, wv_ref, wo_ref,
                h_all, dy_all, o_all, ht, d_kv, d_qa, d_qb, wo_out, wq_out, kv_all, qa_all, qb_all, res, gx, gg,
                pos_all, pos_sems, gg_row, gg_all, gg_sems, x_sems, h_sems, dy_sems, o_sems, kv_sems, qa_sems, qb_sems):
    near = Neighbours()
    seq_len = d_kv.shape[0]

    def gather_of(src, dst, sems):
        return Gather(near, lambda c: src.at[pl.ds(c * (seq_len // CHUNKS), seq_len // CHUNKS), :], dst, seq_len, sems)

    gathers = [gather_of(d_qa, qa_all, qa_sems), gather_of(d_qb, qb_all, qb_sems), gather_of(d_kv, kv_all, kv_sems)]

    def first(*scratch):
        attention_part(heads, near, gathers[0], x_ref, gain_ref, pos_ref, freq_ref, dy_ref, wq_ref, wk_ref, wv_ref, wo_ref,
                       h_all, dy_all, o_all, ht, d_kv, d_qa, d_qb, pos_all, pos_sems, h_sems, dy_sems, o_sems, *scratch)

    def second(*scratch):
        products_part(heads, near, gathers, o_all, ht, dy_all, d_kv, d_qa, d_qb, x_ref, dy_ref, gain_ref, wo_ref, wk_ref, wv_ref, wq_ref,
                      wo_out, wq_out, kv_all, qa_all, qb_all, res, gx, gg, gg_row, gg_all, gg_sems, x_sems, *scratch)

    pl.run_scoped(first, *first_scratch)
    pl.run_scoped(second, *second_scratch)


def step(x, gain, positions, grad_out, w_q, w_k, w_v, w_o, sp_size, heads):
    rows, width = x.shape
    seq_len = rows * sp_size
    q_cols = heads * HEAD_DIM
    all_cols = q_cols * sp_size
    half = width // 2
    cols = 4 * HEAD_DIM
    n_all = (width + all_cols) // cols
    any_spec = pl.BlockSpec(memory_space=pl.ANY)
    vmem = pl.BlockSpec(memory_space=pltpu.VMEM)
    dma = pltpu.SemaphoreType.DMA
    inv_freq = ROPE_THETA ** (-np.arange(0, HEAD_DIM, 2) / HEAD_DIM)
    freq = jnp.asarray(np.concatenate([inv_freq, inv_freq])[None, :], F32)
    pairs = heads * seq_len * (seq_len + rows) // 2
    out = lambda *shape, dtype=BF16: jax.ShapeDtypeStruct(shape, dtype)
    array = lambda *shape, dtype=BF16: pltpu.VMEM(shape, dtype)
    blocks = lambda *shape, dtype=BF16: pltpu.VMEM((sp_size,) + shape, dtype)
    first_scratch = [array(rows, width), array(rows, width), dma((CHUNKS,)), dma((3,)), blocks(rows, HEAD_DIM, dtype=F32),
                     blocks(rows, HEAD_DIM, dtype=F32), array(width, q_cols + 2 * HEAD_DIM), array(q_cols, width), dma((4,)),
                     array(2, rows, width), dma((2,)), array(2, width, rows), dma((2,)),
                     blocks(rows, q_cols), blocks(rows, HEAD_DIM), blocks(rows, HEAD_DIM), blocks(HEAD_DIM, rows), blocks(HEAD_DIM, rows),
                     array(q_cols, seq_len), blocks(8, rows, dtype=F32), array(heads, HEAD_DIM, rows, dtype=F32),
                     blocks(rows, q_cols), blocks(rows, HEAD_DIM, dtype=F32), blocks(rows, HEAD_DIM, dtype=F32),
                     array(2, rows, q_cols), dma((2, 2)), array(seq_len, 2 * HEAD_DIM)]
    second_scratch = [array(half, seq_len), array(2, seq_len, cols), array(2, half, cols, dtype=F32), dma, dma((2, 2)), dma((2,)),
                      array(seq_len, 2 * HEAD_DIM), dma((2,)), array(all_cols, rows), array(rows, all_cols), array(rows, width),
                      dma((4,)), blocks(rows, 2 * HEAD_DIM), dma((sp_size, 2)), array(2, width, 2 * HEAD_DIM), dma((2, 2)),
                      array(rows, width, dtype=F32), array(8, width, dtype=F32)]
    return pl.pallas_call(
        functools.partial(step_kernel, heads, first_scratch, second_scratch),
        in_specs=[any_spec, vmem, vmem, vmem] + [any_spec] * 5,
        out_specs=[any_spec] * 14 + [vmem],
        out_shape=[out(seq_len, width), out(seq_len, width), out(all_cols, seq_len), out(width, seq_len), out(seq_len, 2 * HEAD_DIM),
                   out(seq_len, q_cols - HEAD_DIM), out(seq_len, HEAD_DIM), out(all_cols, width, dtype=F32), out(width, all_cols, dtype=F32),
                   out(sp_size * seq_len, 2 * HEAD_DIM), out(sp_size * seq_len, q_cols - HEAD_DIM), out(sp_size * seq_len, HEAD_DIM),
                   out(rows, width), out(rows, width), out(1, width, dtype=F32)],
        scratch_shapes=[blocks(8, rows, dtype=jnp.int32), dma((2, 7)), array(1, width, dtype=F32), blocks(1, width, dtype=F32), dma((2, 7)),
                        dma((2, n_all))] + [SEMS] * 6,
        compiler_params=pltpu.CompilerParams(vmem_limit_bytes=VMEM_LIMIT, collective_id=0, has_side_effects=True),
        cost_estimate=pl.CostEstimate(flops=28 * pairs * HEAD_DIM + 2 * half * cols * seq_len * n_all, bytes_accessed=20 * seq_len * width,
                                      transcendentals=2 * pairs),
        name="step",
    )(x, gain, positions.reshape(1, -1), freq, grad_out, w_q, w_k, w_v, w_o)


def finish_kernel(ht_ref, d_ref, gx_in, res_in, gg_in, wo_in, wq_in, wk_ref, wv_ref, wq_ref, wo_ref, gx_ref, res_ref, gg_ref, d_v, d_sems, ring, ring_sems):
    step = pl.program_id(0) * pl.num_programs(1) + pl.program_id(1)
    high = ring.shape[2]
    per_array = wo_in.shape[0] // (high * RING)

    def copy_in(src, g, n):
        at = pl.ds(pl.multiple_of((lax.rem(g, per_array) * RING + n) * high, high), high)
        return pltpu.make_async_copy(src.at[at, :], ring.at[lax.rem(g, DEPTH), n], ring_sems.at[0, lax.rem(g, DEPTH), n])

    def copy_out(dst, g, n):
        at = pl.ds(pl.multiple_of((lax.rem(g, per_array) * RING + n) * high, high), high)
        return pltpu.make_async_copy(ring.at[lax.rem(g, DEPTH), n], dst.at[at, :], ring_sems.at[1, lax.rem(g, DEPTH), n])

    def start(copy, first, second, g):
        for ref, mine in ((first, g < per_array), (second, g >= per_array)):
            @pl.when(mine)
            def _():
                for n in range(RING):
                    copy(ref, g, n).start()

    def pair_load(p):
        at = pl.ds(2 * p, 2)
        return pltpu.make_async_copy(d_ref.at[at], d_v.at[at], d_sems.at[p])

    @pl.when(step == 0)
    def _():
        for p in range(d_v.shape[0] // 2):
            pair_load(p).start()

    last = pl.num_programs(0) * pl.num_programs(1) - 1

    def free(g):
        for n in range(RING):
            copy_out(wo_ref, g, n).wait()

    def pass_on(g):
        for n in range(RING):
            copy_in(wo_in, g, n).wait()
        start(copy_out, wo_ref, wq_ref, g)

    @pl.when(step == 0)
    def _():
        start(copy_in, wo_in, wq_in, step)

    @pl.when(step >= DEPTH - 1)
    def _():
        free(step + 1 - DEPTH)

    @pl.when(step < last)
    def _():
        start(copy_in, wo_in, wq_in, step + 1)

    @pl.when(step >= 1)
    def _():
        pass_on(step - 1)

    for p in range(d_v.shape[0] // 2):
        @pl.when(step == p)
        def _():
            pair_load(p).wait()

    ht = ht_ref[...]
    pair = 2 * pl.program_id(1)
    wk_ref[...] = dot(ht, lanes(d_v[pair, :, :HEAD_DIM], d_v[pair + 1, :, :HEAD_DIM]))
    wv_ref[...] = dot(ht, lanes(d_v[pair, :, HEAD_DIM:], d_v[pair + 1, :, HEAD_DIM:]))

    @pl.when(step == 0)
    def _():
        gg_ref[...] = gg_in[...]

    @pl.when(step == last)
    def _():
        pass_on(last)
        for back in range(DEPTH - 1):
            free(last - back)

    @pl.when(step < ROW_STEPS)
    def _():
        gx_ref[...] = gx_in[...]
        res_ref[...] = res_in[...]


def finish(ht, d_kv, w_o_grad, w_q_grad, grad_x, result, grad_gain):
    width, seq_len = ht.shape
    groups = d_kv.shape[0]
    n_j = groups // 2
    steps = (width // MROWS) * n_j
    high = width // COPY_ROWS
    assert w_o_grad.shape[0] + w_q_grad.shape[0] == high * RING * steps
    any_spec = pl.BlockSpec(memory_space=pl.ANY)
    rows = pl.BlockSpec((grad_x.shape[0] // ROW_STEPS, width), lambda m, j: (jnp.minimum(m * n_j + j, ROW_STEPS - 1), 0))
    whole = pl.BlockSpec((1, width), lambda m, j: (0, 0))
    kv_out = pl.BlockSpec((MROWS, 2 * HEAD_DIM), lambda m, j: (m, j))
    out = lambda cols: jax.ShapeDtypeStruct((width, cols), F32)
    like = lambda val: jax.ShapeDtypeStruct(val.shape, val.dtype)
    return pl.pallas_call(
        finish_kernel,
        grid=(width // MROWS, n_j),
        in_specs=[pl.BlockSpec((MROWS, seq_len), lambda m, j: (m, 0)), any_spec, rows, rows, whole, any_spec, any_spec],
        out_specs=[kv_out, kv_out, any_spec, any_spec, rows, rows, whole],
        out_shape=[out(groups * HEAD_DIM), out(groups * HEAD_DIM), like(w_q_grad), like(w_o_grad), like(grad_x), like(result), like(grad_gain)],
        scratch_shapes=[pltpu.VMEM(d_kv.shape, BF16), pltpu.SemaphoreType.DMA((groups // 2,)),
                        pltpu.VMEM((DEPTH, RING, high, width), F32), pltpu.SemaphoreType.DMA((2, DEPTH, RING))],
        compiler_params=params(2),
        cost_estimate=pl.CostEstimate(flops=4 * width * seq_len * groups * HEAD_DIM, bytes_accessed=2 * width * seq_len, transcendentals=0),
        name="finish",
    )(ht, d_kv, grad_x, result, grad_gain, w_o_grad, w_q_grad)


def solution(mesh):
    sp_size = mesh.shape['sp']
    seq_spec = P(('dp', 'sp'), None)
    pos_spec = P(('dp', 'sp'))
    replicated = P(None, None)
    part_rows = P('dp', None)

    def local_step(x, grad_out, positions, gain, w_q, w_k, w_v, w_o):
        n_heads = w_q.shape[1] // HEAD_DIM
        heads = n_heads // sp_size
        _, _, _, ht, _, _, _, w_o_grad, w_q_grad, kv_all, _, _, result, grad_x, grad_gain = step(
            x, gain, positions, grad_out, w_q, w_k, w_v, w_o, sp_size, heads)
        grad_wk, grad_wv, grad_wq, grad_wo, grad_x, result, grad_gain = finish(
            ht, kv_all.reshape(sp_size, -1, 2 * HEAD_DIM), w_o_grad, w_q_grad, grad_x, result, grad_gain)
        return result, grad_x, grad_wq, grad_wk, grad_wv, grad_wo, grad_gain.reshape(-1)

    return jax.shard_map(local_step, mesh=mesh,
                         in_specs=(seq_spec, seq_spec, pos_spec, P(None), replicated, replicated, replicated, replicated),
                         out_specs=(seq_spec, seq_spec, part_rows, part_rows, part_rows, part_rows, P('dp')),
                         check_vma=False)
```

```python
import functools

import jax
import jax.numpy as jnp
import numpy as np
from jax import lax
from jax.experimental import pallas as pl
from jax.experimental.pallas import tpu as pltpu
from jax.sharding import PartitionSpec as P

HEAD_DIM = 128
HALF = HEAD_DIM // 2
ROPE_THETA = 1000000.0
NORM_EPS = 1e-05
NEG_LARGE = -1e30
LOG2E = 1.4426950408889634
BLK = 512
CHUNKS = 4
FWD_MIDDLE, BWD_MIDDLE = 5, 27
MROWS = 768
RING = 3
DEPTH = 4
COPY_ROWS = 24
PARTS = 3
ROW_STEPS = 8
F32 = jnp.float32
BF16 = jnp.bfloat16
ROWS_ROWS = (((0,), (0,)), ((), ()))
COLS_COLS = (((1,), (1,)), ((), ()))
ROWS_COLS = (((0,), (1,)), ((), ()))
VMEM_LIMIT = 63 * 1024 * 1024


def dot(a, b, dims=(((1,), (0,)), ((), ()))):
    return lax.dot_general(a, b, dims, preferred_element_type=F32)


def params(axes=1):
    return pltpu.CompilerParams(dimension_semantics=("arbitrary",) * axes, vmem_limit_bytes=VMEM_LIMIT)


class Neighbours:
    def __init__(self):
        self.me = lax.axis_index('sp')
        core, col, row = lax.rem(self.me, 2), lax.rem(self.me // 2, 2), self.me // 4
        self.sib = self.me + 1 - 2 * core
        self.xn = self.me + 2 - 4 * col
        self.yn = self.me + 4 - 8 * row
        self.diag = self.xn + self.yn - self.me

    def meet(self, peers):
        barrier = pltpu.get_barrier_semaphore()
        for peer in peers:
            pl.semaphore_signal(barrier, inc=1, device_id={'sp': peer}, device_id_type=pl.DeviceIdType.MESH)
        pl.semaphore_wait(barrier, len(peers))

    def across(self, r):
        core, col, row = lax.rem(self.me, 2), lax.rem(self.me // 2, 2), self.me // 4
        return (self.me + lax.rem(r, 2) * (1 - 2 * core) + lax.rem(r // 2, 2) * (2 - 4 * col) + (r // 4) * (4 - 8 * row))

    def others(self):
        flip = lambda dev: dev + 1 - 2 * lax.rem(dev, 2)
        return [self.sib, self.xn, flip(self.xn), self.yn, flip(self.yn), self.diag, flip(self.diag)]


def send(src, dst, sems, index, peer):
    return pltpu.make_async_remote_copy(src_ref=src, dst_ref=dst, send_sem=sems.at[0, index], recv_sem=sems.at[1, index],
                                        device_id={'sp': peer}, device_id_type=pl.DeviceIdType.MESH)


class Gather:
    COPIES = 5 * CHUNKS + 2
    HALF_CHUNKS = CHUNKS // 2
    ORDER = [chunk + half * (CHUNKS // 2) for chunk in range(CHUNKS // 2) for half in range(2)]

    def __init__(self, near, own, dst, rows, sems):
        self.near, self.own, self.dst, self.rows, self.sems = near, own, dst, rows, sems

    def block(self, dev, chunk, count=1):
        size = self.rows // CHUNKS
        return self.dst.at[pl.ds(pl.multiple_of(dev * self.rows + chunk * size, size), count * size), :]

    def first(self, chunk, kind):
        peer = (self.near.xn, self.near.yn, self.near.sib)[kind]
        return send(self.own(chunk), self.block(self.near.me, chunk), self.sems, kind * CHUNKS + chunk, peer)

    def onward(self, chunk):
        over_y = chunk < self.HALF_CHUNKS
        rows = self.block(self.near.xn if over_y else self.near.yn, chunk)
        return send(rows, rows, self.sems, 3 * CHUNKS + chunk, self.near.yn if over_y else self.near.xn)

    def share(self, kind):
        rows = self.block((self.near.xn, self.near.yn)[kind], 0, CHUNKS)
        return send(rows, rows, self.sems, 4 * CHUNKS + kind, self.near.sib)

    def share_diag(self, chunk):
        rows = self.block(self.near.diag, chunk)
        return send(rows, rows, self.sems, 4 * CHUNKS + 2 + chunk, self.near.sib)

    def start(self):
        for chunk in range(CHUNKS):
            for kind in (0, 1):
                self.send_first(chunk, kind)
            self.first(chunk, 2).start()

    def send_first(self, turn, kind):
        self.first(turn if kind == 0 else (turn + self.HALF_CHUNKS) % CHUNKS, kind).start()

    def middle(self):
        for chunk in self.ORDER:
            self.first(chunk, 0 if chunk < self.HALF_CHUNKS else 1).wait_recv()
            self.onward(chunk).start()

    def late(self):
        for chunk in range(self.HALF_CHUNKS, CHUNKS):
            self.first(chunk, 0).wait_recv()
        self.share(0).start()
        for chunk in range(self.HALF_CHUNKS):
            self.first(chunk, 1).wait_recv()
        self.share(1).start()

    def end_sib(self):
        for chunk in range(CHUNKS):
            self.first(chunk, 2).wait_recv()

    def end_near(self):
        for kind in range(2):
            self.share(kind).wait_recv()

    def end_far(self):
        for chunk in self.ORDER:
            self.onward(chunk).wait_recv()
            self.share_diag(chunk).start()
        for chunk in range(CHUNKS):
            for kind in range(3):
                self.first(chunk, kind).wait_send()
            self.onward(chunk).wait_send()
        for kind in range(2):
            self.share(kind).wait_send()
        for chunk in range(CHUNKS):
            self.share_diag(chunk).wait()

    def end(self):
        self.end_sib()
        self.end_near()
        self.end_far()


SEMS = pltpu.SemaphoreType.DMA((2, Gather.COPIES))


def masked(scores):
    key = lax.broadcasted_iota(jnp.int32, scores.shape, 0)
    query = lax.broadcasted_iota(jnp.int32, scores.shape, 1)
    return jnp.where(key <= query, scores, NEG_LARGE)


def unrotate(val, cos_t, sin_t):
    return (val * cos_t - pltpu.roll(val, HALF, 1) * sin_t).astype(BF16)


def attention_part(heads, near, gather_next, x_ref, gain_ref, pos_ref, freq_ref, dy_ref, wq_ref, wk_ref, wv_ref, wo_ref,
                   h_all, dy_all, o_all, ht_ref, dkv_ref, dq_a_ref, dq_b_ref, pos_all, pos_sems, h_sems, dy_sems, o_sems,
                   x_v, h_v, x_sems, own_sems, cos_s, sin_s, w_v, wo_v, w_sems, blk, blk_sems, ht_v, ht_sems,
                   q_s, k_s, v_s, vt, kt, ot_s, lse_s, acc, do_s, dk_acc, dv_acc, dq_v, dq_sems, dkv_v):
    rows, width = x_ref.shape
    n_blocks = k_s.shape[0]
    q_cols = heads * HEAD_DIM
    size = rows // CHUNKS
    qk_scale = HEAD_DIM ** -0.5
    to_log2 = qk_scale * LOG2E
    cols = [slice(a * HEAD_DIM, (a + 1) * HEAD_DIM) for a in range(heads)]
    part = lambda ref, chunk, count=size: ref.at[pl.ds(chunk * count, count), :]
    gather_h = Gather(near, lambda chunk: part(h_v, chunk), h_all, rows, h_sems)
    gather_dy = Gather(near, lambda chunk: part(dy_ref, chunk), dy_all, rows, dy_sems)
    gather_o = Gather(near, lambda chunk: part(ot_s, chunk, q_cols // CHUNKS), o_all, q_cols, o_sems)

    loads = [pltpu.make_async_copy(part(x_ref, chunk), part(x_v, chunk), x_sems.at[chunk]) for chunk in range(CHUNKS)]
    for load in loads:
        load.start()
    others = near.others()
    near.meet(others)
    pos_all[near.me] = jnp.broadcast_to(pos_ref[...], pos_all.shape[1:])
    positions = [send(pos_ref, pos_all.at[near.me, pl.ds(0, 1), :], pos_sems, r, peer) for r, peer in enumerate(others)]
    gain = gain_ref[...].astype(F32).reshape(1, width)
    for turn, chunk in enumerate(Gather.ORDER):
        loads[chunk].wait()

        @pl.loop(0, size // 32)
        def _(r):
            at = pl.ds(pl.multiple_of(chunk * size + r * 32, 32), 32)
            x_f = x_v[at, :].astype(F32)
            normed = x_f * lax.rsqrt(jnp.mean(x_f * x_f, axis=-1, keepdims=True) + NORM_EPS)
            h_v[at, :] = (normed * gain).astype(BF16)

        gather_h.send_first(turn // 2, turn % 2)
        gather_h.first(chunk, 2).start()
    for turn in range(Gather.HALF_CHUNKS, CHUNKS):
        for kind in (0, 1):
            gather_h.send_first(turn, kind)
    for copy in positions:
        copy.start()
    own_h = pltpu.make_async_copy(h_v, gather_h.block(near.me, 0, CHUNKS), own_sems.at[0])
    own_h.start()
    w_loads, col = [], 0
    for n, (ref, count) in enumerate(((wq_ref, q_cols), (wk_ref, HEAD_DIM), (wv_ref, HEAD_DIM))):
        at = pl.ds(pl.multiple_of(near.me * count, HEAD_DIM), count)
        w_loads.append(pltpu.make_async_copy(ref.at[:, at], w_v.at[:, pl.ds(col, count)], w_sems.at[n]))
        col += count
    w_loads.append(pltpu.make_async_copy(wo_ref.at[pl.ds(pl.multiple_of(near.me * q_cols, q_cols), q_cols), :], wo_v, w_sems.at[3]))
    stage_in = pltpu.make_async_copy(dy_ref, x_v, own_sems.at[1])
    stage_out = pltpu.make_async_copy(x_v, gather_dy.block(near.me, 0, CHUNKS), own_sems.at[2])
    for load in w_loads + [stage_in]:
        load.start()
    for copy in positions:
        copy.wait()
    sign = jnp.where(lax.broadcasted_iota(jnp.int32, (1, HEAD_DIM), 1) < HALF, -1.0, 1.0)

    @pl.loop(0, n_blocks)
    def _(b):
        pos = jnp.broadcast_to(pos_all[b, 0:1, :].astype(F32), (HEAD_DIM, rows)).T
        angles = pos * freq_ref[...]
        cos_s[b] = jnp.cos(angles)
        sin_s[b] = jnp.sin(angles) * sign

    gather_h.middle()
    for load in w_loads + [stage_in]:
        load.wait()
    stage_out.start()
    own_h.wait()

    def block_load(ref, block, slot):
        return pltpu.make_async_copy(ref.at[pl.ds(pl.multiple_of(block * rows, rows), rows), :], blk.at[slot], blk_sems.at[slot])

    far = n_blocks * 3 // 4

    def arrive(r, ref, gather, before_near=None, before_far=None):
        slot = lax.rem(r, 2)

        @pl.when(r == 1)
        def _():
            gather.end_sib()

        @pl.when(r == 2)
        def _():
            if before_near:
                before_near()
            gather.end_near()

        @pl.when(r == far)
        def _():
            if before_far:
                before_far()
            gather.end_far()

        @pl.when(functools.reduce(jnp.logical_or, [r == first for first in (0, 1, 2, far)]))
        def _():
            block_load(ref, near.across(r), slot).start()

        block_load(ref, 0, slot).wait()

        @pl.when(functools.reduce(jnp.logical_and, [r + 1 != first for first in (1, 2, far, n_blocks)]))
        def _():
            block_load(ref, near.across(r + 1), 1 - slot).start()

    def ht_store(r):
        at = pl.ds(pl.multiple_of(near.across(r) * rows, rows), rows)
        return pltpu.make_async_copy(ht_v.at[lax.rem(r, 2)], ht_ref.at[:, at], ht_sems.at[lax.rem(r, 2)])

    @pl.loop(0, n_blocks)
    def _(r):
        i = near.across(r)
        slot = lax.rem(r, 2)
        arrive(r, h_all, gather_h, gather_h.late, gather_dy.start)

        @pl.when(r >= 2)
        def _():
            ht_store(r - 2).wait()

        ht_v[slot] = blk[slot].T
        ht_store(r).start()
        prod = dot(blk[slot], w_v[...])
        cos_t, sin_t = cos_s[i], sin_s[i]
        for a in range(heads + 1):
            val = prod[:, a * HEAD_DIM:(a + 1) * HEAD_DIM]
            rot = (val * cos_t + pltpu.roll(val, HALF, 1) * sin_t).astype(BF16)
            if a < heads:
                q_s[i, :, cols[a]] = rot
            else:
                k_s[i] = rot
                kt[i] = rot.T
        v_i = prod[:, q_cols + HEAD_DIM:].astype(BF16)
        v_s[i] = v_i
        vt[i] = v_i.T

    def fwd_chunk(i, c, carry, diagonal):
        k_c, vt_c = k_s[c], vt[c]
        scores = [dot(k_c, q_s[i, :, cols[a]], COLS_COLS) * to_log2 for a in range(heads)]
        out = []
        for a in range(heads):
            s = masked(scores[a]) if diagonal else scores[a]
            m_old, l_old = carry[a]
            m_new = jnp.maximum(m_old, jnp.max(s, axis=0, keepdims=True))
            alpha = jnp.exp2(m_old - m_new)
            p = jnp.exp2(s - m_new)
            l_new = l_old * alpha + jnp.sum(p, axis=0, keepdims=True)
            acc[a] = acc[a] * alpha + dot(vt_c, p.astype(BF16))
            out.append((m_new, l_new))
        return tuple(out)

    @pl.loop(0, n_blocks)
    def _(i):
        acc[...] = jnp.zeros_like(acc)
        start = tuple((jnp.full((1, rows), NEG_LARGE, F32), jnp.zeros((1, rows), F32)) for _ in range(heads))
        carry = lax.fori_loop(0, i, lambda c, carry: fwd_chunk(i, c, carry, False), start)
        carry = fwd_chunk(i, i, carry, True)
        at = pl.ds(pl.multiple_of(i * rows, rows), rows)
        for a in range(heads):
            m_a, l_a = carry[a]
            ot_s[cols[a], at] = (acc[a] / l_a).astype(BF16)
            lse_s[i, a:a + 1, :] = m_a + jnp.log2(l_a)

        @pl.when(i == FWD_MIDDLE)
        def _():
            gather_dy.middle()

    gather_dy.late()
    gather_o.start()
    own_o = pltpu.make_async_copy(ot_s, gather_o.block(near.me, 0, CHUNKS), own_sems.at[0])
    own_o.start()

    def bwd_chunk(i, c, delta, diagonal):
        k_c, v_c, kt_c = k_s[c], v_s[c], kt[c]
        dk_c = dv_c = None
        for a in range(heads):
            q_a, do_a = q_s[i, :, cols[a]], do_s[i, :, cols[a]]
            s = dot(k_c, q_a, COLS_COLS) * to_log2
            if diagonal:
                s = masked(s)
            p = jnp.exp2(s - lse_s[i, a:a + 1, :])
            d_p = dot(v_c, do_a, COLS_COLS)
            d_s = (p * (d_p - delta[a])).astype(BF16)
            dv_a = dot(p.astype(BF16), do_a)
            dk_a = dot(d_s, q_a)
            dv_c = dv_a if dv_c is None else dv_c + dv_a
            dk_c = dk_a if dk_c is None else dk_c + dk_a
            acc[a] += dot(kt_c, d_s)
        dk_acc[c] += dk_c
        dv_acc[c] += dv_c

    def dq_stores(r):
        slot = lax.rem(r, 2)
        at = pl.ds(pl.multiple_of(near.across(r) * rows, rows), rows)
        last = q_cols - HEAD_DIM
        return [pltpu.make_async_copy(dq_v.at[slot, :, pl.ds(0, last)], dq_a_ref.at[at, :], dq_sems.at[slot, 0]),
                pltpu.make_async_copy(dq_v.at[slot, :, pl.ds(last, HEAD_DIM)], dq_b_ref.at[at, :], dq_sems.at[slot, 1])]

    def pass_on(done):
        @pl.when(done == BWD_MIDDLE)
        def _():
            gather_o.middle()

    for r in (n_blocks - 2, n_blocks - 1):
        ht_store(jnp.int32(r)).wait()
    dk_acc[...] = jnp.zeros_like(dk_acc)
    dv_acc[...] = jnp.zeros_like(dv_acc)
    stage_out.wait()

    def bwd_block(r, done):
        i = near.across(r)
        slot = lax.rem(r, 2)
        at = pl.ds(pl.multiple_of(i * rows, rows), rows)

        arrive(r, dy_all, gather_dy)
        do_s[i] = dot(blk[slot], wo_v[...], COLS_COLS).astype(BF16)
        acc[...] = jnp.zeros_like(acc)
        delta = [jnp.sum(ot_s[cols[a], at].astype(F32) * do_s[i, :, cols[a]].T.astype(F32), axis=0, keepdims=True) for a in range(heads)]

        @pl.loop(0, i)
        def _(c):
            bwd_chunk(i, c, delta, False)
            pass_on(done + c)

        bwd_chunk(i, i, delta, True)
        pass_on(done + i)

        @pl.when(r >= 2)
        def _():
            for store in dq_stores(r - 2):
                store.wait()

        for a in range(heads):
            dq_v[slot, :, cols[a]] = unrotate(acc[a].T * qk_scale, cos_s[i], sin_s[i])
        for store in dq_stores(r):
            store.start()
        return done + i + 1

    lax.fori_loop(0, n_blocks, bwd_block, jnp.int32(0))
    gather_o.late()
    for r in (n_blocks - 2, n_blocks - 1):
        for store in dq_stores(r):
            store.wait()
    gather_next.start()

    @pl.loop(0, n_blocks)
    def _(c):
        at = pl.ds(pl.multiple_of(c * rows, rows), rows)
        dkv_v[at, :HEAD_DIM] = unrotate(dk_acc[c] * qk_scale, cos_s[c], sin_s[c])
        dkv_v[at, HEAD_DIM:] = dv_acc[c].astype(BF16)

    dkv_store = pltpu.make_async_copy(dkv_v, dkv_ref, own_sems.at[1])
    dkv_store.start()
    own_o.wait()
    gather_o.end()
    dkv_store.wait()


def lanes(*parts):
    return jnp.concatenate(parts, axis=1)


def products_part(heads, near, gathers, ot_ref, ht_ref, dy_ref, d_kv_ref, d_qa_ref, d_qb_ref, x_ref, own_dy_ref, gain_ref, wo_ref, wk_ref, wv_ref, wq_ref,
                  wo_out, wq_out, kv_all, qa_all, qb_all, res_ref, gx_ref, gg_ref, gg_row, gg_all, gg_sems, x_sems,
                  a_buf, b_buf, tile, a_sem, b_sems, t_sems, stage, stage_sems, ot_v, o_v, x_v, io_sems, own, own_sems, w_v, w_sems, acc,
                  gg_v):
    core = lax.rem(near.me, 2)
    half = a_buf.shape[0]
    seq_len = d_kv_ref.shape[0]
    rows, width = x_ref.shape
    n_cols = d_kv_ref.shape[1]
    n_o, n_all = width // (2 * n_cols), x_sems.shape[1]
    n_oa = n_o + (n_all - n_o) * 2 // 3

    local = (d_qa_ref, d_qb_ref, d_kv_ref)

    def stage_in(n):
        return pltpu.make_async_copy(local[n], stage.at[:, pl.ds(0, local[n].shape[1])], stage_sems.at[0])

    def stage_out(n):
        return pltpu.make_async_copy(stage.at[:, pl.ds(0, local[n].shape[1])], gathers[n].block(near.me, 0, CHUNKS), stage_sems.at[1])

    def copy_own(n):
        stage_in(n).wait()
        stage_out(n).start()

    own_rows = pl.ds(pl.multiple_of(core * half, half), half)
    tokens = pl.ds(pl.multiple_of(near.me * rows, rows), rows)
    ot_load = pltpu.make_async_copy(ot_ref.at[:, tokens], ot_v, io_sems.at[0])
    x_load = pltpu.make_async_copy(x_ref, x_v, io_sems.at[1])
    res_store = pltpu.make_async_copy(x_v, res_ref, io_sems.at[2])
    dy_load = pltpu.make_async_copy(own_dy_ref, o_v, io_sems.at[3])
    gx_store = pltpu.make_async_copy(o_v, gx_ref, io_sems.at[0])

    def a_load(ref):
        return pltpu.make_async_copy(ref.at[own_rows, :], a_buf, a_sem)

    def b_loads(source, p, slot, g):
        if source is dy_ref:
            srcs = [dy_ref.at[:, pl.ds(pl.multiple_of((2 * p + g) * n_cols, n_cols), n_cols)]]
        else:
            per = n_cols // source.shape[1]
            srcs = [source.at[pl.ds(pl.multiple_of(((2 * p + g) * per + n) * seq_len, seq_len), seq_len), :] for n in range(per)]
        return [pltpu.make_async_copy(src, b_buf.at[slot, :, pl.ds(g * n_cols + n * src.shape[1], src.shape[1])], b_sems.at[slot, g])
                for n, src in enumerate(srcs)]

    def start_b(step):
        slot = lax.rem(step, 2)
        for source, low, high in ((dy_ref, 0, n_o), (qa_all, n_o, n_oa), (qb_all, n_oa, n_all)):
            @pl.when(jnp.logical_and(step >= low, step < high))
            def _():
                for g in range(2):
                    for load in b_loads(source, step - low, slot, g):
                        load.start()

    def pieces(kind, step):
        wide = (2 * n_cols, n_cols, HEAD_DIM)[kind]
        slot = lax.rem(step, 2)
        out = []
        for n in range(2 * n_cols // wide):
            group = (step - (0, n_o, n_oa)[kind]) * (2 * n_cols // wide) + n
            col = (group * wide, group * heads * HEAD_DIM, (group + 1) * heads * HEAD_DIM - HEAD_DIM)[kind]
            dst = (wo_out, wq_out, wq_out)[kind].at[own_rows, pl.ds(pl.multiple_of(col, HEAD_DIM), wide)]
            src = tile.at[slot, :, pl.ds(n * wide, wide)]
            out.append((pltpu.make_async_copy(src, dst, t_sems.at[slot]), send(src, dst, x_sems, step, near.sib)))
        return out

    def start_tile(step):
        for kind, (low, high) in enumerate(((0, n_o), (n_o, n_oa), (n_oa, n_all))):
            @pl.when(jnp.logical_and(step >= low, step < high))
            def _():
                for keep, give in pieces(kind, step):
                    keep.start()
                    give.start()

    def whole_tile(step):
        slot = lax.rem(step, 2)
        dst = wo_out.at[own_rows, pl.ds(0, 2 * n_cols)]
        return pltpu.make_async_copy(tile.at[slot], dst, t_sems.at[slot]), send(tile.at[slot], dst, x_sems, step, near.sib)

    def wait_tile(step):
        keep, give = whole_tile(step)
        keep.wait()
        give.wait_send()

    def result_part():
        cols = b_buf.shape[2]

        def w_load(n):
            slot = lax.rem(n, 2)
            return pltpu.make_async_copy(wo_ref.at[:, pl.ds(pl.multiple_of(n * cols, cols), cols)], b_buf.at[slot, pl.ds(0, wo_ref.shape[0]), :],
                                         b_sems.at[slot, 0])

        w_load(jnp.int32(0)).start()
        ot_load.wait()

        @pl.loop(0, ot_v.shape[0] // BLK)
        def _(r):
            at = pl.ds(pl.multiple_of(r * BLK, BLK), BLK)
            o_v[:, at] = ot_v[at, :].T

        x_load.wait()

        @pl.loop(0, n_o)
        def _(n):
            w_load(n).wait()

            @pl.when(n + 1 < n_o)
            def _():
                w_load(n + 1).start()

            at = pl.ds(pl.multiple_of(n * cols, cols), cols)
            x_v[:, at] = (x_v[:, at].astype(F32) + dot(o_v[...], b_buf[lax.rem(n, 2), :wo_ref.shape[0], :])).astype(BF16)

        res_store.start()

    def hidden_parts(kind):
        count = own.shape[0] // (2 if kind == 1 else 1)

        def own_load(r, g):
            source = (qa_all, qb_all, kv_all)[kind]
            device, col = (2 * r + g, 0) if kind == 1 else (near.across(r), g * HEAD_DIM)
            at = pl.ds(pl.multiple_of(device * seq_len + near.me * rows, rows), rows)
            return pltpu.make_async_copy(source.at[at, pl.ds(col, HEAD_DIM)], own.at[r, :, pl.ds(g * HEAD_DIM, HEAD_DIM)], own_sems.at[r, g])

        def w_load(r, g):
            source = (wk_ref, wv_ref)[g] if kind == 2 else wq_ref
            col = near.across(r) if kind == 2 else heads * near.across(r) + g if kind == 0 else heads * (2 * r + g + 1) - 1
            slot = lax.rem(r, 2)
            return pltpu.make_async_copy(source.at[:, pl.ds(pl.multiple_of(col * HEAD_DIM, HEAD_DIM), HEAD_DIM)],
                                         w_v.at[slot, :, pl.ds(g * HEAD_DIM, HEAD_DIM)], w_sems.at[slot, g])

        return count, own_load, w_load

    def hidden_start(kind, low=0, high=None):
        count, own_load, w_load = hidden_parts(kind)
        for g in range(2):
            if low == 0:
                w_load(jnp.int32(0), g).start()

            @pl.loop(low, high or count)
            def _(r):
                own_load(r, g).start()

    def hidden_add(kind, low=0, high=None):
        count, own_load, w_load = hidden_parts(kind)

        @pl.loop(low, high or count)
        def _(r):
            for g in range(2):
                w_load(r, g).wait()
                own_load(r, g).wait()

            @pl.when(r + 1 < count)
            def _():
                for g in range(2):
                    w_load(r + 1, g).start()

            for col in range(0, width, width // PARTS):
                at = slice(col, col + width // PARTS)
                acc[:, at] += dot(own[r], w_v[lax.rem(r, 2), at, :], COLS_COLS)

    a_load(ot_ref).start()
    start_b(jnp.int32(0))
    stage_in(0).start()
    ot_load.start()
    x_load.start()
    a_load(ot_ref).wait()

    @pl.loop(0, n_all)
    def _(step):
        slot = lax.rem(step, 2)
        for g in range(2):
            b_loads(dy_ref, 0, slot, g)[0].wait()

        @pl.when(jnp.logical_and(step != n_o - 1, step != n_oa - 1))
        def _():
            start_b(step + 1)

        @pl.when(step >= 2)
        def _():
            wait_tile(step - 2)

        @pl.when(step == n_o)
        def _():
            a_load(ht_ref).wait()

        for r in range(0, half, half // PARTS):
            tile[slot, r:r + half // PARTS, :] = dot(a_buf[r:r + half // PARTS, :], b_buf[slot])
        start_tile(step)

        @pl.when(step == n_o - 4)
        def _():
            acc[...] = jnp.zeros_like(acc)
            copy_own(0)
            gathers[0].middle()

        @pl.when(step == n_o - 1)
        def _():
            a_load(ht_ref).start()
            gathers[0].late()
            gathers[1].start()
            stage_out(0).wait()
            stage_in(1).start()
            result_part()
            gathers[0].end()
            start_b(step + 1)
            hidden_start(0)

        @pl.when(step == n_oa - 4)
        def _():
            copy_own(1)
            gathers[1].middle()

        @pl.when(step == n_oa - 2)
        def _():
            gathers[1].late()
            gathers[2].start()
            stage_out(1).wait()
            stage_in(2).start()

        @pl.when(step == n_oa - 1)
        def _():
            res_store.wait()
            x_load.start()
            dy_load.start()
            gathers[1].end()
            start_b(step + 1)

    hidden_add(0)
    copy_own(2)
    gathers[2].middle()
    hidden_start(1)
    hidden_add(1)
    gathers[2].late()
    stage_out(2).wait()
    gathers[2].end_sib()
    gathers[2].end_near()
    near_count = own.shape[0] * 3 // 4
    hidden_start(2, 0, near_count)
    for step in (n_all - 2, n_all - 1):
        wait_tile(jnp.int32(step))
    hidden_add(2, 0, near_count)
    gathers[2].end_far()
    hidden_start(2, near_count)
    hidden_add(2, near_count)

    gain = gain_ref[...].astype(F32).reshape(1, width)
    gg_v[...] = jnp.zeros_like(gg_v)
    x_load.wait()
    dy_load.wait()

    def normed_rows(r):
        at = pl.ds(pl.multiple_of(r * 32, 32), 32)
        x_f = x_v[at, :].astype(F32)
        inv_rms = lax.rsqrt(jnp.mean(x_f * x_f, axis=-1, keepdims=True) + NORM_EPS)
        return at, inv_rms, x_f * inv_rms

    @pl.loop(0, rows // 32)
    def _(r):
        at, _, normed = normed_rows(r)
        gg_v[...] += jnp.sum((acc[at, :] * normed).reshape(4, 8, width), axis=0)

    gg_row[...] = jnp.sum(gg_v[...], axis=0, keepdims=True)
    gg_all[near.me] = gg_row[...]
    parts = [send(gg_row, gg_all.at[near.me], gg_sems, r, peer) for r, peer in enumerate(near.others())]
    for copy in parts:
        copy.start()

    @pl.loop(0, rows // 32)
    def _(r):
        at, inv_rms, normed = normed_rows(r)
        d_normed = acc[at, :] * gain
        mean = jnp.mean(d_normed * normed, axis=-1, keepdims=True)
        o_v[at, :] = (o_v[at, :].astype(F32) + inv_rms * (d_normed - normed * mean)).astype(BF16)

    gx_store.start()

    @pl.loop(0, n_all)
    def _(step):
        whole_tile(step)[1].wait_recv()

    for copy in parts:
        copy.wait()
    gg_ref[...] = jnp.sum(gg_all[...], axis=0)
    gx_store.wait()


def step_kernel(heads, first_scratch, second_scratch, x_ref, gain_ref, pos_ref, freq_ref, dy_ref, wq_ref, wk_ref, wv_ref, wo_ref,
                h_all, dy_all, o_all, ht, d_kv, d_qa, d_qb, wo_out, wq_out, kv_all, qa_all, qb_all, res, gx, gg,
                pos_all, pos_sems, gg_row, gg_all, gg_sems, x_sems, h_sems, dy_sems, o_sems, kv_sems, qa_sems, qb_sems):
    near = Neighbours()
    seq_len = d_kv.shape[0]

    def gather_of(src, dst, sems):
        return Gather(near, lambda c: src.at[pl.ds(c * (seq_len // CHUNKS), seq_len // CHUNKS), :], dst, seq_len, sems)

    gathers = [gather_of(d_qa, qa_all, qa_sems), gather_of(d_qb, qb_all, qb_sems), gather_of(d_kv, kv_all, kv_sems)]

    def first(*scratch):
        attention_part(heads, near, gathers[0], x_ref, gain_ref, pos_ref, freq_ref, dy_ref, wq_ref, wk_ref, wv_ref, wo_ref,
                       h_all, dy_all, o_all, ht, d_kv, d_qa, d_qb, pos_all, pos_sems, h_sems, dy_sems, o_sems, *scratch)

    def second(*scratch):
        products_part(heads, near, gathers, o_all, ht, dy_all, d_kv, d_qa, d_qb, x_ref, dy_ref, gain_ref, wo_ref, wk_ref, wv_ref, wq_ref,
                      wo_out, wq_out, kv_all, qa_all, qb_all, res, gx, gg, gg_row, gg_all, gg_sems, x_sems, *scratch)

    pl.run_scoped(first, *first_scratch)
    pl.run_scoped(second, *second_scratch)


def step(x, gain, positions, grad_out, w_q, w_k, w_v, w_o, sp_size, heads):
    rows, width = x.shape
    seq_len = rows * sp_size
    q_cols = heads * HEAD_DIM
    all_cols = q_cols * sp_size
    half = width // 2
    cols = 4 * HEAD_DIM
    n_all = (width + all_cols) // cols
    any_spec = pl.BlockSpec(memory_space=pl.ANY)
    vmem = pl.BlockSpec(memory_space=pltpu.VMEM)
    dma = pltpu.SemaphoreType.DMA
    inv_freq = ROPE_THETA ** (-np.arange(0, HEAD_DIM, 2) / HEAD_DIM)
    freq = jnp.asarray(np.concatenate([inv_freq, inv_freq])[None, :], F32)
    pairs = heads * seq_len * (seq_len + rows) // 2
    out = lambda *shape, dtype=BF16: jax.ShapeDtypeStruct(shape, dtype)
    array = lambda *shape, dtype=BF16: pltpu.VMEM(shape, dtype)
    blocks = lambda *shape, dtype=BF16: pltpu.VMEM((sp_size,) + shape, dtype)
    first_scratch = [array(rows, width), array(rows, width), dma((CHUNKS,)), dma((3,)), blocks(rows, HEAD_DIM, dtype=F32),
                     blocks(rows, HEAD_DIM, dtype=F32), array(width, q_cols + 2 * HEAD_DIM), array(q_cols, width), dma((4,)),
                     array(2, rows, width), dma((2,)), array(2, width, rows), dma((2,)),
                     blocks(rows, q_cols), blocks(rows, HEAD_DIM), blocks(rows, HEAD_DIM), blocks(HEAD_DIM, rows), blocks(HEAD_DIM, rows),
                     array(q_cols, seq_len), blocks(8, rows, dtype=F32), array(heads, HEAD_DIM, rows, dtype=F32),
                     blocks(rows, q_cols), blocks(rows, HEAD_DIM, dtype=F32), blocks(rows, HEAD_DIM, dtype=F32),
                     array(2, rows, q_cols), dma((2, 2)), array(seq_len, 2 * HEAD_DIM)]
    second_scratch = [array(half, seq_len), array(2, seq_len, cols), array(2, half, cols, dtype=F32), dma, dma((2, 2)), dma((2,)),
                      array(seq_len, 2 * HEAD_DIM), dma((2,)), array(all_cols, rows), array(rows, all_cols), array(rows, width),
                      dma((4,)), blocks(rows, 2 * HEAD_DIM), dma((sp_size, 2)), array(2, width, 2 * HEAD_DIM), dma((2, 2)),
                      array(rows, width, dtype=F32), array(8, width, dtype=F32)]
    return pl.pallas_call(
        functools.partial(step_kernel, heads, first_scratch, second_scratch),
        in_specs=[any_spec, vmem, vmem, vmem] + [any_spec] * 5,
        out_specs=[any_spec] * 14 + [vmem],
        out_shape=[out(seq_len, width), out(seq_len, width), out(all_cols, seq_len), out(width, seq_len), out(seq_len, 2 * HEAD_DIM),
                   out(seq_len, q_cols - HEAD_DIM), out(seq_len, HEAD_DIM), out(all_cols, width, dtype=F32), out(width, all_cols, dtype=F32),
                   out(sp_size * seq_len, 2 * HEAD_DIM), out(sp_size * seq_len, q_cols - HEAD_DIM), out(sp_size * seq_len, HEAD_DIM),
                   out(rows, width), out(rows, width), out(1, width, dtype=F32)],
        scratch_shapes=[blocks(8, rows, dtype=jnp.int32), dma((2, 7)), array(1, width, dtype=F32), blocks(1, width, dtype=F32), dma((2, 7)),
                        dma((2, n_all))] + [SEMS] * 6,
        compiler_params=pltpu.CompilerParams(vmem_limit_bytes=VMEM_LIMIT, collective_id=0, has_side_effects=True),
        cost_estimate=pl.CostEstimate(flops=28 * pairs * HEAD_DIM + 2 * half * cols * seq_len * n_all, bytes_accessed=20 * seq_len * width,
                                      transcendentals=2 * pairs),
        name="step",
    )(x, gain, positions.reshape(1, -1), freq, grad_out, w_q, w_k, w_v, w_o)


def finish_kernel(ht_ref, d_ref, gx_in, res_in, gg_in, wo_in, wq_in, wk_ref, wv_ref, wq_ref, wo_ref, gx_ref, res_ref, gg_ref, d_v, d_sems, ring, ring_sems):
    step = pl.program_id(0) * pl.num_programs(1) + pl.program_id(1)
    high = ring.shape[2]
    per_array = wo_in.shape[0] // (high * RING)

    def copy_in(src, g, n):
        at = pl.ds(pl.multiple_of((lax.rem(g, per_array) * RING + n) * high, high), high)
        return pltpu.make_async_copy(src.at[at, :], ring.at[lax.rem(g, DEPTH), n], ring_sems.at[0, lax.rem(g, DEPTH), n])

    def copy_out(dst, g, n):
        at = pl.ds(pl.multiple_of((lax.rem(g, per_array) * RING + n) * high, high), high)
        return pltpu.make_async_copy(ring.at[lax.rem(g, DEPTH), n], dst.at[at, :], ring_sems.at[1, lax.rem(g, DEPTH), n])

    def start(copy, first, second, g):
        for ref, mine in ((first, g < per_array), (second, g >= per_array)):
            @pl.when(mine)
            def _():
                for n in range(RING):
                    copy(ref, g, n).start()

    def pair_load(p):
        at = pl.ds(2 * p, 2)
        return pltpu.make_async_copy(d_ref.at[at], d_v.at[at], d_sems.at[p])

    @pl.when(step == 0)
    def _():
        for p in range(d_v.shape[0] // 2):
            pair_load(p).start()

    last = pl.num_programs(0) * pl.num_programs(1) - 1

    def free(g):
        for n in range(RING):
            copy_out(wo_ref, g, n).wait()

    def pass_on(g):
        for n in range(RING):
            copy_in(wo_in, g, n).wait()
        start(copy_out, wo_ref, wq_ref, g)

    @pl.when(step == 0)
    def _():
        start(copy_in, wo_in, wq_in, step)

    @pl.when(step >= DEPTH - 1)
    def _():
        free(step + 1 - DEPTH)

    @pl.when(step < last)
    def _():
        start(copy_in, wo_in, wq_in, step + 1)

    @pl.when(step >= 1)
    def _():
        pass_on(step - 1)

    for p in range(d_v.shape[0] // 2):
        @pl.when(step == p)
        def _():
            pair_load(p).wait()

    ht = ht_ref[...]
    pair = 2 * pl.program_id(1)
    wk_ref[...] = dot(ht, lanes(d_v[pair, :, :HEAD_DIM], d_v[pair + 1, :, :HEAD_DIM]))
    wv_ref[...] = dot(ht, lanes(d_v[pair, :, HEAD_DIM:], d_v[pair + 1, :, HEAD_DIM:]))

    @pl.when(step == 0)
    def _():
        gg_ref[...] = gg_in[...]

    @pl.when(step == last)
    def _():
        pass_on(last)
        for back in range(DEPTH - 1):
            free(last - back)

    @pl.when(step < ROW_STEPS)
    def _():
        gx_ref[...] = gx_in[...]
        res_ref[...] = res_in[...]


def finish(ht, d_kv, w_o_grad, w_q_grad, grad_x, result, grad_gain):
    width, seq_len = ht.shape
    groups = d_kv.shape[0]
    n_j = groups // 2
    steps = (width // MROWS) * n_j
    high = width // COPY_ROWS
    assert w_o_grad.shape[0] + w_q_grad.shape[0] == high * RING * steps
    any_spec = pl.BlockSpec(memory_space=pl.ANY)
    rows = pl.BlockSpec((grad_x.shape[0] // ROW_STEPS, width), lambda m, j: (jnp.minimum(m * n_j + j, ROW_STEPS - 1), 0))
    whole = pl.BlockSpec((1, width), lambda m, j: (0, 0))
    kv_out = pl.BlockSpec((MROWS, 2 * HEAD_DIM), lambda m, j: (m, j))
    out = lambda cols: jax.ShapeDtypeStruct((width, cols), F32)
    like = lambda val: jax.ShapeDtypeStruct(val.shape, val.dtype)
    return pl.pallas_call(
        finish_kernel,
        grid=(width // MROWS, n_j),
        in_specs=[pl.BlockSpec((MROWS, seq_len), lambda m, j: (m, 0)), any_spec, rows, rows, whole, any_spec, any_spec],
        out_specs=[kv_out, kv_out, any_spec, any_spec, rows, rows, whole],
        out_shape=[out(groups * HEAD_DIM), out(groups * HEAD_DIM), like(w_q_grad), like(w_o_grad), like(grad_x), like(result), like(grad_gain)],
        scratch_shapes=[pltpu.VMEM(d_kv.shape, BF16), pltpu.SemaphoreType.DMA((groups // 2,)),
                        pltpu.VMEM((DEPTH, RING, high, width), F32), pltpu.SemaphoreType.DMA((2, DEPTH, RING))],
        compiler_params=params(2),
        cost_estimate=pl.CostEstimate(flops=4 * width * seq_len * groups * HEAD_DIM, bytes_accessed=2 * width * seq_len, transcendentals=0),
        name="finish",
    )(ht, d_kv, grad_x, result, grad_gain, w_o_grad, w_q_grad)


def solution(mesh):
    sp_size = mesh.shape['sp']
    seq_spec = P(('dp', 'sp'), None)
    pos_spec = P(('dp', 'sp'))
    replicated = P(None, None)
    part_rows = P('dp', None)

    def local_step(x, grad_out, positions, gain, w_q, w_k, w_v, w_o):
        n_heads = w_q.shape[1] // HEAD_DIM
        heads = n_heads // sp_size
        _, _, _, ht, _, _, _, w_o_grad, w_q_grad, kv_all, _, _, result, grad_x, grad_gain = step(
            x, gain, positions, grad_out, w_q, w_k, w_v, w_o, sp_size, heads)
        grad_wk, grad_wv, grad_wq, grad_wo, grad_x, result, grad_gain = finish(
            ht, kv_all.reshape(sp_size, -1, 2 * HEAD_DIM), w_o_grad, w_q_grad, grad_x, result, grad_gain)
        return result, grad_x, grad_wq, grad_wk, grad_wv, grad_wo, grad_gain.reshape(-1)

    return jax.shard_map(local_step, mesh=mesh,
                         in_specs=(seq_spec, seq_spec, pos_spec, P(None), replicated, replicated, replicated, replicated),
                         out_specs=(seq_spec, seq_spec, part_rows, part_rows, part_rows, part_rows, P('dp')),
                         check_vma=False)
```

```python
import functools

import jax
import jax.numpy as jnp
import numpy as np
from jax import lax
from jax.experimental import pallas as pl
from jax.experimental.pallas import tpu as pltpu
from jax.sharding import PartitionSpec as P

HEAD_DIM = 128
HALF = HEAD_DIM // 2
ROPE_THETA = 1000000.0
NORM_EPS = 1e-05
NEG_LARGE = -1e30
LOG2E = 1.4426950408889634
BLK = 512
CHUNKS = 4
FWD_MIDDLE, BWD_MIDDLE = 5, 27
MROWS = 768
RING = 3
DEPTH = 5
COPY_ROWS = 24
PARTS = 3
ROW_STEPS = 16
F32 = jnp.float32
BF16 = jnp.bfloat16
ROWS_ROWS = (((0,), (0,)), ((), ()))
COLS_COLS = (((1,), (1,)), ((), ()))
ROWS_COLS = (((0,), (1,)), ((), ()))
VMEM_LIMIT = 63 * 1024 * 1024


def dot(a, b, dims=(((1,), (0,)), ((), ()))):
    return lax.dot_general(a, b, dims, preferred_element_type=F32)


def params(axes=1):
    return pltpu.CompilerParams(dimension_semantics=("arbitrary",) * axes, vmem_limit_bytes=VMEM_LIMIT)


class Neighbours:
    def __init__(self):
        self.me = lax.axis_index('sp')
        core, col, row = lax.rem(self.me, 2), lax.rem(self.me // 2, 2), self.me // 4
        self.sib = self.me + 1 - 2 * core
        self.xn = self.me + 2 - 4 * col
        self.yn = self.me + 4 - 8 * row
        self.diag = self.xn + self.yn - self.me

    def meet(self, peers):
        barrier = pltpu.get_barrier_semaphore()
        for peer in peers:
            pl.semaphore_signal(barrier, inc=1, device_id={'sp': peer}, device_id_type=pl.DeviceIdType.MESH)
        pl.semaphore_wait(barrier, len(peers))

    def across(self, r):
        core, col, row = lax.rem(self.me, 2), lax.rem(self.me // 2, 2), self.me // 4
        return (self.me + lax.rem(r, 2) * (1 - 2 * core) + lax.rem(r // 2, 2) * (2 - 4 * col) + (r // 4) * (4 - 8 * row))

    def others(self):
        flip = lambda dev: dev + 1 - 2 * lax.rem(dev, 2)
        return [self.sib, self.xn, flip(self.xn), self.yn, flip(self.yn), self.diag, flip(self.diag)]


def send(src, dst, sems, index, peer):
    return pltpu.make_async_remote_copy(src_ref=src, dst_ref=dst, send_sem=sems.at[0, index], recv_sem=sems.at[1, index],
                                        device_id={'sp': peer}, device_id_type=pl.DeviceIdType.MESH)


class Gather:
    COPIES = 5 * CHUNKS + 2
    HALF_CHUNKS = CHUNKS // 2
    ORDER = [chunk + half * (CHUNKS // 2) for chunk in range(CHUNKS // 2) for half in range(2)]

    def __init__(self, near, own, dst, rows, sems):
        self.near, self.own, self.dst, self.rows, self.sems = near, own, dst, rows, sems

    def block(self, dev, chunk, count=1):
        size = self.rows // CHUNKS
        return self.dst.at[pl.ds(pl.multiple_of(dev * self.rows + chunk * size, size), count * size), :]

    def first(self, chunk, kind):
        peer = (self.near.xn, self.near.yn, self.near.sib)[kind]
        return send(self.own(chunk), self.block(self.near.me, chunk), self.sems, kind * CHUNKS + chunk, peer)

    def onward(self, chunk):
        over_y = chunk < self.HALF_CHUNKS
        rows = self.block(self.near.xn if over_y else self.near.yn, chunk)
        return send(rows, rows, self.sems, 3 * CHUNKS + chunk, self.near.yn if over_y else self.near.xn)

    def share(self, kind):
        rows = self.block((self.near.xn, self.near.yn)[kind], 0, CHUNKS)
        return send(rows, rows, self.sems, 4 * CHUNKS + kind, self.near.sib)

    def share_diag(self, chunk):
        rows = self.block(self.near.diag, chunk)
        return send(rows, rows, self.sems, 4 * CHUNKS + 2 + chunk, self.near.sib)

    def start(self):
        for chunk in range(CHUNKS):
            for kind in (0, 1):
                self.send_first(chunk, kind)
            self.first(chunk, 2).start()

    def send_first(self, turn, kind):
        self.first(turn if kind == 0 else (turn + self.HALF_CHUNKS) % CHUNKS, kind).start()

    def middle(self):
        for chunk in self.ORDER:
            self.first(chunk, 0 if chunk < self.HALF_CHUNKS else 1).wait_recv()
            self.onward(chunk).start()

    def late(self):
        for chunk in range(self.HALF_CHUNKS, CHUNKS):
            self.first(chunk, 0).wait_recv()
        self.share(0).start()
        for chunk in range(self.HALF_CHUNKS):
            self.first(chunk, 1).wait_recv()
        self.share(1).start()

    def end_sib(self):
        for chunk in range(CHUNKS):
            self.first(chunk, 2).wait_recv()

    def end_near(self):
        for kind in range(2):
            self.share(kind).wait_recv()

    def end_far(self):
        for chunk in self.ORDER:
            self.onward(chunk).wait_recv()
            self.share_diag(chunk).start()
        for chunk in range(CHUNKS):
            for kind in range(3):
                self.first(chunk, kind).wait_send()
            self.onward(chunk).wait_send()
        for kind in range(2):
            self.share(kind).wait_send()
        for chunk in range(CHUNKS):
            self.share_diag(chunk).wait()

    def end(self):
        self.end_sib()
        self.end_near()
        self.end_far()


SEMS = pltpu.SemaphoreType.DMA((2, Gather.COPIES))


def masked(scores):
    key = lax.broadcasted_iota(jnp.int32, scores.shape, 0)
    query = lax.broadcasted_iota(jnp.int32, scores.shape, 1)
    return jnp.where(key <= query, scores, NEG_LARGE)


def unrotate(val, cos_t, sin_t):
    return (val * cos_t - pltpu.roll(val, HALF, 1) * sin_t).astype(BF16)


def attention_part(heads, near, gather_next, x_ref, gain_ref, pos_ref, freq_ref, dy_ref, wq_ref, wk_ref, wv_ref, wo_ref,
                   h_all, dy_all, o_all, ht_ref, dkv_ref, dq_a_ref, dq_b_ref, pos_all, pos_sems, h_sems, dy_sems, o_sems,
                   x_v, h_v, x_sems, own_sems, cos_s, sin_s, w_v, wo_v, w_sems, blk, blk_sems, ht_v, ht_sems,
                   q_s, k_s, v_s, vt, kt, ot_s, lse_s, acc, do_s, dk_acc, dv_acc, dq_v, dq_sems, dkv_v):
    rows, width = x_ref.shape
    n_blocks = k_s.shape[0]
    q_cols = heads * HEAD_DIM
    size = rows // CHUNKS
    qk_scale = HEAD_DIM ** -0.5
    to_log2 = qk_scale * LOG2E
    cols = [slice(a * HEAD_DIM, (a + 1) * HEAD_DIM) for a in range(heads)]
    part = lambda ref, chunk, count=size: ref.at[pl.ds(chunk * count, count), :]
    gather_h = Gather(near, lambda chunk: part(h_v, chunk), h_all, rows, h_sems)
    gather_dy = Gather(near, lambda chunk: part(dy_ref, chunk), dy_all, rows, dy_sems)
    gather_o = Gather(near, lambda chunk: part(ot_s, chunk, q_cols // CHUNKS), o_all, q_cols, o_sems)

    loads = [pltpu.make_async_copy(part(x_ref, chunk), part(x_v, chunk), x_sems.at[chunk]) for chunk in range(CHUNKS)]
    for load in loads:
        load.start()
    others = near.others()
    near.meet(others)
    pos_all[near.me] = jnp.broadcast_to(pos_ref[...], pos_all.shape[1:])
    positions = [send(pos_ref, pos_all.at[near.me, pl.ds(0, 1), :], pos_sems, r, peer) for r, peer in enumerate(others)]
    gain = gain_ref[...].astype(F32).reshape(1, width)
    for turn, chunk in enumerate(Gather.ORDER):
        loads[chunk].wait()

        @pl.loop(0, size // 32)
        def _(r):
            at = pl.ds(pl.multiple_of(chunk * size + r * 32, 32), 32)
            x_f = x_v[at, :].astype(F32)
            normed = x_f * lax.rsqrt(jnp.mean(x_f * x_f, axis=-1, keepdims=True) + NORM_EPS)
            h_v[at, :] = (normed * gain).astype(BF16)

        gather_h.send_first(turn // 2, turn % 2)
        gather_h.first(chunk, 2).start()
    for turn in range(Gather.HALF_CHUNKS, CHUNKS):
        for kind in (0, 1):
            gather_h.send_first(turn, kind)
    for copy in positions:
        copy.start()
    own_h = pltpu.make_async_copy(h_v, gather_h.block(near.me, 0, CHUNKS), own_sems.at[0])
    own_h.start()
    w_loads, col = [], 0
    for n, (ref, count) in enumerate(((wq_ref, q_cols), (wk_ref, HEAD_DIM), (wv_ref, HEAD_DIM))):
        at = pl.ds(pl.multiple_of(near.me * count, HEAD_DIM), count)
        w_loads.append(pltpu.make_async_copy(ref.at[:, at], w_v.at[:, pl.ds(col, count)], w_sems.at[n]))
        col += count
    w_loads.append(pltpu.make_async_copy(wo_ref.at[pl.ds(pl.multiple_of(near.me * q_cols, q_cols), q_cols), :], wo_v, w_sems.at[3]))
    stage_in = pltpu.make_async_copy(dy_ref, x_v, own_sems.at[1])
    stage_out = pltpu.make_async_copy(x_v, gather_dy.block(near.me, 0, CHUNKS), own_sems.at[2])
    for load in w_loads + [stage_in]:
        load.start()
    for copy in positions:
        copy.wait()
    sign = jnp.where(lax.broadcasted_iota(jnp.int32, (1, HEAD_DIM), 1) < HALF, -1.0, 1.0)

    @pl.loop(0, n_blocks)
    def _(b):
        pos = jnp.broadcast_to(pos_all[b, 0:1, :].astype(F32), (HEAD_DIM, rows)).T
        angles = pos * freq_ref[...]
        cos_s[b] = jnp.cos(angles)
        sin_s[b] = jnp.sin(angles) * sign

    gather_h.middle()
    for load in w_loads + [stage_in]:
        load.wait()
    stage_out.start()
    own_h.wait()

    def block_load(ref, block, slot):
        return pltpu.make_async_copy(ref.at[pl.ds(pl.multiple_of(block * rows, rows), rows), :], blk.at[slot], blk_sems.at[slot])

    far = n_blocks * 3 // 4

    def arrive(r, ref, gather, before_near=None, before_far=None):
        slot = lax.rem(r, 2)

        @pl.when(r == 1)
        def _():
            gather.end_sib()

        @pl.when(r == 2)
        def _():
            if before_near:
                before_near()
            gather.end_near()

        @pl.when(r == far)
        def _():
            if before_far:
                before_far()
            gather.end_far()

        @pl.when(functools.reduce(jnp.logical_or, [r == first for first in (0, 1, 2, far)]))
        def _():
            block_load(ref, near.across(r), slot).start()

        block_load(ref, 0, slot).wait()

        @pl.when(functools.reduce(jnp.logical_and, [r + 1 != first for first in (1, 2, far, n_blocks)]))
        def _():
            block_load(ref, near.across(r + 1), 1 - slot).start()

    def ht_store(r):
        at = pl.ds(pl.multiple_of(near.across(r) * rows, rows), rows)
        return pltpu.make_async_copy(ht_v.at[lax.rem(r, 2)], ht_ref.at[:, at], ht_sems.at[lax.rem(r, 2)])

    @pl.loop(0, n_blocks)
    def _(r):
        i = near.across(r)
        slot = lax.rem(r, 2)
        arrive(r, h_all, gather_h, gather_h.late, gather_dy.start)

        @pl.when(r >= 2)
        def _():
            ht_store(r - 2).wait()

        ht_v[slot] = blk[slot].T
        ht_store(r).start()
        prod = dot(blk[slot], w_v[...])
        cos_t, sin_t = cos_s[i], sin_s[i]
        for a in range(heads + 1):
            val = prod[:, a * HEAD_DIM:(a + 1) * HEAD_DIM]
            rot = (val * cos_t + pltpu.roll(val, HALF, 1) * sin_t).astype(BF16)
            if a < heads:
                q_s[i, :, cols[a]] = rot
            else:
                k_s[i] = rot
                kt[i] = rot.T
        v_i = prod[:, q_cols + HEAD_DIM:].astype(BF16)
        v_s[i] = v_i
        vt[i] = v_i.T

    def fwd_chunk(i, c, carry, diagonal):
        k_c, vt_c = k_s[c], vt[c]
        scores = [dot(k_c, q_s[i, :, cols[a]], COLS_COLS) * to_log2 for a in range(heads)]
        out = []
        for a in range(heads):
            s = masked(scores[a]) if diagonal else scores[a]
            m_old, l_old = carry[a]
            m_new = jnp.maximum(m_old, jnp.max(s, axis=0, keepdims=True))
            alpha = jnp.exp2(m_old - m_new)
            p = jnp.exp2(s - m_new)
            l_new = l_old * alpha + jnp.sum(p, axis=0, keepdims=True)
            acc[a] = acc[a] * alpha + dot(vt_c, p.astype(BF16))
            out.append((m_new, l_new))
        return tuple(out)

    @pl.loop(0, n_blocks)
    def _(i):
        acc[...] = jnp.zeros_like(acc)
        start = tuple((jnp.full((1, rows), NEG_LARGE, F32), jnp.zeros((1, rows), F32)) for _ in range(heads))
        carry = lax.fori_loop(0, i, lambda c, carry: fwd_chunk(i, c, carry, False), start)
        carry = fwd_chunk(i, i, carry, True)
        at = pl.ds(pl.multiple_of(i * rows, rows), rows)
        for a in range(heads):
            m_a, l_a = carry[a]
            ot_s[cols[a], at] = (acc[a] / l_a).astype(BF16)
            lse_s[i, a:a + 1, :] = m_a + jnp.log2(l_a)

        @pl.when(i == FWD_MIDDLE)
        def _():
            gather_dy.middle()

    gather_dy.late()
    gather_o.start()
    own_o = pltpu.make_async_copy(ot_s, gather_o.block(near.me, 0, CHUNKS), own_sems.at[0])
    own_o.start()

    def bwd_chunk(i, c, delta, diagonal):
        k_c, v_c, kt_c = k_s[c], v_s[c], kt[c]
        dk_c = dv_c = None
        for a in range(heads):
            q_a, do_a = q_s[i, :, cols[a]], do_s[i, :, cols[a]]
            s = dot(k_c, q_a, COLS_COLS) * to_log2
            if diagonal:
                s = masked(s)
            p = jnp.exp2(s - lse_s[i, a:a + 1, :])
            d_p = dot(v_c, do_a, COLS_COLS)
            d_s = (p * (d_p - delta[a])).astype(BF16)
            dv_a = dot(p.astype(BF16), do_a)
            dk_a = dot(d_s, q_a)
            dv_c = dv_a if dv_c is None else dv_c + dv_a
            dk_c = dk_a if dk_c is None else dk_c + dk_a
            acc[a] += dot(kt_c, d_s)
        dk_acc[c] += dk_c
        dv_acc[c] += dv_c

    def dq_stores(r):
        slot = lax.rem(r, 2)
        at = pl.ds(pl.multiple_of(near.across(r) * rows, rows), rows)
        last = q_cols - HEAD_DIM
        return [pltpu.make_async_copy(dq_v.at[slot, :, pl.ds(0, last)], dq_a_ref.at[at, :], dq_sems.at[slot, 0]),
                pltpu.make_async_copy(dq_v.at[slot, :, pl.ds(last, HEAD_DIM)], dq_b_ref.at[at, :], dq_sems.at[slot, 1])]

    def pass_on(done):
        @pl.when(done == BWD_MIDDLE)
        def _():
            gather_o.middle()

    for r in (n_blocks - 2, n_blocks - 1):
        ht_store(jnp.int32(r)).wait()
    dk_acc[...] = jnp.zeros_like(dk_acc)
    dv_acc[...] = jnp.zeros_like(dv_acc)
    stage_out.wait()

    def bwd_block(r, done):
        i = near.across(r)
        slot = lax.rem(r, 2)
        at = pl.ds(pl.multiple_of(i * rows, rows), rows)

        arrive(r, dy_all, gather_dy)
        do_s[i] = dot(blk[slot], wo_v[...], COLS_COLS).astype(BF16)
        acc[...] = jnp.zeros_like(acc)
        delta = [jnp.sum(ot_s[cols[a], at].astype(F32) * do_s[i, :, cols[a]].T.astype(F32), axis=0, keepdims=True) for a in range(heads)]

        @pl.loop(0, i)
        def _(c):
            bwd_chunk(i, c, delta, False)
            pass_on(done + c)

        bwd_chunk(i, i, delta, True)
        pass_on(done + i)

        @pl.when(r >= 2)
        def _():
            for store in dq_stores(r - 2):
                store.wait()

        for a in range(heads):
            dq_v[slot, :, cols[a]] = unrotate(acc[a].T * qk_scale, cos_s[i], sin_s[i])
        for store in dq_stores(r):
            store.start()
        return done + i + 1

    lax.fori_loop(0, n_blocks, bwd_block, jnp.int32(0))
    gather_o.late()
    for r in (n_blocks - 2, n_blocks - 1):
        for store in dq_stores(r):
            store.wait()
    gather_next.start()

    @pl.loop(0, n_blocks)
    def _(c):
        at = pl.ds(pl.multiple_of(c * rows, rows), rows)
        dkv_v[at, :HEAD_DIM] = unrotate(dk_acc[c] * qk_scale, cos_s[c], sin_s[c])
        dkv_v[at, HEAD_DIM:] = dv_acc[c].astype(BF16)

    dkv_store = pltpu.make_async_copy(dkv_v, dkv_ref, own_sems.at[1])
    dkv_store.start()
    own_o.wait()
    gather_o.end()
    dkv_store.wait()


def lanes(*parts):
    return jnp.concatenate(parts, axis=1)


def products_part(heads, near, gathers, ot_ref, ht_ref, dy_ref, d_kv_ref, d_qa_ref, d_qb_ref, x_ref, own_dy_ref, gain_ref, wo_ref, wk_ref, wv_ref, wq_ref,
                  wo_out, wq_out, kv_all, qa_all, qb_all, res_ref, gx_ref, gg_ref, gg_row, gg_all, gg_sems, x_sems,
                  a_buf, b_buf, tile, a_sem, b_sems, t_sems, stage, stage_sems, ot_v, o_v, x_v, io_sems, own, own_sems, w_v, w_sems, acc,
                  gg_v):
    core = lax.rem(near.me, 2)
    half = a_buf.shape[0]
    seq_len = d_kv_ref.shape[0]
    rows, width = x_ref.shape
    n_cols = d_kv_ref.shape[1]
    n_o, n_all = width // (2 * n_cols), x_sems.shape[1]
    n_oa = n_o + (n_all - n_o) * 2 // 3

    local = (d_qa_ref, d_qb_ref, d_kv_ref)

    def stage_in(n):
        return pltpu.make_async_copy(local[n], stage.at[:, pl.ds(0, local[n].shape[1])], stage_sems.at[0])

    def stage_out(n):
        return pltpu.make_async_copy(stage.at[:, pl.ds(0, local[n].shape[1])], gathers[n].block(near.me, 0, CHUNKS), stage_sems.at[1])

    def copy_own(n):
        stage_in(n).wait()
        stage_out(n).start()

    own_rows = pl.ds(pl.multiple_of(core * half, half), half)
    tokens = pl.ds(pl.multiple_of(near.me * rows, rows), rows)
    ot_load = pltpu.make_async_copy(ot_ref.at[:, tokens], ot_v, io_sems.at[0])
    x_load = pltpu.make_async_copy(x_ref, x_v, io_sems.at[1])
    res_store = pltpu.make_async_copy(x_v, res_ref, io_sems.at[2])
    dy_load = pltpu.make_async_copy(own_dy_ref, o_v, io_sems.at[3])
    gx_store = pltpu.make_async_copy(o_v, gx_ref, io_sems.at[0])

    def a_load(ref):
        return pltpu.make_async_copy(ref.at[own_rows, :], a_buf, a_sem)

    def b_loads(source, p, slot, g):
        if source is dy_ref:
            srcs = [dy_ref.at[:, pl.ds(pl.multiple_of((2 * p + g) * n_cols, n_cols), n_cols)]]
        else:
            per = n_cols // source.shape[1]
            srcs = [source.at[pl.ds(pl.multiple_of(((2 * p + g) * per + n) * seq_len, seq_len), seq_len), :] for n in range(per)]
        return [pltpu.make_async_copy(src, b_buf.at[slot, :, pl.ds(g * n_cols + n * src.shape[1], src.shape[1])], b_sems.at[slot, g])
                for n, src in enumerate(srcs)]

    def start_b(step):
        slot = lax.rem(step, 2)
        for source, low, high in ((dy_ref, 0, n_o), (qa_all, n_o, n_oa), (qb_all, n_oa, n_all)):
            @pl.when(jnp.logical_and(step >= low, step < high))
            def _():
                for g in range(2):
                    for load in b_loads(source, step - low, slot, g):
                        load.start()

    def pieces(kind, step):
        wide = (2 * n_cols, n_cols, HEAD_DIM)[kind]
        slot = lax.rem(step, 2)
        out = []
        for n in range(2 * n_cols // wide):
            group = (step - (0, n_o, n_oa)[kind]) * (2 * n_cols // wide) + n
            col = (group * wide, group * heads * HEAD_DIM, (group + 1) * heads * HEAD_DIM - HEAD_DIM)[kind]
            dst = (wo_out, wq_out, wq_out)[kind].at[own_rows, pl.ds(pl.multiple_of(col, HEAD_DIM), wide)]
            src = tile.at[slot, :, pl.ds(n * wide, wide)]
            out.append((pltpu.make_async_copy(src, dst, t_sems.at[slot]), send(src, dst, x_sems, step, near.sib)))
        return out

    def start_tile(step):
        for kind, (low, high) in enumerate(((0, n_o), (n_o, n_oa), (n_oa, n_all))):
            @pl.when(jnp.logical_and(step >= low, step < high))
            def _():
                for keep, give in pieces(kind, step):
                    keep.start()
                    give.start()

    def whole_tile(step):
        slot = lax.rem(step, 2)
        dst = wo_out.at[own_rows, pl.ds(0, 2 * n_cols)]
        return pltpu.make_async_copy(tile.at[slot], dst, t_sems.at[slot]), send(tile.at[slot], dst, x_sems, step, near.sib)

    def wait_tile(step):
        keep, give = whole_tile(step)
        keep.wait()
        give.wait_send()

    def result_part():
        cols = b_buf.shape[2]

        def w_load(n):
            slot = lax.rem(n, 2)
            return pltpu.make_async_copy(wo_ref.at[:, pl.ds(pl.multiple_of(n * cols, cols), cols)], b_buf.at[slot, pl.ds(0, wo_ref.shape[0]), :],
                                         b_sems.at[slot, 0])

        w_load(jnp.int32(0)).start()
        ot_load.wait()

        @pl.loop(0, ot_v.shape[0] // BLK)
        def _(r):
            at = pl.ds(pl.multiple_of(r * BLK, BLK), BLK)
            o_v[:, at] = ot_v[at, :].T

        x_load.wait()

        @pl.loop(0, n_o)
        def _(n):
            w_load(n).wait()

            @pl.when(n + 1 < n_o)
            def _():
                w_load(n + 1).start()

            at = pl.ds(pl.multiple_of(n * cols, cols), cols)
            x_v[:, at] = (x_v[:, at].astype(F32) + dot(o_v[...], b_buf[lax.rem(n, 2), :wo_ref.shape[0], :])).astype(BF16)

        res_store.start()

    def hidden_parts(kind):
        count = own.shape[0] // (2 if kind == 1 else 1)

        def own_load(r, g):
            source = (qa_all, qb_all, kv_all)[kind]
            device, col = (2 * r + g, 0) if kind == 1 else (near.across(r), g * HEAD_DIM)
            at = pl.ds(pl.multiple_of(device * seq_len + near.me * rows, rows), rows)
            return pltpu.make_async_copy(source.at[at, pl.ds(col, HEAD_DIM)], own.at[r, :, pl.ds(g * HEAD_DIM, HEAD_DIM)], own_sems.at[r, g])

        def w_load(r, g):
            source = (wk_ref, wv_ref)[g] if kind == 2 else wq_ref
            col = near.across(r) if kind == 2 else heads * near.across(r) + g if kind == 0 else heads * (2 * r + g + 1) - 1
            slot = lax.rem(r, 2)
            return pltpu.make_async_copy(source.at[:, pl.ds(pl.multiple_of(col * HEAD_DIM, HEAD_DIM), HEAD_DIM)],
                                         w_v.at[slot, :, pl.ds(g * HEAD_DIM, HEAD_DIM)], w_sems.at[slot, g])

        return count, own_load, w_load

    def hidden_start(kind, low=0, high=None):
        count, own_load, w_load = hidden_parts(kind)
        for g in range(2):
            if low == 0:
                w_load(jnp.int32(0), g).start()

            @pl.loop(low, high or count)
            def _(r):
                own_load(r, g).start()

    def hidden_add(kind, low=0, high=None):
        count, own_load, w_load = hidden_parts(kind)

        @pl.loop(low, high or count)
        def _(r):
            for g in range(2):
                w_load(r, g).wait()
                own_load(r, g).wait()

            @pl.when(r + 1 < count)
            def _():
                for g in range(2):
                    w_load(r + 1, g).start()

            for col in range(0, width, width // PARTS):
                at = slice(col, col + width // PARTS)
                acc[:, at] += dot(own[r], w_v[lax.rem(r, 2), at, :], COLS_COLS)

    a_load(ot_ref).start()
    start_b(jnp.int32(0))
    stage_in(0).start()
    ot_load.start()
    x_load.start()
    a_load(ot_ref).wait()

    @pl.loop(0, n_all)
    def _(step):
        slot = lax.rem(step, 2)
        for g in range(2):
            b_loads(dy_ref, 0, slot, g)[0].wait()

        @pl.when(jnp.logical_and(step != n_o - 1, step != n_oa - 1))
        def _():
            start_b(step + 1)

        @pl.when(step >= 2)
        def _():
            wait_tile(step - 2)

        @pl.when(step == n_o)
        def _():
            a_load(ht_ref).wait()

        for r in range(0, half, half // PARTS):
            tile[slot, r:r + half // PARTS, :] = dot(a_buf[r:r + half // PARTS, :], b_buf[slot])
        start_tile(step)

        @pl.when(step == n_o - 4)
        def _():
            acc[...] = jnp.zeros_like(acc)
            copy_own(0)
            gathers[0].middle()

        @pl.when(step == n_o - 1)
        def _():
            a_load(ht_ref).start()
            gathers[0].late()
            gathers[1].start()
            stage_out(0).wait()
            stage_in(1).start()
            result_part()
            gathers[0].end()
            start_b(step + 1)
            hidden_start(0)

        @pl.when(step == n_oa - 4)
        def _():
            copy_own(1)
            gathers[1].middle()

        @pl.when(step == n_oa - 2)
        def _():
            gathers[1].late()
            gathers[2].start()
            stage_out(1).wait()
            stage_in(2).start()

        @pl.when(step == n_oa - 1)
        def _():
            res_store.wait()
            x_load.start()
            dy_load.start()
            gathers[1].end()
            start_b(step + 1)

    hidden_add(0)
    copy_own(2)
    gathers[2].middle()
    hidden_start(1)
    hidden_add(1)
    gathers[2].late()
    stage_out(2).wait()
    gathers[2].end_sib()
    gathers[2].end_near()
    near_count = own.shape[0] * 3 // 4
    hidden_start(2, 0, near_count)
    for step in (n_all - 2, n_all - 1):
        wait_tile(jnp.int32(step))
    hidden_add(2, 0, near_count)
    gathers[2].end_far()
    hidden_start(2, near_count)
    hidden_add(2, near_count)

    gain = gain_ref[...].astype(F32).reshape(1, width)
    gg_v[...] = jnp.zeros_like(gg_v)
    x_load.wait()
    dy_load.wait()

    def normed_rows(r):
        at = pl.ds(pl.multiple_of(r * 32, 32), 32)
        x_f = x_v[at, :].astype(F32)
        inv_rms = lax.rsqrt(jnp.mean(x_f * x_f, axis=-1, keepdims=True) + NORM_EPS)
        return at, inv_rms, x_f * inv_rms

    @pl.loop(0, rows // 32)
    def _(r):
        at, _, normed = normed_rows(r)
        gg_v[...] += jnp.sum((acc[at, :] * normed).reshape(4, 8, width), axis=0)

    gg_row[...] = jnp.sum(gg_v[...], axis=0, keepdims=True)
    gg_all[near.me] = gg_row[...]
    parts = [send(gg_row, gg_all.at[near.me], gg_sems, r, peer) for r, peer in enumerate(near.others())]
    for copy in parts:
        copy.start()

    @pl.loop(0, rows // 32)
    def _(r):
        at, inv_rms, normed = normed_rows(r)
        d_normed = acc[at, :] * gain
        mean = jnp.mean(d_normed * normed, axis=-1, keepdims=True)
        o_v[at, :] = (o_v[at, :].astype(F32) + inv_rms * (d_normed - normed * mean)).astype(BF16)

    gx_store.start()

    @pl.loop(0, n_all)
    def _(step):
        whole_tile(step)[1].wait_recv()

    for copy in parts:
        copy.wait()
    gg_ref[...] = jnp.sum(gg_all[...], axis=0)
    gx_store.wait()


def step_kernel(heads, first_scratch, second_scratch, x_ref, gain_ref, pos_ref, freq_ref, dy_ref, wq_ref, wk_ref, wv_ref, wo_ref,
                h_all, dy_all, o_all, ht, d_kv, d_qa, d_qb, wo_out, wq_out, kv_all, qa_all, qb_all, res, gx, gg,
                pos_all, pos_sems, gg_row, gg_all, gg_sems, x_sems, h_sems, dy_sems, o_sems, kv_sems, qa_sems, qb_sems):
    near = Neighbours()
    seq_len = d_kv.shape[0]

    def gather_of(src, dst, sems):
        return Gather(near, lambda c: src.at[pl.ds(c * (seq_len // CHUNKS), seq_len // CHUNKS), :], dst, seq_len, sems)

    gathers = [gather_of(d_qa, qa_all, qa_sems), gather_of(d_qb, qb_all, qb_sems), gather_of(d_kv, kv_all, kv_sems)]

    def first(*scratch):
        attention_part(heads, near, gathers[0], x_ref, gain_ref, pos_ref, freq_ref, dy_ref, wq_ref, wk_ref, wv_ref, wo_ref,
                       h_all, dy_all, o_all, ht, d_kv, d_qa, d_qb, pos_all, pos_sems, h_sems, dy_sems, o_sems, *scratch)

    def second(*scratch):
        products_part(heads, near, gathers, o_all, ht, dy_all, d_kv, d_qa, d_qb, x_ref, dy_ref, gain_ref, wo_ref, wk_ref, wv_ref, wq_ref,
                      wo_out, wq_out, kv_all, qa_all, qb_all, res, gx, gg, gg_row, gg_all, gg_sems, x_sems, *scratch)

    pl.run_scoped(first, *first_scratch)
    pl.run_scoped(second, *second_scratch)


def step(x, gain, positions, grad_out, w_q, w_k, w_v, w_o, sp_size, heads):
    rows, width = x.shape
    seq_len = rows * sp_size
    q_cols = heads * HEAD_DIM
    all_cols = q_cols * sp_size
    half = width // 2
    cols = 4 * HEAD_DIM
    n_all = (width + all_cols) // cols
    any_spec = pl.BlockSpec(memory_space=pl.ANY)
    vmem = pl.BlockSpec(memory_space=pltpu.VMEM)
    dma = pltpu.SemaphoreType.DMA
    inv_freq = ROPE_THETA ** (-np.arange(0, HEAD_DIM, 2) / HEAD_DIM)
    freq = jnp.asarray(np.concatenate([inv_freq, inv_freq])[None, :], F32)
    pairs = heads * seq_len * (seq_len + rows) // 2
    out = lambda *shape, dtype=BF16: jax.ShapeDtypeStruct(shape, dtype)
    array = lambda *shape, dtype=BF16: pltpu.VMEM(shape, dtype)
    blocks = lambda *shape, dtype=BF16: pltpu.VMEM((sp_size,) + shape, dtype)
    first_scratch = [array(rows, width), array(rows, width), dma((CHUNKS,)), dma((3,)), blocks(rows, HEAD_DIM, dtype=F32),
                     blocks(rows, HEAD_DIM, dtype=F32), array(width, q_cols + 2 * HEAD_DIM), array(q_cols, width), dma((4,)),
                     array(2, rows, width), dma((2,)), array(2, width, rows), dma((2,)),
                     blocks(rows, q_cols), blocks(rows, HEAD_DIM), blocks(rows, HEAD_DIM), blocks(HEAD_DIM, rows), blocks(HEAD_DIM, rows),
                     array(q_cols, seq_len), blocks(8, rows, dtype=F32), array(heads, HEAD_DIM, rows, dtype=F32),
                     blocks(rows, q_cols), blocks(rows, HEAD_DIM, dtype=F32), blocks(rows, HEAD_DIM, dtype=F32),
                     array(2, rows, q_cols), dma((2, 2)), array(seq_len, 2 * HEAD_DIM)]
    second_scratch = [array(half, seq_len), array(2, seq_len, cols), array(2, half, cols, dtype=F32), dma, dma((2, 2)), dma((2,)),
                      array(seq_len, 2 * HEAD_DIM), dma((2,)), array(all_cols, rows), array(rows, all_cols), array(rows, width),
                      dma((4,)), blocks(rows, 2 * HEAD_DIM), dma((sp_size, 2)), array(2, width, 2 * HEAD_DIM), dma((2, 2)),
                      array(rows, width, dtype=F32), array(8, width, dtype=F32)]
    return pl.pallas_call(
        functools.partial(step_kernel, heads, first_scratch, second_scratch),
        in_specs=[any_spec, vmem, vmem, vmem] + [any_spec] * 5,
        out_specs=[any_spec] * 14 + [vmem],
        out_shape=[out(seq_len, width), out(seq_len, width), out(all_cols, seq_len), out(width, seq_len), out(seq_len, 2 * HEAD_DIM),
                   out(seq_len, q_cols - HEAD_DIM), out(seq_len, HEAD_DIM), out(all_cols, width, dtype=F32), out(width, all_cols, dtype=F32),
                   out(sp_size * seq_len, 2 * HEAD_DIM), out(sp_size * seq_len, q_cols - HEAD_DIM), out(sp_size * seq_len, HEAD_DIM),
                   out(rows, width), out(rows, width), out(1, width, dtype=F32)],
        scratch_shapes=[blocks(8, rows, dtype=jnp.int32), dma((2, 7)), array(1, width, dtype=F32), blocks(1, width, dtype=F32), dma((2, 7)),
                        dma((2, n_all))] + [SEMS] * 6,
        compiler_params=pltpu.CompilerParams(vmem_limit_bytes=VMEM_LIMIT, collective_id=0, has_side_effects=True),
        cost_estimate=pl.CostEstimate(flops=28 * pairs * HEAD_DIM + 2 * half * cols * seq_len * n_all, bytes_accessed=20 * seq_len * width,
                                      transcendentals=2 * pairs),
        name="step",
    )(x, gain, positions.reshape(1, -1), freq, grad_out, w_q, w_k, w_v, w_o)


def finish_kernel(ht_ref, d_ref, gx_in, res_in, gg_in, wo_in, wq_in, wk_ref, wv_ref, wq_ref, wo_ref, gx_ref, res_ref, gg_ref, d_v, d_sems, ring, ring_sems):
    step = pl.program_id(0) * pl.num_programs(1) + pl.program_id(1)
    high = ring.shape[2]
    per_array = wo_in.shape[0] // (high * RING)

    def copy_in(src, g, n):
        at = pl.ds(pl.multiple_of((lax.rem(g, per_array) * RING + n) * high, high), high)
        return pltpu.make_async_copy(src.at[at, :], ring.at[lax.rem(g, DEPTH), n], ring_sems.at[0, lax.rem(g, DEPTH), n])

    def copy_out(dst, g, n):
        at = pl.ds(pl.multiple_of((lax.rem(g, per_array) * RING + n) * high, high), high)
        return pltpu.make_async_copy(ring.at[lax.rem(g, DEPTH), n], dst.at[at, :], ring_sems.at[1, lax.rem(g, DEPTH), n])

    def start(copy, first, second, g):
        for ref, mine in ((first, g < per_array), (second, g >= per_array)):
            @pl.when(mine)
            def _():
                for n in range(RING):
                    copy(ref, g, n).start()

    def pair_load(p):
        at = pl.ds(2 * p, 2)
        return pltpu.make_async_copy(d_ref.at[at], d_v.at[at], d_sems.at[p])

    @pl.when(step == 0)
    def _():
        for p in range(d_v.shape[0] // 2):
            pair_load(p).start()

    last = pl.num_programs(0) * pl.num_programs(1) - 1

    def free(g):
        for n in range(RING):
            copy_out(wo_ref, g, n).wait()

    def pass_on(g):
        for n in range(RING):
            copy_in(wo_in, g, n).wait()
        start(copy_out, wo_ref, wq_ref, g)

    @pl.when(step == 0)
    def _():
        start(copy_in, wo_in, wq_in, step)
        start(copy_in, wo_in, wq_in, step + 1)

    @pl.when(step >= DEPTH - 2)
    def _():
        free(step + 2 - DEPTH)

    @pl.when(step < last - 1)
    def _():
        start(copy_in, wo_in, wq_in, step + 2)

    @pl.when(step >= 1)
    def _():
        pass_on(step - 1)

    for p in range(d_v.shape[0] // 2):
        @pl.when(step == p)
        def _():
            pair_load(p).wait()

    ht = ht_ref[...]
    pair = 2 * pl.program_id(1)
    wk_ref[...] = dot(ht, lanes(d_v[pair, :, :HEAD_DIM], d_v[pair + 1, :, :HEAD_DIM]))
    wv_ref[...] = dot(ht, lanes(d_v[pair, :, HEAD_DIM:], d_v[pair + 1, :, HEAD_DIM:]))

    @pl.when(step == 0)
    def _():
        gg_ref[...] = gg_in[...]

    @pl.when(step == last)
    def _():
        pass_on(last)
        for back in range(DEPTH - 2):
            free(last - back)

    @pl.when(step < ROW_STEPS)
    def _():
        gx_ref[...] = gx_in[...]
        res_ref[...] = res_in[...]


def finish(ht, d_kv, w_o_grad, w_q_grad, grad_x, result, grad_gain):
    width, seq_len = ht.shape
    groups = d_kv.shape[0]
    n_j = groups // 2
    steps = (width // MROWS) * n_j
    high = width // COPY_ROWS
    assert w_o_grad.shape[0] + w_q_grad.shape[0] == high * RING * steps
    any_spec = pl.BlockSpec(memory_space=pl.ANY)
    rows = pl.BlockSpec((grad_x.shape[0] // ROW_STEPS, width), lambda m, j: (jnp.minimum(m * n_j + j, ROW_STEPS - 1), 0))
    whole = pl.BlockSpec((1, width), lambda m, j: (0, 0))
    kv_out = pl.BlockSpec((MROWS, 2 * HEAD_DIM), lambda m, j: (m, j))
    out = lambda cols: jax.ShapeDtypeStruct((width, cols), F32)
    like = lambda val: jax.ShapeDtypeStruct(val.shape, val.dtype)
    return pl.pallas_call(
        finish_kernel,
        grid=(width // MROWS, n_j),
        in_specs=[pl.BlockSpec((MROWS, seq_len), lambda m, j: (m, 0)), any_spec, rows, rows, whole, any_spec, any_spec],
        out_specs=[kv_out, kv_out, any_spec, any_spec, rows, rows, whole],
        out_shape=[out(groups * HEAD_DIM), out(groups * HEAD_DIM), like(w_q_grad), like(w_o_grad), like(grad_x), like(result), like(grad_gain)],
        scratch_shapes=[pltpu.VMEM(d_kv.shape, BF16), pltpu.SemaphoreType.DMA((groups // 2,)),
                        pltpu.VMEM((DEPTH, RING, high, width), F32), pltpu.SemaphoreType.DMA((2, DEPTH, RING))],
        compiler_params=params(2),
        cost_estimate=pl.CostEstimate(flops=4 * width * seq_len * groups * HEAD_DIM, bytes_accessed=2 * width * seq_len, transcendentals=0),
        name="finish",
    )(ht, d_kv, grad_x, result, grad_gain, w_o_grad, w_q_grad)


def solution(mesh):
    sp_size = mesh.shape['sp']
    seq_spec = P(('dp', 'sp'), None)
    pos_spec = P(('dp', 'sp'))
    replicated = P(None, None)
    part_rows = P('dp', None)

    def local_step(x, grad_out, positions, gain, w_q, w_k, w_v, w_o):
        n_heads = w_q.shape[1] // HEAD_DIM
        heads = n_heads // sp_size
        _, _, _, ht, _, _, _, w_o_grad, w_q_grad, kv_all, _, _, result, grad_x, grad_gain = step(
            x, gain, positions, grad_out, w_q, w_k, w_v, w_o, sp_size, heads)
        grad_wk, grad_wv, grad_wq, grad_wo, grad_x, result, grad_gain = finish(
            ht, kv_all.reshape(sp_size, -1, 2 * HEAD_DIM), w_o_grad, w_q_grad, grad_x, result, grad_gain)
        return result, grad_x, grad_wq, grad_wk, grad_wv, grad_wo, grad_gain.reshape(-1)

    return jax.shard_map(local_step, mesh=mesh,
                         in_specs=(seq_spec, seq_spec, pos_spec, P(None), replicated, replicated, replicated, replicated),
                         out_specs=(seq_spec, seq_spec, part_rows, part_rows, part_rows, part_rows, P('dp')),
                         check_vma=False)
```
